8 devices in a mesh: data: 4 (over z, y, x), stage: 2 (over core).
Axes of the slice: x: 2, y: 2, z: 1, core: 2. Of those that a mesh axis runs over, the one named last changes fastest.
Arguments:
- act_in: bfloat16 [4, 4, 64, 2048], P(None, 'data')
- cot_out: bfloat16 [4, 4, 64, 2048], P(None, 'data')
- seq_lens: int32 [4, 4], P(None, 'data')
- w_gate: bfloat16 [2, 2, 2048, 5632], P('stage', None, 'data')
- w_in: bfloat16 [2, 2, 2048, 5632], P('stage', None, 'data')
- w_out: bfloat16 [2, 2, 5632, 2048], P('stage', None, 'data')
Outputs:
- output 1: bfloat16 [4, 4, 64, 2048], P(None, 'data')
- output 2: float32 [2, 2, 2048, 5632], P('stage', None, 'data')
- output 3: float32 [2, 2, 2048, 5632], P('stage', None, 'data')
- output 4: float32 [2, 2, 5632, 2048], P('stage', None, 'data')
All inputs are finite; a program needn't handle non-finite values.
Results may differ from the reference program's by a relative error of at most 0.02.
Values are sent between devices in bfloat16 or wider.
A program may use at most 1 GiB of HBM per device.

```python
import jax
import jax.numpy as jnp
from jax import lax

MICRO = 4
BATCH_ROWS = 4
SEQ_LEN = 64
D_MODEL = 2048
D_FF = 5632
STAGES = 2
LAYERS_STAGE = 2
EPSILON = 1e-6
MIN_LEN = SEQ_LEN // 4


def tn_dot(left, right):
    return jnp.dot(left.T, right, preferred_element_type=jnp.float32)


def nt_dot(left, right):
    return jnp.dot(left, right.T, preferred_element_type=jnp.float32)


def norm_fwd(h_act):
    h_wide = h_act.astype(jnp.float32)
    inv_rms = lax.rsqrt(jnp.mean(h_wide * h_wide, axis=-1, keepdims=True) + EPSILON)
    return h_wide, inv_rms, (h_wide * inv_rms).astype(jnp.bfloat16)


def layer_fwd(h_act, keep_mask, w_gate, w_in, w_out):
    h_wide, inv_rms, normed = norm_fwd(h_act)
    gate_pre = jnp.dot(normed, w_gate, preferred_element_type=jnp.float32)
    in_pre = jnp.dot(normed, w_in, preferred_element_type=jnp.float32)
    hidden = (gate_pre * jax.nn.sigmoid(gate_pre) * in_pre).astype(jnp.bfloat16)
    branch = jnp.dot(hidden, w_out, preferred_element_type=jnp.float32).astype(jnp.bfloat16)
    return (h_wide + keep_mask * branch.astype(jnp.float32)).astype(jnp.bfloat16)


def layer_bwd(h_act, keep_mask, w_gate, w_in, w_out, d_next):
    h_wide, inv_rms, normed = norm_fwd(h_act)
    gate_pre = jnp.dot(normed, w_gate, preferred_element_type=jnp.float32)
    in_pre = jnp.dot(normed, w_in, preferred_element_type=jnp.float32)
    gate_sig = jax.nn.sigmoid(gate_pre)
    gate_act = gate_pre * gate_sig
    hidden = (gate_act * in_pre).astype(jnp.bfloat16)
    d_wide = d_next.astype(jnp.float32)
    d_branch = (keep_mask * d_wide).astype(jnp.bfloat16)
    grad_out = tn_dot(hidden, d_branch)
    d_hidden = nt_dot(d_branch, w_out)
    d_gate = (d_hidden * in_pre * gate_sig * (1.0 + gate_pre * (1.0 - gate_sig))).astype(jnp.bfloat16)
    d_in = (d_hidden * gate_act).astype(jnp.bfloat16)
    grad_gate = tn_dot(normed, d_gate)
    grad_in = tn_dot(normed, d_in)
    d_normed = nt_dot(d_gate, w_gate) + nt_dot(d_in, w_in)
    d_resid = inv_rms * d_normed - h_wide * (inv_rms * inv_rms * inv_rms) * jnp.mean(d_normed * h_wide, axis=-1, keepdims=True)
    return (d_wide + d_resid).astype(jnp.bfloat16), grad_gate, grad_in, grad_out


def draw_lengths(base_key):
    key_cap, key_len, key_hi, key_lo = jax.random.split(base_key, 4)
    len_caps = jax.random.randint(key_cap, (MICRO, 1), MIN_LEN, SEQ_LEN + 1)
    raw_lens = jax.random.randint(key_len, (MICRO, BATCH_ROWS), MIN_LEN, len_caps + 1)
    n_seqs = MICRO * BATCH_ROWS
    idx_hi = jax.random.randint(key_hi, (), 0, n_seqs)
    idx_lo = (idx_hi + 1 + jax.random.randint(key_lo, (), 0, n_seqs - 1)) % n_seqs
    flat_lens = raw_lens.reshape(n_seqs).at[idx_hi].set(SEQ_LEN).at[idx_lo].set(MIN_LEN)
    return flat_lens.reshape(MICRO, BATCH_ROWS).astype(jnp.int32)


def setup_inputs(seed: int = 0) -> dict:
    rand_keys = jax.random.split(jax.random.key(seed), 6)
    act_shape = (MICRO, BATCH_ROWS, SEQ_LEN, D_MODEL)
    act_in = jax.random.normal(rand_keys[0], act_shape, jnp.float32).astype(jnp.bfloat16)
    cot_out = jax.random.normal(rand_keys[1], act_shape, jnp.float32).astype(jnp.bfloat16)
    seq_lens = draw_lengths(rand_keys[2])
    w_gate = (jax.random.normal(rand_keys[3], (STAGES, LAYERS_STAGE, D_MODEL, D_FF), jnp.float32) * D_MODEL ** -0.5).astype(jnp.bfloat16)
    w_in = (jax.random.normal(rand_keys[4], (STAGES, LAYERS_STAGE, D_MODEL, D_FF), jnp.float32) * D_MODEL ** -0.5).astype(jnp.bfloat16)
    w_out = (jax.random.normal(rand_keys[5], (STAGES, LAYERS_STAGE, D_FF, D_MODEL), jnp.float32) * D_FF ** -0.5).astype(jnp.bfloat16)
    return {'act_in': act_in, 'cot_out': cot_out, 'seq_lens': seq_lens, 'w_gate': w_gate, 'w_in': w_in, 'w_out': w_out}


def reference(act_in, cot_out, seq_lens, w_gate, w_in, w_out):
    n_layer = STAGES * LAYERS_STAGE
    gate_all = w_gate.reshape(n_layer, D_MODEL, D_FF)
    in_all = w_in.reshape(n_layer, D_MODEL, D_FF)
    out_all = w_out.reshape(n_layer, D_FF, D_MODEL)
    positions = jnp.arange(SEQ_LEN)
    tokens = BATCH_ROWS * SEQ_LEN

    def micro_step(grad_acc, micro_items):
        x_micro, g_micro, len_micro = micro_items
        keep_mask = (positions[None, :] < len_micro[:, None]).astype(jnp.float32).reshape(tokens, 1)

        def fwd_layer(h_act, layer_weights):
            return layer_fwd(h_act, keep_mask, layer_weights[0], layer_weights[1], layer_weights[2]), h_act

        h_top, saved = lax.scan(fwd_layer, x_micro.reshape(tokens, D_MODEL), (gate_all, in_all, out_all))
        d_top = (g_micro.reshape(tokens, D_MODEL).astype(jnp.float32) * keep_mask).astype(jnp.bfloat16)

        def bwd_layer(d_act, layer_items):
            d_prev, grad_gate, grad_in, grad_out = layer_bwd(layer_items[0], keep_mask, layer_items[1], layer_items[2], layer_items[3], d_act)
            return d_prev, (grad_gate, grad_in, grad_out)

        d_bottom, layer_grads = lax.scan(bwd_layer, d_top, (saved, gate_all, in_all, out_all), reverse=True)
        grad_acc = (grad_acc[0] + layer_grads[0], grad_acc[1] + layer_grads[1], grad_acc[2] + layer_grads[2])
        return grad_acc, d_bottom.reshape(BATCH_ROWS, SEQ_LEN, D_MODEL)

    zero_grads = (jnp.zeros((n_layer, D_MODEL, D_FF), jnp.float32), jnp.zeros((n_layer, D_MODEL, D_FF), jnp.float32), jnp.zeros((n_layer, D_FF, D_MODEL), jnp.float32))
    grad_acc, act_grad = lax.scan(micro_step, zero_grads, (act_in, cot_out, seq_lens))
    return (act_grad,
            grad_acc[0].reshape(STAGES, LAYERS_STAGE, D_MODEL, D_FF),
            grad_acc[1].reshape(STAGES, LAYERS_STAGE, D_MODEL, D_FF),
            grad_acc[2].reshape(STAGES, LAYERS_STAGE, D_FF, D_MODEL))
```

```python
import functools

import jax
import jax.numpy as jnp
from jax import lax
from jax.experimental import pallas as pl
from jax.experimental.pallas import tpu as pltpu
from jax.sharding import PartitionSpec as P

EPSILON = 1e-6
MESH = pl.DeviceIdType.MESH
BF16, F32 = jnp.bfloat16, jnp.float32
LANES = 128
VMEM_LIMIT = 67043328


def nt_dot(left, right):
    return lax.dot_general(left, right, (((1,), (1,)), ((), ())), preferred_element_type=F32)


def place():
    d = lax.axis_index('data')
    s = lax.axis_index('stage')
    x = lax.rem(d, 2)
    y = lax.div(d, 2)
    return d, s, 2 * y + 1 - x, 2 * (1 - y) + x, 3 - d


def meet():
    d, s, xn, yn, dg = place()
    barrier = pltpu.get_barrier_semaphore()
    for chip, core in ((xn, s), (yn, s), (dg, s), (xn, 1 - s), (yn, 1 - s), (dg, 1 - s), (d, 1 - s)):
        pl.semaphore_signal(barrier, inc=1, device_id=(chip, core), device_id_type=MESH)
    pl.semaphore_wait(barrier, 7)


def remote(src, dst, send_sem, recv_sem, device):
    return pltpu.make_async_remote_copy(src_ref=src, dst_ref=dst, send_sem=send_sem, recv_sem=recv_sem, device_id=device, device_id_type=MESH)


def gather_kernel(act, cot, lens, w_gate, w_in, inp_all, lens_all, gate_in, in_in, other, ss, rs, ls):
    d, s, xn, yn, dg = place()
    rows, cols = act.shape[0], gate_in.shape[2]
    half = rows // 2
    meet()
    own_lens = pltpu.make_async_copy(lens, lens_all.at[d], ls.at[0])
    own_lens.start()
    len_sends = [remote(lens, lens_all.at[d], ss.at[4 + i], rs.at[4 + i], (chip, s)) for i, chip in enumerate((xn, yn, dg))]
    for copy in len_sends:
        copy.start()

    def own_sends(src):
        return [remote(src, inp_all.at[d], ss.at[i], rs.at[i], (chip, s)) for i, chip in enumerate((xn, yn))]

    def start_own(src):
        for copy in own_sends(src):
            copy.start()
        pltpu.make_async_copy(src, inp_all.at[d], ls.at[1]).start()

    @pl.when(s == 0)
    def _():
        start_own(act)

    @pl.when(s == 1)
    def _():
        start_own(cot)

    swaps = [remote(w.at[1], other.at[i], ss.at[13 + i], rs.at[13 + i], (d, 1 - s)) for i, w in enumerate((w_gate, w_in))]
    for copy in swaps:
        copy.start()

    def weight_sends():
        out = []
        for i, chip in enumerate((dg, xn, yn)):
            col = pl.ds(pl.multiple_of(chip * cols, LANES), cols)
            out.append(remote(w_gate.at[0, :, col], gate_in.at[d], ss.at[7 + i], rs.at[7 + i], (chip, s)))
            out.append(remote(w_in.at[0, :, col], in_in.at[d], ss.at[10 + i], rs.at[10 + i], (chip, s)))
        return out

    @pl.when(s == 0)
    def _():
        for copy in weight_sends():
            copy.start()

    owns = own_sends(act)
    fwd_y = remote(inp_all.at[xn, pl.ds(0, half)], inp_all.at[xn, pl.ds(0, half)], ss.at[2], rs.at[2], (yn, s))
    fwd_x = remote(inp_all.at[yn, pl.ds(half, half)], inp_all.at[yn, pl.ds(half, half)], ss.at[3], rs.at[3], (xn, s))
    owns[0].wait_recv()
    fwd_y.start()
    owns[1].wait_recv()
    fwd_x.start()
    for copy in owns:
        copy.wait_send()
    for copy in [fwd_y, fwd_x] + len_sends + swaps:
        copy.wait()
    own_lens.wait()
    pltpu.make_async_copy(act, inp_all.at[d], ls.at[1]).wait()

    @pl.when(s == 0)
    def _():
        for copy in weight_sends():
            copy.wait()


def share_rows(buf, d, s, xn, yn, ss, rs, half):
    lo, hi = pl.ds(0, half), pl.ds(half, half)

    def own(part, i):
        return [remote(buf.at[d, part], buf.at[d, part], ss.at[2 * i + n], rs.at[2 * i + n], (chip, s)) for n, chip in enumerate((xn, yn))]

    own_lo, own_hi = own(lo, 0), own(hi, 1)
    fwd_y = remote(buf.at[xn, lo], buf.at[xn, lo], ss.at[4], rs.at[4], (yn, s))
    fwd_x = remote(buf.at[yn, hi], buf.at[yn, hi], ss.at[5], rs.at[5], (xn, s))
    return own_lo, own_hi, fwd_y, fwd_x


def finish_share(share):
    own_lo, own_hi, fwd_y, fwd_x = share
    own_lo[0].wait_recv()
    fwd_y.start()
    own_hi[1].wait_recv()
    fwd_x.start()
    own_hi[0].wait_recv()
    own_lo[1].wait_recv()
    fwd_y.wait_recv()
    fwd_x.wait_recv()
    for copy in own_lo + own_hi + [fwd_y, fwd_x]:
        copy.wait_send()


def forward_kernel(sel, w_gate, w_in, w_out, gate_in, in_in, other,
                   wc, a_s, b_s, u_s, ho_s, no_s, r_s,
                   wv, wov, hb, nb, ub, zp, acc, ab, rv, ra1, rb1, ra2, rb2,
                   wss, wrs, hss, hrs, ass, ars, zss, zrs, lw, lo, lab, lsv, lh):
    d, s, xn, yn, dg = place()
    T = sel.shape[0]
    half = T // 2
    cols = wc.shape[4]
    tiles = cols // LANES
    dm = 512
    lo_rows, hi_rows = pl.ds(0, half), pl.ds(half, half)
    meet()

    pltpu.make_async_copy(w_out.at[0], wov, lo.at[0]).start()

    def column(chip):
        return pl.ds(pl.multiple_of(chip * cols, LANES), cols)

    def weight_sends(layer, src, core):
        out = []
        for i, chip in enumerate((dg, xn, yn)):
            for m in range(2):
                out.append(remote(src[m].at[:, column(chip)], wc.at[layer, m, d], wss.at[layer, m, i], wrs.at[layer, m, i], (chip, core)))
        return out

    other_pair = (other.at[0], other.at[1])
    first_pair = (w_gate.at[0], w_in.at[0])

    @pl.when(s == 1)
    def _():
        for copy in weight_sends(1, other_pair, 0) + weight_sends(0, first_pair, 1):
            copy.start()

    def in_copies():
        return [pltpu.make_async_copy(sel.at[:, pl.ds(c * dm, dm)], hb.at[0, c], lh.at[c]) for c in range(4)]

    def hand_over():
        return [remote(hb.at[2, c], hb.at[0, c], hss.at[i], hrs.at[i], (d, 1 - s)) for i, c in enumerate((d, xn, yn, dg))]

    @pl.when(s == 0)
    def _():
        for copy in in_copies():
            copy.start()
        for copy in in_copies():
            copy.wait()

    @pl.when(s == 1)
    def _():
        for copy in hand_over():
            copy.wait_recv()

    def load_weights(j):
        def body(k, carry):
            col = pl.ds(pl.multiple_of(k * LANES, LANES), LANES)
            own = pl.ds(pl.multiple_of(d * cols + k * LANES, LANES), LANES)
            for m, w in enumerate((w_gate, w_in)):
                pltpu.make_async_copy(w.at[j, :, own], wv.at[m, pl.ds(pl.multiple_of(d * dm, dm), dm), col], lw.at[k]).start()
                for chip in (xn, yn, dg):
                    dst = wv.at[m, pl.ds(pl.multiple_of(chip * dm, dm), dm), col]
                    if j == 0:
                        @pl.when(s == 0)
                        def _():
                            pltpu.make_async_copy((gate_in, in_in)[m].at[chip, :, col], dst, lw.at[k]).start()

                        @pl.when(s == 1)
                        def _():
                            pltpu.make_async_copy(wc.at[0, m, chip, :, col], dst, lw.at[k]).start()
                    else:
                        pltpu.make_async_copy(wc.at[1, m, chip, :, col], dst, lw.at[k]).start()
            return carry
        lax.fori_loop(0, tiles, body, 0)

    def wait_columns(j):
        for i, chip in enumerate((dg, xn, yn)):
            for m in range(2):
                remote(wc.at[j, m, chip], wc.at[j, m, chip], wss.at[j, m, i], wrs.at[j, m, i], (chip, s)).wait_recv()

    for j in range(2):
        if j == 0:
            @pl.when(s == 1)
            def _():
                wait_columns(0)
        else:
            wait_columns(1)
        load_weights(j)

        step = 32

        def norm_body(i, carry):
            rows = pl.ds(pl.multiple_of(i * step, step), step)
            blocks = [hb[j, c, rows, :].astype(F32) for c in range(4)]
            total = sum(jnp.sum(b * b, axis=-1, keepdims=True) for b in blocks)
            inv = lax.rsqrt(total * (1.0 / (4 * dm)) + EPSILON)
            for c in range(4):
                nb[rows, c * dm:(c + 1) * dm] = (blocks[c] * inv).astype(BF16)
            rv[j, rows, :] = jnp.broadcast_to(inv, (step, LANES))
            return carry
        lax.fori_loop(0, T // step, norm_body, 0)
        saves = [
            pltpu.make_async_copy(hb.at[j, d], ho_s.at[j], lsv.at[0]),
            pltpu.make_async_copy(nb.at[:, pl.ds(pl.multiple_of(d * dm, dm), dm)], no_s.at[j], lsv.at[1]),
            pltpu.make_async_copy(rv.at[j], r_s.at[j], lsv.at[2]),
        ]
        for copy in saves:
            copy.start()

        def ab_copies(k, slot):
            return [pltpu.make_async_copy(ab.at[slot, 0], a_s.at[j, k], lab.at[slot, 0]),
                    pltpu.make_async_copy(ab.at[slot, 1], b_s.at[j, k], lab.at[slot, 1])]

        def ab_body(k, carry):
            col = pl.ds(pl.multiple_of(k * LANES, LANES), LANES)
            pltpu.make_async_copy(wv.at[:, :, col], wv.at[:, :, col], lw.at[k]).wait()
            acc[...] = jnp.dot(nb[...], jnp.concatenate([wv[0, :, col], wv[1, :, col]], axis=1), preferred_element_type=F32)
            slot = lax.rem(k, 2)

            @pl.when(k >= 2)
            def _():
                for copy in ab_copies(k, slot):
                    copy.wait()
            a, b = acc[:, :LANES], acc[:, LANES:]
            ab[slot, 0] = a
            ab[slot, 1] = b
            ub[:, col] = (a * jax.nn.sigmoid(a) * b).astype(BF16)
            for copy in ab_copies(k, slot):
                copy.start()
            return carry
        lax.fori_loop(0, tiles, ab_body, 0)
        for k in (tiles - 2, tiles - 1):
            for copy in ab_copies(k, k % 2):
                copy.wait()
        save_u = pltpu.make_async_copy(ub, u_s.at[j], lsv.at[3])
        save_u.start()

        def mix():
            pltpu.make_async_copy(w_out.at[j], wov, lo.at[0]).wait()

            def block(c):
                zp[c] = jnp.dot(ub[...], wov[:, pl.ds(pl.multiple_of(c * dm, dm), dm)], preferred_element_type=F32)

            def send(i, c, rows, dst, chip):
                return remote(zp.at[c, rows], dst, zss.at[i], zrs.at[i], (chip, s))
            first = [send(0, dg, lo_rows, ra1.at[0], xn), send(1, dg, hi_rows, rb1.at[0], yn)]
            second = [send(2, xn, lo_rows, ra1.at[1], xn), send(3, yn, hi_rows, rb1.at[1], yn)]
            third = [send(4, yn, lo_rows, ra2, yn), send(5, xn, hi_rows, rb2, xn)]
            block(dg)
            for copy in first:
                copy.start()
            block(xn)
            second[0].start()
            block(yn)
            second[1].start()
            block(d)
            first[0].wait_recv()
            zp[yn, :half, :] += ra1[0]
            third[0].start()
            first[1].wait_recv()
            zp[xn, half:, :] += rb1[0]
            third[1].start()
            share = share_rows(hb.at[j + 1], d, s, xn, yn, ass, ars, half)
            for n, (rows, one, two) in enumerate(((lo_rows, ra1, ra2), (hi_rows, rb1, rb2))):
                second[n].wait_recv()
                third[n].wait_recv()
                branch = (zp[d, rows, :] + one[1] + two[...]).astype(BF16).astype(F32)
                hb[j + 1, d, rows, :] = (hb[j, d, rows, :].astype(F32) + branch).astype(BF16)
                for copy in share[n]:
                    copy.start()
            finish_share(share)
            for copy in first + second + third:
                copy.wait_send()

        if j == 0:
            mix()

            @pl.when(s == 0)
            def _():
                pltpu.make_async_copy(w_out.at[1], wov, lo.at[0]).start()
        else:
            @pl.when(s == 0)
            def _():
                mix()
                hands = hand_over()
                for copy in hands:
                    copy.start()
                sends = weight_sends(1, other_pair, 1)
                for copy in sends:
                    copy.start()
                for copy in hands + sends:
                    copy.wait_send()
        for copy in saves:
            copy.wait()
        save_u.wait()

    @pl.when(s == 1)
    def _():
        for copy in weight_sends(1, other_pair, 0) + weight_sends(0, first_pair, 1):
            copy.wait_send()


def backward_kernel(sel, w_gate, w_in, w_out, a_s, b_s, ho_s, r_s,
                    da_o, db_o, e_o, e_bot,
                    wgv, wiv, wov, eb, daf, ab, dn, hov, rv, sq, sv,
                    dss, drs, fss, frs, ess, ers, hss, hrs, sss, srs, lw, lab, lout, lh, le):
    d, s, xn, yn, dg = place()
    T = sel.shape[0]
    half = T // 2
    cols = daf.shape[3]
    dm = 512
    wide = 2 * LANES
    n_full = cols // wide
    tail = cols - n_full * wide
    pad = sq.shape[0]
    lo_rows, hi_rows = pl.ds(0, half), pl.ds(half, half)
    meet()

    def weight_loads(j):
        return [pltpu.make_async_copy(w_out.at[j], wov, lw.at[0]), pltpu.make_async_copy(w_gate.at[j], wgv, lw.at[1]),
                pltpu.make_async_copy(w_in.at[j], wiv, lw.at[2])]
    for copy in weight_loads(1):
        copy.start()

    def in_copies():
        return [pltpu.make_async_copy(sel.at[:, pl.ds(c * dm, dm)], eb.at[2, c], lh.at[c]) for c in range(4)]

    def hand_over():
        return [remote(eb.at[0, c], eb.at[2, c], hss.at[i], hrs.at[i], (d, 1 - s)) for i, c in enumerate((d, xn, yn, dg))]

    @pl.when(s == 1)
    def _():
        for copy in in_copies():
            copy.start()
        for copy in in_copies():
            copy.wait()

    for j in (1, 0):
        small = [pltpu.make_async_copy(ho_s.at[j], hov, le.at[0]), pltpu.make_async_copy(r_s.at[j], rv, le.at[1])]
        for copy in small:
            copy.start()

        def ab_loads(c, slot, width):
            out = []
            for n in range(width // LANES):
                for m, src in enumerate((a_s, b_s)):
                    out.append(pltpu.make_async_copy(src.at[j, 2 * c + n], ab.at[slot, m, n], lab.at[slot, m, n]))
            return out
        for copy in ab_loads(0, 0, wide):
            copy.start()
        if j == 1:
            @pl.when(s == 0)
            def _():
                for copy in hand_over():
                    copy.wait_recv()
        e_saves = [pltpu.make_async_copy(eb.at[j + 1, c], e_o.at[j, :, pl.ds(c * dm, dm)], le.at[2 + c]) for c in range(4)]
        for copy in e_saves:
            copy.start()
        weight_loads(j)[0].wait()

        def own_sends(c, col):
            out = []
            for m in range(2):
                for n, chip in enumerate((xn, yn)):
                    out.append(remote(daf.at[m, d, :, col], daf.at[m, d, :, col], dss.at[m, n, c], drs.at[m, n, c], (chip, s)))
            return out

        def forwards(c, col):
            return [remote(daf.at[0, xn, :, col], daf.at[0, xn, :, col], fss.at[1, c], frs.at[1, c], (yn, s)),
                    remote(daf.at[1, yn, :, col], daf.at[1, yn, :, col], fss.at[0, c], frs.at[0, c], (xn, s))]

        def columns(c, width):
            return pl.ds(pl.multiple_of(c * wide, LANES), width)

        def du_tile(c, slot, width):
            col = columns(c, width)
            e_all = jnp.concatenate([eb[j + 1, n] for n in range(4)], axis=1)
            dn[:, :width] = nt_dot(e_all, wov[col, :])
            for copy in ab_loads(c, slot, width):
                copy.wait()
            for n in range(width // LANES):
                lane = pl.ds(pl.multiple_of(c * wide + n * LANES, LANES), LANES)
                a, b, du = ab[slot, 0, n], ab[slot, 1, n], dn[:, n * LANES:(n + 1) * LANES]
                sig = jax.nn.sigmoid(a)
                daf[0, d, :, lane] = (du * b * sig * (1.0 + a * (1.0 - sig))).astype(BF16)
                daf[1, d, :, lane] = (du * (a * sig)).astype(BF16)
            for copy in own_sends(c, col):
                copy.start()

        def du_body(c, carry):
            slot = lax.rem(c, 2)

            @pl.when(c < n_full - 1)
            def _():
                for copy in ab_loads(c + 1, 1 - slot, wide):
                    copy.start()

            @pl.when(c == n_full - 1)
            def _():
                for copy in ab_loads(n_full, n_full % 2, tail):
                    copy.start()
            du_tile(c, slot, wide)
            return carry
        lax.fori_loop(0, n_full, du_body, 0)
        du_tile(n_full, n_full % 2, tail)

        outs = (da_o, db_o)

        def save_tile(m, chip, col, c, width):
            dst = outs[m].at[j, :, pl.ds(pl.multiple_of(chip * cols + c * wide, LANES), width)]
            pltpu.make_async_copy(daf.at[m, chip, :, col], dst, lout).start()

        def part(m, chip, c, width):
            col = columns(c, width)
            w = (wgv, wiv)[m]
            return nt_dot(daf[m, chip, :, col], w[:, pl.ds(pl.multiple_of(chip * cols + c * wide, LANES), width)])

        weight_loads(j)[1].wait()
        weight_loads(j)[2].wait()
        for m in range(2):
            save_tile(m, d, pl.ds(0, cols), 0, cols)

        def own_part(c, width, first):
            val = part(0, d, c, width) + part(1, d, c, width)
            dn[...] = val if first else dn[...] + val
        own_part(0, wide, True)
        lax.fori_loop(1, n_full, lambda c, carry: (own_part(c, wide, False), carry)[1], 0)
        own_part(n_full, tail, False)

        def near(c, width):
            col = columns(c, width)
            fwd_y, fwd_x = forwards(c, col)

            def came(m, n, chip):
                remote(daf.at[m, chip, :, col], daf.at[m, chip, :, col], dss.at[m, n, c], drs.at[m, n, c], (chip, s)).wait_recv()
            came(0, 0, xn)
            fwd_y.start()
            came(1, 1, yn)
            fwd_x.start()
            came(1, 0, xn)
            came(0, 1, yn)
            for chip in (xn, yn):
                for m in range(2):
                    save_tile(m, chip, col, c, width)
            dn[...] += (part(0, xn, c, width) + part(1, xn, c, width)) + (part(0, yn, c, width) + part(1, yn, c, width))
        lax.fori_loop(0, n_full, lambda c, carry: (near(c, wide), carry)[1], 0)
        near(n_full, tail)

        def far(c, width):
            col = columns(c, width)
            remote(daf.at[0, dg, :, col], daf.at[0, dg, :, col], fss.at[1, c], frs.at[1, c], (yn, s)).wait_recv()
            remote(daf.at[1, dg, :, col], daf.at[1, dg, :, col], fss.at[0, c], frs.at[0, c], (xn, s)).wait_recv()
            for m in range(2):
                save_tile(m, dg, col, c, width)
            dn[...] += part(0, dg, c, width) + part(1, dg, c, width)
        lax.fori_loop(0, n_full, lambda c, carry: (far(c, wide), carry)[1], 0)
        far(n_full, tail)
        if j == 1:
            for copy in weight_loads(0):
                copy.start()

        for copy in small:
            copy.wait()
        prod = dn[...] * hov[...].astype(F32)
        sq[:T, :] = (prod[:, :LANES] + prod[:, LANES:2 * LANES]) + (prod[:, 2 * LANES:3 * LANES] + prod[:, 3 * LANES:])
        sv[0] = jnp.broadcast_to(jnp.sum(sq[...].T, axis=0, keepdims=True), (8, pad))
        sums = [remote(sv.at[0], sv.at[1 + i], sss.at[i], srs.at[i], (chip, s)) for i, chip in enumerate((xn, yn, dg))]
        for copy in sums:
            copy.start()
        pltpu.make_async_copy(daf, daf, lout).wait()

        def drain(c, width):
            col = columns(c, width)
            for copy in own_sends(c, col) + forwards(c, col):
                copy.wait_send()
        lax.fori_loop(0, n_full, lambda c, carry: (drain(c, wide), carry)[1], 0)
        drain(n_full, tail)
        for copy in sums:
            copy.wait()
        mean = ((sv[0, 0:1, :] + sv[1, 0:1, :]) + (sv[2, 0:1, :] + sv[3, 0:1, :])) * (1.0 / (4 * dm))
        sq[...] = jnp.broadcast_to(mean, (LANES, pad)).T
        share = share_rows(eb.at[j], d, s, xn, yn, ess, ers, half)
        for n, base in enumerate((0, half)):
            rows = pl.ds(base, half)
            inv, avg = rv[rows, :], sq[rows, :]
            for c in range(4):
                lane = slice(c * LANES, (c + 1) * LANES)
                resid = inv * dn[rows, lane] - hov[rows, lane].astype(F32) * (inv * inv * inv) * avg
                eb[j, d, rows, lane] = (eb[j + 1, d, rows, lane].astype(F32) + resid).astype(BF16)
            for copy in share[n]:
                copy.start()
        finish_share(share)
        for copy in e_saves:
            copy.wait()

    def last_copies():
        return [pltpu.make_async_copy(eb.at[0, c], e_bot.at[:, pl.ds(c * dm, dm)], lh.at[c]) for c in range(4)]

    def last_sends():
        return [remote(eb.at[0, c], e_bot.at[:, pl.ds(c * dm, dm)], hss.at[4 + c], hrs.at[4 + c], (d, 1 - s)) for c in range(4)]

    @pl.when(s == 1)
    def _():
        hands = hand_over()
        for copy in hands:
            copy.start()
        for copy in hands:
            copy.wait_send()
        for copy in last_sends():
            copy.wait_recv()

    @pl.when(s == 0)
    def _():
        for copy in last_sends() + last_copies():
            copy.start()
        for copy in last_sends():
            copy.wait_send()
        for copy in last_copies():
            copy.wait()


ANY = pl.BlockSpec(memory_space=pl.ANY)
DMA = pltpu.SemaphoreType.DMA


def comm_call(kernel, name, cid, outs, n_in, scratch):
    return pl.pallas_call(
        kernel, name=name, out_shape=[jax.ShapeDtypeStruct(*o) for o in outs], in_specs=[ANY] * n_in, out_specs=[ANY] * len(outs),
        scratch_shapes=scratch, compiler_params=pltpu.CompilerParams(collective_id=cid, has_side_effects=True, vmem_limit_bytes=VMEM_LIMIT))


def gather_call(act, cot, lens, w_gate, w_in):
    rows, dmod = act.shape
    _, dsh, dff = w_gate.shape
    cols = dff // 4
    outs = [((4, rows, dmod), BF16), ((4,) + lens.shape, jnp.int32), ((4, dsh, cols), BF16), ((4, dsh, cols), BF16), ((2, dsh, dff), BF16)]
    return comm_call(gather_kernel, 'gather', 0, outs, 5, [DMA((15,)), DMA((15,)), DMA((2,))])(act, cot, lens, w_gate, w_in)


def forward_call(cid, sel, w_gate, w_in, w_out, gate_in, in_in, other):
    T, dmod = sel.shape
    _, dsh, dff = w_gate.shape
    cols = dff // 4
    half = T // 2
    tiles = cols // LANES
    outs = [((2, 2, 4, dsh, cols), BF16), ((2, tiles, T, LANES), F32), ((2, tiles, T, LANES), F32), ((2, T, cols), BF16),
            ((2, T, dsh), BF16), ((2, T, dsh), BF16), ((2, T, LANES), F32)]
    V = pltpu.VMEM
    scratch = [V((2, dmod, cols), BF16), V((cols, dmod), BF16), V((3, 4, T, dsh), BF16), V((T, dmod), BF16), V((T, cols), BF16),
               V((4, T, dsh), F32), V((T, 2 * LANES), F32), V((2, 2, T, LANES), F32), V((2, T, LANES), F32),
               V((2, half, dsh), F32), V((2, half, dsh), F32), V((half, dsh), F32), V((half, dsh), F32),
               DMA((2, 2, 3)), DMA((2, 2, 3)), DMA((4,)), DMA((4,)), DMA((6,)), DMA((6,)), DMA((6,)), DMA((6,)),
               DMA((tiles,)), DMA((1,)), DMA((2, 2)), DMA((4,)), DMA((4,))]
    return comm_call(forward_kernel, f'forward_{T}', cid, outs, 7, scratch)(sel, w_gate, w_in, w_out, gate_in, in_in, other)


def backward_call(cid, sel, w_gate, w_in, w_out, a_s, b_s, ho_s, r_s):
    T, dmod = sel.shape
    _, dsh, dff = w_gate.shape
    cols = dff // 4
    tiles = cols // LANES
    chunks = (tiles + 1) // 2
    pad = -(-T // LANES) * LANES
    outs = [((2, T, dff), BF16), ((2, T, dff), BF16), ((2, T, dmod), BF16), ((T, dmod), BF16)]
    V = pltpu.VMEM
    scratch = [V((dsh, dff), BF16), V((dsh, dff), BF16), V((cols, dmod), BF16), V((3, 4, T, dsh), BF16), V((2, 4, T, cols), BF16),
               V((2, 2, 2, T, LANES), F32), V((T, dsh), F32), V((T, dsh), BF16), V((T, LANES), F32), V((pad, LANES), F32), V((4, 8, pad), F32),
               DMA((2, 2, chunks)), DMA((2, 2, chunks)), DMA((2, chunks)), DMA((2, chunks)), DMA((6,)), DMA((6,)), DMA((8,)), DMA((8,)),
               DMA((3,)), DMA((3,)), DMA((3,)), DMA((2, 2, 2)), DMA, DMA((4,)), DMA((6,))]
    return comm_call(backward_kernel, f'backward_{T}', cid, outs, 8, scratch)(sel, w_gate, w_in, w_out, a_s, b_s, ho_s, r_s)


def solution(mesh, buckets=(992,)):
    act_spec = P(None, 'data')
    weight_spec = P('stage', None, 'data', None)

    def local_step(act_in, cot_out, seq_lens, w_gate, w_in, w_out):
        n_micro, n_rows, seq_len, dmod = act_in.shape
        rows = n_micro * n_rows * seq_len
        w_gate, w_in, w_out = w_gate[0], w_in[0], w_out[0]
        lens = jnp.zeros((8, LANES), jnp.int32).at[0, :n_micro].set(seq_lens[:, 0])
        inp_all, lens_all, gate_in, in_in, other = gather_call(act_in.reshape(rows, dmod), cot_out.reshape(rows, dmod), lens, w_gate, w_in)
        lens_all = lens_all[:, 0, :n_micro].reshape(-1)
        starts = jnp.cumsum(lens_all) - lens_all
        pos = jnp.arange(seq_len, dtype=jnp.int32)
        slot = jnp.where(pos[None, :] < lens_all[:, None], starts[:, None] + pos[None, :], -1).reshape(-1)
        count = jnp.sum(lens_all)

        def branch(which, T):
            def run(_):
                pick = (jnp.arange(T, dtype=jnp.int32)[:, None] == slot[None, :]).astype(BF16)
                sel = jnp.dot(pick, inp_all.reshape(-1, dmod), preferred_element_type=F32).astype(BF16)
                wc, a_s, b_s, u_s, ho_s, no_s, r_s = forward_call(1 + 2 * which, sel, w_gate, w_in, w_out, gate_in, in_in, other)
                da, db, e_o, e_bot = backward_call(2 + 2 * which, sel, w_gate, w_in, w_out, a_s, b_s, ho_s, r_s)
                own = lax.dynamic_slice_in_dim(slot, lax.axis_index('data') * rows, rows)
                back = (own[:, None] == jnp.arange(T, dtype=jnp.int32)[None, :]).astype(BF16)
                act_grad = jnp.dot(back, e_bot, preferred_element_type=F32).astype(BF16)

                def outer(left, right):
                    return lax.dot_general(left, right, (((1,), (1,)), ((0,), (0,))), preferred_element_type=F32)
                return act_grad.reshape(act_in.shape), outer(no_s, da)[None], outer(no_s, db)[None], outer(u_s, e_o)[None]
            return run
        if len(buckets) == 1:
            return branch(0, buckets[0])(0)
        which = sum((count > b).astype(jnp.int32) for b in buckets[:-1])
        return lax.switch(which, [branch(i, b) for i, b in enumerate(buckets)], 0)

    return jax.shard_map(local_step, mesh=mesh, in_specs=(act_spec, act_spec, act_spec, weight_spec, weight_spec, weight_spec), out_specs=(act_spec, weight_spec, weight_spec, weight_spec), check_vma=False)
```

```python
import functools

import jax
import jax.numpy as jnp
from jax import lax
from jax.experimental import pallas as pl
from jax.experimental.pallas import tpu as pltpu
from jax.sharding import PartitionSpec as P

EPSILON = 1e-6
MESH = pl.DeviceIdType.MESH
BF16, F32 = jnp.bfloat16, jnp.float32
LANES = 128
VMEM_LIMIT = 67043328
BUCKETS = (448, 512, 576, 640, 992)


def nt_dot(left, right):
    return lax.dot_general(left, right, (((1,), (1,)), ((), ())), preferred_element_type=F32)


def place():
    d = lax.axis_index('data')
    s = lax.axis_index('stage')
    x = lax.rem(d, 2)
    y = lax.div(d, 2)
    return d, s, 2 * y + 1 - x, 2 * (1 - y) + x, 3 - d


def meet():
    d, s, xn, yn, dg = place()
    barrier = pltpu.get_barrier_semaphore()
    for chip, core in ((xn, s), (yn, s), (dg, s), (xn, 1 - s), (yn, 1 - s), (dg, 1 - s), (d, 1 - s)):
        pl.semaphore_signal(barrier, inc=1, device_id=(chip, core), device_id_type=MESH)
    pl.semaphore_wait(barrier, 7)


def remote(src, dst, send_sem, recv_sem, device):
    return pltpu.make_async_remote_copy(src_ref=src, dst_ref=dst, send_sem=send_sem, recv_sem=recv_sem, device_id=device, device_id_type=MESH)


def lens_kernel(lens, slot, count, mine, everyone, ss, rs):
    d, s, xn, yn, dg = place()
    meet()
    seqs, tokens = lens.shape[0], mine.shape[0] * LANES
    each = tokens // seqs
    index = lax.broadcasted_iota(jnp.int32, mine.shape, 0) * LANES + lax.broadcasted_iota(jnp.int32, mine.shape, 1)
    length = jnp.zeros(mine.shape, jnp.int32)
    for i in range(seqs):
        length = jnp.where((index >= i * each) & (index < (i + 1) * each), lens[i], length)
    mine[...] = jnp.where(lax.rem(index, each) < length, 1, 0)
    everyone[d] = mine[...]
    sends = [remote(mine, everyone.at[d], ss.at[i], rs.at[i], (chip, s)) for i, chip in enumerate((xn, yn, dg))]
    for copy in sends:
        copy.start()
    for copy in sends:
        copy.wait()
    rows = 4 * mine.shape[0]
    live = everyone[...].reshape(rows, LANES)
    lane, row = lax.broadcasted_iota(jnp.int32, live.shape, 1), lax.broadcasted_iota(jnp.int32, live.shape, 0)
    upto = live
    shift = 1
    while shift < LANES:
        upto = upto + jnp.where(lane >= shift, pltpu.roll(upto, shift, 1), 0)
        shift *= 2
    whole = jnp.broadcast_to(jnp.sum(live, axis=1, keepdims=True), live.shape)
    before = whole
    shift = 1
    while shift < rows:
        before = before + jnp.where(row >= shift, pltpu.roll(before, shift, 0), 0)
        shift *= 2
    place_of = jnp.where(live > 0, before - whole + upto - 1, -1)
    for i in range(rows):
        slot[:, i * LANES:(i + 1) * LANES] = place_of[i:i + 1, :]
    count[0] = jnp.sum(live)


def share_rows(buf, d, s, xn, yn, ss, rs, lo, hi):
    def own(part, i):
        return [remote(buf.at[d, part], buf.at[d, part], ss.at[2 * i + n], rs.at[2 * i + n], (chip, s)) for n, chip in enumerate((xn, yn))]

    fwd_y = remote(buf.at[xn, lo], buf.at[xn, lo], ss.at[4], rs.at[4], (yn, s))
    fwd_x = remote(buf.at[yn, hi], buf.at[yn, hi], ss.at[5], rs.at[5], (xn, s))
    return own(lo, 0), own(hi, 1), fwd_y, fwd_x


def near_share(share):
    own_lo, own_hi, fwd_y, fwd_x = share
    own_lo[0].wait_recv()
    fwd_y.start()
    own_hi[1].wait_recv()
    fwd_x.start()


def far_share(share):
    own_lo, own_hi, fwd_y, fwd_x = share
    own_hi[0].wait_recv()
    own_lo[1].wait_recv()
    fwd_y.wait_recv()
    fwd_x.wait_recv()
    for copy in own_lo + own_hi + [fwd_y, fwd_x]:
        copy.wait_send()


def forward_kernel(act, cot, slot, w_gate, w_in, w_out,
                   sel_o, a_s, b_s, u_s, ho_s, no_s, r_s, other,
                   wv, wov, hb, nb, ub, zp, acc, ab, rv, ra1, rb1, ra2, rb2,
                   wss, wrs, iss, irs, xss, xrs, hss, hrs, ass, ars, zss, zrs, lw, lo, lab, lsv, lin, go):
    d, s, xn, yn, dg = place()
    T = nb.shape[0]
    half = T // 2
    cols = ub.shape[1]
    tiles = cols // LANES
    dm = hb.shape[3]
    rows_in = act.shape[0]
    lo_rows, hi_rows = pl.ds(0, half), pl.ds(half, half)
    chips = (dg, xn, yn)
    first_tiles, early_tiles = 3, 2

    def block_of(chip):
        return pl.ds(pl.multiple_of(chip * dm, dm), dm)

    def input_rows(chip, base=0, size=rows_in):
        return pl.ds(pl.multiple_of(chip * rows_in + base, LANES), size)

    def own_loads(j):
        return [pltpu.make_async_copy(w.at[j, :, pl.ds(pl.multiple_of(d * cols, LANES), cols)], wv.at[j, m, block_of(d)], lw.at[j, m])
                for m, w in enumerate((w_gate, w_in))]

    def start_weights(layer, src, core, sem, first, last):
        def body(k, carry):
            col = pl.ds(pl.multiple_of(k * LANES, LANES), LANES)
            for chip in chips:
                from_col = pl.ds(pl.multiple_of(chip * cols + k * LANES, LANES), LANES)
                for m in range(2):
                    remote(src[m].at[:, from_col], wv.at[layer, m, block_of(d), col], wss.at[sem], wrs.at[layer, k], (chip, core)).start()
            return carry
        lax.fori_loop(first, last, body, 0)

    def wait_sent(sem, count):
        sent = wv.at[0, :, pl.ds(0, 3 * dm), pl.ds(0, count * LANES)]
        pltpu.make_async_copy(sent, sent, wss.at[sem]).wait()

    def wait_tile(layer, k, col):
        came = wv.at[layer, :, pl.ds(0, 3 * dm), col]
        pltpu.make_async_copy(came, came, wrs.at[layer, k]).wait()

    other_pair = (other.at[0], other.at[1])
    first_pair, second_pair = (w_gate.at[0], w_in.at[0]), (w_gate.at[1], w_in.at[1])

    def input_sends(src):
        return [remote(src, wov.at[input_rows(d)], iss.at[n], irs.at[n], (chip, s)) for n, chip in enumerate((xn, yn))]

    part = rows_in // 2
    pass_y = remote(wov.at[input_rows(xn, 0, part)], wov.at[input_rows(xn, 0, part)], iss.at[2], irs.at[2], (yn, s))
    pass_x = remote(wov.at[input_rows(yn, part, part)], wov.at[input_rows(yn, part, part)], iss.at[3], irs.at[3], (xn, s))
    own_input = pltpu.make_async_copy(act, wov.at[input_rows(d)], lin.at[0])
    meet()
    for n, src in enumerate((act, cot)):
        @pl.when(s == n)
        def _():
            for copy in input_sends(src):
                copy.start()
            pltpu.make_async_copy(src, wov.at[input_rows(d)], lin.at[0]).start()
    swaps = [remote(w.at[1], other.at[m], xss.at[m], xrs.at[m], (d, 1 - s)) for m, w in enumerate((w_gate, w_in))]
    for copy in swaps + own_loads(0) + own_loads(1):
        copy.start()

    @pl.when(s == 0)
    def _():
        start_weights(0, first_pair, 0, 0, 0, first_tiles)
    owns = input_sends(act)
    owns[0].wait_recv()
    pass_y.start()
    owns[1].wait_recv()
    pass_x.start()

    @pl.when(s == 0)
    def _():
        start_weights(0, first_pair, 0, 0, first_tiles, tiles)
    for copy in owns + [pass_y, pass_x]:
        copy.wait_send()
    pass_y.wait_recv()
    pass_x.wait_recv()
    own_input.wait()

    tokens = slot.shape[1]

    def pick_body(i, carry):
        base = pl.multiple_of(lax.div(i, 4) * half, 16)
        c = lax.rem(i, 4)
        pick = (lax.broadcasted_iota(jnp.int32, (half, tokens), 0) + base == slot[...]).astype(BF16)
        hb[s, c, pl.ds(base, half), :] = jnp.dot(pick, wov[:tokens, block_of(c)], preferred_element_type=F32).astype(BF16)
        return carry
    lax.fori_loop(0, 8, pick_body, 0)
    pltpu.make_async_copy(w_out.at[0], wov, lo.at[0]).start()
    for copy in swaps:
        copy.wait()

    def hand_over():
        return [remote(hb.at[0, c], hb.at[0, c], hss.at[i], hrs.at[i], (d, 1 - s)) for i, c in enumerate((d, xn, yn, dg))]

    @pl.when(s == 1)
    def _():
        top = [pltpu.make_async_copy(hb.at[1, c], sel_o.at[:, pl.ds(c * dm, dm)], lin.at[c]) for c in range(4)]
        for copy in top:
            copy.start()
        pl.semaphore_wait(go, 1)
        start_weights(1, other_pair, 0, 0, 0, tiles)
        start_weights(0, first_pair, 1, 1, 0, tiles)
        start_weights(1, second_pair, 1, 2, 0, early_tiles)
        for copy in top:
            copy.wait()
        for copy in hand_over():
            copy.wait_recv()

    def layer(j, carry):
        nxt = 1 - j
        step = 32

        def norm_body(i, carry):
            rows = pl.ds(pl.multiple_of(i * step, step), step)
            blocks = [hb[j, c, rows, :].astype(F32) for c in range(4)]
            total = sum(jnp.sum(b * b, axis=-1, keepdims=True) for b in blocks)
            inv = lax.rsqrt(total * (1.0 / (4 * dm)) + EPSILON)
            for c in range(4):
                nb[rows, c * dm:(c + 1) * dm] = (blocks[c] * inv).astype(BF16)
            rv[rows, :] = jnp.broadcast_to(inv, (step, LANES))
            return carry
        lax.fori_loop(0, T // step, norm_body, 0)
        saves = [
            pltpu.make_async_copy(hb.at[j, d], ho_s.at[j], lsv.at[0]),
            pltpu.make_async_copy(nb.at[:, block_of(d)], no_s.at[j], lsv.at[1]),
            pltpu.make_async_copy(rv, r_s.at[j], lsv.at[2]),
        ]
        for copy in saves:
            copy.start()
        for copy in own_loads(j):
            copy.wait()

        def ab_copies(k, side):
            return [pltpu.make_async_copy(ab.at[side, 0], a_s.at[j, k], lab.at[side, 0]),
                    pltpu.make_async_copy(ab.at[side, 1], b_s.at[j, k], lab.at[side, 1])]

        def ab_body(k, carry):
            col = pl.ds(pl.multiple_of(k * LANES, LANES), LANES)
            wait_tile(j, k, col)

            @pl.when((j == 0) & (s == 0) & (k == tiles - 2))
            def _():
                pl.semaphore_signal(go, inc=1, device_id=(d, 1), device_id_type=MESH)
            acc[...] = jnp.dot(nb[...], jnp.concatenate([wv[j, 0, :, col], wv[j, 1, :, col]], axis=1), preferred_element_type=F32)
            side = lax.rem(k, 2)

            @pl.when(k >= 2)
            def _():
                for copy in ab_copies(k, side):
                    copy.wait()
            a, b = acc[:, :LANES], acc[:, LANES:]
            ab[side, 0] = a
            ab[side, 1] = b
            ub[:, col] = (a * jax.nn.sigmoid(a) * b).astype(BF16)
            for copy in ab_copies(k, side):
                copy.start()
            return carry
        lax.fori_loop(0, tiles, ab_body, 0)
        for k in (tiles - 2, tiles - 1):
            for copy in ab_copies(k, k % 2):
                copy.wait()
        save_u = pltpu.make_async_copy(ub, u_s.at[j], lsv.at[3])
        save_u.start()

        @pl.when((j == 0) | (s == 0))
        def _():
            pltpu.make_async_copy(w_out.at[j], wov, lo.at[0]).wait()

            def send(i, c, rows, dst, chip):
                return remote(zp.at[c, rows], dst, zss.at[i], zrs.at[i], (chip, s))
            first = [send(0, dg, lo_rows, ra1.at[0], xn), send(1, dg, hi_rows, rb1.at[0], yn)]
            second = [send(2, xn, lo_rows, ra1.at[1], xn), send(3, yn, hi_rows, rb1.at[1], yn)]
            third = [send(4, yn, lo_rows, ra2, yn), send(5, xn, hi_rows, rb2, xn)]
            x, y = lax.rem(d, 2), lax.div(d, 2)
            wide = 2 * LANES

            def block_body(i, carry):
                rel, part_of = 3 - lax.div(i, 2), lax.rem(i, 2)
                c = 2 * lax.rem(y + lax.rem(rel, 2), 2) + lax.rem(x + lax.div(rel, 2), 2)
                zp[c, :, pl.ds(pl.multiple_of(part_of * wide, wide), wide)] = jnp.dot(
                    ub[...], wov[:, pl.ds(pl.multiple_of(c * dm + part_of * wide, wide), wide)], preferred_element_type=F32)
                for at, copies in ((1, first), (3, second[:1]), (5, second[1:])):
                    @pl.when(i == at)
                    def _():
                        for copy in copies:
                            copy.start()
                return carry
            lax.fori_loop(0, 8, block_body, 0)
            first[0].wait_recv()
            zp[yn, :half, :] += ra1[0]
            third[0].start()
            first[1].wait_recv()
            zp[xn, half:, :] += rb1[0]
            third[1].start()
            share = share_rows(hb.at[nxt], d, s, xn, yn, ass, ars, lo_rows, hi_rows)
            for n, (rows, one, two) in enumerate(((lo_rows, ra1, ra2), (hi_rows, rb1, rb2))):
                second[n].wait_recv()
                third[n].wait_recv()
                branch = (zp[d, rows, :] + one[1] + two[...]).astype(BF16).astype(F32)
                hb[nxt, d, rows, :] = (hb[j, d, rows, :].astype(F32) + branch).astype(BF16)
                for copy in share[n]:
                    copy.start()
            near_share(share)
            far_share(share)
            for copy in first + second + third:
                copy.wait_send()

        @pl.when((j == 0) & (s == 0))
        def _():
            pltpu.make_async_copy(w_out.at[1], wov, lo.at[0]).start()

        @pl.when((j == 1) & (s == 0))
        def _():
            hands = hand_over()
            for copy in hands:
                copy.start()
            start_weights(1, other_pair, 1, 1, early_tiles, tiles)
            for copy in hands:
                copy.wait_send()
        for copy in saves:
            copy.wait()
        save_u.wait()
        return carry
    lax.fori_loop(0, 2, layer, 0)
    wait_sent(0, tiles)

    @pl.when(s == 0)
    def _():
        wait_sent(1, tiles - early_tiles)

    @pl.when(s == 1)
    def _():
        wait_sent(1, tiles)
        wait_sent(2, early_tiles)


def backward_kernel(sel, slot, w_gate, w_in, w_out, a_s, b_s, ho_s, r_s,
                    da_o, db_o, e_o, act_o,
                    wgv, wov, eb, daf, ab, dn, hov, rv, sq, sv, agv,
                    dss, drs, fss, frs, ess, ers, hss, hrs, sss, srs, ass, ars, lw, lab, lout, lh, le, lsm):
    d, s, xn, yn, dg = place()
    T = sel.shape[0]
    part_rows = T // 2
    lo_n = -(-part_rows // 32) * 16
    cols = daf.shape[3]
    dm = dn.shape[1]
    wide = 2 * LANES
    n_full = cols // wide
    tail = cols - n_full * wide
    n_early = n_full // 2
    n_mid = n_early + 2
    pad = sq.shape[1]
    w_slots = wgv.shape[0]
    ab_slots = ab.shape[0]

    def wo_load(j):
        return pltpu.make_async_copy(w_out.at[j], wov, lw.at[0, 0])

    def slot_of(j, n):
        return j if n == 2 else 0

    def gate_loads(j):
        return [pltpu.make_async_copy(w.at[j], wgv.at[slot_of(j, w_slots), m], lw.at[1 + slot_of(j, w_slots), m]) for m, w in enumerate((w_gate, w_in))]

    def rows_of(g, base=0, size=part_rows):
        return pl.ds(pl.multiple_of(g * part_rows + base, 16), size)

    def in_copies():
        return [pltpu.make_async_copy(sel.at[:, pl.ds(c * dm, dm)], eb.at[2, c], lh.at[c]) for c in range(4)]

    def hand_over(g):
        return [remote(eb.at[0, c, rows_of(g)], eb.at[2, c, rows_of(g)], hss.at[g, i], hrs.at[g, i], (d, 1 - s)) for i, c in enumerate((d, xn, yn, dg))]

    def ab_loads(j, g):
        side = slot_of(g, ab_slots)
        return [pltpu.make_async_copy(src.at[j, :, rows_of(g)], ab.at[side, m], lab.at[side, m]) for m, src in enumerate((a_s, b_s))]

    @pl.when(s == 1)
    def _():
        for copy in in_copies():
            copy.start()
    wo_load(1).start()
    small = [pltpu.make_async_copy(ho_s, hov, lsm.at[0]), pltpu.make_async_copy(r_s, rv, lsm.at[1])]
    for g in range(ab_slots):
        for copy in ab_loads(1, g):
            copy.start()
    for copy in gate_loads(1) + small:
        copy.start()
    if w_slots == 2:
        for copy in gate_loads(0):
            copy.start()
    meet()

    @pl.when(s == 1)
    def _():
        for copy in in_copies():
            copy.wait()

    def columns(c, width):
        return pl.ds(pl.multiple_of(c * wide, LANES), width)

    def each_chunk(body, first=0, last=n_full):
        lax.fori_loop(first, last, lambda c, carry: (body(c, wide), carry)[1], 0)

    class Piece:
        def __init__(self, j, g):
            self.j, self.g, self.rows = j, g, rows_of(g)
            parts = (rows_of(g, 0, lo_n), rows_of(g, lo_n, part_rows - lo_n))
            self.share = share_rows(eb.at[j], d, s, xn, yn, ess.at[g], ers.at[g], *parts)
            self.e_saves = [pltpu.make_async_copy(eb.at[j + 1, c, self.rows], e_o.at[j, self.rows, pl.ds(c * dm, dm)], le.at[j, g, c]) for c in range(4)]
            self.sums = [remote(sv.at[g, 0], sv.at[g, 1 + i], sss.at[g, i], srs.at[g, i], (chip, s)) for i, chip in enumerate((xn, yn, dg))]

        def own_sends(self, c, col):
            g, out = self.g, []
            for m in range(2):
                for n, chip in enumerate((xn, yn)):
                    here = daf.at[m, d, self.rows, col]
                    out.append(remote(here, here, dss.at[g, m, n, c], drs.at[g, m, n, c], (chip, s)))
            return out

        def forwards(self, c, col):
            g = self.g
            from_x, from_y = daf.at[0, xn, self.rows, col], daf.at[1, yn, self.rows, col]
            return [remote(from_x, from_x, fss.at[g, 1, c], frs.at[g, 1, c], (yn, s)), remote(from_y, from_y, fss.at[g, 0, c], frs.at[g, 0, c], (xn, s))]

        def make(self):
            j, g, rows, side = self.j, self.g, self.rows, slot_of(self.g, ab_slots)
            for copy in self.e_saves:
                copy.start()

            @pl.when(g == 0)
            def _():
                wo_load(j).wait()
            for copy in ab_loads(j, g):
                copy.wait()

            def tile(c, width):
                e_all = jnp.concatenate([eb[j + 1, n, rows, :] for n in range(4)], axis=1)
                dn[rows, :width] = nt_dot(e_all, wov[columns(c, width), :])
                for n in range(width // LANES):
                    lane = pl.ds(pl.multiple_of(c * wide + n * LANES, LANES), LANES)
                    a, b, du = ab[side, 0, 2 * c + n], ab[side, 1, 2 * c + n], dn[rows, n * LANES:(n + 1) * LANES]
                    sig = jax.nn.sigmoid(a)
                    daf[0, d, rows, lane] = (du * b * sig * (1.0 + a * (1.0 - sig))).astype(BF16)
                    daf[1, d, rows, lane] = (du * (a * sig)).astype(BF16)

            def body(c, width):
                tile(c, wide)

                @pl.when(c < n_early)
                def _():
                    for copy in self.own_sends(c, columns(c, wide)):
                        copy.start()
            each_chunk(body)
            tile(n_full, tail)

        def send(self, first, last):
            def body(c, width):
                for copy in self.own_sends(c, columns(c, width)):
                    copy.start()
            each_chunk(body, first, last)

        def save_tile(self, m, chip, col, c, width):
            dst = (da_o, db_o)[m].at[self.j, self.rows, pl.ds(pl.multiple_of(chip * cols + c * wide, LANES), width)]
            pltpu.make_async_copy(daf.at[m, chip, self.rows, col], dst, lout.at[self.g]).start()

        def part(self, m, chip, c, width):
            w = wgv[slot_of(self.j, w_slots), m, :, pl.ds(pl.multiple_of(chip * cols + c * wide, LANES), width)]
            return nt_dot(daf[m, chip, self.rows, columns(c, width)], w)

        def add(self, chip, c, width):
            dn[self.rows, :] += self.part(0, chip, c, width) + self.part(1, chip, c, width)

        def own(self):
            @pl.when(self.g == 0)
            def _():
                for copy in gate_loads(self.j):
                    copy.wait()
            for m in range(2):
                self.save_tile(m, d, pl.ds(0, cols), 0, cols)
            dn[self.rows, :] = self.part(0, d, n_full, tail) + self.part(1, d, n_full, tail)
            each_chunk(lambda c, width: self.add(d, c, width))

        def near(self, c, width):
            col = columns(c, width)
            fwd_y, fwd_x = self.forwards(c, col)

            def came(m, n, chip):
                there = daf.at[m, chip, self.rows, col]
                remote(there, there, dss.at[self.g, m, n, c], drs.at[self.g, m, n, c], (chip, s)).wait_recv()
            came(0, 0, xn)
            fwd_y.start()
            came(1, 1, yn)
            fwd_x.start()
            came(1, 0, xn)
            came(0, 1, yn)
            for chip in (xn, yn):
                for m in range(2):
                    self.save_tile(m, chip, col, c, width)
            self.add(xn, c, width)
            self.add(yn, c, width)

        def far(self):
            j, g, rows = self.j, self.g, self.rows

            def body(c, width):
                col = columns(c, width)
                there = [daf.at[m, dg, rows, col] for m in range(2)]
                remote(there[0], there[0], fss.at[g, 1, c], frs.at[g, 1, c], (yn, s)).wait_recv()
                remote(there[1], there[1], fss.at[g, 0, c], frs.at[g, 0, c], (xn, s)).wait_recv()
                for m in range(2):
                    self.save_tile(m, dg, col, c, width)
                self.add(dg, c, width)
            each_chunk(body)
            body(n_full, tail)

            @pl.when((j == 1) & (g == 0))
            def _():
                for copy in small:
                    copy.wait()
            prod = dn[rows, :] * hov[j, rows, :].astype(F32)
            sq[g, :part_rows, :] = (prod[:, :LANES] + prod[:, LANES:2 * LANES]) + (prod[:, 2 * LANES:3 * LANES] + prod[:, 3 * LANES:])
            sv[g, 0] = jnp.broadcast_to(jnp.sum(sq[g].T, axis=0, keepdims=True), (8, pad))
            for copy in self.sums:
                copy.start()
            if w_slots == 1:
                @pl.when((j == 1) & (g == 1))
                def _():
                    for copy in gate_loads(0):
                        copy.start()

        def finish(self):
            j, g = self.j, self.g
            whole = daf.at[:, :, self.rows]
            pltpu.make_async_copy(whole, whole, lout.at[g]).wait()

            def drain(c, width):
                col = columns(c, width)
                for copy in self.own_sends(c, col) + self.forwards(c, col):
                    copy.wait_send()
            each_chunk(drain)
            drain(n_full, tail)
            for copy in self.sums:
                copy.wait()
            mean = ((sv[g, 0, 0:1, :] + sv[g, 1, 0:1, :]) + (sv[g, 2, 0:1, :] + sv[g, 3, 0:1, :])) * (1.0 / (4 * dm))
            sq[g] = jnp.broadcast_to(mean, (LANES, pad)).T
            for n, (base, size) in enumerate(((0, lo_n), (lo_n, part_rows - lo_n))):
                at = rows_of(g, base, size)
                inv, avg = rv[j, at, :], sq[g, base:base + size, :]
                for c in range(4):
                    lane = slice(c * LANES, (c + 1) * LANES)
                    resid = inv * dn[at, lane] - hov[j, at, lane].astype(F32) * (inv * inv * inv) * avg
                    eb[j, d, at, lane] = (eb[j + 1, d, at, lane].astype(F32) + resid).astype(BF16)
                for copy in self.share[n]:
                    copy.start()

    def step(i, carry):
        g = lax.rem(i, 2)
        cur = Piece(1 - lax.div(i, 2), g)
        prev = Piece(1 - lax.div(i - 1, 2), 1 - g)
        live, later = i < 4, i > 0

        @pl.when(live)
        def _():
            @pl.when((i < 2) & (s == 0))
            def _():
                for copy in hand_over(g):
                    copy.wait_recv()

            @pl.when(i >= 2)
            def _():
                far_share(Piece(1, g).share)
            cur.make()

            @pl.when(i == 1)
            def _():
                wo_load(0).start()
            coming = i + ab_slots

            @pl.when(coming < 4)
            def _():
                for copy in ab_loads(1 - lax.div(coming, 2), lax.rem(coming, 2)):
                    copy.start()

        @pl.when(i == 4)
        def _():
            far_share(Piece(0, 0).share)

            @pl.when(s == 1)
            def _():
                for copy in hand_over(0):
                    copy.start()

        @pl.when(later)
        def _():
            prev.far()

        @pl.when(live)
        def _():
            cur.send(n_early, n_mid)
            cur.own()

        def halves(h, carry):
            @pl.when(live)
            def _():
                each_chunk(cur.near, h * n_early, n_early + h * (n_full - n_early))

            @pl.when(h == 0)
            def _():
                @pl.when(later)
                def _():
                    prev.finish()

                @pl.when(live)
                def _():
                    cur.send(n_mid, n_full)
                    for copy in cur.own_sends(n_full, columns(n_full, tail)):
                        copy.start()

                @pl.when(later)
                def _():
                    near_share(prev.share)
            return carry
        lax.fori_loop(0, 2, halves, 0)

        @pl.when(live)
        def _():
            cur.near(n_full, tail)
        return carry
    lax.fori_loop(0, 5, step, 0)

    def act_copies(i, c):
        col = pl.ds(pl.multiple_of(c * dm, dm), dm)
        return remote(agv.at[c], act_o.at[:, col], ass.at[i], ars.at[i], (d, 1 - s)), pltpu.make_async_copy(agv.at[c], act_o.at[:, col], lh.at[i])

    @pl.when(s == 1)
    def _():
        far_share(Piece(0, 1).share)
        for copy in hand_over(1):
            copy.start()
        for i, c in enumerate((d, xn, yn, dg)):
            act_copies(i, c)[0].wait_recv()

    @pl.when(s == 0)
    def _():
        own_lo, own_hi, fwd_y, fwd_x = Piece(0, 1).share
        rows_out = agv.shape[1]
        own_slots = slot[:, pl.ds(pl.multiple_of(d * rows_out, LANES), rows_out)]
        back = (lax.broadcasted_iota(jnp.int32, (T, rows_out), 0) == own_slots).astype(BF16)
        for i, c in enumerate((d, xn, yn, dg)):
            for copy in ((), (own_hi[0],), (own_lo[1],), (fwd_y, fwd_x))[i]:
                copy.wait_recv()
            agv[c] = lax.dot_general(back, eb[0, c], (((0,), (0,)), ((), ())), preferred_element_type=F32).astype(BF16)
            for copy in act_copies(i, c):
                copy.start()
        for copy in own_lo + own_hi + [fwd_y, fwd_x]:
            copy.wait_send()
        for i, c in enumerate((d, xn, yn, dg)):
            away, here = act_copies(i, c)
            away.wait_send()
            here.wait()
    for j in range(2):
        for g in range(2):
            for copy in Piece(j, g).e_saves:
                copy.wait()

    @pl.when(s == 1)
    def _():
        for g in range(2):
            for copy in hand_over(g):
                copy.wait_send()


def outer_kernel(n_out, left, *refs):
    flipped = refs[-1]

    @pl.when(pl.program_id(1) == 0)
    def _():
        flipped[...] = left[0].T
    for right, out in zip(refs[:n_out], refs[n_out:]):
        out[0] = jnp.dot(flipped[...], right[0], preferred_element_type=F32)


def outer_call(name, left, rights, width):
    layers, T, dl = left.shape
    dr = rights[0].shape[2]
    n = len(rights)
    moved = 2 * layers * T * (dl + n * dr) + 4 * n * layers * dl * dr
    return pl.pallas_call(
        functools.partial(outer_kernel, n), name=name, grid=(layers, dr // width),
        in_specs=[pl.BlockSpec((1, T, dl), lambda j, c: (j, 0, 0))] + [pl.BlockSpec((1, T, width), lambda j, c: (j, 0, c))] * n,
        out_specs=[pl.BlockSpec((1, dl, width), lambda j, c: (j, 0, c))] * n,
        out_shape=[jax.ShapeDtypeStruct((layers, dl, dr), F32)] * n,
        scratch_shapes=[pltpu.VMEM((dl, T), BF16)],
        cost_estimate=pl.CostEstimate(flops=2 * n * layers * T * dl * dr, bytes_accessed=moved, transcendentals=0),
        compiler_params=pltpu.CompilerParams(vmem_limit_bytes=VMEM_LIMIT))(left, *rights)


ANY = pl.BlockSpec(memory_space=pl.ANY)
DMA = pltpu.SemaphoreType.DMA


def comm_call(kernel, name, cid, outs, in_specs, scratch):
    return pl.pallas_call(
        kernel, name=name, out_shape=[jax.ShapeDtypeStruct(*o) for o in outs], in_specs=in_specs, out_specs=[ANY] * len(outs),
        scratch_shapes=scratch, compiler_params=pltpu.CompilerParams(collective_id=cid, has_side_effects=True, vmem_limit_bytes=VMEM_LIMIT))


def lens_call(lens, tokens):
    smem, vmem = pl.BlockSpec(memory_space=pltpu.SMEM), pl.BlockSpec(memory_space=pltpu.VMEM)
    rows = tokens // LANES
    return pl.pallas_call(
        lens_kernel, name='lens', out_shape=[jax.ShapeDtypeStruct((1, 4 * tokens), jnp.int32), jax.ShapeDtypeStruct((1,), jnp.int32)],
        in_specs=[smem], out_specs=[vmem, smem],
        scratch_shapes=[pltpu.VMEM((rows, LANES), jnp.int32), pltpu.VMEM((4, rows, LANES), jnp.int32), DMA((3,)), DMA((3,))],
        compiler_params=pltpu.CompilerParams(collective_id=0, has_side_effects=True))(lens)


def forward_call(cid, T, act, cot, slot, w_gate, w_in, w_out):
    rows, dmod = act.shape
    _, dsh, dff = w_gate.shape
    cols = dff // 4
    half = T // 2
    tiles = cols // LANES
    outs = [((T, dmod), BF16), ((2, tiles, T, LANES), F32), ((2, tiles, T, LANES), F32), ((2, T, cols), BF16),
            ((2, T, dsh), BF16), ((2, T, dsh), BF16), ((2, T, LANES), F32), ((2, dsh, dff), BF16)]
    V = pltpu.VMEM
    scratch = [V((2, 2, dmod, cols), BF16), V((cols, dmod), BF16), V((2, 4, T, dsh), BF16), V((T, dmod), BF16), V((T, cols), BF16),
               V((4, T, dsh), F32), V((T, 2 * LANES), F32), V((2, 2, T, LANES), F32), V((T, LANES), F32),
               V((2, half, dsh), F32), V((2, half, dsh), F32), V((half, dsh), F32), V((half, dsh), F32),
               DMA((3,)), DMA((2, tiles)), DMA((4,)), DMA((4,)), DMA((2,)), DMA((2,)), DMA((4,)), DMA((4,)), DMA((6,)), DMA((6,)), DMA((6,)), DMA((6,)),
               DMA((2, 2)), DMA((1,)), DMA((2, 2)), DMA((4,)), DMA((4,)), pltpu.SemaphoreType.REGULAR]
    specs = [ANY, ANY, pl.BlockSpec(memory_space=pltpu.VMEM)] + [ANY] * 3
    return comm_call(forward_kernel, f'forward_{T}', cid, outs, specs, scratch)(act, cot, slot, w_gate, w_in, w_out)


def backward_call(cid, sel, slot, w_gate, w_in, w_out, a_s, b_s, ho_s, r_s):
    T, dmod = sel.shape
    _, dsh, dff = w_gate.shape
    cols = dff // 4
    tiles = cols // LANES
    chunks = (tiles + 1) // 2
    pad = -(-(T // 2) // LANES) * LANES
    slots = 2 if T <= 640 else 1
    ab_slots = 2 if T <= 832 else 1
    outs = [((2, T, dff), BF16), ((2, T, dff), BF16), ((2, T, dmod), BF16), ((slot.shape[1] // 4, dmod), BF16)]
    V = pltpu.VMEM
    scratch = [V((slots, 2, dsh, dff), BF16), V((cols, dmod), BF16), V((3, 4, T, dsh), BF16), V((2, 4, T, cols), BF16),
               V((ab_slots, 2, tiles, T // 2, LANES), F32), V((T, dsh), F32), V((2, T, dsh), BF16), V((2, T, LANES), F32), V((2, pad, LANES), F32), V((2, 4, 8, pad), F32), V((4, slot.shape[1] // 4, dsh), BF16),
               DMA((2, 2, 2, chunks)), DMA((2, 2, 2, chunks)), DMA((2, 2, chunks)), DMA((2, 2, chunks)), DMA((2, 6)), DMA((2, 6)), DMA((2, 4)), DMA((2, 4)),
               DMA((2, 3)), DMA((2, 3)), DMA((4,)), DMA((4,)), DMA((3, 2)), DMA((2, 2)), DMA((2,)), DMA((4,)), DMA((2, 2, 4)), DMA((2,))]
    return comm_call(backward_kernel, f'backward_{T}', cid, outs, [ANY, pl.BlockSpec(memory_space=pltpu.VMEM)] + [ANY] * 7, scratch)(sel, slot, w_gate, w_in, w_out, a_s, b_s, ho_s, r_s)


def solution(mesh, buckets=BUCKETS):
    act_spec = P(None, 'data')
    weight_spec = P('stage', None, 'data', None)

    def local_step(act_in, cot_out, seq_lens, w_gate, w_in, w_out):
        n_micro, n_rows, seq_len, dmod = act_in.shape
        rows = n_micro * n_rows * seq_len
        w_gate, w_in, w_out = w_gate[0], w_in[0], w_out[0]
        act, cot = act_in.reshape(rows, dmod), cot_out.reshape(rows, dmod)
        slot, count = lens_call(seq_lens.reshape(n_micro), rows)

        def branch(which, T):
            def run(_):
                sel, a_s, b_s, u_s, ho_s, no_s, r_s, _ = forward_call(1 + 2 * which, T, act, cot, slot, w_gate, w_in, w_out)
                da, db, e_o, act_grad = backward_call(2 + 2 * which, sel, slot, w_gate, w_in, w_out, a_s, b_s, ho_s, r_s)
                gate_grad, in_grad = outer_call(f'gate_in_grad_{T}', no_s, (da, db), 512)
                out_grad, = outer_call(f'out_grad_{T}', u_s, (e_o,), 512)
                return act_grad.reshape(act_in.shape), gate_grad[None], in_grad[None], out_grad[None]
            return run
        if len(buckets) == 1:
            return branch(0, buckets[0])(0)
        which = sum((count[0] > b).astype(jnp.int32) for b in buckets[:-1])
        return lax.switch(which, [branch(i, b) for i, b in enumerate(buckets)], 0)

    return jax.shard_map(local_step, mesh=mesh, in_specs=(act_spec, act_spec, act_spec, weight_spec, weight_spec, weight_spec), out_specs=(act_spec, weight_spec, weight_spec, weight_spec), check_vma=False)
```

```python
import functools

import jax
import jax.numpy as jnp
from jax import lax
from jax.experimental import pallas as pl
from jax.experimental.pallas import tpu as pltpu
from jax.sharding import PartitionSpec as P

EPSILON = 1e-6
MESH = pl.DeviceIdType.MESH
BF16, F32 = jnp.bfloat16, jnp.float32
LANES = 128
VMEM_LIMIT = 67043328
BUCKETS = (416, 480, 544, 640, 992)


def nt_dot(left, right):
    return lax.dot_general(left, right, (((1,), (1,)), ((), ())), preferred_element_type=F32)


def place():
    d = lax.axis_index('data')
    s = lax.axis_index('stage')
    x = lax.rem(d, 2)
    y = lax.div(d, 2)
    return d, s, 2 * y + 1 - x, 2 * (1 - y) + x, 3 - d


def meet():
    d, s, xn, yn, dg = place()
    barrier = pltpu.get_barrier_semaphore()
    for chip, core in ((xn, s), (yn, s), (dg, s), (xn, 1 - s), (yn, 1 - s), (dg, 1 - s), (d, 1 - s)):
        pl.semaphore_signal(barrier, inc=1, device_id=(chip, core), device_id_type=MESH)
    pl.semaphore_wait(barrier, 7)


def remote(src, dst, send_sem, recv_sem, device):
    return pltpu.make_async_remote_copy(src_ref=src, dst_ref=dst, send_sem=send_sem, recv_sem=recv_sem, device_id=device, device_id_type=MESH)


def lens_kernel(lens, slot, count, mine, everyone, ss, rs):
    d, s, xn, yn, dg = place()
    meet()
    seqs, tokens = lens.shape[0], mine.shape[0] * LANES
    each = tokens // seqs
    index = lax.broadcasted_iota(jnp.int32, mine.shape, 0) * LANES + lax.broadcasted_iota(jnp.int32, mine.shape, 1)
    length = jnp.zeros(mine.shape, jnp.int32)
    for i in range(seqs):
        length = jnp.where((index >= i * each) & (index < (i + 1) * each), lens[i], length)
    mine[...] = jnp.where(lax.rem(index, each) < length, 1, 0)
    everyone[d] = mine[...]
    sends = [remote(mine, everyone.at[d], ss.at[i], rs.at[i], (chip, s)) for i, chip in enumerate((xn, yn, dg))]
    for copy in sends:
        copy.start()
    for copy in sends:
        copy.wait()
    rows = 4 * mine.shape[0]
    live = everyone[...].reshape(rows, LANES)
    lane, row = lax.broadcasted_iota(jnp.int32, live.shape, 1), lax.broadcasted_iota(jnp.int32, live.shape, 0)
    upto = live
    shift = 1
    while shift < LANES:
        upto = upto + jnp.where(lane >= shift, pltpu.roll(upto, shift, 1), 0)
        shift *= 2
    whole = jnp.broadcast_to(jnp.sum(live, axis=1, keepdims=True), live.shape)
    before = whole
    shift = 1
    while shift < rows:
        before = before + jnp.where(row >= shift, pltpu.roll(before, shift, 0), 0)
        shift *= 2
    place_of = jnp.where(live > 0, before - whole + upto - 1, -1)
    for i in range(rows):
        slot[:, i * LANES:(i + 1) * LANES] = place_of[i:i + 1, :]
    count[0] = jnp.sum(live)


def share_rows(buf, d, s, xn, yn, ss, rs, lo, hi):
    def own(part, i):
        return [remote(buf.at[d, part], buf.at[d, part], ss.at[2 * i + n], rs.at[2 * i + n], (chip, s)) for n, chip in enumerate((xn, yn))]

    fwd_y = remote(buf.at[xn, lo], buf.at[xn, lo], ss.at[4], rs.at[4], (yn, s))
    fwd_x = remote(buf.at[yn, hi], buf.at[yn, hi], ss.at[5], rs.at[5], (xn, s))
    return own(lo, 0), own(hi, 1), fwd_y, fwd_x


def near_share(share):
    own_lo, own_hi, fwd_y, fwd_x = share
    own_lo[0].wait_recv()
    fwd_y.start()
    own_hi[1].wait_recv()
    fwd_x.start()


def far_share(share):
    own_lo, own_hi, fwd_y, fwd_x = share
    own_hi[0].wait_recv()
    own_lo[1].wait_recv()
    fwd_y.wait_recv()
    fwd_x.wait_recv()
    for copy in own_lo + own_hi + [fwd_y, fwd_x]:
        copy.wait_send()


def forward_kernel(act, cot, slot, w_gate, w_in, w_out,
                   sel_o, a_s, b_s, u_s, ho_s, no_s, r_s, other,
                   wv, wov, hb, nb, ub, zp, acc, ab, rv, ra1, rb1, ra2, rb2, inpv,
                   wss, wrs, iss, irs, xss, xrs, hss, hrs, ass, ars, zss, zrs, lw, lo, lab, lsv, lin, go):
    d, s, xn, yn, dg = place()
    T = nb.shape[0]
    half = T // 2
    piece = T if T <= 640 else half
    cols = ub.shape[1]
    tiles = cols // LANES
    dm = hb.shape[3]
    rows_in = act.shape[0]
    lo_rows, hi_rows = pl.ds(0, half), pl.ds(half, half)
    chips = (dg, xn, yn)
    cuts, early_tiles = (2, 5), 2

    def block_of(chip):
        return pl.ds(pl.multiple_of(chip * dm, dm), dm)

    def input_rows(chip):
        return pl.ds(pl.multiple_of(chip * rows_in, LANES), rows_in)

    def own_loads(j):
        return [pltpu.make_async_copy(w.at[j, :, pl.ds(pl.multiple_of(d * cols, LANES), cols)], wv.at[j, m, block_of(d)], lw.at[j, m])
                for m, w in enumerate((w_gate, w_in))]

    def start_weights(layer, src, core, sem, first, last):
        def body(k, carry):
            col = pl.ds(pl.multiple_of(k * LANES, LANES), LANES)
            for chip in chips:
                from_col = pl.ds(pl.multiple_of(chip * cols + k * LANES, LANES), LANES)
                for m in range(2):
                    remote(src[m].at[:, from_col], wv.at[layer, m, block_of(d), col], wss.at[sem], wrs.at[layer, k], (chip, core)).start()
            return carry
        lax.fori_loop(first, last, body, 0)

    def wait_sent(sem, count):
        sent = wv.at[0, :, pl.ds(0, 3 * dm), pl.ds(0, count * LANES)]
        pltpu.make_async_copy(sent, sent, wss.at[sem]).wait()

    def wait_tile(layer, k, col):
        came = wv.at[layer, :, pl.ds(0, 3 * dm), col]
        pltpu.make_async_copy(came, came, wrs.at[layer, k]).wait()

    other_pair = (other.at[0], other.at[1])
    first_pair, second_pair = (w_gate.at[0], w_in.at[0]), (w_gate.at[1], w_in.at[1])

    def input_sends(src):
        return [remote(src.at[:, block_of(chip)], inpv.at[input_rows(d)], iss.at[i], irs.at[i], (chip, s)) for i, chip in enumerate(chips)]

    def own_input(src):
        return pltpu.make_async_copy(src.at[:, block_of(d)], inpv.at[input_rows(d)], lin.at[0])
    share = share_rows(hb.at[s], d, s, xn, yn, ass, ars, lo_rows, hi_rows)

    def first_weights(first, last):
        @pl.when(s == 0)
        def _():
            start_weights(0, first_pair, 0, 0, first, last)
    meet()
    for n, src in enumerate((act, cot)):
        @pl.when(s == n)
        def _():
            for copy in input_sends(src) + [own_input(src)]:
                copy.start()
    first_weights(0, cuts[0])
    swaps = [remote(w.at[1], other.at[m], xss.at[m], xrs.at[m], (d, 1 - s)) for m, w in enumerate((w_gate, w_in))]
    for copy in own_loads(0) + own_loads(1) + swaps:
        copy.start()
    pltpu.make_async_copy(w_out.at[0], wov, lo.at[0]).start()
    for copy in input_sends(act):
        copy.wait()
    own_input(act).wait()
    tokens = slot.shape[1]

    def pick_body(i, carry):
        base = pl.multiple_of(i * half, 16)
        pick = (lax.broadcasted_iota(jnp.int32, (half, tokens), 0) + base == slot[...]).astype(BF16)
        hb[s, d, pl.ds(base, half), :] = jnp.dot(pick, inpv[...], preferred_element_type=F32).astype(BF16)
        return carry
    lax.fori_loop(0, 2, pick_body, 0)
    for copy in share[0] + share[1]:
        copy.start()
    first_weights(cuts[0], cuts[1])
    near_share(share)
    first_weights(cuts[1], tiles)
    far_share(share)
    for copy in swaps:
        copy.wait()

    def hand_over():
        return [remote(hb.at[0, c], hb.at[0, c], hss.at[i], hrs.at[i], (d, 1 - s)) for i, c in enumerate((d, xn, yn, dg))]

    @pl.when(s == 1)
    def _():
        top = [pltpu.make_async_copy(hb.at[1, c], sel_o.at[:, pl.ds(c * dm, dm)], lin.at[c]) for c in range(4)]
        for copy in top:
            copy.start()
        pl.semaphore_wait(go, 1)
        start_weights(1, other_pair, 0, 0, 0, tiles)
        start_weights(0, first_pair, 1, 1, 0, tiles)
        start_weights(1, second_pair, 1, 2, 0, early_tiles)
        for copy in top:
            copy.wait()
        for copy in hand_over():
            copy.wait_recv()

    def layer(j, carry):
        nxt = 1 - j
        step = 32

        def norm_body(i, carry):
            rows = pl.ds(pl.multiple_of(i * step, step), step)
            blocks = [hb[j, c, rows, :].astype(F32) for c in range(4)]
            total = sum(jnp.sum(b * b, axis=-1, keepdims=True) for b in blocks)
            inv = lax.rsqrt(total * (1.0 / (4 * dm)) + EPSILON)
            for c in range(4):
                nb[rows, c * dm:(c + 1) * dm] = (blocks[c] * inv).astype(BF16)
            rv[rows, :] = jnp.broadcast_to(inv, (step, LANES))
            return carry
        lax.fori_loop(0, T // step, norm_body, 0)
        saves = [
            pltpu.make_async_copy(hb.at[j, d], ho_s.at[j], lsv.at[0]),
            pltpu.make_async_copy(nb.at[:, block_of(d)], no_s.at[j], lsv.at[1]),
            pltpu.make_async_copy(rv, r_s.at[j], lsv.at[2]),
        ]
        for copy in saves:
            copy.start()
        for copy in own_loads(j):
            copy.wait()

        def ab_copies(k, side):
            return [pltpu.make_async_copy(ab.at[side, 0], a_s.at[j, k], lab.at[side, 0]),
                    pltpu.make_async_copy(ab.at[side, 1], b_s.at[j, k], lab.at[side, 1])]

        def ab_body(k, carry):
            col = pl.ds(pl.multiple_of(k * LANES, LANES), LANES)
            wait_tile(j, k, col)

            @pl.when((j == 0) & (s == 0) & (k == tiles - 2))
            def _():
                pl.semaphore_signal(go, inc=1, device_id=(d, 1), device_id_type=MESH)

            def ab_rows(i, carry):
                rows = pl.ds(pl.multiple_of(i * piece, 16), piece)
                acc[rows, :] = jnp.dot(nb[rows, :], jnp.concatenate([wv[j, 0, :, col], wv[j, 1, :, col]], axis=1), preferred_element_type=F32)
                return carry
            lax.fori_loop(0, T // piece, ab_rows, 0)
            side = lax.rem(k, 2)

            @pl.when(k >= 2)
            def _():
                for copy in ab_copies(k, side):
                    copy.wait()
            a, b = acc[:, :LANES], acc[:, LANES:]
            ab[side, 0] = a
            ab[side, 1] = b
            ub[:, col] = (a * jax.nn.sigmoid(a) * b).astype(BF16)
            for copy in ab_copies(k, side):
                copy.start()
            return carry
        lax.fori_loop(0, tiles, ab_body, 0)
        for k in (tiles - 2, tiles - 1):
            for copy in ab_copies(k, k % 2):
                copy.wait()
        save_u = pltpu.make_async_copy(ub, u_s.at[j], lsv.at[3])
        save_u.start()

        @pl.when((j == 0) | (s == 0))
        def _():
            pltpu.make_async_copy(w_out.at[j], wov, lo.at[0]).wait()

            def send(i, c, rows, dst, chip):
                return remote(zp.at[c, rows], dst, zss.at[i], zrs.at[i], (chip, s))
            first = [send(0, dg, lo_rows, ra1.at[0], xn), send(1, dg, hi_rows, rb1.at[0], yn)]
            second = [send(2, xn, lo_rows, ra1.at[1], xn), send(3, yn, hi_rows, rb1.at[1], yn)]
            third = [send(4, yn, lo_rows, ra2, yn), send(5, xn, hi_rows, rb2, xn)]
            x, y = lax.rem(d, 2), lax.div(d, 2)
            wide = 2 * LANES

            def block_body(i, carry):
                rel, part_of = 3 - lax.div(i, 2), lax.rem(i, 2)
                c = 2 * lax.rem(y + lax.rem(rel, 2), 2) + lax.rem(x + lax.div(rel, 2), 2)

                def zp_rows(n, carry):
                    rows = pl.ds(pl.multiple_of(n * piece, 16), piece)
                    zp[c, rows, pl.ds(pl.multiple_of(part_of * wide, wide), wide)] = jnp.dot(
                        ub[rows, :], wov[:, pl.ds(pl.multiple_of(c * dm + part_of * wide, wide), wide)], preferred_element_type=F32)
                    return carry
                lax.fori_loop(0, T // piece, zp_rows, 0)
                for at, copies in ((1, first), (3, second[:1]), (5, second[1:])):
                    @pl.when(i == at)
                    def _():
                        for copy in copies:
                            copy.start()
                return carry
            lax.fori_loop(0, 8, block_body, 0)
            first[0].wait_recv()
            zp[yn, :half, :] += ra1[0]
            third[0].start()
            first[1].wait_recv()
            zp[xn, half:, :] += rb1[0]
            third[1].start()
            share = share_rows(hb.at[nxt], d, s, xn, yn, ass, ars, lo_rows, hi_rows)
            for n, (rows, one, two) in enumerate(((lo_rows, ra1, ra2), (hi_rows, rb1, rb2))):
                second[n].wait_recv()
                third[n].wait_recv()
                branch = (zp[d, rows, :] + one[1] + two[...]).astype(BF16).astype(F32)
                hb[nxt, d, rows, :] = (hb[j, d, rows, :].astype(F32) + branch).astype(BF16)
                for copy in share[n]:
                    copy.start()
            near_share(share)
            far_share(share)
            for copy in first + second + third:
                copy.wait_send()

        @pl.when((j == 0) & (s == 0))
        def _():
            pltpu.make_async_copy(w_out.at[1], wov, lo.at[0]).start()

        @pl.when((j == 1) & (s == 0))
        def _():
            hands = hand_over()
            for copy in hands:
                copy.start()
            start_weights(1, other_pair, 1, 1, early_tiles, tiles)
            for copy in hands:
                copy.wait_send()
        for copy in saves:
            copy.wait()
        save_u.wait()
        return carry
    lax.fori_loop(0, 2, layer, 0)
    wait_sent(0, tiles)

    @pl.when(s == 0)
    def _():
        wait_sent(1, tiles - early_tiles)

    @pl.when(s == 1)
    def _():
        wait_sent(1, tiles)
        wait_sent(2, early_tiles)


def backward_kernel(sel, slot, w_gate, w_in, w_out, a_s, b_s, ho_s, r_s,
                    da_o, db_o, e_o, act_o,
                    wgv, wov, eb, daf, ab, dn, hov, rv, sq, sv, agv, back_v,
                    dss, drs, fss, frs, ess, ers, hss, hrs, sss, srs, ass, ars, lw, lab, lout, lh, le, lsm):
    d, s, xn, yn, dg = place()
    T = sel.shape[0]
    part_rows = T // 2
    lo_n = -(-part_rows // 32) * 16
    cols = daf.shape[3]
    dm = dn.shape[1]
    wide = 2 * LANES
    n_full = cols // wide
    tail = cols - n_full * wide
    n_early = n_full // 2
    n_mid = n_early + 2
    pad = sq.shape[1]
    w_slots = wgv.shape[0]
    ab_slots = ab.shape[0]

    def wo_load(j):
        return pltpu.make_async_copy(w_out.at[j], wov, lw.at[0, 0])

    def slot_of(j, n):
        return j if n == 2 else 0

    def gate_loads(j):
        return [pltpu.make_async_copy(w.at[j], wgv.at[slot_of(j, w_slots), m], lw.at[1 + slot_of(j, w_slots), m]) for m, w in enumerate((w_gate, w_in))]

    def rows_of(g, base=0, size=part_rows):
        return pl.ds(pl.multiple_of(g * part_rows + base, 16), size)

    def in_copies():
        return [pltpu.make_async_copy(sel.at[:, pl.ds(c * dm, dm)], eb.at[2, c], lh.at[c]) for c in range(4)]

    def hand_over(g):
        return [remote(eb.at[0, c, rows_of(g)], eb.at[2, c, rows_of(g)], hss.at[g, i], hrs.at[g, i], (d, 1 - s)) for i, c in enumerate((d, xn, yn, dg))]

    def ab_loads(j, g):
        side = slot_of(g, ab_slots)
        return [pltpu.make_async_copy(src.at[j, :, rows_of(g)], ab.at[side, m], lab.at[side, m]) for m, src in enumerate((a_s, b_s))]

    @pl.when(s == 1)
    def _():
        for copy in in_copies():
            copy.start()
    wo_load(1).start()
    small = [pltpu.make_async_copy(ho_s, hov, lsm.at[0]), pltpu.make_async_copy(r_s, rv, lsm.at[1])]
    for g in range(ab_slots):
        for copy in ab_loads(1, g):
            copy.start()
    for copy in gate_loads(1) + small:
        copy.start()
    if w_slots == 2:
        for copy in gate_loads(0):
            copy.start()
    meet()

    @pl.when(s == 1)
    def _():
        for copy in in_copies():
            copy.wait()

    def columns(c, width):
        return pl.ds(pl.multiple_of(c * wide, LANES), width)

    def each_chunk(body, first=0, last=n_full):
        lax.fori_loop(first, last, lambda c, carry: (body(c, wide), carry)[1], 0)

    class Piece:
        def __init__(self, j, g):
            self.j, self.g, self.rows = j, g, rows_of(g)
            parts = (rows_of(g, 0, lo_n), rows_of(g, lo_n, part_rows - lo_n))
            self.share = share_rows(eb.at[j], d, s, xn, yn, ess.at[g], ers.at[g], *parts)
            self.e_saves = [pltpu.make_async_copy(eb.at[j + 1, c, self.rows], e_o.at[j, self.rows, pl.ds(c * dm, dm)], le.at[j, g, c]) for c in range(4)]
            self.sums = [remote(sv.at[g, 0], sv.at[g, 1 + i], sss.at[g, i], srs.at[g, i], (chip, s)) for i, chip in enumerate((xn, yn, dg))]

        def own_sends(self, c, col):
            g, out = self.g, []
            for m in range(2):
                for n, chip in enumerate((xn, yn)):
                    here = daf.at[m, d, self.rows, col]
                    out.append(remote(here, here, dss.at[g, m, n, c], drs.at[g, m, n, c], (chip, s)))
            return out

        def forwards(self, c, col):
            g = self.g
            from_x, from_y = daf.at[0, xn, self.rows, col], daf.at[1, yn, self.rows, col]
            return [remote(from_x, from_x, fss.at[g, 1, c], frs.at[g, 1, c], (yn, s)), remote(from_y, from_y, fss.at[g, 0, c], frs.at[g, 0, c], (xn, s))]

        def make(self):
            j, g, rows, side = self.j, self.g, self.rows, slot_of(self.g, ab_slots)
            for copy in self.e_saves:
                copy.start()

            @pl.when(g == 0)
            def _():
                wo_load(j).wait()
            for copy in ab_loads(j, g):
                copy.wait()

            def tile(c, width):
                e_all = jnp.concatenate([eb[j + 1, n, rows, :] for n in range(4)], axis=1)
                dn[rows, :width] = nt_dot(e_all, wov[columns(c, width), :])
                for n in range(width // LANES):
                    lane = pl.ds(pl.multiple_of(c * wide + n * LANES, LANES), LANES)
                    a, b, du = ab[side, 0, 2 * c + n], ab[side, 1, 2 * c + n], dn[rows, n * LANES:(n + 1) * LANES]
                    sig = jax.nn.sigmoid(a)
                    daf[0, d, rows, lane] = (du * b * sig * (1.0 + a * (1.0 - sig))).astype(BF16)
                    daf[1, d, rows, lane] = (du * (a * sig)).astype(BF16)

            def body(c, width):
                tile(c, wide)

                @pl.when(c < n_early)
                def _():
                    for copy in self.own_sends(c, columns(c, wide)):
                        copy.start()
            each_chunk(body)
            tile(n_full, tail)

        def send(self, first, last):
            def body(c, width):
                for copy in self.own_sends(c, columns(c, width)):
                    copy.start()
            each_chunk(body, first, last)

        def save_tile(self, m, chip, col, c, width):
            dst = (da_o, db_o)[m].at[self.j, self.rows, pl.ds(pl.multiple_of(chip * cols + c * wide, LANES), width)]
            pltpu.make_async_copy(daf.at[m, chip, self.rows, col], dst, lout.at[self.g]).start()

        def add(self, chip, c, width):
            def body(m, carry):
                w = wgv[slot_of(self.j, w_slots), m, :, pl.ds(pl.multiple_of(chip * cols + c * wide, LANES), width)]
                dn[self.rows, :] += nt_dot(daf[m, chip, self.rows, columns(c, width)], w)
                return carry
            lax.fori_loop(0, 2, body, 0)

        def own(self):
            @pl.when(self.g == 0)
            def _():
                for copy in gate_loads(self.j):
                    copy.wait()
            for m in range(2):
                self.save_tile(m, d, pl.ds(0, cols), 0, cols)
            dn[self.rows, :] = jnp.zeros((part_rows, dm), F32)
            each_chunk(lambda c, width: self.add(d, c, width))
            self.add(d, n_full, tail)

        def near(self, c, width):
            col = columns(c, width)
            fwd_y, fwd_x = self.forwards(c, col)

            def came(m, n, chip):
                there = daf.at[m, chip, self.rows, col]
                remote(there, there, dss.at[self.g, m, n, c], drs.at[self.g, m, n, c], (chip, s)).wait_recv()
            came(0, 0, xn)
            fwd_y.start()
            came(1, 1, yn)
            fwd_x.start()
            came(1, 0, xn)
            came(0, 1, yn)
            for chip in (xn, yn):
                for m in range(2):
                    self.save_tile(m, chip, col, c, width)
            lax.fori_loop(0, 2, lambda i, carry: (self.add(xn + i * (yn - xn), c, width), carry)[1], 0)

        def far(self):
            j, g, rows = self.j, self.g, self.rows

            def body(c, width):
                col = columns(c, width)
                there = [daf.at[m, dg, rows, col] for m in range(2)]
                remote(there[0], there[0], fss.at[g, 1, c], frs.at[g, 1, c], (yn, s)).wait_recv()
                remote(there[1], there[1], fss.at[g, 0, c], frs.at[g, 0, c], (xn, s)).wait_recv()
                for m in range(2):
                    self.save_tile(m, dg, col, c, width)
                self.add(dg, c, width)
            each_chunk(body)
            body(n_full, tail)

            @pl.when((j == 1) & (g == 0))
            def _():
                for copy in small:
                    copy.wait()
            prod = dn[rows, :] * hov[j, rows, :].astype(F32)
            sq[g, :part_rows, :] = (prod[:, :LANES] + prod[:, LANES:2 * LANES]) + (prod[:, 2 * LANES:3 * LANES] + prod[:, 3 * LANES:])
            sv[g, 0] = jnp.broadcast_to(jnp.sum(sq[g].T, axis=0, keepdims=True), (8, pad))
            for copy in self.sums:
                copy.start()
            if w_slots == 1:
                @pl.when((j == 1) & (g == 1))
                def _():
                    for copy in gate_loads(0):
                        copy.start()

        def finish(self):
            j, g = self.j, self.g
            whole = daf.at[:, :, self.rows]
            pltpu.make_async_copy(whole, whole, lout.at[g]).wait()

            def drain(c, width):
                col = columns(c, width)
                for copy in self.own_sends(c, col) + self.forwards(c, col):
                    copy.wait_send()
            each_chunk(drain)
            drain(n_full, tail)
            for copy in self.sums:
                copy.wait()
            mean = ((sv[g, 0, 0:1, :] + sv[g, 1, 0:1, :]) + (sv[g, 2, 0:1, :] + sv[g, 3, 0:1, :])) * (1.0 / (4 * dm))
            sq[g] = jnp.broadcast_to(mean, (LANES, pad)).T
            for n, (base, size) in enumerate(((0, lo_n), (lo_n, part_rows - lo_n))):
                at = rows_of(g, base, size)
                inv, avg = rv[j, at, :], sq[g, base:base + size, :]
                for c in range(4):
                    lane = slice(c * LANES, (c + 1) * LANES)
                    resid = inv * dn[at, lane] - hov[j, at, lane].astype(F32) * (inv * inv * inv) * avg
                    eb[j, d, at, lane] = (eb[j + 1, d, at, lane].astype(F32) + resid).astype(BF16)
                for copy in self.share[n]:
                    copy.start()

    def step(i, carry):
        g = lax.rem(i, 2)
        cur = Piece(1 - lax.div(i, 2), g)
        prev = Piece(1 - lax.div(i - 1, 2), 1 - g)
        live, later = i < 4, i > 0

        @pl.when(live)
        def _():
            @pl.when((i < 2) & (s == 0))
            def _():
                for copy in hand_over(g):
                    copy.wait_recv()

            @pl.when(i >= 2)
            def _():
                far_share(Piece(1, g).share)
            cur.make()

            @pl.when(i == 1)
            def _():
                wo_load(0).start()
            coming = i + ab_slots

            @pl.when(coming < 4)
            def _():
                for copy in ab_loads(1 - lax.div(coming, 2), lax.rem(coming, 2)):
                    copy.start()

        @pl.when(i == 4)
        def _():
            far_share(Piece(0, 0).share)

            @pl.when(s == 1)
            def _():
                for copy in hand_over(0):
                    copy.start()

        @pl.when(later)
        def _():
            prev.far()

        @pl.when(live)
        def _():
            cur.send(n_early, n_mid)
            cur.own()

        def halves(h, carry):
            @pl.when(live)
            def _():
                each_chunk(cur.near, h * n_early, n_early + h * (n_full - n_early))

            @pl.when(h == 0)
            def _():
                @pl.when(later)
                def _():
                    prev.finish()

                @pl.when(live)
                def _():
                    cur.send(n_mid, n_full)
                    for copy in cur.own_sends(n_full, columns(n_full, tail)):
                        copy.start()

                @pl.when(later)
                def _():
                    near_share(prev.share)
            return carry
        lax.fori_loop(0, 2, halves, 0)

        @pl.when(live)
        def _():
            cur.near(n_full, tail)
        return carry
    lax.fori_loop(0, 5, step, 0)

    def act_copies(i, c):
        col = pl.ds(pl.multiple_of(c * dm, dm), dm)
        return remote(agv.at[c], act_o.at[:, col], ass.at[i], ars.at[i], (d, 1 - s)), pltpu.make_async_copy(agv.at[c], act_o.at[:, col], lh.at[i])

    @pl.when(s == 1)
    def _():
        far_share(Piece(0, 1).share)
        for copy in hand_over(1):
            copy.start()
        for i, c in enumerate((d, xn, yn, dg)):
            act_copies(i, c)[0].wait_recv()

    @pl.when(s == 0)
    def _():
        own_lo, own_hi, fwd_y, fwd_x = Piece(0, 1).share
        rows_out = agv.shape[1]
        own_slots = slot[:, pl.ds(pl.multiple_of(d * rows_out, LANES), rows_out)]
        back = (lax.broadcasted_iota(jnp.int32, (T, rows_out), 0) == own_slots).astype(BF16)
        back_v[...] = back
        came = ((), (own_hi[0],), (own_lo[1],), (fwd_y, fwd_x))
        x, y = lax.rem(d, 2), lax.div(d, 2)

        def spread(i, carry):
            for n in range(1, 4):
                @pl.when(i == n)
                def _():
                    for copy in came[n]:
                        copy.wait_recv()
            c = 2 * lax.rem(y + lax.div(i, 2), 2) + lax.rem(x + lax.rem(i, 2), 2)
            agv[c] = lax.dot_general(back_v[...], eb[0, c], (((0,), (0,)), ((), ())), preferred_element_type=F32).astype(BF16)
            for copy in act_copies(i, c):
                copy.start()
            return carry
        lax.fori_loop(0, 4, spread, 0)
        for copy in own_lo + own_hi + [fwd_y, fwd_x]:
            copy.wait_send()
        for i, c in enumerate((d, xn, yn, dg)):
            away, here = act_copies(i, c)
            away.wait_send()
            here.wait()
    for j in range(2):
        for g in range(2):
            for copy in Piece(j, g).e_saves:
                copy.wait()

    @pl.when(s == 1)
    def _():
        for g in range(2):
            for copy in hand_over(g):
                copy.wait_send()


def grads_kernel(no_s, u_s, da, db, e_o, act, gate_o, in_o, out_o, act_o, nv, uv, ev, av, nt, ut, ring, og, oo, ln, lr, lg, lo):
    layers = nv.shape[0]
    wide = ring.shape[3]
    n_gate, n_out = da.shape[2] // wide, e_o.shape[2] // wide
    slots, g_slots, o_slots = ring.shape[0], og.shape[0], oo.shape[0]
    rows = oo.shape[2]

    def flip(src, dst):
        def body(i, carry):
            lane = pl.ds(pl.multiple_of(i * LANES, LANES), LANES)
            dst[lane, :] = src[:, lane].T
            return carry
        lax.fori_loop(0, dst.shape[0] // LANES, body, 0)
    wholes = [pltpu.make_async_copy(src, dst, ln.at[i]) for i, (src, dst) in enumerate(((no_s, nv), (u_s, uv), (e_o, ev), (act, av)))]
    act_store = pltpu.make_async_copy(av, act_o, ln.at[4])

    def tile_at(c):
        return pl.ds(pl.multiple_of(c * wide, wide), wide)

    def loads(t):
        slot = lax.rem(t, slots)
        return [pltpu.make_async_copy(src.at[lax.div(t, n_gate), :, tile_at(lax.rem(t, n_gate))], ring.at[slot, m], lr.at[slot, m]) for m, src in enumerate((da, db))]

    def gate_stores(t):
        slot = lax.rem(t, g_slots)
        return [pltpu.make_async_copy(og.at[slot, m], dst.at[lax.div(t, n_gate), :, tile_at(lax.rem(t, n_gate))], lg.at[slot, m]) for m, dst in enumerate((gate_o, in_o))]

    def out_stores(t):
        slot = lax.rem(t, o_slots)
        return [pltpu.make_async_copy(oo.at[slot, m], out_o.at[lax.div(t, n_out), pl.ds(m * rows, rows), tile_at(lax.rem(t, n_out))], lo.at[slot, m]) for m in range(2)]

    def start(copies):
        for copy in copies:
            copy.start()

    def wait(copies):
        for copy in copies:
            copy.wait()
    wholes[0].start()
    for t in range(slots - 1):
        start(loads(t))
    start(wholes[1:])
    wholes[0].wait()

    def gate_body(t, carry):
        j, c, slot, at = lax.div(t, n_gate), lax.rem(t, n_gate), lax.rem(t, slots), lax.rem(t, g_slots)

        @pl.when(t + slots - 1 < layers * n_gate)
        def _():
            start(loads(t + slots - 1))

        @pl.when(c == 0)
        def _():
            flip(nv.at[j], nt)
        wait(loads(t))

        @pl.when(t >= g_slots)
        def _():
            wait(gate_stores(t - g_slots))
        for m in range(2):
            og[at, m] = jnp.dot(nt[...], ring[slot, m], preferred_element_type=F32)
        start(gate_stores(t))
        return carry
    lax.fori_loop(0, layers * n_gate, gate_body, 0)
    wait(wholes[1:])
    act_store.start()

    def out_body(t, carry):
        j, c, at = lax.div(t, n_out), lax.rem(t, n_out), lax.rem(t, o_slots)

        @pl.when(c == 0)
        def _():
            flip(uv.at[j], ut)

        @pl.when(t >= o_slots)
        def _():
            wait(out_stores(t - o_slots))

        def half(m, carry):
            oo[at, m] = jnp.dot(ut[pl.ds(pl.multiple_of(m * rows, 64), rows), :], ev[j, :, tile_at(c)], preferred_element_type=F32)
            return carry
        lax.fori_loop(0, 2, half, 0)
        start(out_stores(t))
        return carry
    lax.fori_loop(0, layers * n_out, out_body, 0)
    act_store.wait()
    for t in range(layers * n_gate - g_slots, layers * n_gate):
        wait(gate_stores(t))
    for t in range(layers * n_out - o_slots, layers * n_out):
        wait(out_stores(t))


def grads_call(no_s, u_s, da, db, e_o, act):
    layers, T, dsh = no_s.shape
    cols, dff, dmod = u_s.shape[2], da.shape[2], e_o.shape[2]
    V, wide = pltpu.VMEM, 4 * LANES
    moved = 2 * layers * T * (dsh + cols + 2 * dff + dmod) + 4 * layers * (2 * dsh * dff + cols * dmod)
    return pl.pallas_call(
        grads_kernel, name=f'grads_{T}', in_specs=[ANY] * 6, out_specs=[ANY] * 4,
        out_shape=[jax.ShapeDtypeStruct((layers, dsh, dff), F32), jax.ShapeDtypeStruct((layers, dsh, dff), F32), jax.ShapeDtypeStruct((layers, cols, dmod), F32),
                   jax.ShapeDtypeStruct(act.shape, BF16)],
        scratch_shapes=[V((layers, T, dsh), BF16), V((layers, T, cols), BF16), V((layers, T, dmod), BF16), V(act.shape, BF16), V((dsh, T), BF16), V((cols, T), BF16),
                        V((4, 2, T, wide), BF16), V((3, 2, dsh, wide), F32), V((2, 2, cols // 2, wide), F32), DMA((5,)), DMA((4, 2)), DMA((3, 2)), DMA((2, 2))],
        cost_estimate=pl.CostEstimate(flops=2 * layers * T * (2 * dsh * dff + cols * dmod), bytes_accessed=moved, transcendentals=0),
        compiler_params=pltpu.CompilerParams(vmem_limit_bytes=VMEM_LIMIT))(no_s, u_s, da, db, e_o, act)


ANY = pl.BlockSpec(memory_space=pl.ANY)
DMA = pltpu.SemaphoreType.DMA


def comm_call(kernel, name, cid, outs, in_specs, scratch):
    return pl.pallas_call(
        kernel, name=name, out_shape=[jax.ShapeDtypeStruct(*o) for o in outs], in_specs=in_specs, out_specs=[ANY] * len(outs),
        scratch_shapes=scratch, compiler_params=pltpu.CompilerParams(collective_id=cid, has_side_effects=True, vmem_limit_bytes=VMEM_LIMIT))


def lens_call(lens, tokens):
    smem, vmem = pl.BlockSpec(memory_space=pltpu.SMEM), pl.BlockSpec(memory_space=pltpu.VMEM)
    rows = tokens // LANES
    return pl.pallas_call(
        lens_kernel, name='lens', out_shape=[jax.ShapeDtypeStruct((1, 4 * tokens), jnp.int32), jax.ShapeDtypeStruct((1,), jnp.int32)],
        in_specs=[smem], out_specs=[vmem, smem],
        scratch_shapes=[pltpu.VMEM((rows, LANES), jnp.int32), pltpu.VMEM((4, rows, LANES), jnp.int32), DMA((3,)), DMA((3,))],
        compiler_params=pltpu.CompilerParams(collective_id=0, has_side_effects=True))(lens)


def forward_call(cid, T, act, cot, slot, w_gate, w_in, w_out):
    rows, dmod = act.shape
    _, dsh, dff = w_gate.shape
    cols = dff // 4
    half = T // 2
    tiles = cols // LANES
    outs = [((T, dmod), BF16), ((2, tiles, T, LANES), F32), ((2, tiles, T, LANES), F32), ((2, T, cols), BF16),
            ((2, T, dsh), BF16), ((2, T, dsh), BF16), ((2, T, LANES), F32), ((2, dsh, dff), BF16)]
    V = pltpu.VMEM
    scratch = [V((2, 2, dmod, cols), BF16), V((cols, dmod), BF16), V((2, 4, T, dsh), BF16), V((T, dmod), BF16), V((T, cols), BF16),
               V((4, T, dsh), F32), V((T, 2 * LANES), F32), V((2, 2, T, LANES), F32), V((T, LANES), F32),
               V((2, half, dsh), F32), V((2, half, dsh), F32), V((half, dsh), F32), V((half, dsh), F32), V((4 * rows, dsh), BF16),
               DMA((3,)), DMA((2, tiles)), DMA((3,)), DMA((3,)), DMA((2,)), DMA((2,)), DMA((4,)), DMA((4,)), DMA((6,)), DMA((6,)), DMA((6,)), DMA((6,)),
               DMA((2, 2)), DMA((1,)), DMA((2, 2)), DMA((4,)), DMA((4,)), pltpu.SemaphoreType.REGULAR]
    specs = [ANY, ANY, pl.BlockSpec(memory_space=pltpu.VMEM)] + [ANY] * 3
    return comm_call(forward_kernel, f'forward_{T}', cid, outs, specs, scratch)(act, cot, slot, w_gate, w_in, w_out)


def backward_call(cid, sel, slot, w_gate, w_in, w_out, a_s, b_s, ho_s, r_s):
    T, dmod = sel.shape
    _, dsh, dff = w_gate.shape
    cols = dff // 4
    tiles = cols // LANES
    chunks = (tiles + 1) // 2
    pad = -(-(T // 2) // LANES) * LANES
    slots = 2 if T <= 640 else 1
    ab_slots = 2 if T <= 832 else 1
    outs = [((2, T, dff), BF16), ((2, T, dff), BF16), ((2, T, dmod), BF16), ((slot.shape[1] // 4, dmod), BF16)]
    V = pltpu.VMEM
    scratch = [V((slots, 2, dsh, dff), BF16), V((cols, dmod), BF16), V((3, 4, T, dsh), BF16), V((2, 4, T, cols), BF16),
               V((ab_slots, 2, tiles, T // 2, LANES), F32), V((T, dsh), F32), V((2, T, dsh), BF16), V((2, T, LANES), F32), V((2, pad, LANES), F32), V((2, 4, 8, pad), F32), V((4, slot.shape[1] // 4, dsh), BF16), V((T, slot.shape[1] // 4), BF16),
               DMA((2, 2, 2, chunks)), DMA((2, 2, 2, chunks)), DMA((2, 2, chunks)), DMA((2, 2, chunks)), DMA((2, 6)), DMA((2, 6)), DMA((2, 4)), DMA((2, 4)),
               DMA((2, 3)), DMA((2, 3)), DMA((4,)), DMA((4,)), DMA((3, 2)), DMA((2, 2)), DMA((2,)), DMA((4,)), DMA((2, 2, 4)), DMA((2,))]
    return comm_call(backward_kernel, f'backward_{T}', cid, outs, [ANY, pl.BlockSpec(memory_space=pltpu.VMEM)] + [ANY] * 7, scratch)(sel, slot, w_gate, w_in, w_out, a_s, b_s, ho_s, r_s)


def solution(mesh, buckets=BUCKETS):
    act_spec = P(None, 'data')
    weight_spec = P('stage', None, 'data', None)

    def local_step(act_in, cot_out, seq_lens, w_gate, w_in, w_out):
        n_micro, n_rows, seq_len, dmod = act_in.shape
        rows = n_micro * n_rows * seq_len
        w_gate, w_in, w_out = w_gate[0], w_in[0], w_out[0]
        act, cot = act_in.reshape(rows, dmod), cot_out.reshape(rows, dmod)
        slot, count = lens_call(seq_lens.reshape(n_micro), rows)

        def branch(which, T):
            def run(_):
                sel, a_s, b_s, u_s, ho_s, no_s, r_s, _ = forward_call(1 + 2 * which, T, act, cot, slot, w_gate, w_in, w_out)
                da, db, e_o, act_grad = backward_call(2 + 2 * which, sel, slot, w_gate, w_in, w_out, a_s, b_s, ho_s, r_s)
                gate_grad, in_grad, out_grad, act_grad = grads_call(no_s, u_s, da, db, e_o, act_grad)
                return act_grad.reshape(act_in.shape), gate_grad[None], in_grad[None], out_grad[None]
            return run
        if len(buckets) == 1:
            return branch(0, buckets[0])(0)
        which = sum((count[0] > b).astype(jnp.int32) for b in buckets[:-1])
        return lax.switch(which, [branch(i, b) for i, b in enumerate(buckets)], 0)

    return jax.shard_map(local_step, mesh=mesh, in_specs=(act_spec, act_spec, act_spec, weight_spec, weight_spec, weight_spec), out_specs=(act_spec, weight_spec, weight_spec, weight_spec), check_vma=False)
```

```python
import functools

import jax
import jax.numpy as jnp
from jax import lax
from jax.experimental import pallas as pl
from jax.experimental.pallas import tpu as pltpu
from jax.sharding import PartitionSpec as P

EPSILON = 1e-6
MESH = pl.DeviceIdType.MESH
BF16, F32 = jnp.bfloat16, jnp.float32
LANES = 128
VMEM_LIMIT = 67043328
BUCKETS = (416, 480, 544, 640, 992)


def nt_dot(left, right):
    return lax.dot_general(left, right, (((1,), (1,)), ((), ())), preferred_element_type=F32)


def place():
    d = lax.axis_index('data')
    s = lax.axis_index('stage')
    x = lax.rem(d, 2)
    y = lax.div(d, 2)
    return d, s, 2 * y + 1 - x, 2 * (1 - y) + x, 3 - d


def meet(same_core=False):
    d, s, xn, yn, dg = place()
    barrier = pltpu.get_barrier_semaphore()
    peers = [(xn, s), (yn, s), (dg, s)]
    if not same_core:
        peers += [(xn, 1 - s), (yn, 1 - s), (dg, 1 - s), (d, 1 - s)]
    for chip, core in peers:
        pl.semaphore_signal(barrier, inc=1, device_id=(chip, core), device_id_type=MESH)
    pl.semaphore_wait(barrier, len(peers))


def remote(src, dst, send_sem, recv_sem, device):
    return pltpu.make_async_remote_copy(src_ref=src, dst_ref=dst, send_sem=send_sem, recv_sem=recv_sem, device_id=device, device_id_type=MESH)


def lens_kernel(lens, slot, count, mine, everyone, ss, rs):
    d, s, xn, yn, dg = place()
    meet(same_core=True)
    seqs, tokens = lens.shape[0], mine.shape[0] * LANES
    each = tokens // seqs
    index = lax.broadcasted_iota(jnp.int32, mine.shape, 0) * LANES + lax.broadcasted_iota(jnp.int32, mine.shape, 1)
    length = jnp.zeros(mine.shape, jnp.int32)
    for i in range(seqs):
        length = jnp.where((index >= i * each) & (index < (i + 1) * each), lens[i], length)
    mine[...] = jnp.where(lax.rem(index, each) < length, 1, 0)
    everyone[d] = mine[...]
    sends = [remote(mine, everyone.at[d], ss.at[i], rs.at[i], (chip, s)) for i, chip in enumerate((xn, yn, dg))]
    for copy in sends:
        copy.start()
    for copy in sends:
        copy.wait()
    rows = 4 * mine.shape[0]
    live = everyone[...].reshape(rows, LANES)
    lane, row = lax.broadcasted_iota(jnp.int32, live.shape, 1), lax.broadcasted_iota(jnp.int32, live.shape, 0)
    upto = live
    shift = 1
    while shift < LANES:
        upto = upto + jnp.where(lane >= shift, pltpu.roll(upto, shift, 1), 0)
        shift *= 2
    whole = jnp.broadcast_to(jnp.sum(live, axis=1, keepdims=True), live.shape)
    before = whole
    shift = 1
    while shift < rows:
        before = before + jnp.where(row >= shift, pltpu.roll(before, shift, 0), 0)
        shift *= 2
    place_of = jnp.where(live > 0, before - whole + upto - 1, -1)
    for i in range(rows):
        slot[:, i * LANES:(i + 1) * LANES] = place_of[i:i + 1, :]
    count[0] = jnp.sum(live)


def share_rows(buf, d, s, xn, yn, ss, rs, lo, hi):
    def own(part, i):
        return [remote(buf.at[d, part], buf.at[d, part], ss.at[2 * i + n], rs.at[2 * i + n], (chip, s)) for n, chip in enumerate((xn, yn))]

    fwd_y = remote(buf.at[xn, lo], buf.at[xn, lo], ss.at[4], rs.at[4], (yn, s))
    fwd_x = remote(buf.at[yn, hi], buf.at[yn, hi], ss.at[5], rs.at[5], (xn, s))
    return own(lo, 0), own(hi, 1), fwd_y, fwd_x


def near_share(share):
    own_lo, own_hi, fwd_y, fwd_x = share
    own_lo[0].wait_recv()
    fwd_y.start()
    own_hi[1].wait_recv()
    fwd_x.start()


def far_share(share):
    own_lo, own_hi, fwd_y, fwd_x = share
    own_hi[0].wait_recv()
    own_lo[1].wait_recv()
    fwd_y.wait_recv()
    fwd_x.wait_recv()
    for copy in own_lo + own_hi + [fwd_y, fwd_x]:
        copy.wait_send()


def forward_kernel(act, cot, slot, w_gate, w_in, w_out,
                   sel_o, a_s, b_s, u_s, ho_s, no_s, r_s, other,
                   wv, wov, hb, nb, ub, zp, acc, ab, rv, near_in, far_in, inpv,
                   wss, wrs, iss, irs, xss, xrs, hss, hrs, ass, ars, zss, zrs, lw, lo, lab, lsv, lin, go):
    d, s, xn, yn, dg = place()
    T = nb.shape[0]
    half = T // 2
    piece = T if T <= 640 else half
    cols = ub.shape[1]
    tiles = cols // LANES
    dm = hb.shape[3]
    rows_in = act.shape[0]
    lo_rows, hi_rows = pl.ds(0, half), pl.ds(half, half)
    chips = (dg, xn, yn)
    cuts, early_tiles = (2, 5), 2

    def block_of(chip):
        return pl.ds(pl.multiple_of(chip * dm, dm), dm)

    def input_rows(chip):
        return pl.ds(pl.multiple_of(chip * rows_in, LANES), rows_in)

    def own_loads(j):
        return [pltpu.make_async_copy(w.at[j, :, pl.ds(pl.multiple_of(d * cols, LANES), cols)], wv.at[j, m, block_of(d)], lw.at[j, m])
                for m, w in enumerate((w_gate, w_in))]

    def start_weights(layer, src, core, sem, first, last):
        def body(k, carry):
            col = pl.ds(pl.multiple_of(k * LANES, LANES), LANES)
            for chip in chips:
                from_col = pl.ds(pl.multiple_of(chip * cols + k * LANES, LANES), LANES)
                for m in range(2):
                    remote(src[m].at[:, from_col], wv.at[layer, m, block_of(d), col], wss.at[sem], wrs.at[layer, k], (chip, core)).start()
            return carry
        lax.fori_loop(first, last, body, 0)

    def wait_sent(sem, count):
        sent = wv.at[0, :, pl.ds(0, 3 * dm), pl.ds(0, count * LANES)]
        pltpu.make_async_copy(sent, sent, wss.at[sem]).wait()

    def wait_tile(layer, k, col):
        came = wv.at[layer, :, pl.ds(0, 3 * dm), col]
        pltpu.make_async_copy(came, came, wrs.at[layer, k]).wait()

    other_pair = (other.at[0], other.at[1])
    first_pair, second_pair = (w_gate.at[0], w_in.at[0]), (w_gate.at[1], w_in.at[1])

    def input_sends(src):
        return [remote(src.at[:, block_of(chip)], inpv.at[input_rows(d)], iss.at[i], irs.at[i], (chip, s)) for i, chip in enumerate(chips)]

    def own_input(src):
        return pltpu.make_async_copy(src.at[:, block_of(d)], inpv.at[input_rows(d)], lin.at[0])
    share = share_rows(hb.at[s], d, s, xn, yn, ass, ars, lo_rows, hi_rows)

    def first_weights(first, last):
        @pl.when(s == 0)
        def _():
            start_weights(0, first_pair, 0, 0, first, last)
    meet()
    for n, src in enumerate((act, cot)):
        @pl.when(s == n)
        def _():
            for copy in input_sends(src) + [own_input(src)]:
                copy.start()
    first_weights(0, cuts[0])
    swaps = [remote(w.at[1], other.at[m], xss.at[m], xrs.at[m], (d, 1 - s)) for m, w in enumerate((w_gate, w_in))]
    for copy in own_loads(0) + own_loads(1) + swaps:
        copy.start()
    pltpu.make_async_copy(w_out.at[0], wov, lo.at[0]).start()
    for copy in input_sends(act):
        copy.wait()
    own_input(act).wait()
    tokens = slot.shape[1]

    def pick_body(i, carry):
        base = pl.multiple_of(i * half, 16)
        pick = (lax.broadcasted_iota(jnp.int32, (half, tokens), 0) + base == slot[...]).astype(BF16)
        hb[s, d, pl.ds(base, half), :] = jnp.dot(pick, inpv[...], preferred_element_type=F32).astype(BF16)
        return carry
    lax.fori_loop(0, 2, pick_body, 0)
    for copy in share[0] + share[1]:
        copy.start()
    first_weights(cuts[0], cuts[1])
    near_share(share)
    first_weights(cuts[1], tiles)
    far_share(share)
    for copy in swaps:
        copy.wait()

    def hand_over():
        return [remote(hb.at[0, c], hb.at[0, c], hss.at[i], hrs.at[i], (d, 1 - s)) for i, c in enumerate((d, xn, yn, dg))]

    @pl.when(s == 1)
    def _():
        top = [pltpu.make_async_copy(hb.at[1, c], sel_o.at[:, pl.ds(c * dm, dm)], lin.at[c]) for c in range(4)]
        for copy in top:
            copy.start()
        pl.semaphore_wait(go, 1)
        start_weights(1, other_pair, 0, 0, 0, tiles)
        start_weights(0, first_pair, 1, 1, 0, tiles)
        start_weights(1, second_pair, 1, 2, 0, early_tiles)
        for copy in top:
            copy.wait()
        for copy in hand_over():
            copy.wait_recv()

    def layer(j, carry):
        nxt = 1 - j
        step = 32

        def norm_body(i, carry):
            rows = pl.ds(pl.multiple_of(i * step, step), step)
            blocks = [hb[j, c, rows, :].astype(F32) for c in range(4)]
            total = sum(jnp.sum(b * b, axis=-1, keepdims=True) for b in blocks)
            inv = lax.rsqrt(total * (1.0 / (4 * dm)) + EPSILON)
            for c in range(4):
                nb[rows, c * dm:(c + 1) * dm] = (blocks[c] * inv).astype(BF16)
            rv[rows, :] = jnp.broadcast_to(inv, (step, LANES))
            return carry
        lax.fori_loop(0, T // step, norm_body, 0)
        saves = [
            pltpu.make_async_copy(hb.at[j, d], ho_s.at[j], lsv.at[0]),
            pltpu.make_async_copy(nb.at[:, block_of(d)], no_s.at[j], lsv.at[1]),
            pltpu.make_async_copy(rv, r_s.at[j], lsv.at[2]),
        ]
        for copy in saves:
            copy.start()
        for copy in own_loads(j):
            copy.wait()

        def ab_copies(k, side):
            return [pltpu.make_async_copy(ab.at[side, 0], a_s.at[j, k], lab.at[side, 0]),
                    pltpu.make_async_copy(ab.at[side, 1], b_s.at[j, k], lab.at[side, 1])]

        def ab_body(k, carry):
            col = pl.ds(pl.multiple_of(k * LANES, LANES), LANES)
            wait_tile(j, k, col)

            @pl.when((j == 0) & (s == 0) & (k == tiles - 2))
            def _():
                pl.semaphore_signal(go, inc=1, device_id=(d, 1), device_id_type=MESH)

            def ab_rows(i, carry):
                rows = pl.ds(pl.multiple_of(i * piece, 16), piece)
                acc[rows, :] = jnp.dot(nb[rows, :], jnp.concatenate([wv[j, 0, :, col], wv[j, 1, :, col]], axis=1), preferred_element_type=F32)
                return carry
            lax.fori_loop(0, T // piece, ab_rows, 0)
            side = lax.rem(k, 2)

            @pl.when(k >= 2)
            def _():
                for copy in ab_copies(k, side):
                    copy.wait()
            a, b = acc[:, :LANES], acc[:, LANES:]
            ab[side, 0] = a
            ab[side, 1] = b
            ub[:, col] = (a * jax.nn.sigmoid(a) * b).astype(BF16)
            for copy in ab_copies(k, side):
                copy.start()
            return carry
        lax.fori_loop(0, tiles, ab_body, 0)
        for k in (tiles - 2, tiles - 1):
            for copy in ab_copies(k, k % 2):
                copy.wait()
        save_u = pltpu.make_async_copy(ub, u_s.at[j], lsv.at[3])
        save_u.start()

        @pl.when((j == 0) | (s == 0))
        def _():
            pltpu.make_async_copy(w_out.at[j], wov, lo.at[0]).wait()

            def send(i, c, rows, dst, chip):
                return remote(zp.at[c, rows], dst, zss.at[i], zrs.at[i], (chip, s))
            first = [send(0, dg, lo_rows, near_in.at[0, 0], xn), send(1, dg, hi_rows, near_in.at[1, 0], yn)]
            second = [send(2, xn, lo_rows, near_in.at[0, 1], xn), send(3, yn, hi_rows, near_in.at[1, 1], yn)]
            third = [send(4, yn, lo_rows, far_in.at[0], yn), send(5, xn, hi_rows, far_in.at[1], xn)]
            x, y = lax.rem(d, 2), lax.div(d, 2)
            wide = 2 * LANES

            def block_body(i, carry):
                rel, part_of = 3 - lax.div(i, 2), lax.rem(i, 2)
                c = 2 * lax.rem(y + lax.rem(rel, 2), 2) + lax.rem(x + lax.div(rel, 2), 2)

                def zp_rows(n, carry):
                    rows = pl.ds(pl.multiple_of(n * piece, 16), piece)
                    zp[c, rows, pl.ds(pl.multiple_of(part_of * wide, wide), wide)] = jnp.dot(
                        ub[rows, :], wov[:, pl.ds(pl.multiple_of(c * dm + part_of * wide, wide), wide)], preferred_element_type=F32)
                    return carry
                lax.fori_loop(0, T // piece, zp_rows, 0)
                for at, copies in ((1, first), (3, second[:1]), (5, second[1:])):
                    @pl.when(i == at)
                    def _():
                        for copy in copies:
                            copy.start()
                return carry
            lax.fori_loop(0, 8, block_body, 0)
            share = share_rows(hb.at[nxt], d, s, xn, yn, ass, ars, lo_rows, hi_rows)

            def both(n, stage):
                for at in range(2):
                    @pl.when(n == at)
                    def _():
                        stage(at)

            def half_rows(n):
                return pl.ds(pl.multiple_of(n * half, 16), half)

            def relay(n, carry):
                both(n, lambda at: first[at].wait_recv())
                c, rows = yn + n * (xn - yn), half_rows(n)
                zp[c, rows, :] += near_in[n, 0]
                both(n, lambda at: third[at].start())
                return carry
            lax.fori_loop(0, 2, relay, 0)

            def settle(n, carry):
                both(n, lambda at: (second[at].wait_recv(), third[at].wait_recv()))
                rows = half_rows(n)
                branch = (zp[d, rows, :] + near_in[n, 1] + far_in[n]).astype(BF16).astype(F32)
                hb[nxt, d, rows, :] = (hb[j, d, rows, :].astype(F32) + branch).astype(BF16)
                both(n, lambda at: [copy.start() for copy in share[at]])
                return carry
            lax.fori_loop(0, 2, settle, 0)
            near_share(share)
            far_share(share)
            for copy in first + second + third:
                copy.wait_send()

        @pl.when((j == 0) & (s == 0))
        def _():
            pltpu.make_async_copy(w_out.at[1], wov, lo.at[0]).start()

        @pl.when((j == 1) & (s == 0))
        def _():
            hands = hand_over()
            for copy in hands:
                copy.start()
            start_weights(1, other_pair, 1, 1, early_tiles, tiles)
            for copy in hands:
                copy.wait_send()
        for copy in saves:
            copy.wait()
        save_u.wait()
        return carry
    lax.fori_loop(0, 2, layer, 0)
    wait_sent(0, tiles)

    @pl.when(s == 0)
    def _():
        wait_sent(1, tiles - early_tiles)

    @pl.when(s == 1)
    def _():
        wait_sent(1, tiles)
        wait_sent(2, early_tiles)


def backward_kernel(sel, slot, w_gate, w_in, w_out, a_s, b_s, ho_s, r_s,
                    da_o, db_o, e_o, act_o,
                    wgv, wov, eb, daf, ab, dn, hov, rv, sq, sv, agv, back_v,
                    dss, drs, fss, frs, ess, ers, hss, hrs, sss, srs, ass, ars, lw, lab, lout, lh, le, lsm):
    d, s, xn, yn, dg = place()
    T = sel.shape[0]
    part_rows = T // 2
    lo_n = -(-part_rows // 32) * 16
    cols = daf.shape[3]
    dm = dn.shape[1]
    wide = 2 * LANES
    n_full = cols // wide
    tail = cols - n_full * wide
    n_early = n_full // 2
    n_mid = n_early + 2
    pad = sq.shape[1]
    w_slots = wgv.shape[0]
    ab_slots = ab.shape[0]

    def wo_load(j):
        return pltpu.make_async_copy(w_out.at[j], wov, lw.at[0, 0])

    def slot_of(j, n):
        return j if n == 2 else 0

    def gate_loads(j):
        return [pltpu.make_async_copy(w.at[j], wgv.at[slot_of(j, w_slots), m], lw.at[1 + slot_of(j, w_slots), m]) for m, w in enumerate((w_gate, w_in))]

    def rows_of(g, base=0, size=part_rows):
        return pl.ds(pl.multiple_of(g * part_rows + base, 16), size)

    def in_copies(g):
        return [pltpu.make_async_copy(sel.at[rows_of(g), pl.ds(c * dm, dm)], eb.at[2, c, rows_of(g)], lh.at[g, c]) for c in range(4)]

    def hand_over(g):
        return [remote(eb.at[0, c, rows_of(g)], eb.at[2, c, rows_of(g)], hss.at[g, i], hrs.at[g, i], (d, 1 - s)) for i, c in enumerate((d, xn, yn, dg))]

    def ab_loads(j, g):
        side = slot_of(g, ab_slots)
        return [pltpu.make_async_copy(src.at[j, :, rows_of(g)], ab.at[side, m], lab.at[side, m]) for m, src in enumerate((a_s, b_s))]

    @pl.when(s == 1)
    def _():
        for copy in in_copies(0):
            copy.start()
    wo_load(1).start()
    small = [pltpu.make_async_copy(ho_s, hov, lsm.at[0]), pltpu.make_async_copy(r_s, rv, lsm.at[1])]
    for copy in ab_loads(1, 0):
        copy.start()
    meet()

    def columns(c, width):
        return pl.ds(pl.multiple_of(c * wide, LANES), width)

    def each_chunk(body, first=0, last=n_full):
        lax.fori_loop(first, last, lambda c, carry: (body(c, wide), carry)[1], 0)

    class Piece:
        def __init__(self, j, g):
            self.j, self.g, self.rows = j, g, rows_of(g)
            parts = (rows_of(g, 0, lo_n), rows_of(g, lo_n, part_rows - lo_n))
            self.share = share_rows(eb.at[j], d, s, xn, yn, ess.at[g], ers.at[g], *parts)
            self.e_saves = [pltpu.make_async_copy(eb.at[j + 1, c, self.rows], e_o.at[j, self.rows, pl.ds(c * dm, dm)], le.at[j, g, c]) for c in range(4)]
            self.sums = [remote(sv.at[g, 0], sv.at[g, 1 + i], sss.at[g, i], srs.at[g, i], (chip, s)) for i, chip in enumerate((xn, yn, dg))]

        def own_sends(self, c, col):
            g, out = self.g, []
            for m in range(2):
                for n, chip in enumerate((xn, yn)):
                    here = daf.at[m, d, self.rows, col]
                    out.append(remote(here, here, dss.at[g, m, n, c], drs.at[g, m, n, c], (chip, s)))
            return out

        def forwards(self, c, col):
            g = self.g
            from_x, from_y = daf.at[0, xn, self.rows, col], daf.at[1, yn, self.rows, col]
            return [remote(from_x, from_x, fss.at[g, 1, c], frs.at[g, 1, c], (yn, s)), remote(from_y, from_y, fss.at[g, 0, c], frs.at[g, 0, c], (xn, s))]

        def make(self):
            j, g, rows, side = self.j, self.g, self.rows, slot_of(self.g, ab_slots)
            for copy in self.e_saves:
                copy.start()

            @pl.when(g == 0)
            def _():
                wo_load(j).wait()
            for copy in ab_loads(j, g):
                copy.wait()

            @pl.when((j == 1) & (g == 0))
            def _():
                if ab_slots == 2:
                    for copy in ab_loads(1, 1):
                        copy.start()

                @pl.when(s == 1)
                def _():
                    for copy in in_copies(1):
                        copy.start()
                for copy in gate_loads(1) + small:
                    copy.start()
            if w_slots == 2:
                @pl.when((j == 1) & (g == 1))
                def _():
                    for copy in gate_loads(0):
                        copy.start()

            def tile(c, width):
                e_all = jnp.concatenate([eb[j + 1, n, rows, :] for n in range(4)], axis=1)
                dn[rows, :width] = nt_dot(e_all, wov[columns(c, width), :])
                for n in range(width // LANES):
                    lane = pl.ds(pl.multiple_of(c * wide + n * LANES, LANES), LANES)
                    a, b, du = ab[side, 0, 2 * c + n], ab[side, 1, 2 * c + n], dn[rows, n * LANES:(n + 1) * LANES]
                    sig = jax.nn.sigmoid(a)
                    daf[0, d, rows, lane] = (du * b * sig * (1.0 + a * (1.0 - sig))).astype(BF16)
                    daf[1, d, rows, lane] = (du * (a * sig)).astype(BF16)

            def body(c, width):
                tile(c, wide)

                @pl.when(c < n_early)
                def _():
                    for copy in self.own_sends(c, columns(c, wide)):
                        copy.start()
            each_chunk(body)
            tile(n_full, tail)

        def send(self, first, last):
            def body(c, width):
                for copy in self.own_sends(c, columns(c, width)):
                    copy.start()
            each_chunk(body, first, last)

        def save_tile(self, m, chip, col, c, width):
            dst = (da_o, db_o)[m].at[self.j, self.rows, pl.ds(pl.multiple_of(chip * cols + c * wide, LANES), width)]
            pltpu.make_async_copy(daf.at[m, chip, self.rows, col], dst, lout.at[self.g]).start()

        def add(self, chip, c, width):
            def body(m, carry):
                w = wgv[slot_of(self.j, w_slots), m, :, pl.ds(pl.multiple_of(chip * cols + c * wide, LANES), width)]
                dn[self.rows, :] += nt_dot(daf[m, chip, self.rows, columns(c, width)], w)
                return carry
            lax.fori_loop(0, 2, body, 0)

        def own(self):
            @pl.when(self.g == 0)
            def _():
                for copy in gate_loads(self.j):
                    copy.wait()
            for m in range(2):
                self.save_tile(m, d, pl.ds(0, cols), 0, cols)
            dn[self.rows, :] = jnp.zeros((part_rows, dm), F32)
            each_chunk(lambda c, width: self.add(d, c, width))
            self.add(d, n_full, tail)

        def near(self, c, width):
            col = columns(c, width)
            fwd_y, fwd_x = self.forwards(c, col)

            def came(m, n, chip):
                there = daf.at[m, chip, self.rows, col]
                remote(there, there, dss.at[self.g, m, n, c], drs.at[self.g, m, n, c], (chip, s)).wait_recv()
            came(0, 0, xn)
            fwd_y.start()
            came(1, 1, yn)
            fwd_x.start()
            came(1, 0, xn)
            came(0, 1, yn)
            for chip in (xn, yn):
                for m in range(2):
                    self.save_tile(m, chip, col, c, width)
            lax.fori_loop(0, 2, lambda i, carry: (self.add(xn + i * (yn - xn), c, width), carry)[1], 0)

        def far(self):
            j, g, rows = self.j, self.g, self.rows

            def body(c, width):
                col = columns(c, width)
                there = [daf.at[m, dg, rows, col] for m in range(2)]
                remote(there[0], there[0], fss.at[g, 1, c], frs.at[g, 1, c], (yn, s)).wait_recv()
                remote(there[1], there[1], fss.at[g, 0, c], frs.at[g, 0, c], (xn, s)).wait_recv()
                for m in range(2):
                    self.save_tile(m, dg, col, c, width)
                self.add(dg, c, width)
            each_chunk(body)
            body(n_full, tail)

            @pl.when((j == 1) & (g == 0))
            def _():
                for copy in small:
                    copy.wait()
            prod = dn[rows, :] * hov[j, rows, :].astype(F32)
            sq[g, :part_rows, :] = (prod[:, :LANES] + prod[:, LANES:2 * LANES]) + (prod[:, 2 * LANES:3 * LANES] + prod[:, 3 * LANES:])
            sv[g, 0] = jnp.broadcast_to(jnp.sum(sq[g].T, axis=0, keepdims=True), (8, pad))
            for copy in self.sums:
                copy.start()
            if w_slots == 1:
                @pl.when((j == 1) & (g == 1))
                def _():
                    for copy in gate_loads(0):
                        copy.start()

        def finish(self):
            j, g = self.j, self.g
            whole = daf.at[:, :, self.rows]
            pltpu.make_async_copy(whole, whole, lout.at[g]).wait()

            def drain(c, width):
                col = columns(c, width)
                for copy in self.own_sends(c, col) + self.forwards(c, col):
                    copy.wait_send()
            each_chunk(drain)
            drain(n_full, tail)
            for copy in self.sums:
                copy.wait()
            mean = ((sv[g, 0, 0:1, :] + sv[g, 1, 0:1, :]) + (sv[g, 2, 0:1, :] + sv[g, 3, 0:1, :])) * (1.0 / (4 * dm))
            sq[g] = jnp.broadcast_to(mean, (LANES, pad)).T
            for n, (base, size) in enumerate(((0, lo_n), (lo_n, part_rows - lo_n))):
                at = rows_of(g, base, size)
                inv, avg = rv[j, at, :], sq[g, base:base + size, :]
                for c in range(4):
                    lane = slice(c * LANES, (c + 1) * LANES)
                    resid = inv * dn[at, lane] - hov[j, at, lane].astype(F32) * (inv * inv * inv) * avg
                    eb[j, d, at, lane] = (eb[j + 1, d, at, lane].astype(F32) + resid).astype(BF16)
                for copy in self.share[n]:
                    copy.start()

    def step(i, carry):
        g = lax.rem(i, 2)
        cur = Piece(1 - lax.div(i, 2), g)
        prev = Piece(1 - lax.div(i - 1, 2), 1 - g)
        live, later = i < 4, i > 0

        @pl.when(i >= 2)
        def _():
            far_share(Piece(1 - lax.div(i - 2, 2), g).share)

        @pl.when((i == 4) & (s == 1))
        def _():
            for copy in hand_over(0):
                copy.start()

        @pl.when(live)
        def _():
            @pl.when((i < 2) & (s == 0))
            def _():
                for copy in hand_over(g):
                    copy.wait_recv()

            @pl.when((i < 2) & (s == 1))
            def _():
                for copy in in_copies(g):
                    copy.wait()

            cur.make()

            @pl.when(i == 1)
            def _():
                wo_load(0).start()
            coming = i + ab_slots

            @pl.when(coming < 4)
            def _():
                for copy in ab_loads(1 - lax.div(coming, 2), lax.rem(coming, 2)):
                    copy.start()

        @pl.when(later)
        def _():
            prev.far()

        def halves(h, carry):
            @pl.when(live)
            def _():
                cur.send(n_early + h * (n_mid - n_early), n_mid + h * (n_full - n_mid))

            @pl.when(live & (h == 0))
            def _():
                cur.own()

            @pl.when(live & (h == 1))
            def _():
                for copy in cur.own_sends(n_full, columns(n_full, tail)):
                    copy.start()

            @pl.when(later & (h == 1))
            def _():
                near_share(prev.share)

            @pl.when(live)
            def _():
                each_chunk(cur.near, h * n_early, n_early + h * (n_full - n_early))

            @pl.when(later & (h == 0))
            def _():
                prev.finish()
            return carry
        lax.fori_loop(0, 2, halves, 0)

        @pl.when(live)
        def _():
            cur.near(n_full, tail)
        return carry
    lax.fori_loop(0, 5, step, 0)

    def act_copies(i, c):
        col = pl.ds(pl.multiple_of(c * dm, dm), dm)
        return remote(agv.at[c], act_o.at[:, col], ass.at[i], ars.at[i], (d, 1 - s)), pltpu.make_async_copy(agv.at[c], act_o.at[:, col], lh.at[0, i])

    @pl.when(s == 1)
    def _():
        far_share(Piece(0, 1).share)
        for copy in hand_over(1):
            copy.start()
        for i, c in enumerate((d, xn, yn, dg)):
            act_copies(i, c)[0].wait_recv()

    @pl.when(s == 0)
    def _():
        own_lo, own_hi, fwd_y, fwd_x = Piece(0, 1).share
        rows_out = agv.shape[1]
        own_slots = slot[:, pl.ds(pl.multiple_of(d * rows_out, LANES), rows_out)]
        back = (lax.broadcasted_iota(jnp.int32, (T, rows_out), 0) == own_slots).astype(BF16)
        back_v[...] = back
        came = ((), (own_hi[0],), (own_lo[1],), (fwd_y, fwd_x))
        x, y = lax.rem(d, 2), lax.div(d, 2)

        def spread(i, carry):
            for n in range(1, 4):
                @pl.when(i == n)
                def _():
                    for copy in came[n]:
                        copy.wait_recv()
            c = 2 * lax.rem(y + lax.div(i, 2), 2) + lax.rem(x + lax.rem(i, 2), 2)
            agv[c] = lax.dot_general(back_v[...], eb[0, c], (((0,), (0,)), ((), ())), preferred_element_type=F32).astype(BF16)
            for copy in act_copies(i, c):
                copy.start()
            return carry
        lax.fori_loop(0, 4, spread, 0)
        for copy in own_lo + own_hi + [fwd_y, fwd_x]:
            copy.wait_send()
        for i, c in enumerate((d, xn, yn, dg)):
            away, here = act_copies(i, c)
            away.wait_send()
            here.wait()
    def saved(i, carry):
        for copy in Piece(lax.div(i, 2), lax.rem(i, 2)).e_saves:
            copy.wait()
        return carry
    lax.fori_loop(0, 4, saved, 0)

    @pl.when(s == 1)
    def _():
        for g in range(2):
            for copy in hand_over(g):
                copy.wait_send()


def grads_kernel(no_s, u_s, da, db, e_o, act, gate_o, in_o, out_o, act_o, nv, uv, ev, av, nt, ut, ring, og, oo, ln, lr, lg, lo):
    layers = nv.shape[0]
    wide = ring.shape[3]
    n_gate, n_out = da.shape[2] // wide, e_o.shape[2] // wide
    slots, g_slots, o_slots = ring.shape[0], og.shape[0], oo.shape[0]
    rows = oo.shape[2]

    def flip(src, dst):
        def body(i, carry):
            lane = pl.ds(pl.multiple_of(i * LANES, LANES), LANES)
            dst[lane, :] = src[:, lane].T
            return carry
        lax.fori_loop(0, dst.shape[0] // LANES, body, 0)
    wholes = [pltpu.make_async_copy(src, dst, ln.at[i]) for i, (src, dst) in enumerate(((no_s, nv), (u_s, uv), (e_o, ev), (act, av)))]
    act_store = pltpu.make_async_copy(av, act_o, ln.at[4])

    def tile_at(c):
        return pl.ds(pl.multiple_of(c * wide, wide), wide)

    def loads(t):
        slot = lax.rem(t, slots)
        return [pltpu.make_async_copy(src.at[lax.div(t, n_gate), :, tile_at(lax.rem(t, n_gate))], ring.at[slot, m], lr.at[slot, m]) for m, src in enumerate((da, db))]

    def gate_stores(t):
        slot = lax.rem(t, g_slots)
        return [pltpu.make_async_copy(og.at[slot, m], dst.at[lax.div(t, n_gate), :, tile_at(lax.rem(t, n_gate))], lg.at[slot, m]) for m, dst in enumerate((gate_o, in_o))]

    def out_stores(t):
        slot = lax.rem(t, o_slots)
        return [pltpu.make_async_copy(oo.at[slot, m], out_o.at[lax.div(t, n_out), pl.ds(m * rows, rows), tile_at(lax.rem(t, n_out))], lo.at[slot, m]) for m in range(2)]

    def start(copies):
        for copy in copies:
            copy.start()

    def wait(copies):
        for copy in copies:
            copy.wait()
    wholes[0].start()
    for t in range(slots - 1):
        start(loads(t))
    start(wholes[1:])
    wholes[0].wait()

    def gate_body(t, carry):
        j, c, slot, at = lax.div(t, n_gate), lax.rem(t, n_gate), lax.rem(t, slots), lax.rem(t, g_slots)

        @pl.when(t + slots - 1 < layers * n_gate)
        def _():
            start(loads(t + slots - 1))

        @pl.when(c == 0)
        def _():
            flip(nv.at[j], nt)
        wait(loads(t))

        @pl.when(t >= g_slots)
        def _():
            wait(gate_stores(t - g_slots))

        def side(m, carry):
            og[at, m] = jnp.dot(nt[...], ring[slot, m], preferred_element_type=F32)
            return carry
        lax.fori_loop(0, 2, side, 0)
        start(gate_stores(t))
        return carry
    lax.fori_loop(0, layers * n_gate, gate_body, 0)
    wait(wholes[1:])
    act_store.start()

    def out_body(t, carry):
        j, c, at = lax.div(t, n_out), lax.rem(t, n_out), lax.rem(t, o_slots)

        @pl.when(c == 0)
        def _():
            flip(uv.at[j], ut)

        @pl.when(t >= o_slots)
        def _():
            wait(out_stores(t - o_slots))

        def half(m, carry):
            oo[at, m] = jnp.dot(ut[pl.ds(pl.multiple_of(m * rows, 64), rows), :], ev[j, :, tile_at(c)], preferred_element_type=F32)
            return carry
        lax.fori_loop(0, 2, half, 0)
        start(out_stores(t))
        return carry
    lax.fori_loop(0, layers * n_out, out_body, 0)
    act_store.wait()
    for t in range(layers * n_gate - g_slots, layers * n_gate):
        wait(gate_stores(t))
    for t in range(layers * n_out - o_slots, layers * n_out):
        wait(out_stores(t))


def grads_call(no_s, u_s, da, db, e_o, act):
    layers, T, dsh = no_s.shape
    cols, dff, dmod = u_s.shape[2], da.shape[2], e_o.shape[2]
    V, wide = pltpu.VMEM, 4 * LANES
    moved = 2 * layers * T * (dsh + cols + 2 * dff + dmod) + 4 * layers * (2 * dsh * dff + cols * dmod)
    return pl.pallas_call(
        grads_kernel, name=f'grads_{T}', in_specs=[ANY] * 6, out_specs=[ANY] * 4,
        out_shape=[jax.ShapeDtypeStruct((layers, dsh, dff), F32), jax.ShapeDtypeStruct((layers, dsh, dff), F32), jax.ShapeDtypeStruct((layers, cols, dmod), F32),
                   jax.ShapeDtypeStruct(act.shape, BF16)],
        scratch_shapes=[V((layers, T, dsh), BF16), V((layers, T, cols), BF16), V((layers, T, dmod), BF16), V(act.shape, BF16), V((dsh, T), BF16), V((cols, T), BF16),
                        V((6, 2, T, wide), BF16), V((4, 2, dsh, wide), F32), V((3, 2, cols // 2, wide), F32), DMA((5,)), DMA((6, 2)), DMA((4, 2)), DMA((3, 2))],
        cost_estimate=pl.CostEstimate(flops=2 * layers * T * (2 * dsh * dff + cols * dmod), bytes_accessed=moved, transcendentals=0),
        compiler_params=pltpu.CompilerParams(vmem_limit_bytes=VMEM_LIMIT))(no_s, u_s, da, db, e_o, act)


ANY = pl.BlockSpec(memory_space=pl.ANY)
DMA = pltpu.SemaphoreType.DMA


def comm_call(kernel, name, cid, outs, in_specs, scratch):
    return pl.pallas_call(
        kernel, name=name, out_shape=[jax.ShapeDtypeStruct(*o) for o in outs], in_specs=in_specs, out_specs=[ANY] * len(outs),
        scratch_shapes=scratch, compiler_params=pltpu.CompilerParams(collective_id=cid, has_side_effects=True, vmem_limit_bytes=VMEM_LIMIT))


def lens_call(lens, tokens):
    smem, vmem = pl.BlockSpec(memory_space=pltpu.SMEM), pl.BlockSpec(memory_space=pltpu.VMEM)
    rows = tokens // LANES
    return pl.pallas_call(
        lens_kernel, name='lens', out_shape=[jax.ShapeDtypeStruct((1, 4 * tokens), jnp.int32), jax.ShapeDtypeStruct((1,), jnp.int32)],
        in_specs=[smem], out_specs=[vmem, smem],
        scratch_shapes=[pltpu.VMEM((rows, LANES), jnp.int32), pltpu.VMEM((4, rows, LANES), jnp.int32), DMA((3,)), DMA((3,))],
        compiler_params=pltpu.CompilerParams(collective_id=0, has_side_effects=True))(lens)


def forward_call(cid, T, act, cot, slot, w_gate, w_in, w_out):
    rows, dmod = act.shape
    _, dsh, dff = w_gate.shape
    cols = dff // 4
    half = T // 2
    tiles = cols // LANES
    outs = [((T, dmod), BF16), ((2, tiles, T, LANES), F32), ((2, tiles, T, LANES), F32), ((2, T, cols), BF16),
            ((2, T, dsh), BF16), ((2, T, dsh), BF16), ((2, T, LANES), F32), ((2, dsh, dff), BF16)]
    V = pltpu.VMEM
    scratch = [V((2, 2, dmod, cols), BF16), V((cols, dmod), BF16), V((2, 4, T, dsh), BF16), V((T, dmod), BF16), V((T, cols), BF16),
               V((4, T, dsh), F32), V((T, 2 * LANES), F32), V((2, 2, T, LANES), F32), V((T, LANES), F32),
               V((2, 2, half, dsh), F32), V((2, half, dsh), F32), V((4 * rows, dsh), BF16),
               DMA((3,)), DMA((2, tiles)), DMA((3,)), DMA((3,)), DMA((2,)), DMA((2,)), DMA((4,)), DMA((4,)), DMA((6,)), DMA((6,)), DMA((6,)), DMA((6,)),
               DMA((2, 2)), DMA((1,)), DMA((2, 2)), DMA((4,)), DMA((4,)), pltpu.SemaphoreType.REGULAR]
    specs = [ANY, ANY, pl.BlockSpec(memory_space=pltpu.VMEM)] + [ANY] * 3
    return comm_call(forward_kernel, f'forward_{T}', cid, outs, specs, scratch)(act, cot, slot, w_gate, w_in, w_out)


def backward_call(cid, sel, slot, w_gate, w_in, w_out, a_s, b_s, ho_s, r_s):
    T, dmod = sel.shape
    _, dsh, dff = w_gate.shape
    cols = dff // 4
    tiles = cols // LANES
    chunks = (tiles + 1) // 2
    pad = -(-(T // 2) // LANES) * LANES
    slots = 2 if T <= 640 else 1
    ab_slots = 2 if T <= 832 else 1
    outs = [((2, T, dff), BF16), ((2, T, dff), BF16), ((2, T, dmod), BF16), ((slot.shape[1] // 4, dmod), BF16)]
    V = pltpu.VMEM
    scratch = [V((slots, 2, dsh, dff), BF16), V((cols, dmod), BF16), V((3, 4, T, dsh), BF16), V((2, 4, T, cols), BF16),
               V((ab_slots, 2, tiles, T // 2, LANES), F32), V((T, dsh), F32), V((2, T, dsh), BF16), V((2, T, LANES), F32), V((2, pad, LANES), F32), V((2, 4, 8, pad), F32), V((4, slot.shape[1] // 4, dsh), BF16), V((T, slot.shape[1] // 4), BF16),
               DMA((2, 2, 2, chunks)), DMA((2, 2, 2, chunks)), DMA((2, 2, chunks)), DMA((2, 2, chunks)), DMA((2, 6)), DMA((2, 6)), DMA((2, 4)), DMA((2, 4)),
               DMA((2, 3)), DMA((2, 3)), DMA((4,)), DMA((4,)), DMA((3, 2)), DMA((2, 2)), DMA((2,)), DMA((2, 4)), DMA((2, 2, 4)), DMA((2,))]
    return comm_call(backward_kernel, f'backward_{T}', cid, outs, [ANY, pl.BlockSpec(memory_space=pltpu.VMEM)] + [ANY] * 7, scratch)(sel, slot, w_gate, w_in, w_out, a_s, b_s, ho_s, r_s)


def solution(mesh, buckets=BUCKETS):
    act_spec = P(None, 'data')
    weight_spec = P('stage', None, 'data', None)

    def local_step(act_in, cot_out, seq_lens, w_gate, w_in, w_out):
        n_micro, n_rows, seq_len, dmod = act_in.shape
        rows = n_micro * n_rows * seq_len
        w_gate, w_in, w_out = w_gate[0], w_in[0], w_out[0]
        act, cot = act_in.reshape(rows, dmod), cot_out.reshape(rows, dmod)
        slot, count = lens_call(seq_lens.reshape(n_micro), rows)

        def branch(which, T):
            def run(_):
                sel, a_s, b_s, u_s, ho_s, no_s, r_s, _ = forward_call(1 + 2 * which, T, act, cot, slot, w_gate, w_in, w_out)
                da, db, e_o, act_grad = backward_call(2 + 2 * which, sel, slot, w_gate, w_in, w_out, a_s, b_s, ho_s, r_s)
                gate_grad, in_grad, out_grad, act_grad = grads_call(no_s, u_s, da, db, e_o, act_grad)
                return act_grad.reshape(act_in.shape), gate_grad[None], in_grad[None], out_grad[None]
            return run
        if len(buckets) == 1:
            return branch(0, buckets[0])(0)
        which = sum((count[0] > b).astype(jnp.int32) for b in buckets[:-1])
        return lax.switch(which, [branch(i, b) for i, b in enumerate(buckets)], 0)

    return jax.shard_map(local_step, mesh=mesh, in_specs=(act_spec, act_spec, act_spec, weight_spec, weight_spec, weight_spec), out_specs=(act_spec, weight_spec, weight_spec, weight_spec), check_vma=False)
```

```python
import functools

import jax
import jax.numpy as jnp
from jax import lax
from jax.experimental import pallas as pl
from jax.experimental.pallas import tpu as pltpu
from jax.sharding import PartitionSpec as P

EPSILON = 1e-6
MESH = pl.DeviceIdType.MESH
BF16, F32 = jnp.bfloat16, jnp.float32
LANES = 128
VMEM_LIMIT = 67043328
BUCKETS = (448, 480, 512, 544, 608, 992)


def nt_dot(left, right):
    return lax.dot_general(left, right, (((1,), (1,)), ((), ())), preferred_element_type=F32)


def place():
    d = lax.axis_index('data')
    s = lax.axis_index('stage')
    x = lax.rem(d, 2)
    y = lax.div(d, 2)
    return d, s, 2 * y + 1 - x, 2 * (1 - y) + x, 3 - d


def meet(same_core=False):
    d, s, xn, yn, dg = place()
    barrier = pltpu.get_barrier_semaphore()
    peers = [(xn, s), (yn, s), (dg, s)]
    if not same_core:
        peers += [(xn, 1 - s), (yn, 1 - s), (dg, 1 - s), (d, 1 - s)]
    for chip, core in peers:
        pl.semaphore_signal(barrier, inc=1, device_id=(chip, core), device_id_type=MESH)
    pl.semaphore_wait(barrier, len(peers))


def remote(src, dst, send_sem, recv_sem, device):
    return pltpu.make_async_remote_copy(src_ref=src, dst_ref=dst, send_sem=send_sem, recv_sem=recv_sem, device_id=device, device_id_type=MESH)


def lens_kernel(lens, slot, count, mine, everyone, ss, rs):
    d, s, xn, yn, dg = place()
    meet(same_core=True)
    seqs, tokens = lens.shape[0], mine.shape[0] * LANES
    each = tokens // seqs
    index = lax.broadcasted_iota(jnp.int32, mine.shape, 0) * LANES + lax.broadcasted_iota(jnp.int32, mine.shape, 1)
    length = jnp.zeros(mine.shape, jnp.int32)
    for i in range(seqs):
        length = jnp.where((index >= i * each) & (index < (i + 1) * each), lens[i], length)
    mine[...] = jnp.where(lax.rem(index, each) < length, 1, 0)
    everyone[d] = mine[...]
    sends = [remote(mine, everyone.at[d], ss.at[i], rs.at[i], (chip, s)) for i, chip in enumerate((xn, yn, dg))]
    for copy in sends:
        copy.start()
    for copy in sends:
        copy.wait()
    rows = 4 * mine.shape[0]
    live = everyone[...].reshape(rows, LANES)
    lane, row = lax.broadcasted_iota(jnp.int32, live.shape, 1), lax.broadcasted_iota(jnp.int32, live.shape, 0)
    upto = live
    shift = 1
    while shift < LANES:
        upto = upto + jnp.where(lane >= shift, pltpu.roll(upto, shift, 1), 0)
        shift *= 2
    whole = jnp.broadcast_to(jnp.sum(live, axis=1, keepdims=True), live.shape)
    before = whole
    shift = 1
    while shift < rows:
        before = before + jnp.where(row >= shift, pltpu.roll(before, shift, 0), 0)
        shift *= 2
    place_of = jnp.where(live > 0, before - whole + upto - 1, -1)
    for i in range(rows):
        slot[:, i * LANES:(i + 1) * LANES] = place_of[i:i + 1, :]
    count[0] = jnp.sum(live)


def share_rows(buf, d, s, xn, yn, ss, rs, lo, hi):
    def own(part, i):
        return [remote(buf.at[d, part], buf.at[d, part], ss.at[2 * i + n], rs.at[2 * i + n], (chip, s)) for n, chip in enumerate((xn, yn))]

    fwd_y = remote(buf.at[xn, lo], buf.at[xn, lo], ss.at[4], rs.at[4], (yn, s))
    fwd_x = remote(buf.at[yn, hi], buf.at[yn, hi], ss.at[5], rs.at[5], (xn, s))
    return own(lo, 0), own(hi, 1), fwd_y, fwd_x


def near_share(share):
    own_lo, own_hi, fwd_y, fwd_x = share
    own_lo[0].wait_recv()
    fwd_y.start()
    own_hi[1].wait_recv()
    fwd_x.start()


def far_share(share):
    own_lo, own_hi, fwd_y, fwd_x = share
    own_hi[0].wait_recv()
    own_lo[1].wait_recv()
    fwd_y.wait_recv()
    fwd_x.wait_recv()
    for copy in own_lo + own_hi + [fwd_y, fwd_x]:
        copy.wait_send()


def forward_kernel(act, cot, slot, w_gate, w_in, w_out,
                   sel_o, a_s, b_s, u_s, ho_s, no_s, r_s, other,
                   wv, wov, hb, nb, ub, zp, acc, ab, rv, near_in, far_in, inpv,
                   wss, wrs, iss, irs, xss, xrs, hss, hrs, ass, ars, zss, zrs, lw, lo, lab, lsv, lin, go):
    d, s, xn, yn, dg = place()
    T = nb.shape[0]
    half = T // 2
    piece = T if T <= 512 else half
    cols = ub.shape[1]
    tiles = cols // LANES
    dm = hb.shape[3]
    rows_in = act.shape[0]
    lo_rows, hi_rows = pl.ds(0, half), pl.ds(half, half)
    chips = (dg, xn, yn)
    cuts, early_tiles = (2, 5), 2

    def block_of(chip):
        return pl.ds(pl.multiple_of(chip * dm, dm), dm)

    def input_rows(chip):
        return pl.ds(pl.multiple_of(chip * rows_in, LANES), rows_in)

    def own_loads(j):
        return [pltpu.make_async_copy(w.at[j, :, pl.ds(pl.multiple_of(d * cols, LANES), cols)], wv.at[j, m, block_of(d)], lw.at[j, m])
                for m, w in enumerate((w_gate, w_in))]

    def start_weights(layer, src, core, sem, first, last):
        def body(k, carry):
            col = pl.ds(pl.multiple_of(k * LANES, LANES), LANES)
            for chip in chips:
                from_col = pl.ds(pl.multiple_of(chip * cols + k * LANES, LANES), LANES)
                for m in range(2):
                    remote(src[m].at[:, from_col], wv.at[layer, m, block_of(d), col], wss.at[sem], wrs.at[layer, k], (chip, core)).start()
            return carry
        lax.fori_loop(first, last, body, 0)

    def wait_sent(sem, count):
        sent = wv.at[0, :, pl.ds(0, 3 * dm), pl.ds(0, count * LANES)]
        pltpu.make_async_copy(sent, sent, wss.at[sem]).wait()

    def wait_tile(layer, k, col):
        came = wv.at[layer, :, pl.ds(0, 3 * dm), col]
        pltpu.make_async_copy(came, came, wrs.at[layer, k]).wait()

    other_pair = (other.at[0], other.at[1])
    first_pair, second_pair = (w_gate.at[0], w_in.at[0]), (w_gate.at[1], w_in.at[1])

    def input_sends(src):
        return [remote(src.at[:, block_of(chip)], inpv.at[input_rows(d)], iss.at[i], irs.at[i], (chip, s)) for i, chip in enumerate(chips)]

    def own_input(src):
        return pltpu.make_async_copy(src.at[:, block_of(d)], inpv.at[input_rows(d)], lin.at[0])
    share = share_rows(hb.at[s], d, s, xn, yn, ass, ars, lo_rows, hi_rows)

    def first_weights(first, last):
        @pl.when(s == 0)
        def _():
            start_weights(0, first_pair, 0, 0, first, last)
    meet()
    for n, src in enumerate((act, cot)):
        @pl.when(s == n)
        def _():
            for copy in input_sends(src) + [own_input(src)]:
                copy.start()
    first_weights(0, cuts[0])
    swaps = [remote(w.at[1], other.at[m], xss.at[m], xrs.at[m], (d, 1 - s)) for m, w in enumerate((w_gate, w_in))]
    for copy in own_loads(0) + own_loads(1) + swaps:
        copy.start()
    pltpu.make_async_copy(w_out.at[0], wov, lo.at[0]).start()
    for copy in input_sends(act):
        copy.wait()
    own_input(act).wait()
    tokens = slot.shape[1]

    def pick_body(i, carry):
        base = pl.multiple_of(lax.div(i, 2) * half, 16)
        pick = (lax.broadcasted_iota(jnp.int32, (half, tokens), 0) + base == slot[...]).astype(BF16)
        lane = pl.ds(pl.multiple_of(lax.rem(i, 2) * (dm // 2), LANES), dm // 2)
        hb[s, d, pl.ds(base, half), lane] = jnp.dot(pick, inpv[:, lane], preferred_element_type=F32).astype(BF16)
        return carry
    lax.fori_loop(0, 4, pick_body, 0)
    for copy in share[0] + share[1]:
        copy.start()
    first_weights(cuts[0], cuts[1])
    near_share(share)
    first_weights(cuts[1], tiles)
    far_share(share)
    for copy in swaps:
        copy.wait()

    def hand_over():
        return [remote(hb.at[0, c], hb.at[0, c], hss.at[i], hrs.at[i], (d, 1 - s)) for i, c in enumerate((d, xn, yn, dg))]

    @pl.when(s == 1)
    def _():
        top = [pltpu.make_async_copy(hb.at[1, c], sel_o.at[:, pl.ds(c * dm, dm)], lin.at[c]) for c in range(4)]
        for copy in top:
            copy.start()
        pl.semaphore_wait(go, 1)
        start_weights(1, other_pair, 0, 0, 0, tiles)
        start_weights(0, first_pair, 1, 1, 0, tiles)
        start_weights(1, second_pair, 1, 2, 0, early_tiles)
        for copy in top:
            copy.wait()
        for copy in hand_over():
            copy.wait_recv()

    def layer(j, carry):
        nxt = 1 - j
        step = 32

        def norm_body(i, carry):
            rows = pl.ds(pl.multiple_of(i * step, step), step)
            blocks = [hb[j, c, rows, :].astype(F32) for c in range(4)]
            total = sum(jnp.sum(b * b, axis=-1, keepdims=True) for b in blocks)
            inv = lax.rsqrt(total * (1.0 / (4 * dm)) + EPSILON)
            for c in range(4):
                nb[rows, c * dm:(c + 1) * dm] = (blocks[c] * inv).astype(BF16)
            rv[rows, :] = jnp.broadcast_to(inv, (step, LANES))
            return carry
        lax.fori_loop(0, T // step, norm_body, 0)
        saves = [
            pltpu.make_async_copy(hb.at[j, d], ho_s.at[j], lsv.at[0]),
            pltpu.make_async_copy(nb.at[:, block_of(d)], no_s.at[j], lsv.at[1]),
            pltpu.make_async_copy(rv, r_s.at[j], lsv.at[2]),
        ]
        for copy in saves:
            copy.start()
        for copy in own_loads(j):
            copy.wait()

        def ab_copies(k, side):
            return [pltpu.make_async_copy(ab.at[side, 0], a_s.at[j, k], lab.at[side, 0]),
                    pltpu.make_async_copy(ab.at[side, 1], b_s.at[j, k], lab.at[side, 1])]

        def ab_body(k, carry):
            col = pl.ds(pl.multiple_of(k * LANES, LANES), LANES)
            wait_tile(j, k, col)

            @pl.when((j == 0) & (s == 0) & (k == tiles - 2))
            def _():
                pl.semaphore_signal(go, inc=1, device_id=(d, 1), device_id_type=MESH)

            def ab_rows(i, carry):
                rows = pl.ds(pl.multiple_of(i * piece, 16), piece)
                acc[rows, :] = jnp.dot(nb[rows, :], jnp.concatenate([wv[j, 0, :, col], wv[j, 1, :, col]], axis=1), preferred_element_type=F32)
                return carry
            lax.fori_loop(0, T // piece, ab_rows, 0)
            side = lax.rem(k, 2)

            @pl.when(k >= 2)
            def _():
                for copy in ab_copies(k, side):
                    copy.wait()
            a, b = acc[:, :LANES], acc[:, LANES:]
            ab[side, 0] = a
            ab[side, 1] = b
            ub[:, col] = (a * jax.nn.sigmoid(a) * b).astype(BF16)
            for copy in ab_copies(k, side):
                copy.start()
            return carry
        lax.fori_loop(0, tiles, ab_body, 0)
        for k in (tiles - 2, tiles - 1):
            for copy in ab_copies(k, k % 2):
                copy.wait()
        save_u = pltpu.make_async_copy(ub, u_s.at[j], lsv.at[3])
        save_u.start()

        @pl.when((j == 0) | (s == 0))
        def _():
            pltpu.make_async_copy(w_out.at[j], wov, lo.at[0]).wait()

            def send(i, c, rows, dst, chip):
                return remote(zp.at[c, rows], dst, zss.at[i], zrs.at[i], (chip, s))
            first = [send(0, dg, lo_rows, near_in.at[0, 0], xn), send(1, dg, hi_rows, near_in.at[1, 0], yn)]
            second = [send(2, xn, lo_rows, near_in.at[0, 1], xn), send(3, yn, hi_rows, near_in.at[1, 1], yn)]
            third = [send(4, yn, lo_rows, far_in.at[0], yn), send(5, xn, hi_rows, far_in.at[1], xn)]
            x, y = lax.rem(d, 2), lax.div(d, 2)
            wide = 2 * LANES

            def block_body(i, carry):
                rel, part_of = 3 - lax.div(i, 2), lax.rem(i, 2)
                c = 2 * lax.rem(y + lax.rem(rel, 2), 2) + lax.rem(x + lax.div(rel, 2), 2)

                def zp_rows(n, carry):
                    rows = pl.ds(pl.multiple_of(n * half, 16), half)
                    zp[c, rows, pl.ds(pl.multiple_of(part_of * wide, wide), wide)] = jnp.dot(
                        ub[rows, :], wov[:, pl.ds(pl.multiple_of(c * dm + part_of * wide, wide), wide)], preferred_element_type=F32)
                    return carry
                lax.fori_loop(0, 2, zp_rows, 0)
                for at, copies in ((1, first), (3, second[:1]), (5, second[1:])):
                    @pl.when(i == at)
                    def _():
                        for copy in copies:
                            copy.start()
                return carry
            lax.fori_loop(0, 8, block_body, 0)
            share = share_rows(hb.at[nxt], d, s, xn, yn, ass, ars, lo_rows, hi_rows)

            def both(n, stage):
                for at in range(2):
                    @pl.when(n == at)
                    def _():
                        stage(at)

            def half_rows(n):
                return pl.ds(pl.multiple_of(n * half, 16), half)

            def relay(n, carry):
                both(n, lambda at: first[at].wait_recv())
                c, rows = yn + n * (xn - yn), half_rows(n)
                zp[c, rows, :] += near_in[n, 0]
                both(n, lambda at: third[at].start())
                return carry
            lax.fori_loop(0, 2, relay, 0)

            def settle(n, carry):
                both(n, lambda at: (second[at].wait_recv(), third[at].wait_recv()))
                rows = half_rows(n)
                branch = (zp[d, rows, :] + near_in[n, 1] + far_in[n]).astype(BF16).astype(F32)
                hb[nxt, d, rows, :] = (hb[j, d, rows, :].astype(F32) + branch).astype(BF16)
                both(n, lambda at: [copy.start() for copy in share[at]])
                return carry
            lax.fori_loop(0, 2, settle, 0)
            near_share(share)
            far_share(share)
            for copy in first + second + third:
                copy.wait_send()

        @pl.when((j == 0) & (s == 0))
        def _():
            pltpu.make_async_copy(w_out.at[1], wov, lo.at[0]).start()

        @pl.when((j == 1) & (s == 0))
        def _():
            hands = hand_over()
            for copy in hands:
                copy.start()
            start_weights(1, other_pair, 1, 1, early_tiles, tiles)
            for copy in hands:
                copy.wait_send()
        for copy in saves:
            copy.wait()
        save_u.wait()
        return carry
    lax.fori_loop(0, 2, layer, 0)
    wait_sent(0, tiles)

    @pl.when(s == 0)
    def _():
        wait_sent(1, tiles - early_tiles)

    @pl.when(s == 1)
    def _():
        wait_sent(1, tiles)
        wait_sent(2, early_tiles)


def backward_kernel(sel, slot, w_gate, w_in, w_out, a_s, b_s, ho_s, r_s,
                    da_o, db_o, e_o, act_o,
                    wgv, wov, eb, daf, ab, dn, hov, rv, sq, sv, agv, back_v,
                    dss, drs, fss, frs, ess, ers, hss, hrs, sss, srs, ass, ars, lw, lab, lout, lh, le, lsm):
    d, s, xn, yn, dg = place()
    T = sel.shape[0]
    part_rows = T // 2
    lo_n = -(-part_rows // 32) * 16
    cols = daf.shape[3]
    dm = dn.shape[1]
    wide = 2 * LANES
    n_full = cols // wide
    tail = cols - n_full * wide
    n_early = n_full // 2
    n_mid = n_early + 2
    splits, one_loop = (1 if T <= 640 else 2), T > 512
    pad = sq.shape[1]
    w_slots = wgv.shape[0]
    ab_slots = ab.shape[0]

    def wo_load(j):
        return pltpu.make_async_copy(w_out.at[j], wov, lw.at[0, 0])

    def slot_of(j, n):
        return j if n == 2 else 0

    def gate_loads(j):
        return [pltpu.make_async_copy(w.at[j], wgv.at[slot_of(j, w_slots), m], lw.at[1 + slot_of(j, w_slots), m]) for m, w in enumerate((w_gate, w_in))]

    def rows_of(g, base=0, size=part_rows):
        return pl.ds(pl.multiple_of(g * part_rows + base, 16), size)

    def in_copies(g):
        return [pltpu.make_async_copy(sel.at[rows_of(g), pl.ds(c * dm, dm)], eb.at[2, c, rows_of(g)], lh.at[g, c]) for c in range(4)]

    def hand_over(g):
        return [remote(eb.at[0, c, rows_of(g)], eb.at[2, c, rows_of(g)], hss.at[g, i], hrs.at[g, i], (d, 1 - s)) for i, c in enumerate((d, xn, yn, dg))]

    def ab_loads(j, g):
        side = slot_of(g, ab_slots)
        return [pltpu.make_async_copy(src.at[j, :, rows_of(g)], ab.at[side, m], lab.at[side, m]) for m, src in enumerate((a_s, b_s))]

    @pl.when(s == 1)
    def _():
        for copy in in_copies(0):
            copy.start()
    wo_load(1).start()
    small = [pltpu.make_async_copy(ho_s, hov, lsm.at[0]), pltpu.make_async_copy(r_s, rv, lsm.at[1])]
    for copy in ab_loads(1, 0):
        copy.start()
    meet()

    def columns(c, width):
        return pl.ds(pl.multiple_of(c * wide, LANES), width)

    def each_chunk(body, first=0, last=n_full):
        lax.fori_loop(first, last, lambda c, carry: (body(c, wide), carry)[1], 0)

    class Piece:
        def __init__(self, j, g):
            self.j, self.g, self.rows = j, g, rows_of(g)
            parts = (rows_of(g, 0, lo_n), rows_of(g, lo_n, part_rows - lo_n))
            self.share = share_rows(eb.at[j], d, s, xn, yn, ess.at[g], ers.at[g], *parts)
            self.e_saves = [pltpu.make_async_copy(eb.at[j + 1, c, self.rows], e_o.at[j, self.rows, pl.ds(c * dm, dm)], le.at[j, g, c]) for c in range(4)]
            self.sums = [remote(sv.at[g, 0], sv.at[g, 1 + i], sss.at[g, i], srs.at[g, i], (chip, s)) for i, chip in enumerate((xn, yn, dg))]

        def own_sends(self, c, col):
            g, out = self.g, []
            for m in range(2):
                for n, chip in enumerate((xn, yn)):
                    here = daf.at[m, d, self.rows, col]
                    out.append(remote(here, here, dss.at[g, m, n, c], drs.at[g, m, n, c], (chip, s)))
            return out

        def forwards(self, c, col):
            g = self.g
            from_x, from_y = daf.at[0, xn, self.rows, col], daf.at[1, yn, self.rows, col]
            return [remote(from_x, from_x, fss.at[g, 1, c], frs.at[g, 1, c], (yn, s)), remote(from_y, from_y, fss.at[g, 0, c], frs.at[g, 0, c], (xn, s))]

        def make(self):
            j, g, rows, side = self.j, self.g, self.rows, slot_of(self.g, ab_slots)
            for copy in self.e_saves:
                copy.start()

            @pl.when(g == 0)
            def _():
                wo_load(j).wait()
            for copy in ab_loads(j, g):
                copy.wait()

            @pl.when((j == 1) & (g == 0))
            def _():
                if ab_slots == 2:
                    for copy in ab_loads(1, 1):
                        copy.start()

                @pl.when(s == 1)
                def _():
                    for copy in in_copies(1):
                        copy.start()
                for copy in gate_loads(1) + small:
                    copy.start()
            if w_slots == 2:
                @pl.when((j == 1) & (g == 1))
                def _():
                    for copy in gate_loads(0):
                        copy.start()

            def tile(c, width=wide):
                base = jnp.minimum(c * wide, cols - wide) if one_loop else c * wide
                def du(blocks, lanes):
                    e_part = jnp.concatenate([eb[j + 1, n, rows, :] for n in blocks], axis=1)
                    return nt_dot(e_part, wov[pl.ds(pl.multiple_of(base, LANES), width), lanes])
                if splits == 1:
                    dn[rows, :width] = du(range(4), slice(None))
                else:
                    dn[rows, :width] = jnp.zeros((part_rows, width), F32)

                    def du_part(n, carry):
                        dn[rows, :width] += du((2 * n, 2 * n + 1), pl.ds(pl.multiple_of(n * 2 * dm, dm), 2 * dm))
                        return carry
                    lax.fori_loop(0, 2, du_part, 0)
                def lanes(n):
                    lane = pl.ds(pl.multiple_of(base + n * LANES, LANES), LANES)
                    at = lax.div(base, LANES) + n
                    a, b, du = ab[side, 0, at], ab[side, 1, at], dn[rows, n * LANES:(n + 1) * LANES]
                    sig = jax.nn.sigmoid(a)
                    daf[0, d, rows, lane] = (du * b * sig * (1.0 + a * (1.0 - sig))).astype(BF16)
                    daf[1, d, rows, lane] = (du * (a * sig)).astype(BF16)

                if one_loop:
                    @pl.when(c < n_full)
                    def _():
                        lanes(0)
                    lanes(1)
                else:
                    for n in range(width // LANES):
                        lanes(n)

            def body(c, width):
                tile(c, wide)

                @pl.when(c < n_early)
                def _():
                    for copy in self.own_sends(c, columns(c, wide)):
                        copy.start()
            each_chunk(body, 0, n_full + 1 if one_loop else n_full)
            if not one_loop:
                tile(n_full, tail)

        def send(self, first, last):
            def body(c, width):
                for copy in self.own_sends(c, columns(c, width)):
                    copy.start()
            each_chunk(body, first, last)

        def save_tile(self, m, chip, col, c, width):
            dst = (da_o, db_o)[m].at[self.j, self.rows, pl.ds(pl.multiple_of(chip * cols + c * wide, LANES), width)]
            pltpu.make_async_copy(daf.at[m, chip, self.rows, col], dst, lout.at[self.g]).start()

        def add(self, chip, c, width):
            def body(i, carry):
                m, at = lax.div(i, splits), pl.ds(pl.multiple_of(lax.rem(i, splits) * (dm // splits), LANES), dm // splits)
                w = wgv[slot_of(self.j, w_slots), m, at, pl.ds(pl.multiple_of(chip * cols + c * wide, LANES), width)]
                dn[self.rows, at] += nt_dot(daf[m, chip, self.rows, columns(c, width)], w)
                return carry
            lax.fori_loop(0, 2 * splits, body, 0)

        def own(self):
            @pl.when(self.g == 0)
            def _():
                for copy in gate_loads(self.j):
                    copy.wait()
            for m in range(2):
                self.save_tile(m, d, pl.ds(0, cols), 0, cols)
            dn[self.rows, :] = jnp.zeros((part_rows, dm), F32)
            each_chunk(lambda c, width: self.add(d, c, width))
            self.add(d, n_full, tail)

        def near(self, c, width):
            col = columns(c, width)
            fwd_y, fwd_x = self.forwards(c, col)

            def came(m, n, chip):
                there = daf.at[m, chip, self.rows, col]
                remote(there, there, dss.at[self.g, m, n, c], drs.at[self.g, m, n, c], (chip, s)).wait_recv()
            came(0, 0, xn)
            fwd_y.start()
            came(1, 1, yn)
            fwd_x.start()
            came(1, 0, xn)
            came(0, 1, yn)
            for chip in (xn, yn):
                for m in range(2):
                    self.save_tile(m, chip, col, c, width)
            lax.fori_loop(0, 2, lambda i, carry: (self.add(xn + i * (yn - xn), c, width), carry)[1], 0)

        def far(self):
            j, g, rows = self.j, self.g, self.rows

            def body(c, width):
                col = columns(c, width)
                there = [daf.at[m, dg, rows, col] for m in range(2)]
                remote(there[0], there[0], fss.at[g, 1, c], frs.at[g, 1, c], (yn, s)).wait_recv()
                remote(there[1], there[1], fss.at[g, 0, c], frs.at[g, 0, c], (xn, s)).wait_recv()
                for m in range(2):
                    self.save_tile(m, dg, col, c, width)
                self.add(dg, c, width)
            each_chunk(body)
            body(n_full, tail)

            @pl.when((j == 1) & (g == 0))
            def _():
                for copy in small:
                    copy.wait()
            prod = dn[rows, :] * hov[j, rows, :].astype(F32)
            sq[g, :part_rows, :] = (prod[:, :LANES] + prod[:, LANES:2 * LANES]) + (prod[:, 2 * LANES:3 * LANES] + prod[:, 3 * LANES:])
            sv[g, 0] = jnp.broadcast_to(jnp.sum(sq[g].T, axis=0, keepdims=True), (8, pad))
            for copy in self.sums:
                copy.start()
            if w_slots == 1:
                @pl.when((j == 1) & (g == 1))
                def _():
                    for copy in gate_loads(0):
                        copy.start()

        def finish(self):
            j, g = self.j, self.g
            whole = daf.at[:, :, self.rows]
            pltpu.make_async_copy(whole, whole, lout.at[g]).wait()

            def drain(c, width):
                col = columns(c, width)
                for copy in self.own_sends(c, col) + self.forwards(c, col):
                    copy.wait_send()
            each_chunk(drain)
            drain(n_full, tail)
            for copy in self.sums:
                copy.wait()
            mean = ((sv[g, 0, 0:1, :] + sv[g, 1, 0:1, :]) + (sv[g, 2, 0:1, :] + sv[g, 3, 0:1, :])) * (1.0 / (4 * dm))
            sq[g] = jnp.broadcast_to(mean, (LANES, pad)).T
            for n, (base, size) in enumerate(((0, lo_n), (lo_n, part_rows - lo_n))):
                at = rows_of(g, base, size)
                inv, avg = rv[j, at, :], sq[g, base:base + size, :]
                for c in range(4):
                    lane = slice(c * LANES, (c + 1) * LANES)
                    resid = inv * dn[at, lane] - hov[j, at, lane].astype(F32) * (inv * inv * inv) * avg
                    eb[j, d, at, lane] = (eb[j + 1, d, at, lane].astype(F32) + resid).astype(BF16)
                for copy in self.share[n]:
                    copy.start()

    def step(i, carry):
        g = lax.rem(i, 2)
        cur = Piece(1 - lax.div(i, 2), g)
        prev = Piece(1 - lax.div(i - 1, 2), 1 - g)
        live, later = i < 4, i > 0

        @pl.when(i >= 2)
        def _():
            far_share(Piece(1 - lax.div(i - 2, 2), g).share)

        @pl.when((i == 4) & (s == 1))
        def _():
            for copy in hand_over(0):
                copy.start()

        @pl.when(live)
        def _():
            @pl.when((i < 2) & (s == 0))
            def _():
                for copy in hand_over(g):
                    copy.wait_recv()

            @pl.when((i < 2) & (s == 1))
            def _():
                for copy in in_copies(g):
                    copy.wait()

            cur.make()

            @pl.when(i == 1)
            def _():
                wo_load(0).start()
            coming = i + ab_slots

            @pl.when(coming < 4)
            def _():
                for copy in ab_loads(1 - lax.div(coming, 2), lax.rem(coming, 2)):
                    copy.start()

        @pl.when(later)
        def _():
            prev.far()

        def halves(h, carry):
            @pl.when(live)
            def _():
                cur.send(n_early + h * (n_mid - n_early), n_mid + h * (n_full - n_mid))

            @pl.when(live & (h == 0))
            def _():
                cur.own()

            @pl.when(live & (h == 1))
            def _():
                for copy in cur.own_sends(n_full, columns(n_full, tail)):
                    copy.start()

            @pl.when(later & (h == 1))
            def _():
                near_share(prev.share)

            @pl.when(live)
            def _():
                each_chunk(cur.near, h * n_early, n_early + h * (n_full - n_early))

            @pl.when(later & (h == 0))
            def _():
                prev.finish()
            return carry
        lax.fori_loop(0, 2, halves, 0)

        @pl.when(live)
        def _():
            cur.near(n_full, tail)
        return carry
    lax.fori_loop(0, 5, step, 0)

    def act_copies(i, c):
        col = pl.ds(pl.multiple_of(c * dm, dm), dm)
        return remote(agv.at[c], act_o.at[:, col], ass.at[i], ars.at[i], (d, 1 - s)), pltpu.make_async_copy(agv.at[c], act_o.at[:, col], lh.at[0, i])

    @pl.when(s == 1)
    def _():
        far_share(Piece(0, 1).share)
        for copy in hand_over(1):
            copy.start()
        for i, c in enumerate((d, xn, yn, dg)):
            act_copies(i, c)[0].wait_recv()

    @pl.when(s == 0)
    def _():
        own_lo, own_hi, fwd_y, fwd_x = Piece(0, 1).share
        rows_out = agv.shape[1]
        own_slots = slot[:, pl.ds(pl.multiple_of(d * rows_out, LANES), rows_out)]
        back = (lax.broadcasted_iota(jnp.int32, (T, rows_out), 0) == own_slots).astype(BF16)
        back_v[...] = back
        came = ((), (own_hi[0],), (own_lo[1],), (fwd_y, fwd_x))
        x, y = lax.rem(d, 2), lax.div(d, 2)

        def spread(i, carry):
            for n in range(1, 4):
                @pl.when(i == n)
                def _():
                    for copy in came[n]:
                        copy.wait_recv()
            c = 2 * lax.rem(y + lax.div(i, 2), 2) + lax.rem(x + lax.rem(i, 2), 2)
            agv[c] = lax.dot_general(back_v[...], eb[0, c], (((0,), (0,)), ((), ())), preferred_element_type=F32).astype(BF16)
            for copy in act_copies(i, c):
                copy.start()
            return carry
        lax.fori_loop(0, 4, spread, 0)
        for copy in own_lo + own_hi + [fwd_y, fwd_x]:
            copy.wait_send()
        for i, c in enumerate((d, xn, yn, dg)):
            away, here = act_copies(i, c)
            away.wait_send()
            here.wait()
    def saved(i, carry):
        for copy in Piece(lax.div(i, 2), lax.rem(i, 2)).e_saves:
            copy.wait()
        return carry
    lax.fori_loop(0, 4, saved, 0)

    @pl.when(s == 1)
    def _():
        for g in range(2):
            for copy in hand_over(g):
                copy.wait_send()


def grads_kernel(no_s, u_s, da, db, e_o, act, gate_o, in_o, out_o, act_o, nv, uv, ev, av, nt, ut, ring, og, oo, ln, lr, lg, lo):
    layers = nv.shape[0]
    wide = ring.shape[3]
    n_gate, n_out = da.shape[2] // wide, e_o.shape[2] // wide
    slots, g_slots, o_slots = ring.shape[0], og.shape[0], oo.shape[0]
    rows = oo.shape[2]

    def put(ref, at, value):
        ref[at] = value

    def for_rows(count, body):
        parts = 1 if nv.shape[1] <= 640 else 2
        size = count // parts
        if parts == 1:
            body(pl.ds(0, size))
        else:
            lax.fori_loop(0, parts, lambda i, carry: (body(pl.ds(pl.multiple_of(i * size, 32), size)), carry)[1], 0)

    def flip(src, dst):
        def body(i, carry):
            lane = pl.ds(pl.multiple_of(i * LANES, LANES), LANES)
            dst[lane, :] = src[:, lane].T
            return carry
        lax.fori_loop(0, dst.shape[0] // LANES, body, 0)
    wholes = [pltpu.make_async_copy(src, dst, ln.at[i]) for i, (src, dst) in enumerate(((no_s, nv), (u_s, uv), (e_o, ev), (act, av)))]
    act_store = pltpu.make_async_copy(av, act_o, ln.at[4])

    def tile_at(c):
        return pl.ds(pl.multiple_of(c * wide, wide), wide)

    def loads(t):
        slot = lax.rem(t, slots)
        return [pltpu.make_async_copy(src.at[lax.div(t, n_gate), :, tile_at(lax.rem(t, n_gate))], ring.at[slot, m], lr.at[slot, m]) for m, src in enumerate((da, db))]

    def gate_stores(t):
        slot = lax.rem(t, g_slots)
        return [pltpu.make_async_copy(og.at[slot, m], dst.at[lax.div(t, n_gate), :, tile_at(lax.rem(t, n_gate))], lg.at[slot, m]) for m, dst in enumerate((gate_o, in_o))]

    def out_stores(t):
        slot = lax.rem(t, o_slots)
        return [pltpu.make_async_copy(oo.at[slot, m], out_o.at[lax.div(t, n_out), pl.ds(m * rows, rows), tile_at(lax.rem(t, n_out))], lo.at[slot, m]) for m in range(2)]

    def start(copies):
        for copy in copies:
            copy.start()

    def wait(copies):
        for copy in copies:
            copy.wait()
    wholes[0].start()
    for t in range(slots - 1):
        start(loads(t))
    start(wholes[1:])
    wholes[0].wait()

    def gate_body(t, carry):
        j, c, slot, at = lax.div(t, n_gate), lax.rem(t, n_gate), lax.rem(t, slots), lax.rem(t, g_slots)

        @pl.when(t + slots - 1 < layers * n_gate)
        def _():
            start(loads(t + slots - 1))

        @pl.when(c == 0)
        def _():
            flip(nv.at[j], nt)
        wait(loads(t))

        @pl.when(t >= g_slots)
        def _():
            wait(gate_stores(t - g_slots))

        def side(m, carry):
            for_rows(og.shape[2], lambda at_rows: put(og, (at, m, at_rows), jnp.dot(nt[at_rows, :], ring[slot, m], preferred_element_type=F32)))
            return carry
        lax.fori_loop(0, 2, side, 0)
        start(gate_stores(t))
        return carry
    lax.fori_loop(0, layers * n_gate, gate_body, 0)
    wait(wholes[1:])
    act_store.start()

    def out_body(t, carry):
        j, c, at = lax.div(t, n_out), lax.rem(t, n_out), lax.rem(t, o_slots)

        @pl.when(c == 0)
        def _():
            flip(uv.at[j], ut)

        @pl.when(t >= o_slots)
        def _():
            wait(out_stores(t - o_slots))

        def half(m, carry):
            for_rows(rows, lambda at_rows: put(oo, (at, m, at_rows), jnp.dot(
                ut[pl.ds(pl.multiple_of(m * rows + at_rows.start, 32), at_rows.size), :], ev[j, :, tile_at(c)], preferred_element_type=F32)))
            return carry
        lax.fori_loop(0, 2, half, 0)
        start(out_stores(t))
        return carry
    lax.fori_loop(0, layers * n_out, out_body, 0)
    act_store.wait()
    for t in range(layers * n_gate - g_slots, layers * n_gate):
        wait(gate_stores(t))
    for t in range(layers * n_out - o_slots, layers * n_out):
        wait(out_stores(t))


def grads_call(no_s, u_s, da, db, e_o, act):
    layers, T, dsh = no_s.shape
    cols, dff, dmod = u_s.shape[2], da.shape[2], e_o.shape[2]
    V, wide = pltpu.VMEM, 4 * LANES
    moved = 2 * layers * T * (dsh + cols + 2 * dff + dmod) + 4 * layers * (2 * dsh * dff + cols * dmod)
    return pl.pallas_call(
        grads_kernel, name=f'grads_{T}', in_specs=[ANY] * 6, out_specs=[ANY] * 4,
        out_shape=[jax.ShapeDtypeStruct((layers, dsh, dff), F32), jax.ShapeDtypeStruct((layers, dsh, dff), F32), jax.ShapeDtypeStruct((layers, cols, dmod), F32),
                   jax.ShapeDtypeStruct(act.shape, BF16)],
        scratch_shapes=[V((layers, T, dsh), BF16), V((layers, T, cols), BF16), V((layers, T, dmod), BF16), V(act.shape, BF16), V((dsh, T), BF16), V((cols, T), BF16),
                        V((6, 2, T, wide), BF16), V((4, 2, dsh, wide), F32), V((3, 2, cols // 2, wide), F32), DMA((5,)), DMA((6, 2)), DMA((4, 2)), DMA((3, 2))],
        cost_estimate=pl.CostEstimate(flops=2 * layers * T * (2 * dsh * dff + cols * dmod), bytes_accessed=moved, transcendentals=0),
        compiler_params=pltpu.CompilerParams(vmem_limit_bytes=VMEM_LIMIT))(no_s, u_s, da, db, e_o, act)


ANY = pl.BlockSpec(memory_space=pl.ANY)
DMA = pltpu.SemaphoreType.DMA


def comm_call(kernel, name, cid, outs, in_specs, scratch):
    return pl.pallas_call(
        kernel, name=name, out_shape=[jax.ShapeDtypeStruct(*o) for o in outs], in_specs=in_specs, out_specs=[ANY] * len(outs),
        scratch_shapes=scratch, compiler_params=pltpu.CompilerParams(collective_id=cid, has_side_effects=True, vmem_limit_bytes=VMEM_LIMIT))


def lens_call(lens, tokens):
    smem, vmem = pl.BlockSpec(memory_space=pltpu.SMEM), pl.BlockSpec(memory_space=pltpu.VMEM)
    rows = tokens // LANES
    return pl.pallas_call(
        lens_kernel, name='lens', out_shape=[jax.ShapeDtypeStruct((1, 4 * tokens), jnp.int32), jax.ShapeDtypeStruct((1,), jnp.int32)],
        in_specs=[smem], out_specs=[vmem, smem],
        scratch_shapes=[pltpu.VMEM((rows, LANES), jnp.int32), pltpu.VMEM((4, rows, LANES), jnp.int32), DMA((3,)), DMA((3,))],
        compiler_params=pltpu.CompilerParams(collective_id=0, has_side_effects=True))(lens)


def forward_call(cid, T, act, cot, slot, w_gate, w_in, w_out):
    rows, dmod = act.shape
    _, dsh, dff = w_gate.shape
    cols = dff // 4
    half = T // 2
    tiles = cols // LANES
    outs = [((T, dmod), BF16), ((2, tiles, T, LANES), F32), ((2, tiles, T, LANES), F32), ((2, T, cols), BF16),
            ((2, T, dsh), BF16), ((2, T, dsh), BF16), ((2, T, LANES), F32), ((2, dsh, dff), BF16)]
    V = pltpu.VMEM
    scratch = [V((2, 2, dmod, cols), BF16), V((cols, dmod), BF16), V((2, 4, T, dsh), BF16), V((T, dmod), BF16), V((T, cols), BF16),
               V((4, T, dsh), F32), V((T, 2 * LANES), F32), V((2, 2, T, LANES), F32), V((T, LANES), F32),
               V((2, 2, half, dsh), F32), V((2, half, dsh), F32), V((4 * rows, dsh), BF16),
               DMA((3,)), DMA((2, tiles)), DMA((3,)), DMA((3,)), DMA((2,)), DMA((2,)), DMA((4,)), DMA((4,)), DMA((6,)), DMA((6,)), DMA((6,)), DMA((6,)),
               DMA((2, 2)), DMA((1,)), DMA((2, 2)), DMA((4,)), DMA((4,)), pltpu.SemaphoreType.REGULAR]
    specs = [ANY, ANY, pl.BlockSpec(memory_space=pltpu.VMEM)] + [ANY] * 3
    return comm_call(forward_kernel, f'forward_{T}', cid, outs, specs, scratch)(act, cot, slot, w_gate, w_in, w_out)


def backward_call(cid, sel, slot, w_gate, w_in, w_out, a_s, b_s, ho_s, r_s):
    T, dmod = sel.shape
    _, dsh, dff = w_gate.shape
    cols = dff // 4
    tiles = cols // LANES
    chunks = (tiles + 1) // 2
    pad = -(-(T // 2) // LANES) * LANES
    slots = 2 if T <= 640 else 1
    ab_slots = 2 if T <= 832 else 1
    outs = [((2, T, dff), BF16), ((2, T, dff), BF16), ((2, T, dmod), BF16), ((slot.shape[1] // 4, dmod), BF16)]
    V = pltpu.VMEM
    scratch = [V((slots, 2, dsh, dff), BF16), V((cols, dmod), BF16), V((3, 4, T, dsh), BF16), V((2, 4, T, cols), BF16),
               V((ab_slots, 2, tiles, T // 2, LANES), F32), V((T, dsh), F32), V((2, T, dsh), BF16), V((2, T, LANES), F32), V((2, pad, LANES), F32), V((2, 4, 8, pad), F32), V((4, slot.shape[1] // 4, dsh), BF16), V((T, slot.shape[1] // 4), BF16),
               DMA((2, 2, 2, chunks)), DMA((2, 2, 2, chunks)), DMA((2, 2, chunks)), DMA((2, 2, chunks)), DMA((2, 6)), DMA((2, 6)), DMA((2, 4)), DMA((2, 4)),
               DMA((2, 3)), DMA((2, 3)), DMA((4,)), DMA((4,)), DMA((3, 2)), DMA((2, 2)), DMA((2,)), DMA((2, 4)), DMA((2, 2, 4)), DMA((2,))]
    return comm_call(backward_kernel, f'backward_{T}', cid, outs, [ANY, pl.BlockSpec(memory_space=pltpu.VMEM)] + [ANY] * 7, scratch)(sel, slot, w_gate, w_in, w_out, a_s, b_s, ho_s, r_s)


def solution(mesh, buckets=BUCKETS):
    act_spec = P(None, 'data')
    weight_spec = P('stage', None, 'data', None)

    def local_step(act_in, cot_out, seq_lens, w_gate, w_in, w_out):
        n_micro, n_rows, seq_len, dmod = act_in.shape
        rows = n_micro * n_rows * seq_len
        w_gate, w_in, w_out = w_gate[0], w_in[0], w_out[0]
        act, cot = act_in.reshape(rows, dmod), cot_out.reshape(rows, dmod)
        slot, count = lens_call(seq_lens.reshape(n_micro), rows)

        def branch(which, T):
            def run(_):
                sel, a_s, b_s, u_s, ho_s, no_s, r_s, _ = forward_call(1 + 2 * which, T, act, cot, slot, w_gate, w_in, w_out)
                da, db, e_o, act_grad = backward_call(2 + 2 * which, sel, slot, w_gate, w_in, w_out, a_s, b_s, ho_s, r_s)
                gate_grad, in_grad, out_grad, act_grad = grads_call(no_s, u_s, da, db, e_o, act_grad)
                return act_grad.reshape(act_in.shape), gate_grad[None], in_grad[None], out_grad[None]
            return run
        if len(buckets) == 1:
            return branch(0, buckets[0])(0)
        which = sum((count[0] > b).astype(jnp.int32) for b in buckets[:-1])
        return lax.switch(which, [branch(i, b) for i, b in enumerate(buckets)], 0)

    return jax.shard_map(local_step, mesh=mesh, in_specs=(act_spec, act_spec, act_spec, weight_spec, weight_spec, weight_spec), out_specs=(act_spec, weight_spec, weight_spec, weight_spec), check_vma=False)
```

```python
import functools

import jax
import jax.numpy as jnp
from jax import lax
from jax.experimental import pallas as pl
from jax.experimental.pallas import tpu as pltpu
from jax.sharding import PartitionSpec as P

EPSILON = 1e-6
MESH = pl.DeviceIdType.MESH
BF16, F32 = jnp.bfloat16, jnp.float32
LANES = 128
VMEM_LIMIT = 67043328
BUCKETS = (448, 480, 512, 544, 608, 992)


def nt_dot(left, right):
    return lax.dot_general(left, right, (((1,), (1,)), ((), ())), preferred_element_type=F32)


def place():
    d = lax.axis_index('data')
    s = lax.axis_index('stage')
    x = lax.rem(d, 2)
    y = lax.div(d, 2)
    return d, s, 2 * y + 1 - x, 2 * (1 - y) + x, 3 - d


def meet(same_core=False):
    d, s, xn, yn, dg = place()
    barrier = pltpu.get_barrier_semaphore()
    peers = [(xn, s), (yn, s), (dg, s)]
    if not same_core:
        peers += [(xn, 1 - s), (yn, 1 - s), (dg, 1 - s), (d, 1 - s)]
    for chip, core in peers:
        pl.semaphore_signal(barrier, inc=1, device_id=(chip, core), device_id_type=MESH)
    pl.semaphore_wait(barrier, len(peers))


def remote(src, dst, send_sem, recv_sem, device):
    return pltpu.make_async_remote_copy(src_ref=src, dst_ref=dst, send_sem=send_sem, recv_sem=recv_sem, device_id=device, device_id_type=MESH)


def lens_kernel(lens, slot, count, mine, everyone, ss, rs):
    d, s, xn, yn, dg = place()
    meet(same_core=True)
    seqs, tokens = lens.shape[0], mine.shape[0] * LANES
    each = tokens // seqs
    index = lax.broadcasted_iota(jnp.int32, mine.shape, 0) * LANES + lax.broadcasted_iota(jnp.int32, mine.shape, 1)
    length = jnp.zeros(mine.shape, jnp.int32)
    for i in range(seqs):
        length = jnp.where((index >= i * each) & (index < (i + 1) * each), lens[i], length)
    mine[...] = jnp.where(lax.rem(index, each) < length, 1, 0)
    everyone[d] = mine[...]
    sends = [remote(mine, everyone.at[d], ss.at[i], rs.at[i], (chip, s)) for i, chip in enumerate((xn, yn, dg))]
    for copy in sends:
        copy.start()
    for copy in sends:
        copy.wait()
    rows = 4 * mine.shape[0]
    live = everyone[...].reshape(rows, LANES)
    lane, row = lax.broadcasted_iota(jnp.int32, live.shape, 1), lax.broadcasted_iota(jnp.int32, live.shape, 0)
    upto = live
    shift = 1
    while shift < LANES:
        upto = upto + jnp.where(lane >= shift, pltpu.roll(upto, shift, 1), 0)
        shift *= 2
    whole = jnp.broadcast_to(jnp.sum(live, axis=1, keepdims=True), live.shape)
    before = whole
    shift = 1
    while shift < rows:
        before = before + jnp.where(row >= shift, pltpu.roll(before, shift, 0), 0)
        shift *= 2
    place_of = jnp.where(live > 0, before - whole + upto - 1, -1)
    for i in range(rows):
        slot[:, i * LANES:(i + 1) * LANES] = place_of[i:i + 1, :]
    count[0] = jnp.sum(live)


def share_rows(buf, d, s, xn, yn, ss, rs, lo, hi):
    def own(part, i):
        return [remote(buf.at[d, part], buf.at[d, part], ss.at[2 * i + n], rs.at[2 * i + n], (chip, s)) for n, chip in enumerate((xn, yn))]

    fwd_y = remote(buf.at[xn, lo], buf.at[xn, lo], ss.at[4], rs.at[4], (yn, s))
    fwd_x = remote(buf.at[yn, hi], buf.at[yn, hi], ss.at[5], rs.at[5], (xn, s))
    return own(lo, 0), own(hi, 1), fwd_y, fwd_x


def near_share(share):
    own_lo, own_hi, fwd_y, fwd_x = share
    own_lo[0].wait_recv()
    fwd_y.start()
    own_hi[1].wait_recv()
    fwd_x.start()


def far_share(share):
    own_lo, own_hi, fwd_y, fwd_x = share
    own_hi[0].wait_recv()
    own_lo[1].wait_recv()
    fwd_y.wait_recv()
    fwd_x.wait_recv()
    for copy in own_lo + own_hi + [fwd_y, fwd_x]:
        copy.wait_send()


def forward_kernel(act, cot, slot, w_gate, w_in, w_out,
                   sel_o, a_s, b_s, u_s, ho_s, no_s, r_s, other,
                   wv, wov, hb, nb, ub, zp, acc, ab, rv, near_in, far_in, inpv,
                   wss, wrs, iss, irs, xss, xrs, hss, hrs, ass, ars, zss, zrs, lw, lo, lab, lsv, lin, go):
    d, s, xn, yn, dg = place()
    T = nb.shape[0]
    half = T // 2
    piece = T if T <= 512 else half
    cols = ub.shape[1]
    tiles = cols // LANES
    dm = hb.shape[3]
    rows_in = act.shape[0]
    lo_rows, hi_rows = pl.ds(0, half), pl.ds(half, half)
    chips = (dg, xn, yn)
    early_tiles, held_tiles = (1, 2) if T <= 480 else (2, 3)

    def block_of(chip):
        return pl.ds(pl.multiple_of(chip * dm, dm), dm)

    def input_rows(chip):
        return pl.ds(pl.multiple_of(chip * rows_in, LANES), rows_in)

    def own_loads(j):
        return [pltpu.make_async_copy(w.at[j, :, pl.ds(pl.multiple_of(d * cols, LANES), cols)], wv.at[j, m, block_of(d)], lw.at[j, m])
                for m, w in enumerate((w_gate, w_in))]

    def start_weights(layer, src, core, sem, first, last):
        def body(k, carry):
            col = pl.ds(pl.multiple_of(k * LANES, LANES), LANES)
            for chip in chips:
                from_col = pl.ds(pl.multiple_of(chip * cols + k * LANES, LANES), LANES)
                for m in range(2):
                    remote(src[m].at[:, from_col], wv.at[layer, m, block_of(d), col], wss.at[sem], wrs.at[layer, k], (chip, core)).start()
            return carry
        lax.fori_loop(first, last, body, 0)

    def wait_sent(sem, count):
        sent = wv.at[0, :, pl.ds(0, 3 * dm), pl.ds(0, count * LANES)]
        pltpu.make_async_copy(sent, sent, wss.at[sem]).wait()

    def wait_tile(layer, k, col):
        came = wv.at[layer, :, pl.ds(0, 3 * dm), col]
        pltpu.make_async_copy(came, came, wrs.at[layer, k]).wait()

    other_pair = (other.at[0], other.at[1])
    first_pair = (w_gate.at[0], w_in.at[0])

    def input_sends(src):
        return [remote(src.at[:, block_of(chip)], inpv.at[input_rows(d)], iss.at[i], irs.at[i], (chip, s)) for i, chip in enumerate(chips)]

    def own_input(src):
        return pltpu.make_async_copy(src.at[:, block_of(d)], inpv.at[input_rows(d)], lin.at[0])
    share = share_rows(hb.at[s], d, s, xn, yn, ass, ars, lo_rows, hi_rows)

    def first_weights(first, last):
        @pl.when(s == 0)
        def _():
            start_weights(0, first_pair, 0, 0, first, last)
    meet()
    for n, src in enumerate((act, cot)):
        @pl.when(s == n)
        def _():
            for copy in input_sends(src) + [own_input(src)]:
                copy.start()
    swaps = [remote(w.at[1], other.at[m], xss.at[m], xrs.at[m], (d, 1 - s)) for m, w in enumerate((w_gate, w_in))]
    for copy in own_loads(0) + own_loads(1) + swaps:
        copy.start()
    pltpu.make_async_copy(w_out.at[0], wov, lo.at[0]).start()
    tokens = slot.shape[1]

    def pick_body(i, carry):
        base = pl.multiple_of(lax.div(i, 2) * half, 16)
        pick = (lax.broadcasted_iota(jnp.int32, (half, tokens), 0) + base == slot[...]).astype(BF16)
        lane = pl.ds(pl.multiple_of(lax.rem(i, 2) * (dm // 2), LANES), dm // 2)
        hb[s, d, pl.ds(base, half), lane] = jnp.dot(pick, inpv[:, lane], preferred_element_type=F32).astype(BF16)
        return carry

    def opening(q, carry):
        @pl.when(q == 1)
        def _():
            for copy in input_sends(act):
                copy.wait()
            own_input(act).wait()
            lax.fori_loop(0, 4, pick_body, 0)
            for copy in share[0] + share[1]:
                copy.start()

        @pl.when(q == 2)
        def _():
            near_share(share)
        first_weights(3 * q, 3 * q + 3 + lax.div(q, 2) * (tiles - 9))
        return carry
    lax.fori_loop(0, 3, opening, 0)
    far_share(share)
    for copy in swaps:
        copy.wait()

    def hand_over():
        return [remote(hb.at[0, c], hb.at[0, c], hss.at[i], hrs.at[i], (d, 1 - s)) for i, c in enumerate((d, xn, yn, dg))]

    @pl.when(s == 1)
    def _():
        top = [pltpu.make_async_copy(hb.at[1, c], sel_o.at[:, pl.ds(c * dm, dm)], lin.at[c]) for c in range(4)]
        for copy in top:
            copy.start()
        pl.semaphore_wait(go, 1)
        start_weights(1, other_pair, 0, 0, 0, tiles)

        def own_layers(q, carry):
            start_weights(q, (w_gate.at[q], w_in.at[q]), 1, 1 + q, 0, tiles - q * (tiles - early_tiles))
            return carry
        lax.fori_loop(0, 2, own_layers, 0)
        for copy in top:
            copy.wait()
        for copy in hand_over():
            copy.wait_recv()

    def layer(j, carry):
        nxt = 1 - j
        step = 32

        def norm_body(i, carry):
            rows = pl.ds(pl.multiple_of(i * step, step), step)
            blocks = [hb[j, c, rows, :].astype(F32) for c in range(4)]
            total = sum(jnp.sum(b * b, axis=-1, keepdims=True) for b in blocks)
            inv = lax.rsqrt(total * (1.0 / (4 * dm)) + EPSILON)
            for c in range(4):
                nb[rows, c * dm:(c + 1) * dm] = (blocks[c] * inv).astype(BF16)
            rv[rows, :] = jnp.broadcast_to(inv, (step, LANES))
            return carry
        lax.fori_loop(0, T // step, norm_body, 0)
        saves = [
            pltpu.make_async_copy(hb.at[j, d], ho_s.at[j], lsv.at[0]),
            pltpu.make_async_copy(nb.at[:, block_of(d)], no_s.at[j], lsv.at[1]),
            pltpu.make_async_copy(rv, r_s.at[j], lsv.at[2]),
        ]
        for copy in saves:
            copy.start()
        for copy in own_loads(j):
            copy.wait()

        def ab_copies(k, side):
            return [pltpu.make_async_copy(ab.at[side, 0], a_s.at[j, k], lab.at[side, 0]),
                    pltpu.make_async_copy(ab.at[side, 1], b_s.at[j, k], lab.at[side, 1])]

        def ab_body(k, carry):
            col = pl.ds(pl.multiple_of(k * LANES, LANES), LANES)
            wait_tile(j, k, col)

            @pl.when((j == 0) & (s == 0) & (k == tiles - 2))
            def _():
                pl.semaphore_signal(go, inc=1, device_id=(d, 1), device_id_type=MESH)

            def ab_rows(i, carry):
                rows = pl.ds(pl.multiple_of(i * piece, 16), piece)
                acc[rows, :] = jnp.dot(nb[rows, :], jnp.concatenate([wv[j, 0, :, col], wv[j, 1, :, col]], axis=1), preferred_element_type=F32)
                return carry
            lax.fori_loop(0, T // piece, ab_rows, 0)
            side = lax.rem(k, 2)

            @pl.when(k >= 2)
            def _():
                for copy in ab_copies(k, side):
                    copy.wait()
            a, b = acc[:, :LANES], acc[:, LANES:]
            ab[side, 0] = a
            ab[side, 1] = b
            ub[:, col] = (a * jax.nn.sigmoid(a) * b).astype(BF16)
            for copy in ab_copies(k, side):
                copy.start()
            return carry
        lax.fori_loop(0, tiles, ab_body, 0)
        for k in (tiles - 2, tiles - 1):
            for copy in ab_copies(k, k % 2):
                copy.wait()
        save_u = pltpu.make_async_copy(ub, u_s.at[j], lsv.at[3])
        save_u.start()

        @pl.when((j == 0) | (s == 0))
        def _():
            pltpu.make_async_copy(w_out.at[j], wov, lo.at[0]).wait()

            def send(i, c, rows, dst, chip):
                return remote(zp.at[c, rows], dst, zss.at[i], zrs.at[i], (chip, s))
            first = [send(0, dg, lo_rows, near_in.at[0, 0], xn), send(1, dg, hi_rows, near_in.at[1, 0], yn)]
            second = [send(2, xn, lo_rows, near_in.at[0, 1], xn), send(3, yn, hi_rows, near_in.at[1, 1], yn)]
            third = [send(4, yn, lo_rows, far_in.at[0], yn), send(5, xn, hi_rows, far_in.at[1], xn)]
            x, y = lax.rem(d, 2), lax.div(d, 2)
            wide = 2 * LANES

            def block_body(i, carry):
                rel, part_of = 3 - lax.div(i, 2), lax.rem(i, 2)
                c = 2 * lax.rem(y + lax.rem(rel, 2), 2) + lax.rem(x + lax.div(rel, 2), 2)

                def zp_rows(n, carry):
                    rows = pl.ds(pl.multiple_of(n * half, 16), half)
                    zp[c, rows, pl.ds(pl.multiple_of(part_of * wide, wide), wide)] = jnp.dot(
                        ub[rows, :], wov[:, pl.ds(pl.multiple_of(c * dm + part_of * wide, wide), wide)], preferred_element_type=F32)
                    return carry
                lax.fori_loop(0, 2, zp_rows, 0)
                for at, copies in ((1, first), (3, second[:1]), (5, second[1:])):
                    @pl.when(i == at)
                    def _():
                        for copy in copies:
                            copy.start()
                return carry
            lax.fori_loop(0, 8, block_body, 0)
            share = share_rows(hb.at[nxt], d, s, xn, yn, ass, ars, lo_rows, hi_rows)

            def both(n, stage):
                for at in range(2):
                    @pl.when(n == at)
                    def _():
                        stage(at)

            def half_rows(n):
                return pl.ds(pl.multiple_of(n * half, 16), half)

            def relay(n, carry):
                both(n, lambda at: first[at].wait_recv())
                c, rows = yn + n * (xn - yn), half_rows(n)
                zp[c, rows, :] += near_in[n, 0]
                both(n, lambda at: third[at].start())
                return carry
            lax.fori_loop(0, 2, relay, 0)

            def settle(n, carry):
                both(n, lambda at: (second[at].wait_recv(), third[at].wait_recv()))
                rows = half_rows(n)
                branch = (zp[d, rows, :] + near_in[n, 1] + far_in[n]).astype(BF16).astype(F32)
                hb[nxt, d, rows, :] = (hb[j, d, rows, :].astype(F32) + branch).astype(BF16)
                both(n, lambda at: [copy.start() for copy in share[at]])
                return carry
            lax.fori_loop(0, 2, settle, 0)
            near_share(share)

            @pl.when((j == 0) & (s == 1))
            def _():
                pl.semaphore_signal(go, inc=1, device_id=(d, 0), device_id_type=MESH)
            far_share(share)
            for copy in first + second + third:
                copy.wait_send()

        @pl.when((j == 0) & (s == 0))
        def _():
            pltpu.make_async_copy(w_out.at[1], wov, lo.at[0]).start()

        @pl.when((j == 1) & (s == 0))
        def _():
            hands = hand_over()
            for copy in hands:
                copy.start()

            def last_layer(q, carry):
                @pl.when(q == 1)
                def _():
                    pl.semaphore_wait(go, 1)
                start_weights(1, other_pair, 1, 1, early_tiles + q * (tiles - held_tiles - early_tiles), tiles - held_tiles + q * held_tiles)
                return carry
            lax.fori_loop(0, 2, last_layer, 0)
            for copy in hands:
                copy.wait_send()
        for copy in saves:
            copy.wait()
        save_u.wait()
        return carry
    lax.fori_loop(0, 2, layer, 0)
    wait_sent(0, tiles)

    @pl.when(s == 0)
    def _():
        wait_sent(1, tiles - early_tiles)

    @pl.when(s == 1)
    def _():
        wait_sent(1, tiles)
        wait_sent(2, early_tiles)


def backward_kernel(sel, slot, w_gate, w_in, w_out, a_s, b_s, ho_s, r_s,
                    da_o, db_o, e_o, act_o,
                    wgv, wov, eb, daf, ab, dn, hov, rv, sq, sv, agv, back_v,
                    dss, drs, fss, frs, ess, ers, hss, hrs, sss, srs, ass, ars, lw, lab, lout, lh, le, lsm):
    d, s, xn, yn, dg = place()
    T = sel.shape[0]
    part_rows = T // 2
    lo_n = -(-part_rows // 32) * 16
    cols = daf.shape[3]
    dm = dn.shape[1]
    wide = 2 * LANES
    n_full = cols // wide
    tail = cols - n_full * wide
    n_early = n_full // 2
    n_mid = n_early + 2
    splits, one_loop = (1 if T <= 640 else 2), T > 512
    pad = sq.shape[1]
    w_slots = wgv.shape[0]
    ab_slots = ab.shape[0]

    def wo_load(j):
        return pltpu.make_async_copy(w_out.at[j], wov, lw.at[0, 0])

    def slot_of(j, n):
        return j if n == 2 else 0

    def gate_loads(j):
        return [pltpu.make_async_copy(w.at[j], wgv.at[slot_of(j, w_slots), m], lw.at[1 + slot_of(j, w_slots), m]) for m, w in enumerate((w_gate, w_in))]

    def rows_of(g, base=0, size=part_rows):
        return pl.ds(pl.multiple_of(g * part_rows + base, 16), size)

    def in_copies(g):
        return [pltpu.make_async_copy(sel.at[rows_of(g), pl.ds(c * dm, dm)], eb.at[2, c, rows_of(g)], lh.at[g, c]) for c in range(4)]

    def hand_over(g):
        return [remote(eb.at[0, c, rows_of(g)], eb.at[2, c, rows_of(g)], hss.at[g, i], hrs.at[g, i], (d, 1 - s)) for i, c in enumerate((d, xn, yn, dg))]

    def ab_loads(j, g):
        side = slot_of(g, ab_slots)
        return [pltpu.make_async_copy(src.at[j, :, rows_of(g)], ab.at[side, m], lab.at[side, m]) for m, src in enumerate((a_s, b_s))]

    @pl.when(s == 1)
    def _():
        for copy in in_copies(0):
            copy.start()
    wo_load(1).start()
    small = [pltpu.make_async_copy(ho_s, hov, lsm.at[0]), pltpu.make_async_copy(r_s, rv, lsm.at[1])]
    for copy in ab_loads(1, 0):
        copy.start()
    meet()

    def columns(c, width):
        return pl.ds(pl.multiple_of(c * wide, LANES), width)

    def each_chunk(body, first=0, last=n_full):
        lax.fori_loop(first, last, lambda c, carry: (body(c, wide), carry)[1], 0)

    class Piece:
        def __init__(self, j, g):
            self.j, self.g, self.rows = j, g, rows_of(g)
            parts = (rows_of(g, 0, lo_n), rows_of(g, lo_n, part_rows - lo_n))
            self.share = share_rows(eb.at[j], d, s, xn, yn, ess.at[g], ers.at[g], *parts)
            self.e_saves = [pltpu.make_async_copy(eb.at[j + 1, c, self.rows], e_o.at[j, self.rows, pl.ds(c * dm, dm)], le.at[j, g, c]) for c in range(4)]
            self.sums = [remote(sv.at[g, 0], sv.at[g, 1 + i], sss.at[g, i], srs.at[g, i], (chip, s)) for i, chip in enumerate((xn, yn, dg))]

        def own_sends(self, c, col):
            g, out = self.g, []
            for m in range(2):
                for n, chip in enumerate((xn, yn)):
                    here = daf.at[m, d, self.rows, col]
                    out.append(remote(here, here, dss.at[g, m, n, c], drs.at[g, m, n, c], (chip, s)))
            return out

        def forwards(self, c, col):
            g = self.g
            from_x, from_y = daf.at[0, xn, self.rows, col], daf.at[1, yn, self.rows, col]
            return [remote(from_x, from_x, fss.at[g, 1, c], frs.at[g, 1, c], (yn, s)), remote(from_y, from_y, fss.at[g, 0, c], frs.at[g, 0, c], (xn, s))]

        def make(self):
            j, g, rows, side = self.j, self.g, self.rows, slot_of(self.g, ab_slots)
            for copy in self.e_saves:
                copy.start()

            @pl.when(g == 0)
            def _():
                wo_load(j).wait()
            for copy in ab_loads(j, g):
                copy.wait()

            @pl.when((j == 1) & (g == 0))
            def _():
                if ab_slots == 2:
                    for copy in ab_loads(1, 1):
                        copy.start()

                @pl.when(s == 1)
                def _():
                    for copy in in_copies(1):
                        copy.start()
                for copy in gate_loads(1) + small:
                    copy.start()
            if w_slots == 2:
                @pl.when((j == 1) & (g == 1))
                def _():
                    for copy in gate_loads(0):
                        copy.start()

            def tile(c, width=wide):
                base = jnp.minimum(c * wide, cols - wide) if one_loop else c * wide
                def du(blocks, lanes):
                    e_part = jnp.concatenate([eb[j + 1, n, rows, :] for n in blocks], axis=1)
                    return nt_dot(e_part, wov[pl.ds(pl.multiple_of(base, LANES), width), lanes])
                if splits == 1:
                    dn[rows, :width] = du(range(4), slice(None))
                else:
                    dn[rows, :width] = jnp.zeros((part_rows, width), F32)

                    def du_part(n, carry):
                        dn[rows, :width] += du((2 * n, 2 * n + 1), pl.ds(pl.multiple_of(n * 2 * dm, dm), 2 * dm))
                        return carry
                    lax.fori_loop(0, 2, du_part, 0)
                def lanes(n):
                    lane = pl.ds(pl.multiple_of(base + n * LANES, LANES), LANES)
                    at = lax.div(base, LANES) + n
                    a, b, du = ab[side, 0, at], ab[side, 1, at], dn[rows, n * LANES:(n + 1) * LANES]
                    sig = jax.nn.sigmoid(a)
                    daf[0, d, rows, lane] = (du * b * sig * (1.0 + a * (1.0 - sig))).astype(BF16)
                    daf[1, d, rows, lane] = (du * (a * sig)).astype(BF16)

                if one_loop:
                    @pl.when(c < n_full)
                    def _():
                        lanes(0)
                    lanes(1)
                else:
                    for n in range(width // LANES):
                        lanes(n)

            def body(c, width):
                tile(c, wide)

                @pl.when(c < n_early)
                def _():
                    for copy in self.own_sends(c, columns(c, wide)):
                        copy.start()
            each_chunk(body, 0, n_full + 1 if one_loop else n_full)
            if not one_loop:
                tile(n_full, tail)

        def send(self, first, last):
            def body(c, width):
                for copy in self.own_sends(c, columns(c, width)):
                    copy.start()
            each_chunk(body, first, last)

        def save_tile(self, m, chip, col, c, width):
            dst = (da_o, db_o)[m].at[self.j, self.rows, pl.ds(pl.multiple_of(chip * cols + c * wide, LANES), width)]
            pltpu.make_async_copy(daf.at[m, chip, self.rows, col], dst, lout.at[self.g]).start()

        def add(self, chip, c, width):
            def body(i, carry):
                m, at = lax.div(i, splits), pl.ds(pl.multiple_of(lax.rem(i, splits) * (dm // splits), LANES), dm // splits)
                w = wgv[slot_of(self.j, w_slots), m, at, pl.ds(pl.multiple_of(chip * cols + c * wide, LANES), width)]
                dn[self.rows, at] += nt_dot(daf[m, chip, self.rows, columns(c, width)], w)
                return carry
            lax.fori_loop(0, 2 * splits, body, 0)

        def own(self):
            @pl.when(self.g == 0)
            def _():
                for copy in gate_loads(self.j):
                    copy.wait()
            for m in range(2):
                self.save_tile(m, d, pl.ds(0, cols), 0, cols)
            dn[self.rows, :] = jnp.zeros((part_rows, dm), F32)
            each_chunk(lambda c, width: self.add(d, c, width))
            self.add(d, n_full, tail)

        def near(self, c, width):
            col = columns(c, width)
            fwd_y, fwd_x = self.forwards(c, col)

            def came(m, n, chip):
                there = daf.at[m, chip, self.rows, col]
                remote(there, there, dss.at[self.g, m, n, c], drs.at[self.g, m, n, c], (chip, s)).wait_recv()
            came(0, 0, xn)
            fwd_y.start()
            came(1, 1, yn)
            fwd_x.start()
            came(1, 0, xn)
            came(0, 1, yn)
            for chip in (xn, yn):
                for m in range(2):
                    self.save_tile(m, chip, col, c, width)
            lax.fori_loop(0, 2, lambda i, carry: (self.add(xn + i * (yn - xn), c, width), carry)[1], 0)

        def far(self):
            j, g, rows = self.j, self.g, self.rows

            def body(c, width):
                col = columns(c, width)
                there = [daf.at[m, dg, rows, col] for m in range(2)]
                remote(there[0], there[0], fss.at[g, 1, c], frs.at[g, 1, c], (yn, s)).wait_recv()
                remote(there[1], there[1], fss.at[g, 0, c], frs.at[g, 0, c], (xn, s)).wait_recv()
                for m in range(2):
                    self.save_tile(m, dg, col, c, width)
                self.add(dg, c, width)
            each_chunk(body)
            body(n_full, tail)

            @pl.when((j == 1) & (g == 0))
            def _():
                for copy in small:
                    copy.wait()
            prod = dn[rows, :] * hov[j, rows, :].astype(F32)
            sq[g, :part_rows, :] = (prod[:, :LANES] + prod[:, LANES:2 * LANES]) + (prod[:, 2 * LANES:3 * LANES] + prod[:, 3 * LANES:])
            sv[g, 0] = jnp.broadcast_to(jnp.sum(sq[g].T, axis=0, keepdims=True), (8, pad))
            for copy in self.sums:
                copy.start()
            if w_slots == 1:
                @pl.when((j == 1) & (g == 1))
                def _():
                    for copy in gate_loads(0):
                        copy.start()

        def finish(self):
            j, g = self.j, self.g
            whole = daf.at[:, :, self.rows]
            pltpu.make_async_copy(whole, whole, lout.at[g]).wait()

            def drain(c, width):
                col = columns(c, width)
                for copy in self.own_sends(c, col) + self.forwards(c, col):
                    copy.wait_send()
            each_chunk(drain)
            drain(n_full, tail)
            for copy in self.sums:
                copy.wait()
            mean = ((sv[g, 0, 0:1, :] + sv[g, 1, 0:1, :]) + (sv[g, 2, 0:1, :] + sv[g, 3, 0:1, :])) * (1.0 / (4 * dm))
            sq[g] = jnp.broadcast_to(mean, (LANES, pad)).T
            for n, (base, size) in enumerate(((0, lo_n), (lo_n, part_rows - lo_n))):
                at = rows_of(g, base, size)
                inv, avg = rv[j, at, :], sq[g, base:base + size, :]
                for c in range(4):
                    lane = slice(c * LANES, (c + 1) * LANES)
                    resid = inv * dn[at, lane] - hov[j, at, lane].astype(F32) * (inv * inv * inv) * avg
                    eb[j, d, at, lane] = (eb[j + 1, d, at, lane].astype(F32) + resid).astype(BF16)
                for copy in self.share[n]:
                    copy.start()

    def step(i, carry):
        g = lax.rem(i, 2)
        cur = Piece(1 - lax.div(i, 2), g)
        prev = Piece(1 - lax.div(i - 1, 2), 1 - g)
        live, later = i < 4, i > 0

        @pl.when(i >= 2)
        def _():
            far_share(Piece(1 - lax.div(i - 2, 2), g).share)

        @pl.when((i == 4) & (s == 1))
        def _():
            for copy in hand_over(0):
                copy.start()

        @pl.when(live)
        def _():
            @pl.when((i < 2) & (s == 0))
            def _():
                for copy in hand_over(g):
                    copy.wait_recv()

            @pl.when((i < 2) & (s == 1))
            def _():
                for copy in in_copies(g):
                    copy.wait()

            cur.make()

            @pl.when(i == 1)
            def _():
                wo_load(0).start()
            coming = i + ab_slots

            @pl.when(coming < 4)
            def _():
                for copy in ab_loads(1 - lax.div(coming, 2), lax.rem(coming, 2)):
                    copy.start()

        @pl.when(later)
        def _():
            prev.far()

        def halves(h, carry):
            @pl.when(live)
            def _():
                cur.send(n_early + h * (n_mid - n_early), n_mid + h * (n_full - n_mid))

            @pl.when(live & (h == 0))
            def _():
                cur.own()

            @pl.when(live & (h == 1))
            def _():
                for copy in cur.own_sends(n_full, columns(n_full, tail)):
                    copy.start()

            @pl.when(later & (h == 1))
            def _():
                near_share(prev.share)

            @pl.when(live)
            def _():
                each_chunk(cur.near, h * n_early, n_early + h * (n_full - n_early))

            @pl.when(later & (h == 0))
            def _():
                prev.finish()
            return carry
        lax.fori_loop(0, 2, halves, 0)

        @pl.when(live)
        def _():
            cur.near(n_full, tail)
        return carry
    lax.fori_loop(0, 5, step, 0)

    def act_copies(i, c):
        col = pl.ds(pl.multiple_of(c * dm, dm), dm)
        return remote(agv.at[c], act_o.at[:, col], ass.at[i], ars.at[i], (d, 1 - s)), pltpu.make_async_copy(agv.at[c], act_o.at[:, col], lh.at[0, i])

    @pl.when(s == 1)
    def _():
        far_share(Piece(0, 1).share)
        for copy in hand_over(1):
            copy.start()
        for i, c in enumerate((d, xn, yn, dg)):
            act_copies(i, c)[0].wait_recv()

    @pl.when(s == 0)
    def _():
        own_lo, own_hi, fwd_y, fwd_x = Piece(0, 1).share
        rows_out = agv.shape[1]
        own_slots = slot[:, pl.ds(pl.multiple_of(d * rows_out, LANES), rows_out)]
        back = (lax.broadcasted_iota(jnp.int32, (T, rows_out), 0) == own_slots).astype(BF16)
        back_v[...] = back
        came = ((), (own_hi[0],), (own_lo[1],), (fwd_y, fwd_x))
        x, y = lax.rem(d, 2), lax.div(d, 2)

        def spread(i, carry):
            for n in range(1, 4):
                @pl.when(i == n)
                def _():
                    for copy in came[n]:
                        copy.wait_recv()
            c = 2 * lax.rem(y + lax.div(i, 2), 2) + lax.rem(x + lax.rem(i, 2), 2)
            agv[c] = lax.dot_general(back_v[...], eb[0, c], (((0,), (0,)), ((), ())), preferred_element_type=F32).astype(BF16)
            for copy in act_copies(i, c):
                copy.start()
            return carry
        lax.fori_loop(0, 4, spread, 0)
        for copy in own_lo + own_hi + [fwd_y, fwd_x]:
            copy.wait_send()
        for i, c in enumerate((d, xn, yn, dg)):
            away, here = act_copies(i, c)
            away.wait_send()
            here.wait()
    def saved(i, carry):
        for copy in Piece(lax.div(i, 2), lax.rem(i, 2)).e_saves:
            copy.wait()
        return carry
    lax.fori_loop(0, 4, saved, 0)

    @pl.when(s == 1)
    def _():
        for g in range(2):
            for copy in hand_over(g):
                copy.wait_send()


def grads_kernel(no_s, u_s, da, db, e_o, act, gate_o, in_o, out_o, act_o, nv, uv, ev, av, nt, ut, ring, og, oo, ln, lr, lg, lo):
    layers = nv.shape[0]
    wide = ring.shape[3]
    n_gate, n_out = da.shape[2] // wide, e_o.shape[2] // wide
    slots, g_slots, o_slots = ring.shape[0], og.shape[0], oo.shape[0]
    rows = oo.shape[2]

    def put(ref, at, value):
        ref[at] = value

    def for_rows(count, body):
        parts = 1 if nv.shape[1] <= 640 else 2
        size = count // parts
        if parts == 1:
            body(pl.ds(0, size))
        else:
            lax.fori_loop(0, parts, lambda i, carry: (body(pl.ds(pl.multiple_of(i * size, 32), size)), carry)[1], 0)

    def flip(src, dst):
        def body(i, carry):
            lane = pl.ds(pl.multiple_of(i * LANES, LANES), LANES)
            dst[lane, :] = src[:, lane].T
            return carry
        lax.fori_loop(0, dst.shape[0] // LANES, body, 0)
    wholes = [pltpu.make_async_copy(src, dst, ln.at[i]) for i, (src, dst) in enumerate(((no_s, nv), (u_s, uv), (e_o, ev), (act, av)))]
    act_store = pltpu.make_async_copy(av, act_o, ln.at[4])

    def tile_at(c):
        return pl.ds(pl.multiple_of(c * wide, wide), wide)

    def loads(t):
        slot = lax.rem(t, slots)
        return [pltpu.make_async_copy(src.at[lax.div(t, n_gate), :, tile_at(lax.rem(t, n_gate))], ring.at[slot, m], lr.at[slot, m]) for m, src in enumerate((da, db))]

    def gate_stores(t):
        slot = lax.rem(t, g_slots)
        return [pltpu.make_async_copy(og.at[slot, m], dst.at[lax.div(t, n_gate), :, tile_at(lax.rem(t, n_gate))], lg.at[slot, m]) for m, dst in enumerate((gate_o, in_o))]

    def out_stores(t):
        slot = lax.rem(t, o_slots)
        return [pltpu.make_async_copy(oo.at[slot, m], out_o.at[lax.div(t, n_out), pl.ds(m * rows, rows), tile_at(lax.rem(t, n_out))], lo.at[slot, m]) for m in range(2)]

    def start(copies):
        for copy in copies:
            copy.start()

    def wait(copies):
        for copy in copies:
            copy.wait()
    wholes[0].start()
    for t in range(slots - 1):
        start(loads(t))
    start(wholes[1:])
    wholes[0].wait()

    def gate_body(t, carry):
        j, c, slot, at = lax.div(t, n_gate), lax.rem(t, n_gate), lax.rem(t, slots), lax.rem(t, g_slots)

        @pl.when(t + slots - 1 < layers * n_gate)
        def _():
            start(loads(t + slots - 1))

        @pl.when(c == 0)
        def _():
            flip(nv.at[j], nt)
        wait(loads(t))

        @pl.when(t >= g_slots)
        def _():
            wait(gate_stores(t - g_slots))

        def side(m, carry):
            for_rows(og.shape[2], lambda at_rows: put(og, (at, m, at_rows), jnp.dot(nt[at_rows, :], ring[slot, m], preferred_element_type=F32)))
            return carry
        lax.fori_loop(0, 2, side, 0)
        start(gate_stores(t))
        return carry
    lax.fori_loop(0, layers * n_gate, gate_body, 0)
    wait(wholes[1:])
    act_store.start()

    def out_body(t, carry):
        j, c, at = lax.div(t, n_out), lax.rem(t, n_out), lax.rem(t, o_slots)

        @pl.when(c == 0)
        def _():
            flip(uv.at[j], ut)

        @pl.when(t >= o_slots)
        def _():
            wait(out_stores(t - o_slots))

        def half(m, carry):
            for_rows(rows, lambda at_rows: put(oo, (at, m, at_rows), jnp.dot(
                ut[pl.ds(pl.multiple_of(m * rows + at_rows.start, 32), at_rows.size), :], ev[j, :, tile_at(c)], preferred_element_type=F32)))
            return carry
        lax.fori_loop(0, 2, half, 0)
        start(out_stores(t))
        return carry
    lax.fori_loop(0, layers * n_out, out_body, 0)
    act_store.wait()
    for t in range(layers * n_gate - g_slots, layers * n_gate):
        wait(gate_stores(t))
    for t in range(layers * n_out - o_slots, layers * n_out):
        wait(out_stores(t))


def grads_call(no_s, u_s, da, db, e_o, act):
    layers, T, dsh = no_s.shape
    cols, dff, dmod = u_s.shape[2], da.shape[2], e_o.shape[2]
    V, wide = pltpu.VMEM, 4 * LANES
    moved = 2 * layers * T * (dsh + cols + 2 * dff + dmod) + 4 * layers * (2 * dsh * dff + cols * dmod)
    return pl.pallas_call(
        grads_kernel, name=f'grads_{T}', in_specs=[ANY] * 6, out_specs=[ANY] * 4,
        out_shape=[jax.ShapeDtypeStruct((layers, dsh, dff), F32), jax.ShapeDtypeStruct((layers, dsh, dff), F32), jax.ShapeDtypeStruct((layers, cols, dmod), F32),
                   jax.ShapeDtypeStruct(act.shape, BF16)],
        scratch_shapes=[V((layers, T, dsh), BF16), V((layers, T, cols), BF16), V((layers, T, dmod), BF16), V(act.shape, BF16), V((dsh, T), BF16), V((cols, T), BF16),
                        V((6, 2, T, wide), BF16), V((4, 2, dsh, wide), F32), V((3, 2, cols // 2, wide), F32), DMA((5,)), DMA((6, 2)), DMA((4, 2)), DMA((3, 2))],
        cost_estimate=pl.CostEstimate(flops=2 * layers * T * (2 * dsh * dff + cols * dmod), bytes_accessed=moved, transcendentals=0),
        compiler_params=pltpu.CompilerParams(vmem_limit_bytes=VMEM_LIMIT))(no_s, u_s, da, db, e_o, act)


ANY = pl.BlockSpec(memory_space=pl.ANY)
DMA = pltpu.SemaphoreType.DMA


def comm_call(kernel, name, cid, outs, in_specs, scratch):
    return pl.pallas_call(
        kernel, name=name, out_shape=[jax.ShapeDtypeStruct(*o) for o in outs], in_specs=in_specs, out_specs=[ANY] * len(outs),
        scratch_shapes=scratch, compiler_params=pltpu.CompilerParams(collective_id=cid, has_side_effects=True, vmem_limit_bytes=VMEM_LIMIT))


def lens_call(lens, tokens):
    smem, vmem = pl.BlockSpec(memory_space=pltpu.SMEM), pl.BlockSpec(memory_space=pltpu.VMEM)
    rows = tokens // LANES
    return pl.pallas_call(
        lens_kernel, name='lens', out_shape=[jax.ShapeDtypeStruct((1, 4 * tokens), jnp.int32), jax.ShapeDtypeStruct((1,), jnp.int32)],
        in_specs=[smem], out_specs=[vmem, smem],
        scratch_shapes=[pltpu.VMEM((rows, LANES), jnp.int32), pltpu.VMEM((4, rows, LANES), jnp.int32), DMA((3,)), DMA((3,))],
        compiler_params=pltpu.CompilerParams(collective_id=0, has_side_effects=True))(lens)


def forward_call(cid, T, act, cot, slot, w_gate, w_in, w_out):
    rows, dmod = act.shape
    _, dsh, dff = w_gate.shape
    cols = dff // 4
    half = T // 2
    tiles = cols // LANES
    outs = [((T, dmod), BF16), ((2, tiles, T, LANES), F32), ((2, tiles, T, LANES), F32), ((2, T, cols), BF16),
            ((2, T, dsh), BF16), ((2, T, dsh), BF16), ((2, T, LANES), F32), ((2, dsh, dff), BF16)]
    V = pltpu.VMEM
    scratch = [V((2, 2, dmod, cols), BF16), V((cols, dmod), BF16), V((2, 4, T, dsh), BF16), V((T, dmod), BF16), V((T, cols), BF16),
               V((4, T, dsh), F32), V((T, 2 * LANES), F32), V((2, 2, T, LANES), F32), V((T, LANES), F32),
               V((2, 2, half, dsh), F32), V((2, half, dsh), F32), V((4 * rows, dsh), BF16),
               DMA((3,)), DMA((2, tiles)), DMA((3,)), DMA((3,)), DMA((2,)), DMA((2,)), DMA((4,)), DMA((4,)), DMA((6,)), DMA((6,)), DMA((6,)), DMA((6,)),
               DMA((2, 2)), DMA((1,)), DMA((2, 2)), DMA((4,)), DMA((4,)), pltpu.SemaphoreType.REGULAR]
    specs = [ANY, ANY, pl.BlockSpec(memory_space=pltpu.VMEM)] + [ANY] * 3
    return comm_call(forward_kernel, f'forward_{T}', cid, outs, specs, scratch)(act, cot, slot, w_gate, w_in, w_out)


def backward_call(cid, sel, slot, w_gate, w_in, w_out, a_s, b_s, ho_s, r_s):
    T, dmod = sel.shape
    _, dsh, dff = w_gate.shape
    cols = dff // 4
    tiles = cols // LANES
    chunks = (tiles + 1) // 2
    pad = -(-(T // 2) // LANES) * LANES
    slots = 2 if T <= 640 else 1
    ab_slots = 2 if T <= 832 else 1
    outs = [((2, T, dff), BF16), ((2, T, dff), BF16), ((2, T, dmod), BF16), ((slot.shape[1] // 4, dmod), BF16)]
    V = pltpu.VMEM
    scratch = [V((slots, 2, dsh, dff), BF16), V((cols, dmod), BF16), V((3, 4, T, dsh), BF16), V((2, 4, T, cols), BF16),
               V((ab_slots, 2, tiles, T // 2, LANES), F32), V((T, dsh), F32), V((2, T, dsh), BF16), V((2, T, LANES), F32), V((2, pad, LANES), F32), V((2, 4, 8, pad), F32), V((4, slot.shape[1] // 4, dsh), BF16), V((T, slot.shape[1] // 4), BF16),
               DMA((2, 2, 2, chunks)), DMA((2, 2, 2, chunks)), DMA((2, 2, chunks)), DMA((2, 2, chunks)), DMA((2, 6)), DMA((2, 6)), DMA((2, 4)), DMA((2, 4)),
               DMA((2, 3)), DMA((2, 3)), DMA((4,)), DMA((4,)), DMA((3, 2)), DMA((2, 2)), DMA((2,)), DMA((2, 4)), DMA((2, 2, 4)), DMA((2,))]
    return comm_call(backward_kernel, f'backward_{T}', cid, outs, [ANY, pl.BlockSpec(memory_space=pltpu.VMEM)] + [ANY] * 7, scratch)(sel, slot, w_gate, w_in, w_out, a_s, b_s, ho_s, r_s)


def solution(mesh, buckets=BUCKETS):
    act_spec = P(None, 'data')
    weight_spec = P('stage', None, 'data', None)

    def local_step(act_in, cot_out, seq_lens, w_gate, w_in, w_out):
        n_micro, n_rows, seq_len, dmod = act_in.shape
        rows = n_micro * n_rows * seq_len
        w_gate, w_in, w_out = w_gate[0], w_in[0], w_out[0]
        act, cot = act_in.reshape(rows, dmod), cot_out.reshape(rows, dmod)
        slot, count = lens_call(seq_lens.reshape(n_micro), rows)

        def branch(which, T):
            def run(_):
                sel, a_s, b_s, u_s, ho_s, no_s, r_s, _ = forward_call(1 + 2 * which, T, act, cot, slot, w_gate, w_in, w_out)
                da, db, e_o, act_grad = backward_call(2 + 2 * which, sel, slot, w_gate, w_in, w_out, a_s, b_s, ho_s, r_s)
                gate_grad, in_grad, out_grad, act_grad = grads_call(no_s, u_s, da, db, e_o, act_grad)
                return act_grad.reshape(act_in.shape), gate_grad[None], in_grad[None], out_grad[None]
            return run
        if len(buckets) == 1:
            return branch(0, buckets[0])(0)
        which = sum((count[0] > b).astype(jnp.int32) for b in buckets[:-1])
        return lax.switch(which, [branch(i, b) for i, b in enumerate(buckets)], 0)

    return jax.shard_map(local_step, mesh=mesh, in_specs=(act_spec, act_spec, act_spec, weight_spec, weight_spec, weight_spec), out_specs=(act_spec, weight_spec, weight_spec, weight_spec), check_vma=False)
```

```python
import functools

import jax
import jax.numpy as jnp
from jax import lax
from jax.experimental import pallas as pl
from jax.experimental.pallas import tpu as pltpu
from jax.sharding import PartitionSpec as P

EPSILON = 1e-6
MESH = pl.DeviceIdType.MESH
BF16, F32 = jnp.bfloat16, jnp.float32
LANES = 128
VMEM_LIMIT = 67043328
BUCKETS = (448, 480, 512, 544, 608, 992)


def nt_dot(left, right):
    return lax.dot_general(left, right, (((1,), (1,)), ((), ())), preferred_element_type=F32)


def place():
    d = lax.axis_index('data')
    s = lax.axis_index('stage')
    x = lax.rem(d, 2)
    y = lax.div(d, 2)
    return d, s, 2 * y + 1 - x, 2 * (1 - y) + x, 3 - d


def meet(same_core=False):
    d, s, xn, yn, dg = place()
    barrier = pltpu.get_barrier_semaphore()
    peers = [(xn, s), (yn, s), (dg, s)]
    if not same_core:
        peers += [(xn, 1 - s), (yn, 1 - s), (dg, 1 - s), (d, 1 - s)]
    for chip, core in peers:
        pl.semaphore_signal(barrier, inc=1, device_id=(chip, core), device_id_type=MESH)
    pl.semaphore_wait(barrier, len(peers))


def remote(src, dst, send_sem, recv_sem, device):
    return pltpu.make_async_remote_copy(src_ref=src, dst_ref=dst, send_sem=send_sem, recv_sem=recv_sem, device_id=device, device_id_type=MESH)


def lens_kernel(sizes, lens, slot, which, mine, everyone, ss, rs):
    d, s, xn, yn, dg = place()
    meet(same_core=True)
    seqs, tokens = lens.shape[0], mine.shape[0] * LANES
    each = tokens // seqs
    index = lax.broadcasted_iota(jnp.int32, mine.shape, 0) * LANES + lax.broadcasted_iota(jnp.int32, mine.shape, 1)
    length = jnp.zeros(mine.shape, jnp.int32)
    for i in range(seqs):
        length = jnp.where((index >= i * each) & (index < (i + 1) * each), lens[i], length)
    mine[...] = jnp.where(lax.rem(index, each) < length, 1, 0)
    everyone[d] = mine[...]
    sends = [remote(mine, everyone.at[d], ss.at[i], rs.at[i], (chip, s)) for i, chip in enumerate((xn, yn, dg))]
    for copy in sends:
        copy.start()
    for copy in sends:
        copy.wait()
    rows = 4 * mine.shape[0]
    live = everyone[...].reshape(rows, LANES)
    lane, row = lax.broadcasted_iota(jnp.int32, live.shape, 1), lax.broadcasted_iota(jnp.int32, live.shape, 0)
    upto = live
    shift = 1
    while shift < LANES:
        upto = upto + jnp.where(lane >= shift, pltpu.roll(upto, shift, 1), 0)
        shift *= 2
    whole = jnp.broadcast_to(jnp.sum(live, axis=1, keepdims=True), live.shape)
    before = whole
    shift = 1
    while shift < rows:
        before = before + jnp.where(row >= shift, pltpu.roll(before, shift, 0), 0)
        shift *= 2
    place_of = jnp.where(live > 0, before - whole + upto - 1, -1)
    for i in range(rows):
        slot[:, i * LANES:(i + 1) * LANES] = place_of[i:i + 1, :]
    total = jnp.sum(live)
    which[0] = sum((total > size).astype(jnp.int32) for size in sizes[:-1]) if len(sizes) > 1 else 0


def share_rows(buf, d, s, xn, yn, ss, rs, lo, hi):
    def own(part, i):
        return [remote(buf.at[d, part], buf.at[d, part], ss.at[2 * i + n], rs.at[2 * i + n], (chip, s)) for n, chip in enumerate((xn, yn))]

    fwd_y = remote(buf.at[xn, lo], buf.at[xn, lo], ss.at[4], rs.at[4], (yn, s))
    fwd_x = remote(buf.at[yn, hi], buf.at[yn, hi], ss.at[5], rs.at[5], (xn, s))
    return own(lo, 0), own(hi, 1), fwd_y, fwd_x


def near_share(share):
    own_lo, own_hi, fwd_y, fwd_x = share
    own_lo[0].wait_recv()
    fwd_y.start()
    own_hi[1].wait_recv()
    fwd_x.start()


def far_share(share):
    own_lo, own_hi, fwd_y, fwd_x = share
    own_hi[0].wait_recv()
    own_lo[1].wait_recv()
    fwd_y.wait_recv()
    fwd_x.wait_recv()
    for copy in own_lo + own_hi + [fwd_y, fwd_x]:
        copy.wait_send()


def forward_kernel(act, cot, slot, w_gate, w_in, w_out,
                   sel_o, a_s, b_s, u_s, ho_s, no_s, r_s, other,
                   wv, wov, hb, nb, ub, zp, acc, ab, rv, near_in, far_in, inpv,
                   wss, wrs, iss, irs, xss, xrs, hss, hrs, ass, ars, zss, zrs, lw, lo, lab, lsv, lin, go):
    d, s, xn, yn, dg = place()
    T = nb.shape[0]
    half = T // 2
    piece = T if T <= 512 else half
    cols = ub.shape[1]
    tiles = cols // LANES
    dm = hb.shape[3]
    rows_in = act.shape[0]
    lo_rows, hi_rows = pl.ds(0, half), pl.ds(half, half)
    chips = (dg, xn, yn)
    early_tiles, held_tiles = (1, 2) if T <= 448 else (2, 3)

    def block_of(chip):
        return pl.ds(pl.multiple_of(chip * dm, dm), dm)

    def input_rows(chip):
        return pl.ds(pl.multiple_of(chip * rows_in, LANES), rows_in)

    def own_loads(j):
        return [pltpu.make_async_copy(w.at[j, :, pl.ds(pl.multiple_of(d * cols, LANES), cols)], wv.at[j, m, block_of(d)], lw.at[j, m])
                for m, w in enumerate((w_gate, w_in))]

    def start_weights(layer, src, core, sem, first, last):
        def body(k, carry):
            col = pl.ds(pl.multiple_of(k * LANES, LANES), LANES)
            for chip in chips:
                from_col = pl.ds(pl.multiple_of(chip * cols + k * LANES, LANES), LANES)
                for m in range(2):
                    remote(src[m].at[:, from_col], wv.at[layer, m, block_of(d), col], wss.at[sem], wrs.at[layer, k], (chip, core)).start()
            return carry
        lax.fori_loop(first, last, body, 0)

    def wait_sent(sem, count):
        sent = wv.at[0, :, pl.ds(0, 3 * dm), pl.ds(0, count * LANES)]
        pltpu.make_async_copy(sent, sent, wss.at[sem]).wait()

    def wait_tile(layer, k, col):
        came = wv.at[layer, :, pl.ds(0, 3 * dm), col]
        pltpu.make_async_copy(came, came, wrs.at[layer, k]).wait()

    other_pair = (other.at[0], other.at[1])
    first_pair = (w_gate.at[0], w_in.at[0])

    def input_sends(src):
        return [remote(src.at[:, block_of(chip)], inpv.at[input_rows(d)], iss.at[i], irs.at[i], (chip, s)) for i, chip in enumerate(chips)]

    def own_input(src):
        return pltpu.make_async_copy(src.at[:, block_of(d)], inpv.at[input_rows(d)], lin.at[0])
    share = share_rows(hb.at[s], d, s, xn, yn, ass, ars, lo_rows, hi_rows)

    def first_weights(first, last):
        @pl.when(s == 0)
        def _():
            start_weights(0, first_pair, 0, 0, first, last)
    meet()
    for n, src in enumerate((act, cot)):
        @pl.when(s == n)
        def _():
            for copy in input_sends(src) + [own_input(src)]:
                copy.start()
    swaps = [remote(w.at[1], other.at[m], xss.at[m], xrs.at[m], (d, 1 - s)) for m, w in enumerate((w_gate, w_in))]
    for copy in own_loads(0) + own_loads(1) + swaps:
        copy.start()
    pltpu.make_async_copy(w_out.at[0], wov, lo.at[0]).start()
    tokens = slot.shape[1]

    def pick_body(i, carry):
        base = pl.multiple_of(lax.div(i, 2) * half, 16)
        pick = (lax.broadcasted_iota(jnp.int32, (half, tokens), 0) + base == slot[...]).astype(BF16)
        lane = pl.ds(pl.multiple_of(lax.rem(i, 2) * (dm // 2), LANES), dm // 2)
        hb[s, d, pl.ds(base, half), lane] = jnp.dot(pick, inpv[:, lane], preferred_element_type=F32).astype(BF16)
        return carry

    def opening(q, carry):
        @pl.when(q == 1)
        def _():
            for copy in input_sends(act):
                copy.wait()
            own_input(act).wait()
            lax.fori_loop(0, 4, pick_body, 0)
            for copy in share[0] + share[1]:
                copy.start()

        @pl.when(q == 2)
        def _():
            near_share(share)
        first_weights(3 * q, 3 * q + 3 + lax.div(q, 2) * (tiles - 9))
        return carry
    lax.fori_loop(0, 3, opening, 0)
    far_share(share)
    for copy in swaps:
        copy.wait()

    def hand_over():
        return [remote(hb.at[0, c], hb.at[0, c], hss.at[i], hrs.at[i], (d, 1 - s)) for i, c in enumerate((d, xn, yn, dg))]

    @pl.when(s == 1)
    def _():
        top = [pltpu.make_async_copy(hb.at[1, c], sel_o.at[:, pl.ds(c * dm, dm)], lin.at[c]) for c in range(4)]
        for copy in top:
            copy.start()
        pl.semaphore_wait(go, 1)
        start_weights(1, other_pair, 0, 0, 0, tiles)

        def own_layers(q, carry):
            start_weights(q, (w_gate.at[q], w_in.at[q]), 1, 1 + q, 0, tiles - q * (tiles - early_tiles))
            return carry
        lax.fori_loop(0, 2, own_layers, 0)
        for copy in top:
            copy.wait()
        for copy in hand_over():
            copy.wait_recv()

    def layer(j, carry):
        nxt = 1 - j
        step = 32

        def norm_body(i, carry):
            rows = pl.ds(pl.multiple_of(i * step, step), step)
            blocks = [hb[j, c, rows, :].astype(F32) for c in range(4)]
            total = sum(jnp.sum(b * b, axis=-1, keepdims=True) for b in blocks)
            inv = lax.rsqrt(total * (1.0 / (4 * dm)) + EPSILON)
            for c in range(4):
                nb[rows, c * dm:(c + 1) * dm] = (blocks[c] * inv).astype(BF16)
            rv[rows, :] = jnp.broadcast_to(inv, (step, LANES))
            return carry
        lax.fori_loop(0, T // step, norm_body, 0)
        saves = [
            pltpu.make_async_copy(hb.at[j, d], ho_s.at[j], lsv.at[0]),
            pltpu.make_async_copy(nb.at[:, block_of(d)], no_s.at[j], lsv.at[1]),
            pltpu.make_async_copy(rv, r_s.at[j], lsv.at[2]),
        ]
        for copy in saves:
            copy.start()
        for copy in own_loads(j):
            copy.wait()

        def ab_copies(k, side):
            return [pltpu.make_async_copy(ab.at[side, 0], a_s.at[j, k], lab.at[side, 0]),
                    pltpu.make_async_copy(ab.at[side, 1], b_s.at[j, k], lab.at[side, 1])]

        def ab_body(k, carry):
            col = pl.ds(pl.multiple_of(k * LANES, LANES), LANES)
            wait_tile(j, k, col)

            @pl.when((j == 0) & (s == 0) & (k == tiles - 2))
            def _():
                pl.semaphore_signal(go, inc=1, device_id=(d, 1), device_id_type=MESH)

            def ab_rows(i, carry):
                rows = pl.ds(pl.multiple_of(i * piece, 16), piece)
                acc[rows, :] = jnp.dot(nb[rows, :], jnp.concatenate([wv[j, 0, :, col], wv[j, 1, :, col]], axis=1), preferred_element_type=F32)
                return carry
            lax.fori_loop(0, T // piece, ab_rows, 0)
            side = lax.rem(k, 2)

            @pl.when(k >= 2)
            def _():
                for copy in ab_copies(k, side):
                    copy.wait()
            a, b = acc[:, :LANES], acc[:, LANES:]
            ab[side, 0] = a
            ab[side, 1] = b
            ub[:, col] = (a * jax.nn.sigmoid(a) * b).astype(BF16)
            for copy in ab_copies(k, side):
                copy.start()
            return carry
        lax.fori_loop(0, tiles, ab_body, 0)
        for k in (tiles - 2, tiles - 1):
            for copy in ab_copies(k, k % 2):
                copy.wait()
        save_u = pltpu.make_async_copy(ub, u_s.at[j], lsv.at[3])
        save_u.start()

        @pl.when((j == 0) | (s == 0))
        def _():
            pltpu.make_async_copy(w_out.at[j], wov, lo.at[0]).wait()

            def send(i, c, rows, dst, chip):
                return remote(zp.at[c, rows], dst, zss.at[i], zrs.at[i], (chip, s))
            first = [send(0, dg, lo_rows, near_in.at[0, 0], xn), send(1, dg, hi_rows, near_in.at[1, 0], yn)]
            second = [send(2, xn, lo_rows, near_in.at[0, 1], xn), send(3, yn, hi_rows, near_in.at[1, 1], yn)]
            third = [send(4, yn, lo_rows, far_in.at[0], yn), send(5, xn, hi_rows, far_in.at[1], xn)]
            x, y = lax.rem(d, 2), lax.div(d, 2)
            wide = 2 * LANES

            def block_body(i, carry):
                rel, part_of = 3 - lax.div(i, 2), lax.rem(i, 2)
                c = 2 * lax.rem(y + lax.rem(rel, 2), 2) + lax.rem(x + lax.div(rel, 2), 2)

                def zp_rows(n, carry):
                    rows = pl.ds(pl.multiple_of(n * half, 16), half)
                    zp[c, rows, pl.ds(pl.multiple_of(part_of * wide, wide), wide)] = jnp.dot(
                        ub[rows, :], wov[:, pl.ds(pl.multiple_of(c * dm + part_of * wide, wide), wide)], preferred_element_type=F32)
                    return carry
                lax.fori_loop(0, 2, zp_rows, 0)
                for at, copies in ((1, first), (3, second[:1]), (5, second[1:])):
                    @pl.when(i == at)
                    def _():
                        for copy in copies:
                            copy.start()
                return carry
            lax.fori_loop(0, 8, block_body, 0)
            share = share_rows(hb.at[nxt], d, s, xn, yn, ass, ars, lo_rows, hi_rows)

            def both(n, stage):
                for at in range(2):
                    @pl.when(n == at)
                    def _():
                        stage(at)

            def half_rows(n):
                return pl.ds(pl.multiple_of(n * half, 16), half)

            def relay(n, carry):
                both(n, lambda at: first[at].wait_recv())
                c, rows = yn + n * (xn - yn), half_rows(n)
                zp[c, rows, :] += near_in[n, 0]
                both(n, lambda at: third[at].start())
                return carry
            lax.fori_loop(0, 2, relay, 0)

            def settle(n, carry):
                both(n, lambda at: (second[at].wait_recv(), third[at].wait_recv()))
                rows = half_rows(n)
                branch = (zp[d, rows, :] + near_in[n, 1] + far_in[n]).astype(BF16).astype(F32)
                hb[nxt, d, rows, :] = (hb[j, d, rows, :].astype(F32) + branch).astype(BF16)
                both(n, lambda at: [copy.start() for copy in share[at]])
                return carry
            lax.fori_loop(0, 2, settle, 0)
            near_share(share)

            @pl.when((j == 0) & (s == 1))
            def _():
                pl.semaphore_signal(go, inc=1, device_id=(d, 0), device_id_type=MESH)
            far_share(share)
            for copy in first + second + third:
                copy.wait_send()

        @pl.when((j == 0) & (s == 0))
        def _():
            pltpu.make_async_copy(w_out.at[1], wov, lo.at[0]).start()

        @pl.when((j == 1) & (s == 0))
        def _():
            hands = hand_over()
            for copy in hands:
                copy.start()

            def last_layer(q, carry):
                @pl.when(q == 1)
                def _():
                    pl.semaphore_wait(go, 1)
                start_weights(1, other_pair, 1, 1, early_tiles + q * (tiles - held_tiles - early_tiles), tiles - held_tiles + q * held_tiles)
                return carry
            lax.fori_loop(0, 2, last_layer, 0)
            for copy in hands:
                copy.wait_send()
        for copy in saves:
            copy.wait()
        save_u.wait()
        return carry
    lax.fori_loop(0, 2, layer, 0)
    wait_sent(0, tiles)

    @pl.when(s == 0)
    def _():
        wait_sent(1, tiles - early_tiles)

    @pl.when(s == 1)
    def _():
        wait_sent(1, tiles)
        wait_sent(2, early_tiles)


def backward_kernel(sel, slot, w_gate, w_in, w_out, a_s, b_s, ho_s, r_s,
                    da_o, db_o, e_o, act_o,
                    wgv, wov, eb, daf, ab, dn, hov, rv, sq, sv, agv, back_v,
                    dss, drs, fss, frs, ess, ers, hss, hrs, sss, srs, ass, ars, lw, lab, lout, lh, le, lsm):
    d, s, xn, yn, dg = place()
    T = sel.shape[0]
    part_rows = T // 2
    lo_n = -(-part_rows // 32) * 16
    cols = daf.shape[3]
    dm = dn.shape[1]
    wide = 2 * LANES
    n_full = cols // wide
    tail = cols - n_full * wide
    n_early = n_full // 2
    n_mid = n_early + 2
    splits, one_loop = (1 if T <= 640 else 2), T > 512
    pad = sq.shape[1]
    w_slots = wgv.shape[0]
    ab_slots = ab.shape[0]

    def wo_load(j):
        return pltpu.make_async_copy(w_out.at[j], wov, lw.at[0, 0])

    def slot_of(j, n):
        return j if n == 2 else 0

    def gate_loads(j):
        return [pltpu.make_async_copy(w.at[j], wgv.at[slot_of(j, w_slots), m], lw.at[1 + slot_of(j, w_slots), m]) for m, w in enumerate((w_gate, w_in))]

    def rows_of(g, base=0, size=part_rows):
        return pl.ds(pl.multiple_of(g * part_rows + base, 16), size)

    def in_copies(g):
        return [pltpu.make_async_copy(sel.at[rows_of(g), pl.ds(c * dm, dm)], eb.at[2, c, rows_of(g)], lh.at[g, c]) for c in range(4)]

    def hand_over(g):
        return [remote(eb.at[0, c, rows_of(g)], eb.at[2, c, rows_of(g)], hss.at[g, i], hrs.at[g, i], (d, 1 - s)) for i, c in enumerate((d, xn, yn, dg))]

    def ab_loads(j, g):
        side = slot_of(g, ab_slots)
        return [pltpu.make_async_copy(src.at[j, :, rows_of(g)], ab.at[side, m], lab.at[side, m]) for m, src in enumerate((a_s, b_s))]

    @pl.when(s == 1)
    def _():
        for copy in in_copies(0):
            copy.start()
    wo_load(1).start()
    small = [pltpu.make_async_copy(ho_s, hov, lsm.at[0]), pltpu.make_async_copy(r_s, rv, lsm.at[1])]
    for copy in ab_loads(1, 0):
        copy.start()
    meet()

    def columns(c, width):
        return pl.ds(pl.multiple_of(c * wide, LANES), width)

    def each_chunk(body, first=0, last=n_full):
        lax.fori_loop(first, last, lambda c, carry: (body(c, wide), carry)[1], 0)

    class Piece:
        def __init__(self, j, g):
            self.j, self.g, self.rows = j, g, rows_of(g)
            parts = (rows_of(g, 0, lo_n), rows_of(g, lo_n, part_rows - lo_n))
            self.share = share_rows(eb.at[j], d, s, xn, yn, ess.at[g], ers.at[g], *parts)
            self.e_saves = [pltpu.make_async_copy(eb.at[j + 1, c, self.rows], e_o.at[j, self.rows, pl.ds(c * dm, dm)], le.at[j, g, c]) for c in range(4)]
            self.sums = [remote(sv.at[g, 0], sv.at[g, 1 + i], sss.at[g, i], srs.at[g, i], (chip, s)) for i, chip in enumerate((xn, yn, dg))]

        def own_sends(self, c, col):
            g, out = self.g, []
            for m in range(2):
                for n, chip in enumerate((xn, yn)):
                    here = daf.at[m, d, self.rows, col]
                    out.append(remote(here, here, dss.at[g, m, n, c], drs.at[g, m, n, c], (chip, s)))
            return out

        def forwards(self, c, col):
            g = self.g
            from_x, from_y = daf.at[0, xn, self.rows, col], daf.at[1, yn, self.rows, col]
            return [remote(from_x, from_x, fss.at[g, 1, c], frs.at[g, 1, c], (yn, s)), remote(from_y, from_y, fss.at[g, 0, c], frs.at[g, 0, c], (xn, s))]

        def make(self):
            j, g, rows, side = self.j, self.g, self.rows, slot_of(self.g, ab_slots)
            for copy in self.e_saves:
                copy.start()

            @pl.when(g == 0)
            def _():
                wo_load(j).wait()
            for copy in ab_loads(j, g):
                copy.wait()

            @pl.when((j == 1) & (g == 0))
            def _():
                if ab_slots == 2:
                    for copy in ab_loads(1, 1):
                        copy.start()

                @pl.when(s == 1)
                def _():
                    for copy in in_copies(1):
                        copy.start()
                for copy in gate_loads(1) + small:
                    copy.start()
            if w_slots == 2:
                @pl.when((j == 1) & (g == 1))
                def _():
                    for copy in gate_loads(0):
                        copy.start()

            def tile(c, width=wide):
                base = jnp.minimum(c * wide, cols - wide) if one_loop else c * wide
                def du(blocks, lanes):
                    e_part = jnp.concatenate([eb[j + 1, n, rows, :] for n in blocks], axis=1)
                    return nt_dot(e_part, wov[pl.ds(pl.multiple_of(base, LANES), width), lanes])
                if splits == 1:
                    dn[rows, :width] = du(range(4), slice(None))
                else:
                    dn[rows, :width] = jnp.zeros((part_rows, width), F32)

                    def du_part(n, carry):
                        dn[rows, :width] += du((2 * n, 2 * n + 1), pl.ds(pl.multiple_of(n * 2 * dm, dm), 2 * dm))
                        return carry
                    lax.fori_loop(0, 2, du_part, 0)
                def lanes(n):
                    lane = pl.ds(pl.multiple_of(base + n * LANES, LANES), LANES)
                    at = lax.div(base, LANES) + n
                    a, b, du = ab[side, 0, at], ab[side, 1, at], dn[rows, n * LANES:(n + 1) * LANES]
                    sig = jax.nn.sigmoid(a)
                    daf[0, d, rows, lane] = (du * b * sig * (1.0 + a * (1.0 - sig))).astype(BF16)
                    daf[1, d, rows, lane] = (du * (a * sig)).astype(BF16)

                if one_loop:
                    @pl.when(c < n_full)
                    def _():
                        lanes(0)
                    lanes(1)
                else:
                    for n in range(width // LANES):
                        lanes(n)

            def body(c, width):
                tile(c, wide)

                @pl.when(c < n_early)
                def _():
                    for copy in self.own_sends(c, columns(c, wide)):
                        copy.start()
            each_chunk(body, 0, n_full + 1 if one_loop else n_full)
            if not one_loop:
                tile(n_full, tail)

        def send(self, first, last):
            def body(c, width):
                for copy in self.own_sends(c, columns(c, width)):
                    copy.start()
            each_chunk(body, first, last)

        def save_tile(self, m, chip, col, c, width):
            dst = (da_o, db_o)[m].at[self.j, self.rows, pl.ds(pl.multiple_of(chip * cols + c * wide, LANES), width)]
            pltpu.make_async_copy(daf.at[m, chip, self.rows, col], dst, lout.at[self.g]).start()

        def add(self, chip, c, width):
            def body(i, carry):
                m, at = lax.div(i, splits), pl.ds(pl.multiple_of(lax.rem(i, splits) * (dm // splits), LANES), dm // splits)
                w = wgv[slot_of(self.j, w_slots), m, at, pl.ds(pl.multiple_of(chip * cols + c * wide, LANES), width)]
                dn[self.rows, at] += nt_dot(daf[m, chip, self.rows, columns(c, width)], w)
                return carry
            lax.fori_loop(0, 2 * splits, body, 0)

        def own(self):
            @pl.when(self.g == 0)
            def _():
                for copy in gate_loads(self.j):
                    copy.wait()
            for m in range(2):
                self.save_tile(m, d, pl.ds(0, cols), 0, cols)
            dn[self.rows, :] = jnp.zeros((part_rows, dm), F32)
            each_chunk(lambda c, width: self.add(d, c, width))
            self.add(d, n_full, tail)

        def near(self, c, width):
            col = columns(c, width)
            fwd_y, fwd_x = self.forwards(c, col)

            def came(m, n, chip):
                there = daf.at[m, chip, self.rows, col]
                remote(there, there, dss.at[self.g, m, n, c], drs.at[self.g, m, n, c], (chip, s)).wait_recv()
            came(0, 0, xn)
            fwd_y.start()
            came(1, 1, yn)
            fwd_x.start()
            came(1, 0, xn)
            came(0, 1, yn)
            for chip in (xn, yn):
                for m in range(2):
                    self.save_tile(m, chip, col, c, width)
            lax.fori_loop(0, 2, lambda i, carry: (self.add(xn + i * (yn - xn), c, width), carry)[1], 0)

        def far(self):
            j, g, rows = self.j, self.g, self.rows

            def body(c, width):
                col = columns(c, width)
                there = [daf.at[m, dg, rows, col] for m in range(2)]
                remote(there[0], there[0], fss.at[g, 1, c], frs.at[g, 1, c], (yn, s)).wait_recv()
                remote(there[1], there[1], fss.at[g, 0, c], frs.at[g, 0, c], (xn, s)).wait_recv()
                for m in range(2):
                    self.save_tile(m, dg, col, c, width)
                self.add(dg, c, width)
            each_chunk(body)
            body(n_full, tail)

            @pl.when((j == 1) & (g == 0))
            def _():
                for copy in small:
                    copy.wait()
            prod = dn[rows, :] * hov[j, rows, :].astype(F32)
            sq[g, :part_rows, :] = (prod[:, :LANES] + prod[:, LANES:2 * LANES]) + (prod[:, 2 * LANES:3 * LANES] + prod[:, 3 * LANES:])
            sv[g, 0] = jnp.broadcast_to(jnp.sum(sq[g].T, axis=0, keepdims=True), (8, pad))
            for copy in self.sums:
                copy.start()
            if w_slots == 1:
                @pl.when((j == 1) & (g == 1))
                def _():
                    for copy in gate_loads(0):
                        copy.start()

        def finish(self):
            j, g = self.j, self.g
            whole = daf.at[:, :, self.rows]
            pltpu.make_async_copy(whole, whole, lout.at[g]).wait()

            def drain(c, width):
                col = columns(c, width)
                for copy in self.own_sends(c, col) + self.forwards(c, col):
                    copy.wait_send()
            each_chunk(drain)
            drain(n_full, tail)
            for copy in self.sums:
                copy.wait()
            mean = ((sv[g, 0, 0:1, :] + sv[g, 1, 0:1, :]) + (sv[g, 2, 0:1, :] + sv[g, 3, 0:1, :])) * (1.0 / (4 * dm))
            sq[g] = jnp.broadcast_to(mean, (LANES, pad)).T
            for n, (base, size) in enumerate(((0, lo_n), (lo_n, part_rows - lo_n))):
                at = rows_of(g, base, size)
                inv, avg = rv[j, at, :], sq[g, base:base + size, :]
                for c in range(4):
                    lane = slice(c * LANES, (c + 1) * LANES)
                    resid = inv * dn[at, lane] - hov[j, at, lane].astype(F32) * (inv * inv * inv) * avg
                    eb[j, d, at, lane] = (eb[j + 1, d, at, lane].astype(F32) + resid).astype(BF16)
                for copy in self.share[n]:
                    copy.start()

    def give(g):
        own_lo, own_hi, fwd_y, fwd_x = Piece(0, g).share
        for copy, came in zip(hand_over(g), ((), (own_hi[0],), (own_lo[1],), (fwd_y, fwd_x))):
            for part in came:
                part.wait_recv()
            copy.start()
        for copy in own_lo + own_hi + [fwd_y, fwd_x]:
            copy.wait_send()

    def step(i, carry):
        g = lax.rem(i, 2)
        cur = Piece(1 - lax.div(i, 2), g)
        prev = Piece(1 - lax.div(i - 1, 2), 1 - g)
        live, later = i < 4, i > 0

        ending = (i == 4) & (s == 1)

        @pl.when(ending)
        def _():
            give(0)

        @pl.when((i >= 2) & jnp.logical_not(ending))
        def _():
            far_share(Piece(1 - lax.div(i - 2, 2), g).share)

        @pl.when(live)
        def _():
            @pl.when((i < 2) & (s == 0))
            def _():
                for copy in hand_over(g):
                    copy.wait_recv()

            @pl.when((i < 2) & (s == 1))
            def _():
                for copy in in_copies(g):
                    copy.wait()

            cur.make()

            @pl.when(i == 1)
            def _():
                wo_load(0).start()
            coming = i + ab_slots

            @pl.when(coming < 4)
            def _():
                for copy in ab_loads(1 - lax.div(coming, 2), lax.rem(coming, 2)):
                    copy.start()

        @pl.when(later)
        def _():
            prev.far()

        def halves(h, carry):
            @pl.when(live)
            def _():
                cur.send(n_early + h * (n_mid - n_early), n_mid + h * (n_full - n_mid))

            @pl.when(live & (h == 0))
            def _():
                cur.own()

            @pl.when(live & (h == 1))
            def _():
                for copy in cur.own_sends(n_full, columns(n_full, tail)):
                    copy.start()

            @pl.when(later & (h == 1))
            def _():
                near_share(prev.share)

            @pl.when(live)
            def _():
                each_chunk(cur.near, h * n_early, n_early + h * (n_full - n_early))

            @pl.when(later & (h == 0))
            def _():
                prev.finish()
            return carry
        lax.fori_loop(0, 2, halves, 0)

        @pl.when(live)
        def _():
            cur.near(n_full, tail)
        return carry
    lax.fori_loop(0, 5, step, 0)

    def act_copies(i, c):
        col = pl.ds(pl.multiple_of(c * dm, dm), dm)
        return remote(agv.at[c], act_o.at[:, col], ass.at[i], ars.at[i], (d, 1 - s)), pltpu.make_async_copy(agv.at[c], act_o.at[:, col], lh.at[0, i])

    @pl.when(s == 1)
    def _():
        give(1)
        for i, c in enumerate((d, xn, yn, dg)):
            act_copies(i, c)[0].wait_recv()

    @pl.when(s == 0)
    def _():
        own_lo, own_hi, fwd_y, fwd_x = Piece(0, 1).share
        rows_out = agv.shape[1]
        own_slots = slot[:, pl.ds(pl.multiple_of(d * rows_out, LANES), rows_out)]
        back = (lax.broadcasted_iota(jnp.int32, (T, rows_out), 0) == own_slots).astype(BF16)
        back_v[...] = back
        came = ((), (own_hi[0],), (own_lo[1],), (fwd_y, fwd_x))
        x, y = lax.rem(d, 2), lax.div(d, 2)

        def spread(i, carry):
            for n in range(1, 4):
                @pl.when(i == n)
                def _():
                    for copy in came[n]:
                        copy.wait_recv()
            c = 2 * lax.rem(y + lax.div(i, 2), 2) + lax.rem(x + lax.rem(i, 2), 2)
            agv[c] = lax.dot_general(back_v[...], eb[0, c], (((0,), (0,)), ((), ())), preferred_element_type=F32).astype(BF16)
            for copy in act_copies(i, c):
                copy.start()
            return carry
        lax.fori_loop(0, 4, spread, 0)
        for copy in own_lo + own_hi + [fwd_y, fwd_x]:
            copy.wait_send()
        for i, c in enumerate((d, xn, yn, dg)):
            away, here = act_copies(i, c)
            away.wait_send()
            here.wait()
    def saved(i, carry):
        for copy in Piece(lax.div(i, 2), lax.rem(i, 2)).e_saves:
            copy.wait()
        return carry
    lax.fori_loop(0, 4, saved, 0)

    @pl.when(s == 1)
    def _():
        for g in range(2):
            for copy in hand_over(g):
                copy.wait_send()


def grads_kernel(no_s, u_s, da, db, e_o, act, gate_o, in_o, out_o, act_o, nv, uv, ev, av, nt, ut, ring, og, oo, ln, lr, lg, lo):
    layers = nv.shape[0]
    wide = ring.shape[3]
    n_gate, n_out = da.shape[2] // wide, e_o.shape[2] // wide
    slots, g_slots, o_slots = ring.shape[0], og.shape[0], oo.shape[0]
    rows = oo.shape[2]

    def put(ref, at, value):
        ref[at] = value

    def for_rows(count, body):
        parts = 1 if nv.shape[1] <= 640 else 2
        size = count // parts
        if parts == 1:
            body(pl.ds(0, size))
        else:
            lax.fori_loop(0, parts, lambda i, carry: (body(pl.ds(pl.multiple_of(i * size, 32), size)), carry)[1], 0)

    def flip(src, dst):
        def body(i, carry):
            lane = pl.ds(pl.multiple_of(i * LANES, LANES), LANES)
            dst[lane, :] = src[:, lane].T
            return carry
        lax.fori_loop(0, dst.shape[0] // LANES, body, 0)
    wholes = [pltpu.make_async_copy(src, dst, ln.at[i]) for i, (src, dst) in enumerate(((no_s, nv), (u_s, uv), (e_o, ev), (act, av)))]
    act_store = pltpu.make_async_copy(av, act_o, ln.at[4])

    def tile_at(c):
        return pl.ds(pl.multiple_of(c * wide, wide), wide)

    def loads(t):
        slot = lax.rem(t, slots)
        return [pltpu.make_async_copy(src.at[lax.div(t, n_gate), :, tile_at(lax.rem(t, n_gate))], ring.at[slot, m], lr.at[slot, m]) for m, src in enumerate((da, db))]

    def gate_stores(t):
        slot = lax.rem(t, g_slots)
        return [pltpu.make_async_copy(og.at[slot, m], dst.at[lax.div(t, n_gate), :, tile_at(lax.rem(t, n_gate))], lg.at[slot, m]) for m, dst in enumerate((gate_o, in_o))]

    def out_stores(t):
        slot = lax.rem(t, o_slots)
        return [pltpu.make_async_copy(oo.at[slot, m], out_o.at[lax.div(t, n_out), pl.ds(m * rows, rows), tile_at(lax.rem(t, n_out))], lo.at[slot, m]) for m in range(2)]

    def start(copies):
        for copy in copies:
            copy.start()

    def wait(copies):
        for copy in copies:
            copy.wait()
    wholes[0].start()
    for t in range(slots - 1):
        start(loads(t))
    start(wholes[1:])
    wholes[0].wait()

    def gate_body(t, carry):
        j, c, slot, at = lax.div(t, n_gate), lax.rem(t, n_gate), lax.rem(t, slots), lax.rem(t, g_slots)

        @pl.when(t + slots - 1 < layers * n_gate)
        def _():
            start(loads(t + slots - 1))

        @pl.when(c == 0)
        def _():
            flip(nv.at[j], nt)
        wait(loads(t))

        @pl.when(t >= g_slots)
        def _():
            wait(gate_stores(t - g_slots))

        def side(m, carry):
            for_rows(og.shape[2], lambda at_rows: put(og, (at, m, at_rows), jnp.dot(nt[at_rows, :], ring[slot, m], preferred_element_type=F32)))
            return carry
        lax.fori_loop(0, 2, side, 0)
        start(gate_stores(t))
        return carry
    lax.fori_loop(0, layers * n_gate, gate_body, 0)
    wait(wholes[1:])
    act_store.start()

    def out_body(t, carry):
        j, c, at = lax.div(t, n_out), lax.rem(t, n_out), lax.rem(t, o_slots)

        @pl.when(c == 0)
        def _():
            flip(uv.at[j], ut)

        @pl.when(t >= o_slots)
        def _():
            wait(out_stores(t - o_slots))

        def half(m, carry):
            for_rows(rows, lambda at_rows: put(oo, (at, m, at_rows), jnp.dot(
                ut[pl.ds(pl.multiple_of(m * rows + at_rows.start, 32), at_rows.size), :], ev[j, :, tile_at(c)], preferred_element_type=F32)))
            return carry
        lax.fori_loop(0, 2, half, 0)
        start(out_stores(t))
        return carry
    lax.fori_loop(0, layers * n_out, out_body, 0)
    act_store.wait()
    for t in range(layers * n_gate - g_slots, layers * n_gate):
        wait(gate_stores(t))
    for t in range(layers * n_out - o_slots, layers * n_out):
        wait(out_stores(t))


def grads_call(no_s, u_s, da, db, e_o, act):
    layers, T, dsh = no_s.shape
    cols, dff, dmod = u_s.shape[2], da.shape[2], e_o.shape[2]
    V, wide = pltpu.VMEM, 4 * LANES
    moved = 2 * layers * T * (dsh + cols + 2 * dff + dmod) + 4 * layers * (2 * dsh * dff + cols * dmod)
    return pl.pallas_call(
        grads_kernel, name=f'grads_{T}', in_specs=[ANY] * 6, out_specs=[ANY] * 4,
        out_shape=[jax.ShapeDtypeStruct((layers, dsh, dff), F32), jax.ShapeDtypeStruct((layers, dsh, dff), F32), jax.ShapeDtypeStruct((layers, cols, dmod), F32),
                   jax.ShapeDtypeStruct(act.shape, BF16)],
        scratch_shapes=[V((layers, T, dsh), BF16), V((layers, T, cols), BF16), V((layers, T, dmod), BF16), V(act.shape, BF16), V((dsh, T), BF16), V((cols, T), BF16),
                        V((6, 2, T, wide), BF16), V((4, 2, dsh, wide), F32), V((3, 2, cols // 2, wide), F32), DMA((5,)), DMA((6, 2)), DMA((4, 2)), DMA((3, 2))],
        cost_estimate=pl.CostEstimate(flops=2 * layers * T * (2 * dsh * dff + cols * dmod), bytes_accessed=moved, transcendentals=0),
        compiler_params=pltpu.CompilerParams(vmem_limit_bytes=VMEM_LIMIT))(no_s, u_s, da, db, e_o, act)


ANY = pl.BlockSpec(memory_space=pl.ANY)
DMA = pltpu.SemaphoreType.DMA


def comm_call(kernel, name, cid, outs, in_specs, scratch):
    return pl.pallas_call(
        kernel, name=name, out_shape=[jax.ShapeDtypeStruct(*o) for o in outs], in_specs=in_specs, out_specs=[ANY] * len(outs),
        scratch_shapes=scratch, compiler_params=pltpu.CompilerParams(collective_id=cid, has_side_effects=True, vmem_limit_bytes=VMEM_LIMIT))


def lens_call(lens, tokens, sizes):
    smem, vmem = pl.BlockSpec(memory_space=pltpu.SMEM), pl.BlockSpec(memory_space=pltpu.VMEM)
    rows = tokens // LANES
    return pl.pallas_call(
        functools.partial(lens_kernel, sizes), name='lens', out_shape=[jax.ShapeDtypeStruct((1, 4 * tokens), jnp.int32), jax.ShapeDtypeStruct((1,), jnp.int32)],
        in_specs=[smem], out_specs=[vmem, smem],
        scratch_shapes=[pltpu.VMEM((rows, LANES), jnp.int32), pltpu.VMEM((4, rows, LANES), jnp.int32), DMA((3,)), DMA((3,))],
        compiler_params=pltpu.CompilerParams(collective_id=0, has_side_effects=True))(lens)


def forward_call(cid, T, act, cot, slot, w_gate, w_in, w_out):
    rows, dmod = act.shape
    _, dsh, dff = w_gate.shape
    cols = dff // 4
    half = T // 2
    tiles = cols // LANES
    outs = [((T, dmod), BF16), ((2, tiles, T, LANES), F32), ((2, tiles, T, LANES), F32), ((2, T, cols), BF16),
            ((2, T, dsh), BF16), ((2, T, dsh), BF16), ((2, T, LANES), F32), ((2, dsh, dff), BF16)]
    V = pltpu.VMEM
    scratch = [V((2, 2, dmod, cols), BF16), V((cols, dmod), BF16), V((2, 4, T, dsh), BF16), V((T, dmod), BF16), V((T, cols), BF16),
               V((4, T, dsh), F32), V((T, 2 * LANES), F32), V((2, 2, T, LANES), F32), V((T, LANES), F32),
               V((2, 2, half, dsh), F32), V((2, half, dsh), F32), V((4 * rows, dsh), BF16),
               DMA((3,)), DMA((2, tiles)), DMA((3,)), DMA((3,)), DMA((2,)), DMA((2,)), DMA((4,)), DMA((4,)), DMA((6,)), DMA((6,)), DMA((6,)), DMA((6,)),
               DMA((2, 2)), DMA((1,)), DMA((2, 2)), DMA((4,)), DMA((4,)), pltpu.SemaphoreType.REGULAR]
    specs = [ANY, ANY, pl.BlockSpec(memory_space=pltpu.VMEM)] + [ANY] * 3
    return comm_call(forward_kernel, f'forward_{T}', cid, outs, specs, scratch)(act, cot, slot, w_gate, w_in, w_out)


def backward_call(cid, sel, slot, w_gate, w_in, w_out, a_s, b_s, ho_s, r_s):
    T, dmod = sel.shape
    _, dsh, dff = w_gate.shape
    cols = dff // 4
    tiles = cols // LANES
    chunks = (tiles + 1) // 2
    pad = -(-(T // 2) // LANES) * LANES
    slots = 2 if T <= 640 else 1
    ab_slots = 2 if T <= 832 else 1
    outs = [((2, T, dff), BF16), ((2, T, dff), BF16), ((2, T, dmod), BF16), ((slot.shape[1] // 4, dmod), BF16)]
    V = pltpu.VMEM
    scratch = [V((slots, 2, dsh, dff), BF16), V((cols, dmod), BF16), V((3, 4, T, dsh), BF16), V((2, 4, T, cols), BF16),
               V((ab_slots, 2, tiles, T // 2, LANES), F32), V((T, dsh), F32), V((2, T, dsh), BF16), V((2, T, LANES), F32), V((2, pad, LANES), F32), V((2, 4, 8, pad), F32), V((4, slot.shape[1] // 4, dsh), BF16), V((T, slot.shape[1] // 4), BF16),
               DMA((2, 2, 2, chunks)), DMA((2, 2, 2, chunks)), DMA((2, 2, chunks)), DMA((2, 2, chunks)), DMA((2, 6)), DMA((2, 6)), DMA((2, 4)), DMA((2, 4)),
               DMA((2, 3)), DMA((2, 3)), DMA((4,)), DMA((4,)), DMA((3, 2)), DMA((2, 2)), DMA((2,)), DMA((2, 4)), DMA((2, 2, 4)), DMA((2,))]
    return comm_call(backward_kernel, f'backward_{T}', cid, outs, [ANY, pl.BlockSpec(memory_space=pltpu.VMEM)] + [ANY] * 7, scratch)(sel, slot, w_gate, w_in, w_out, a_s, b_s, ho_s, r_s)


def solution(mesh, buckets=BUCKETS):
    act_spec = P(None, 'data')
    weight_spec = P('stage', None, 'data', None)

    def local_step(act_in, cot_out, seq_lens, w_gate, w_in, w_out):
        n_micro, n_rows, seq_len, dmod = act_in.shape
        rows = n_micro * n_rows * seq_len
        w_gate, w_in, w_out = w_gate[0], w_in[0], w_out[0]
        act, cot = act_in.reshape(rows, dmod), cot_out.reshape(rows, dmod)
        slot, which = lens_call(seq_lens.reshape(n_micro), rows, buckets)

        def branch(which, T):
            def run(_):
                sel, a_s, b_s, u_s, ho_s, no_s, r_s, _ = forward_call(1 + 2 * which, T, act, cot, slot, w_gate, w_in, w_out)
                da, db, e_o, act_grad = backward_call(2 + 2 * which, sel, slot, w_gate, w_in, w_out, a_s, b_s, ho_s, r_s)
                gate_grad, in_grad, out_grad, act_grad = grads_call(no_s, u_s, da, db, e_o, act_grad)
                return act_grad.reshape(act_in.shape), gate_grad[None], in_grad[None], out_grad[None]
            return run
        if len(buckets) == 1:
            return branch(0, buckets[0])(0)
        return lax.switch(which[0], [branch(i, b) for i, b in enumerate(buckets)], 0)

    return jax.shard_map(local_step, mesh=mesh, in_specs=(act_spec, act_spec, act_spec, weight_spec, weight_spec, weight_spec), out_specs=(act_spec, weight_spec, weight_spec, weight_spec), check_vma=False)
```

```python
import functools

import jax
import jax.numpy as jnp
from jax import lax
from jax.experimental import pallas as pl
from jax.experimental.pallas import tpu as pltpu
from jax.sharding import PartitionSpec as P

EPSILON = 1e-6
MESH = pl.DeviceIdType.MESH
BF16, F32 = jnp.bfloat16, jnp.float32
LANES = 128
VMEM_LIMIT = 67043328
BUCKETS = (448, 480, 512, 544, 608, 992)


def nt_dot(left, right):
    return lax.dot_general(left, right, (((1,), (1,)), ((), ())), preferred_element_type=F32)


def place():
    d = lax.axis_index('data')
    s = lax.axis_index('stage')
    x = lax.rem(d, 2)
    y = lax.div(d, 2)
    return d, s, 2 * y + 1 - x, 2 * (1 - y) + x, 3 - d


def meet(same_core=False):
    d, s, xn, yn, dg = place()
    barrier = pltpu.get_barrier_semaphore()
    peers = [(xn, s), (yn, s), (dg, s)]
    if not same_core:
        peers += [(xn, 1 - s), (yn, 1 - s), (dg, 1 - s), (d, 1 - s)]
    for chip, core in peers:
        pl.semaphore_signal(barrier, inc=1, device_id=(chip, core), device_id_type=MESH)
    pl.semaphore_wait(barrier, len(peers))


def remote(src, dst, send_sem, recv_sem, device):
    return pltpu.make_async_remote_copy(src_ref=src, dst_ref=dst, send_sem=send_sem, recv_sem=recv_sem, device_id=device, device_id_type=MESH)


def lens_kernel(sizes, lens, slot, which, mine, everyone, ss, rs):
    d, s, xn, yn, dg = place()
    meet(same_core=True)
    seqs, tokens = lens.shape[0], mine.shape[0] * LANES
    each = tokens // seqs
    index = lax.broadcasted_iota(jnp.int32, mine.shape, 0) * LANES + lax.broadcasted_iota(jnp.int32, mine.shape, 1)
    length = jnp.zeros(mine.shape, jnp.int32)
    for i in range(seqs):
        length = jnp.where((index >= i * each) & (index < (i + 1) * each), lens[i], length)
    mine[...] = jnp.where(lax.rem(index, each) < length, 1, 0)
    everyone[d] = mine[...]
    sends = [remote(mine, everyone.at[d], ss.at[i], rs.at[i], (chip, s)) for i, chip in enumerate((xn, yn, dg))]
    for copy in sends:
        copy.start()
    for copy in sends:
        copy.wait()
    rows = 4 * mine.shape[0]
    live = everyone[...].reshape(rows, LANES)
    lane, row = lax.broadcasted_iota(jnp.int32, live.shape, 1), lax.broadcasted_iota(jnp.int32, live.shape, 0)
    upto = live
    shift = 1
    while shift < LANES:
        upto = upto + jnp.where(lane >= shift, pltpu.roll(upto, shift, 1), 0)
        shift *= 2
    whole = jnp.broadcast_to(jnp.sum(live, axis=1, keepdims=True), live.shape)
    before = whole
    shift = 1
    while shift < rows:
        before = before + jnp.where(row >= shift, pltpu.roll(before, shift, 0), 0)
        shift *= 2
    place_of = jnp.where(live > 0, before - whole + upto - 1, -1)
    for i in range(rows):
        slot[:, i * LANES:(i + 1) * LANES] = place_of[i:i + 1, :]
    total = jnp.sum(live)
    which[0] = sum((total > size).astype(jnp.int32) for size in sizes[:-1]) if len(sizes) > 1 else 0


def share_rows(buf, d, s, xn, yn, ss, rs, lo, hi):
    def own(part, i):
        return [remote(buf.at[d, part], buf.at[d, part], ss.at[2 * i + n], rs.at[2 * i + n], (chip, s)) for n, chip in enumerate((xn, yn))]

    fwd_y = remote(buf.at[xn, lo], buf.at[xn, lo], ss.at[4], rs.at[4], (yn, s))
    fwd_x = remote(buf.at[yn, hi], buf.at[yn, hi], ss.at[5], rs.at[5], (xn, s))
    return own(lo, 0), own(hi, 1), fwd_y, fwd_x


def near_share(share):
    own_lo, own_hi, fwd_y, fwd_x = share
    own_lo[0].wait_recv()
    fwd_y.start()
    own_hi[1].wait_recv()
    fwd_x.start()


def far_share(share):
    own_lo, own_hi, fwd_y, fwd_x = share
    own_hi[0].wait_recv()
    own_lo[1].wait_recv()
    fwd_y.wait_recv()
    fwd_x.wait_recv()
    for copy in own_lo + own_hi + [fwd_y, fwd_x]:
        copy.wait_send()


def forward_kernel(act, cot, slot, w_gate, w_in, w_out,
                   sel_o, a_s, b_s, u_s, ho_s, no_s, r_s, other,
                   wv, wov, hb, nb, ub, zp, acc, ab, rv, near_in, far_in, inpv,
                   wss, wrs, iss, irs, xss, xrs, hss, hrs, ass, ars, zss, zrs, lw, lo, lab, lsv, lin, go):
    d, s, xn, yn, dg = place()
    T = nb.shape[0]
    half = T // 2
    piece = T if T <= 512 else half
    cols = ub.shape[1]
    tiles = cols // LANES
    dm = hb.shape[3]
    rows_in = act.shape[0]
    lo_rows, hi_rows = pl.ds(0, half), pl.ds(half, half)
    chips = (dg, xn, yn)
    early_tiles, held_tiles = (1, 2) if T <= 448 else (3, 3) if T <= 480 else (4, 3)

    def block_of(chip):
        return pl.ds(pl.multiple_of(chip * dm, dm), dm)

    def input_rows(chip):
        return pl.ds(pl.multiple_of(chip * rows_in, LANES), rows_in)

    def own_loads(j):
        return [pltpu.make_async_copy(w.at[j, :, pl.ds(pl.multiple_of(d * cols, LANES), cols)], wv.at[j, m, block_of(d)], lw.at[j, m])
                for m, w in enumerate((w_gate, w_in))]

    def start_weights(layer, src, core, sem, first, last):
        def body(k, carry):
            col = pl.ds(pl.multiple_of(k * LANES, LANES), LANES)
            for chip in chips:
                from_col = pl.ds(pl.multiple_of(chip * cols + k * LANES, LANES), LANES)
                for m in range(2):
                    remote(src[m].at[:, from_col], wv.at[layer, m, block_of(d), col], wss.at[sem], wrs.at[layer, k], (chip, core)).start()
            return carry
        lax.fori_loop(first, last, body, 0)

    def wait_sent(sem, count):
        sent = wv.at[0, :, pl.ds(0, 3 * dm), pl.ds(0, count * LANES)]
        pltpu.make_async_copy(sent, sent, wss.at[sem]).wait()

    def wait_tile(layer, k, col):
        came = wv.at[layer, :, pl.ds(0, 3 * dm), col]
        pltpu.make_async_copy(came, came, wrs.at[layer, k]).wait()

    other_pair = (other.at[0], other.at[1])
    first_pair = (w_gate.at[0], w_in.at[0])

    def input_sends(src):
        return [remote(src.at[:, block_of(chip)], inpv.at[input_rows(d)], iss.at[i], irs.at[i], (chip, s)) for i, chip in enumerate(chips)]

    def own_input(src):
        return pltpu.make_async_copy(src.at[:, block_of(d)], inpv.at[input_rows(d)], lin.at[0])
    share = share_rows(hb.at[s], d, s, xn, yn, ass, ars, lo_rows, hi_rows)

    def first_weights(first, last):
        @pl.when(s == 0)
        def _():
            start_weights(0, first_pair, 0, 0, first, last)
    meet()
    for n, src in enumerate((act, cot)):
        @pl.when(s == n)
        def _():
            for copy in input_sends(src) + [own_input(src)]:
                copy.start()
    swaps = [remote(w.at[1], other.at[m], xss.at[m], xrs.at[m], (d, 1 - s)) for m, w in enumerate((w_gate, w_in))]
    for copy in own_loads(0) + own_loads(1) + swaps:
        copy.start()
    pltpu.make_async_copy(w_out.at[0], wov, lo.at[0]).start()
    tokens = slot.shape[1]

    def pick_body(i, carry):
        base = pl.multiple_of(lax.div(i, 2) * half, 16)
        pick = (lax.broadcasted_iota(jnp.int32, (half, tokens), 0) + base == slot[...]).astype(BF16)
        lane = pl.ds(pl.multiple_of(lax.rem(i, 2) * (dm // 2), LANES), dm // 2)
        hb[s, d, pl.ds(base, half), lane] = jnp.dot(pick, inpv[:, lane], preferred_element_type=F32).astype(BF16)
        return carry

    def opening(q, carry):
        @pl.when(q == 1)
        def _():
            for copy in input_sends(act):
                copy.wait()
            own_input(act).wait()
            lax.fori_loop(0, 4, pick_body, 0)
            for copy in share[0] + share[1]:
                copy.start()

        @pl.when(q == 2)
        def _():
            near_share(share)
        first_weights(3 * q, 3 * q + 3 + lax.div(q, 2) * (tiles - 9))
        return carry
    lax.fori_loop(0, 3, opening, 0)
    far_share(share)
    for copy in swaps:
        copy.wait()

    def hand_over():
        return [remote(hb.at[0, c], hb.at[0, c], hss.at[i], hrs.at[i], (d, 1 - s)) for i, c in enumerate((d, xn, yn, dg))]

    @pl.when(s == 1)
    def _():
        top = [pltpu.make_async_copy(hb.at[1, c], sel_o.at[:, pl.ds(c * dm, dm)], lin.at[c]) for c in range(4)]
        for copy in top:
            copy.start()
        pl.semaphore_wait(go, 1)
        start_weights(1, other_pair, 0, 0, 0, tiles)

        def own_layers(q, carry):
            start_weights(q, (w_gate.at[q], w_in.at[q]), 1, 1 + q, 0, tiles - q * (tiles - early_tiles))
            return carry
        lax.fori_loop(0, 2, own_layers, 0)
        for copy in top:
            copy.wait()
        for copy in hand_over():
            copy.wait_recv()

    def layer(j, carry):
        nxt = 1 - j
        step = 32

        def norm_body(i, carry):
            rows = pl.ds(pl.multiple_of(i * step, step), step)
            blocks = [hb[j, c, rows, :].astype(F32) for c in range(4)]
            total = sum(jnp.sum(b * b, axis=-1, keepdims=True) for b in blocks)
            inv = lax.rsqrt(total * (1.0 / (4 * dm)) + EPSILON)
            for c in range(4):
                nb[rows, c * dm:(c + 1) * dm] = (blocks[c] * inv).astype(BF16)
            rv[rows, :] = jnp.broadcast_to(inv, (step, LANES))
            return carry
        lax.fori_loop(0, T // step, norm_body, 0)
        saves = [
            pltpu.make_async_copy(hb.at[j, d], ho_s.at[j], lsv.at[0]),
            pltpu.make_async_copy(nb.at[:, block_of(d)], no_s.at[j], lsv.at[1]),
            pltpu.make_async_copy(rv, r_s.at[j], lsv.at[2]),
        ]
        for copy in saves:
            copy.start()
        for copy in own_loads(j):
            copy.wait()

        def ab_copies(k, side):
            return [pltpu.make_async_copy(ab.at[side, 0], a_s.at[j, k], lab.at[side, 0]),
                    pltpu.make_async_copy(ab.at[side, 1], b_s.at[j, k], lab.at[side, 1])]

        def ab_body(k, carry):
            col = pl.ds(pl.multiple_of(k * LANES, LANES), LANES)
            wait_tile(j, k, col)

            @pl.when((j == 0) & (s == 0) & (k == tiles - 2))
            def _():
                pl.semaphore_signal(go, inc=1, device_id=(d, 1), device_id_type=MESH)

            def ab_rows(i, carry):
                rows = pl.ds(pl.multiple_of(i * piece, 16), piece)
                acc[rows, :] = jnp.dot(nb[rows, :], jnp.concatenate([wv[j, 0, :, col], wv[j, 1, :, col]], axis=1), preferred_element_type=F32)
                return carry
            lax.fori_loop(0, T // piece, ab_rows, 0)
            side = lax.rem(k, 2)

            @pl.when(k >= 2)
            def _():
                for copy in ab_copies(k, side):
                    copy.wait()
            a, b = acc[:, :LANES], acc[:, LANES:]
            ab[side, 0] = a
            ab[side, 1] = b
            ub[:, col] = (a * jax.nn.sigmoid(a) * b).astype(BF16)
            for copy in ab_copies(k, side):
                copy.start()
            return carry
        lax.fori_loop(0, tiles, ab_body, 0)
        for k in (tiles - 2, tiles - 1):
            for copy in ab_copies(k, k % 2):
                copy.wait()
        save_u = pltpu.make_async_copy(ub, u_s.at[j], lsv.at[3])
        save_u.start()

        @pl.when((j == 0) | (s == 0))
        def _():
            pltpu.make_async_copy(w_out.at[j], wov, lo.at[0]).wait()

            def send(i, c, rows, dst, chip):
                return remote(zp.at[c, rows], dst, zss.at[i], zrs.at[i], (chip, s))
            first = [send(0, dg, lo_rows, near_in.at[0, 0], xn), send(1, dg, hi_rows, near_in.at[1, 0], yn)]
            second = [send(2, xn, lo_rows, near_in.at[0, 1], xn), send(3, yn, hi_rows, near_in.at[1, 1], yn)]
            third = [send(4, yn, lo_rows, far_in.at[0], yn), send(5, xn, hi_rows, far_in.at[1], xn)]
            x, y = lax.rem(d, 2), lax.div(d, 2)
            wide = 2 * LANES

            def block_body(i, carry):
                rel, part_of = 3 - lax.div(i, 2), lax.rem(i, 2)
                c = 2 * lax.rem(y + lax.rem(rel, 2), 2) + lax.rem(x + lax.div(rel, 2), 2)

                def zp_rows(n, carry):
                    rows = pl.ds(pl.multiple_of(n * half, 16), half)
                    zp[c, rows, pl.ds(pl.multiple_of(part_of * wide, wide), wide)] = jnp.dot(
                        ub[rows, :], wov[:, pl.ds(pl.multiple_of(c * dm + part_of * wide, wide), wide)], preferred_element_type=F32)
                    return carry
                lax.fori_loop(0, 2, zp_rows, 0)
                for at, copies in ((1, first), (3, second[:1]), (5, second[1:])):
                    @pl.when(i == at)
                    def _():
                        for copy in copies:
                            copy.start()
                return carry
            lax.fori_loop(0, 8, block_body, 0)
            share = share_rows(hb.at[nxt], d, s, xn, yn, ass, ars, lo_rows, hi_rows)

            def both(n, stage):
                for at in range(2):
                    @pl.when(n == at)
                    def _():
                        stage(at)

            def half_rows(n):
                return pl.ds(pl.multiple_of(n * half, 16), half)

            def relay(n, carry):
                both(n, lambda at: first[at].wait_recv())
                c, rows = yn + n * (xn - yn), half_rows(n)
                zp[c, rows, :] += near_in[n, 0]
                both(n, lambda at: third[at].start())
                return carry
            lax.fori_loop(0, 2, relay, 0)

            def settle(n, carry):
                both(n, lambda at: (second[at].wait_recv(), third[at].wait_recv()))
                rows = half_rows(n)
                branch = (zp[d, rows, :] + near_in[n, 1] + far_in[n]).astype(BF16).astype(F32)
                hb[nxt, d, rows, :] = (hb[j, d, rows, :].astype(F32) + branch).astype(BF16)
                both(n, lambda at: [copy.start() for copy in share[at]])
                return carry
            lax.fori_loop(0, 2, settle, 0)
            near_share(share)

            @pl.when((j == 0) & (s == 1))
            def _():
                pl.semaphore_signal(go, inc=1, device_id=(d, 0), device_id_type=MESH)
            far_share(share)
            for copy in first + second + third:
                copy.wait_send()

        @pl.when((j == 0) & (s == 0))
        def _():
            pltpu.make_async_copy(w_out.at[1], wov, lo.at[0]).start()

        @pl.when((j == 1) & (s == 0))
        def _():
            hands = hand_over()
            for copy in hands:
                copy.start()

            def last_layer(q, carry):
                @pl.when(q == 1)
                def _():
                    pl.semaphore_wait(go, 1)
                start_weights(1, other_pair, 1, 1, early_tiles + q * (tiles - held_tiles - early_tiles), tiles - held_tiles + q * held_tiles)
                return carry
            lax.fori_loop(0, 2, last_layer, 0)
            for copy in hands:
                copy.wait_send()
        for copy in saves:
            copy.wait()
        save_u.wait()
        return carry
    lax.fori_loop(0, 2, layer, 0)
    wait_sent(0, tiles)

    @pl.when(s == 0)
    def _():
        wait_sent(1, tiles - early_tiles)

    @pl.when(s == 1)
    def _():
        wait_sent(1, tiles)
        wait_sent(2, early_tiles)


def backward_kernel(sel, slot, w_gate, w_in, w_out, a_s, b_s, ho_s, r_s,
                    da_o, db_o, e_o, act_o,
                    wgv, wov, eb, daf, ab, dn, hov, rv, sq, sv, agv, back_v,
                    dss, drs, fss, frs, ess, ers, hss, hrs, sss, srs, ass, ars, lw, lab, lout, lh, le, lsm):
    d, s, xn, yn, dg = place()
    T = sel.shape[0]
    part_rows = T // 2
    lo_n = -(-part_rows // 32) * 16
    cols = daf.shape[3]
    dm = dn.shape[1]
    wide = 2 * LANES
    n_full = cols // wide
    tail = cols - n_full * wide
    n_early = n_full // 2
    n_mid = n_early + 2
    splits, one_loop = (1 if T <= 640 else 2), T > 512
    pad = sq.shape[1]
    w_slots = wgv.shape[0]
    ab_slots = ab.shape[0]

    def wo_load(j):
        return pltpu.make_async_copy(w_out.at[j], wov, lw.at[0, 0])

    def slot_of(j, n):
        return j if n == 2 else 0

    def gate_loads(j):
        return [pltpu.make_async_copy(w.at[j], wgv.at[slot_of(j, w_slots), m], lw.at[1 + slot_of(j, w_slots), m]) for m, w in enumerate((w_gate, w_in))]

    def rows_of(g, base=0, size=part_rows):
        return pl.ds(pl.multiple_of(g * part_rows + base, 16), size)

    def in_copies(g):
        return [pltpu.make_async_copy(sel.at[rows_of(g), pl.ds(c * dm, dm)], eb.at[2, c, rows_of(g)], lh.at[g, c]) for c in range(4)]

    def hand_over(g):
        return [remote(eb.at[0, c, rows_of(g)], eb.at[2, c, rows_of(g)], hss.at[g, i], hrs.at[g, i], (d, 1 - s)) for i, c in enumerate((d, xn, yn, dg))]

    def ab_loads(j, g):
        side = slot_of(g, ab_slots)
        return [pltpu.make_async_copy(src.at[j, :, rows_of(g)], ab.at[side, m], lab.at[side, m]) for m, src in enumerate((a_s, b_s))]

    @pl.when(s == 1)
    def _():
        for copy in in_copies(0):
            copy.start()
    wo_load(1).start()
    small = [pltpu.make_async_copy(ho_s, hov, lsm.at[0]), pltpu.make_async_copy(r_s, rv, lsm.at[1])]
    for copy in ab_loads(1, 0):
        copy.start()
    meet()

    def columns(c, width):
        return pl.ds(pl.multiple_of(c * wide, LANES), width)

    def each_chunk(body, first=0, last=n_full):
        lax.fori_loop(first, last, lambda c, carry: (body(c, wide), carry)[1], 0)

    class Piece:
        def __init__(self, j, g):
            self.j, self.g, self.rows = j, g, rows_of(g)
            parts = (rows_of(g, 0, lo_n), rows_of(g, lo_n, part_rows - lo_n))
            self.share = share_rows(eb.at[j], d, s, xn, yn, ess.at[g], ers.at[g], *parts)
            self.e_saves = [pltpu.make_async_copy(eb.at[j + 1, c, self.rows], e_o.at[j, self.rows, pl.ds(c * dm, dm)], le.at[j, g, c]) for c in range(4)]
            self.sums = [remote(sv.at[g, 0], sv.at[g, 1 + i], sss.at[g, i], srs.at[g, i], (chip, s)) for i, chip in enumerate((xn, yn, dg))]

        def own_sends(self, c, col):
            g, out = self.g, []
            for m in range(2):
                for n, chip in enumerate((xn, yn)):
                    here = daf.at[m, d, self.rows, col]
                    out.append(remote(here, here, dss.at[g, m, n, c], drs.at[g, m, n, c], (chip, s)))
            return out

        def forwards(self, c, col):
            g = self.g
            from_x, from_y = daf.at[0, xn, self.rows, col], daf.at[1, yn, self.rows, col]
            return [remote(from_x, from_x, fss.at[g, 1, c], frs.at[g, 1, c], (yn, s)), remote(from_y, from_y, fss.at[g, 0, c], frs.at[g, 0, c], (xn, s))]

        def make(self):
            j, g, rows, side = self.j, self.g, self.rows, slot_of(self.g, ab_slots)
            for copy in self.e_saves:
                copy.start()

            @pl.when(g == 0)
            def _():
                wo_load(j).wait()
            for copy in ab_loads(j, g):
                copy.wait()

            @pl.when((j == 1) & (g == 0))
            def _():
                if ab_slots == 2:
                    for copy in ab_loads(1, 1):
                        copy.start()

                @pl.when(s == 1)
                def _():
                    for copy in in_copies(1):
                        copy.start()
                for copy in gate_loads(1) + small:
                    copy.start()
            if w_slots == 2:
                @pl.when((j == 1) & (g == 1))
                def _():
                    for copy in gate_loads(0):
                        copy.start()

            def tile(c, width=wide):
                base = jnp.minimum(c * wide, cols - wide) if one_loop else c * wide
                def du(blocks, lanes):
                    e_part = jnp.concatenate([eb[j + 1, n, rows, :] for n in blocks], axis=1)
                    return nt_dot(e_part, wov[pl.ds(pl.multiple_of(base, LANES), width), lanes])
                if splits == 1:
                    dn[rows, :width] = du(range(4), slice(None))
                else:
                    dn[rows, :width] = jnp.zeros((part_rows, width), F32)

                    def du_part(n, carry):
                        dn[rows, :width] += du((2 * n, 2 * n + 1), pl.ds(pl.multiple_of(n * 2 * dm, dm), 2 * dm))
                        return carry
                    lax.fori_loop(0, 2, du_part, 0)
                def lanes(n):
                    lane = pl.ds(pl.multiple_of(base + n * LANES, LANES), LANES)
                    at = lax.div(base, LANES) + n
                    a, b, du = ab[side, 0, at], ab[side, 1, at], dn[rows, n * LANES:(n + 1) * LANES]
                    sig = jax.nn.sigmoid(a)
                    daf[0, d, rows, lane] = (du * b * sig * (1.0 + a * (1.0 - sig))).astype(BF16)
                    daf[1, d, rows, lane] = (du * (a * sig)).astype(BF16)

                if one_loop:
                    @pl.when(c < n_full)
                    def _():
                        lanes(0)
                    lanes(1)
                else:
                    for n in range(width // LANES):
                        lanes(n)

            def body(c, width):
                tile(c, wide)

                @pl.when(c < n_early)
                def _():
                    for copy in self.own_sends(c, columns(c, wide)):
                        copy.start()
            each_chunk(body, 0, n_full + 1 if one_loop else n_full)
            if not one_loop:
                tile(n_full, tail)

        def send(self, first, last):
            def body(c, width):
                for copy in self.own_sends(c, columns(c, width)):
                    copy.start()
            each_chunk(body, first, last)

        def save_tile(self, m, chip, col, c, width):
            dst = (da_o, db_o)[m].at[self.j, self.rows, pl.ds(pl.multiple_of(chip * cols + c * wide, LANES), width)]
            pltpu.make_async_copy(daf.at[m, chip, self.rows, col], dst, lout.at[self.g]).start()

        def add(self, chip, c, width):
            def body(i, carry):
                m, at = lax.div(i, splits), pl.ds(pl.multiple_of(lax.rem(i, splits) * (dm // splits), LANES), dm // splits)
                w = wgv[slot_of(self.j, w_slots), m, at, pl.ds(pl.multiple_of(chip * cols + c * wide, LANES), width)]
                dn[self.rows, at] += nt_dot(daf[m, chip, self.rows, columns(c, width)], w)
                return carry
            lax.fori_loop(0, 2 * splits, body, 0)

        def own(self):
            @pl.when(self.g == 0)
            def _():
                for copy in gate_loads(self.j):
                    copy.wait()
            for m in range(2):
                self.save_tile(m, d, pl.ds(0, cols), 0, cols)
            dn[self.rows, :] = jnp.zeros((part_rows, dm), F32)
            each_chunk(lambda c, width: self.add(d, c, width))
            self.add(d, n_full, tail)

        def near(self, c, width):
            col = columns(c, width)
            fwd_y, fwd_x = self.forwards(c, col)

            def came(m, n, chip):
                there = daf.at[m, chip, self.rows, col]
                remote(there, there, dss.at[self.g, m, n, c], drs.at[self.g, m, n, c], (chip, s)).wait_recv()
            came(0, 0, xn)
            fwd_y.start()
            came(1, 1, yn)
            fwd_x.start()
            came(1, 0, xn)
            came(0, 1, yn)
            for chip in (xn, yn):
                for m in range(2):
                    self.save_tile(m, chip, col, c, width)
            lax.fori_loop(0, 2, lambda i, carry: (self.add(xn + i * (yn - xn), c, width), carry)[1], 0)

        def far(self):
            j, g, rows = self.j, self.g, self.rows

            def body(c, width):
                col = columns(c, width)
                there = [daf.at[m, dg, rows, col] for m in range(2)]
                remote(there[0], there[0], fss.at[g, 1, c], frs.at[g, 1, c], (yn, s)).wait_recv()
                remote(there[1], there[1], fss.at[g, 0, c], frs.at[g, 0, c], (xn, s)).wait_recv()
                for m in range(2):
                    self.save_tile(m, dg, col, c, width)
                self.add(dg, c, width)
            each_chunk(body)
            body(n_full, tail)

            @pl.when((j == 1) & (g == 0))
            def _():
                for copy in small:
                    copy.wait()
            prod = dn[rows, :] * hov[j, rows, :].astype(F32)
            sq[g, :part_rows, :] = (prod[:, :LANES] + prod[:, LANES:2 * LANES]) + (prod[:, 2 * LANES:3 * LANES] + prod[:, 3 * LANES:])
            sv[g, 0] = jnp.broadcast_to(jnp.sum(sq[g].T, axis=0, keepdims=True), (8, pad))
            for copy in self.sums:
                copy.start()
            if w_slots == 1:
                @pl.when((j == 1) & (g == 1))
                def _():
                    for copy in gate_loads(0):
                        copy.start()

        def finish(self):
            j, g = self.j, self.g
            whole = daf.at[:, :, self.rows]
            pltpu.make_async_copy(whole, whole, lout.at[g]).wait()

            def drain(c, width):
                col = columns(c, width)
                for copy in self.own_sends(c, col) + self.forwards(c, col):
                    copy.wait_send()
            each_chunk(drain)
            drain(n_full, tail)
            for copy in self.sums:
                copy.wait()
            mean = ((sv[g, 0, 0:1, :] + sv[g, 1, 0:1, :]) + (sv[g, 2, 0:1, :] + sv[g, 3, 0:1, :])) * (1.0 / (4 * dm))
            sq[g] = jnp.broadcast_to(mean, (LANES, pad)).T
            for n, (base, size) in enumerate(((0, lo_n), (lo_n, part_rows - lo_n))):
                at = rows_of(g, base, size)
                inv, avg = rv[j, at, :], sq[g, base:base + size, :]
                for c in range(4):
                    lane = slice(c * LANES, (c + 1) * LANES)
                    resid = inv * dn[at, lane] - hov[j, at, lane].astype(F32) * (inv * inv * inv) * avg
                    eb[j, d, at, lane] = (eb[j + 1, d, at, lane].astype(F32) + resid).astype(BF16)
                for copy in self.share[n]:
                    copy.start()

    def give(g):
        own_lo, own_hi, fwd_y, fwd_x = Piece(0, g).share
        for copy, came in zip(hand_over(g), ((), (own_hi[0],), (own_lo[1],), (fwd_y, fwd_x))):
            for part in came:
                part.wait_recv()
            copy.start()
        for copy in own_lo + own_hi + [fwd_y, fwd_x]:
            copy.wait_send()

    def step(i, carry):
        g = lax.rem(i, 2)
        cur = Piece(1 - lax.div(i, 2), g)
        prev = Piece(1 - lax.div(i - 1, 2), 1 - g)
        live, later = i < 4, i > 0

        ending = (i == 4) & (s == 1)

        @pl.when(ending)
        def _():
            give(0)

        @pl.when((i >= 2) & jnp.logical_not(ending))
        def _():
            far_share(Piece(1 - lax.div(i - 2, 2), g).share)

        @pl.when(live)
        def _():
            @pl.when((i < 2) & (s == 0))
            def _():
                for copy in hand_over(g):
                    copy.wait_recv()

            @pl.when((i < 2) & (s == 1))
            def _():
                for copy in in_copies(g):
                    copy.wait()

            cur.make()

            @pl.when(i == 1)
            def _():
                wo_load(0).start()
            coming = i + ab_slots

            @pl.when(coming < 4)
            def _():
                for copy in ab_loads(1 - lax.div(coming, 2), lax.rem(coming, 2)):
                    copy.start()

        @pl.when(later)
        def _():
            prev.far()

        def halves(h, carry):
            @pl.when(live)
            def _():
                cur.send(n_early + h * (n_mid - n_early), n_mid + h * (n_full - n_mid))

            @pl.when(live & (h == 0))
            def _():
                cur.own()

            @pl.when(live & (h == 1))
            def _():
                for copy in cur.own_sends(n_full, columns(n_full, tail)):
                    copy.start()

            @pl.when(later & (h == 1))
            def _():
                near_share(prev.share)

            @pl.when(live & (h == 1))
            def _():
                each_chunk(cur.near)

            @pl.when(later & (h == 0))
            def _():
                prev.finish()
            return carry
        lax.fori_loop(0, 2, halves, 0)

        @pl.when(live)
        def _():
            cur.near(n_full, tail)
        return carry
    lax.fori_loop(0, 5, step, 0)

    def act_copies(i, c):
        col = pl.ds(pl.multiple_of(c * dm, dm), dm)
        return remote(agv.at[c], act_o.at[:, col], ass.at[i], ars.at[i], (d, 1 - s)), pltpu.make_async_copy(agv.at[c], act_o.at[:, col], lh.at[0, i])

    @pl.when(s == 1)
    def _():
        give(1)
        for i, c in enumerate((d, xn, yn, dg)):
            act_copies(i, c)[0].wait_recv()

    @pl.when(s == 0)
    def _():
        own_lo, own_hi, fwd_y, fwd_x = Piece(0, 1).share
        rows_out = agv.shape[1]
        own_slots = slot[:, pl.ds(pl.multiple_of(d * rows_out, LANES), rows_out)]
        back = (lax.broadcasted_iota(jnp.int32, (T, rows_out), 0) == own_slots).astype(BF16)
        back_v[...] = back
        came = ((), (own_hi[0],), (own_lo[1],), (fwd_y, fwd_x))
        x, y = lax.rem(d, 2), lax.div(d, 2)

        def spread(i, carry):
            for n in range(1, 4):
                @pl.when(i == n)
                def _():
                    for copy in came[n]:
                        copy.wait_recv()
            c = 2 * lax.rem(y + lax.div(i, 2), 2) + lax.rem(x + lax.rem(i, 2), 2)
            agv[c] = lax.dot_general(back_v[...], eb[0, c], (((0,), (0,)), ((), ())), preferred_element_type=F32).astype(BF16)
            for copy in act_copies(i, c):
                copy.start()
            return carry
        lax.fori_loop(0, 4, spread, 0)
        for copy in own_lo + own_hi + [fwd_y, fwd_x]:
            copy.wait_send()
        for i, c in enumerate((d, xn, yn, dg)):
            away, here = act_copies(i, c)
            away.wait_send()
            here.wait()
    def saved(i, carry):
        for copy in Piece(lax.div(i, 2), lax.rem(i, 2)).e_saves:
            copy.wait()
        return carry
    lax.fori_loop(0, 4, saved, 0)

    @pl.when(s == 1)
    def _():
        for g in range(2):
            for copy in hand_over(g):
                copy.wait_send()


def grads_kernel(no_s, u_s, da, db, e_o, act, gate_o, in_o, out_o, act_o, nv, uv, ev, av, nt, ut, ring, og, oo, ln, lr, lg, lo):
    layers = nv.shape[0]
    wide = ring.shape[3]
    n_gate, n_out = da.shape[2] // wide, e_o.shape[2] // wide
    slots, g_slots, o_slots = ring.shape[0], og.shape[0], oo.shape[0]
    rows = oo.shape[2]
    first_out = layers * n_gate - layers * n_out - 2

    def put(ref, at, value):
        ref[at] = value

    def for_rows(count, body):
        parts = 1 if nv.shape[1] <= 640 else 2
        size = count // parts
        if parts == 1:
            body(pl.ds(0, size))
        else:
            lax.fori_loop(0, parts, lambda i, carry: (body(pl.ds(pl.multiple_of(i * size, 32), size)), carry)[1], 0)

    def flip(src, dst):
        def body(i, carry):
            lane = pl.ds(pl.multiple_of(i * LANES, LANES), LANES)
            dst[lane, :] = src[:, lane].T
            return carry
        lax.fori_loop(0, dst.shape[0] // LANES, body, 0)
    wholes = [pltpu.make_async_copy(src, dst, ln.at[i]) for i, (src, dst) in enumerate(((no_s, nv), (u_s, uv), (e_o, ev), (act, av)))]
    act_store = pltpu.make_async_copy(av, act_o, ln.at[4])

    def tile_at(c):
        return pl.ds(pl.multiple_of(c * wide, wide), wide)

    def loads(t):
        slot = lax.rem(t, slots)
        return [pltpu.make_async_copy(src.at[lax.div(t, n_gate), :, tile_at(lax.rem(t, n_gate))], ring.at[slot, m], lr.at[slot, m]) for m, src in enumerate((da, db))]

    def gate_stores(t):
        slot = lax.rem(t, g_slots)
        return [pltpu.make_async_copy(og.at[slot, m], dst.at[lax.div(t, n_gate), :, tile_at(lax.rem(t, n_gate))], lg.at[slot, m]) for m, dst in enumerate((gate_o, in_o))]

    def out_stores(t):
        slot = lax.rem(t, o_slots)
        return [pltpu.make_async_copy(oo.at[slot, m], out_o.at[lax.div(t, n_out), pl.ds(m * rows, rows), tile_at(lax.rem(t, n_out))], lo.at[slot, m]) for m in range(2)]

    def start(copies):
        for copy in copies:
            copy.start()

    def wait(copies):
        for copy in copies:
            copy.wait()
    wholes[0].start()
    for t in range(slots - 1):
        start(loads(t))
    start(wholes[1:])
    wholes[0].wait()

    def out_tile(t):
        j, c, at = lax.div(t, n_out), lax.rem(t, n_out), lax.rem(t, o_slots)

        @pl.when(c == 0)
        def _():
            flip(uv.at[j], ut)

        @pl.when(t >= o_slots)
        def _():
            wait(out_stores(t - o_slots))

        def half(m, carry):
            for_rows(rows, lambda at_rows: put(oo, (at, m, at_rows), jnp.dot(
                ut[pl.ds(pl.multiple_of(m * rows + at_rows.start, 32), at_rows.size), :], ev[j, :, tile_at(c)], preferred_element_type=F32)))
            return carry
        lax.fori_loop(0, 2, half, 0)
        start(out_stores(t))

    def gate_body(t, carry):
        j, c, slot, at = lax.div(t, n_gate), lax.rem(t, n_gate), lax.rem(t, slots), lax.rem(t, g_slots)

        @pl.when(t + slots - 1 < layers * n_gate)
        def _():
            start(loads(t + slots - 1))

        @pl.when(c == 0)
        def _():
            flip(nv.at[j], nt)
        wait(loads(t))

        @pl.when(t >= g_slots)
        def _():
            wait(gate_stores(t - g_slots))

        def side(m, carry):
            for_rows(og.shape[2], lambda at_rows: put(og, (at, m, at_rows), jnp.dot(nt[at_rows, :], ring[slot, m], preferred_element_type=F32)))
            return carry
        lax.fori_loop(0, 2, side, 0)
        start(gate_stores(t))

        @pl.when(t == first_out)
        def _():
            wait(wholes[1:])
            act_store.start()

        @pl.when((t >= first_out) & (t < first_out + layers * n_out))
        def _():
            out_tile(t - first_out)
        return carry
    lax.fori_loop(0, layers * n_gate, gate_body, 0)
    act_store.wait()
    for t in range(layers * n_gate - g_slots, layers * n_gate):
        wait(gate_stores(t))
    for t in range(layers * n_out - o_slots, layers * n_out):
        wait(out_stores(t))


def grads_call(no_s, u_s, da, db, e_o, act):
    layers, T, dsh = no_s.shape
    cols, dff, dmod = u_s.shape[2], da.shape[2], e_o.shape[2]
    V, wide = pltpu.VMEM, 4 * LANES
    moved = 2 * layers * T * (dsh + cols + 2 * dff + dmod) + 4 * layers * (2 * dsh * dff + cols * dmod)
    return pl.pallas_call(
        grads_kernel, name=f'grads_{T}', in_specs=[ANY] * 6, out_specs=[ANY] * 4,
        out_shape=[jax.ShapeDtypeStruct((layers, dsh, dff), F32), jax.ShapeDtypeStruct((layers, dsh, dff), F32), jax.ShapeDtypeStruct((layers, cols, dmod), F32),
                   jax.ShapeDtypeStruct(act.shape, BF16)],
        scratch_shapes=[V((layers, T, dsh), BF16), V((layers, T, cols), BF16), V((layers, T, dmod), BF16), V(act.shape, BF16), V((dsh, T), BF16), V((cols, T), BF16),
                        V((6, 2, T, wide), BF16), V((4, 2, dsh, wide), F32), V((3, 2, cols // 2, wide), F32), DMA((5,)), DMA((6, 2)), DMA((4, 2)), DMA((3, 2))],
        cost_estimate=pl.CostEstimate(flops=2 * layers * T * (2 * dsh * dff + cols * dmod), bytes_accessed=moved, transcendentals=0),
        compiler_params=pltpu.CompilerParams(vmem_limit_bytes=VMEM_LIMIT))(no_s, u_s, da, db, e_o, act)


ANY = pl.BlockSpec(memory_space=pl.ANY)
DMA = pltpu.SemaphoreType.DMA


def comm_call(kernel, name, cid, outs, in_specs, scratch):
    return pl.pallas_call(
        kernel, name=name, out_shape=[jax.ShapeDtypeStruct(*o) for o in outs], in_specs=in_specs, out_specs=[ANY] * len(outs),
        scratch_shapes=scratch, compiler_params=pltpu.CompilerParams(collective_id=cid, has_side_effects=True, vmem_limit_bytes=VMEM_LIMIT))


def lens_call(lens, tokens, sizes):
    smem, vmem = pl.BlockSpec(memory_space=pltpu.SMEM), pl.BlockSpec(memory_space=pltpu.VMEM)
    rows = tokens // LANES
    return pl.pallas_call(
        functools.partial(lens_kernel, sizes), name='lens', out_shape=[jax.ShapeDtypeStruct((1, 4 * tokens), jnp.int32), jax.ShapeDtypeStruct((1,), jnp.int32)],
        in_specs=[smem], out_specs=[vmem, smem],
        scratch_shapes=[pltpu.VMEM((rows, LANES), jnp.int32), pltpu.VMEM((4, rows, LANES), jnp.int32), DMA((3,)), DMA((3,))],
        compiler_params=pltpu.CompilerParams(collective_id=0, has_side_effects=True))(lens)


def forward_call(cid, T, act, cot, slot, w_gate, w_in, w_out):
    rows, dmod = act.shape
    _, dsh, dff = w_gate.shape
    cols = dff // 4
    half = T // 2
    tiles = cols // LANES
    outs = [((T, dmod), BF16), ((2, tiles, T, LANES), F32), ((2, tiles, T, LANES), F32), ((2, T, cols), BF16),
            ((2, T, dsh), BF16), ((2, T, dsh), BF16), ((2, T, LANES), F32), ((2, dsh, dff), BF16)]
    V = pltpu.VMEM
    scratch = [V((2, 2, dmod, cols), BF16), V((cols, dmod), BF16), V((2, 4, T, dsh), BF16), V((T, dmod), BF16), V((T, cols), BF16),
               V((4, T, dsh), F32), V((T, 2 * LANES), F32), V((2, 2, T, LANES), F32), V((T, LANES), F32),
               V((2, 2, half, dsh), F32), V((2, half, dsh), F32), V((4 * rows, dsh), BF16),
               DMA((3,)), DMA((2, tiles)), DMA((3,)), DMA((3,)), DMA((2,)), DMA((2,)), DMA((4,)), DMA((4,)), DMA((6,)), DMA((6,)), DMA((6,)), DMA((6,)),
               DMA((2, 2)), DMA((1,)), DMA((2, 2)), DMA((4,)), DMA((4,)), pltpu.SemaphoreType.REGULAR]
    specs = [ANY, ANY, pl.BlockSpec(memory_space=pltpu.VMEM)] + [ANY] * 3
    return comm_call(forward_kernel, f'forward_{T}', cid, outs, specs, scratch)(act, cot, slot, w_gate, w_in, w_out)


def backward_call(cid, sel, slot, w_gate, w_in, w_out, a_s, b_s, ho_s, r_s):
    T, dmod = sel.shape
    _, dsh, dff = w_gate.shape
    cols = dff // 4
    tiles = cols // LANES
    chunks = (tiles + 1) // 2
    pad = -(-(T // 2) // LANES) * LANES
    slots = 2 if T <= 640 else 1
    ab_slots = 2 if T <= 832 else 1
    outs = [((2, T, dff), BF16), ((2, T, dff), BF16), ((2, T, dmod), BF16), ((slot.shape[1] // 4, dmod), BF16)]
    V = pltpu.VMEM
    scratch = [V((slots, 2, dsh, dff), BF16), V((cols, dmod), BF16), V((3, 4, T, dsh), BF16), V((2, 4, T, cols), BF16),
               V((ab_slots, 2, tiles, T // 2, LANES), F32), V((T, dsh), F32), V((2, T, dsh), BF16), V((2, T, LANES), F32), V((2, pad, LANES), F32), V((2, 4, 8, pad), F32), V((4, slot.shape[1] // 4, dsh), BF16), V((T, slot.shape[1] // 4), BF16),
               DMA((2, 2, 2, chunks)), DMA((2, 2, 2, chunks)), DMA((2, 2, chunks)), DMA((2, 2, chunks)), DMA((2, 6)), DMA((2, 6)), DMA((2, 4)), DMA((2, 4)),
               DMA((2, 3)), DMA((2, 3)), DMA((4,)), DMA((4,)), DMA((3, 2)), DMA((2, 2)), DMA((2,)), DMA((2, 4)), DMA((2, 2, 4)), DMA((2,))]
    return comm_call(backward_kernel, f'backward_{T}', cid, outs, [ANY, pl.BlockSpec(memory_space=pltpu.VMEM)] + [ANY] * 7, scratch)(sel, slot, w_gate, w_in, w_out, a_s, b_s, ho_s, r_s)


def solution(mesh, buckets=BUCKETS):
    act_spec = P(None, 'data')
    weight_spec = P('stage', None, 'data', None)

    def local_step(act_in, cot_out, seq_lens, w_gate, w_in, w_out):
        n_micro, n_rows, seq_len, dmod = act_in.shape
        rows = n_micro * n_rows * seq_len
        w_gate, w_in, w_out = w_gate[0], w_in[0], w_out[0]
        act, cot = act_in.reshape(rows, dmod), cot_out.reshape(rows, dmod)
        slot, which = lens_call(seq_lens.reshape(n_micro), rows, buckets)

        def branch(which, T):
            def run(_):
                sel, a_s, b_s, u_s, ho_s, no_s, r_s, _ = forward_call(1 + 2 * which, T, act, cot, slot, w_gate, w_in, w_out)
                da, db, e_o, act_grad = backward_call(2 + 2 * which, sel, slot, w_gate, w_in, w_out, a_s, b_s, ho_s, r_s)
                gate_grad, in_grad, out_grad, act_grad = grads_call(no_s, u_s, da, db, e_o, act_grad)
                return act_grad.reshape(act_in.shape), gate_grad[None], in_grad[None], out_grad[None]
            return run
        if len(buckets) == 1:
            return branch(0, buckets[0])(0)
        return lax.switch(which[0], [branch(i, b) for i, b in enumerate(buckets)], 0)

    return jax.shard_map(local_step, mesh=mesh, in_specs=(act_spec, act_spec, act_spec, weight_spec, weight_spec, weight_spec), out_specs=(act_spec, weight_spec, weight_spec, weight_spec), check_vma=False)
```

```python
import functools

import jax
import jax.numpy as jnp
from jax import lax
from jax.experimental import pallas as pl
from jax.experimental.pallas import tpu as pltpu
from jax.sharding import PartitionSpec as P

EPSILON = 1e-6
MESH = pl.DeviceIdType.MESH
BF16, F32 = jnp.bfloat16, jnp.float32
LANES = 128
VMEM_LIMIT = 67043328
BUCKETS = (448, 480, 512, 544, 608, 992)


def nt_dot(left, right):
    return lax.dot_general(left, right, (((1,), (1,)), ((), ())), preferred_element_type=F32)


def place():
    d = lax.axis_index('data')
    s = lax.axis_index('stage')
    x = lax.rem(d, 2)
    y = lax.div(d, 2)
    return d, s, 2 * y + 1 - x, 2 * (1 - y) + x, 3 - d


def meet(same_core=False):
    d, s, xn, yn, dg = place()
    barrier = pltpu.get_barrier_semaphore()
    peers = [(xn, s), (yn, s), (dg, s)]
    if not same_core:
        peers += [(xn, 1 - s), (yn, 1 - s), (dg, 1 - s), (d, 1 - s)]
    for chip, core in peers:
        pl.semaphore_signal(barrier, inc=1, device_id=(chip, core), device_id_type=MESH)
    pl.semaphore_wait(barrier, len(peers))


def remote(src, dst, send_sem, recv_sem, device):
    return pltpu.make_async_remote_copy(src_ref=src, dst_ref=dst, send_sem=send_sem, recv_sem=recv_sem, device_id=device, device_id_type=MESH)


def lens_kernel(sizes, lens, slot, which, mine, everyone, ss, rs):
    d, s, xn, yn, dg = place()
    meet(same_core=True)
    seqs, tokens = lens.shape[0], mine.shape[0] * LANES
    each = tokens // seqs
    index = lax.broadcasted_iota(jnp.int32, mine.shape, 0) * LANES + lax.broadcasted_iota(jnp.int32, mine.shape, 1)
    length = jnp.zeros(mine.shape, jnp.int32)
    for i in range(seqs):
        length = jnp.where((index >= i * each) & (index < (i + 1) * each), lens[i], length)
    mine[...] = jnp.where(lax.rem(index, each) < length, 1, 0)
    everyone[d] = mine[...]
    sends = [remote(mine, everyone.at[d], ss.at[i], rs.at[i], (chip, s)) for i, chip in enumerate((xn, yn, dg))]
    for copy in sends:
        copy.start()
    for copy in sends:
        copy.wait()
    rows = 4 * mine.shape[0]
    live = everyone[...].reshape(rows, LANES)
    lane, row = lax.broadcasted_iota(jnp.int32, live.shape, 1), lax.broadcasted_iota(jnp.int32, live.shape, 0)
    upto = live
    shift = 1
    while shift < LANES:
        upto = upto + jnp.where(lane >= shift, pltpu.roll(upto, shift, 1), 0)
        shift *= 2
    whole = jnp.broadcast_to(jnp.sum(live, axis=1, keepdims=True), live.shape)
    before = whole
    shift = 1
    while shift < rows:
        before = before + jnp.where(row >= shift, pltpu.roll(before, shift, 0), 0)
        shift *= 2
    place_of = jnp.where(live > 0, before - whole + upto - 1, -1)
    for i in range(rows):
        slot[:, i * LANES:(i + 1) * LANES] = place_of[i:i + 1, :]
    total = jnp.sum(live)
    which[0] = sum((total > size).astype(jnp.int32) for size in sizes[:-1]) if len(sizes) > 1 else 0


def share_rows(buf, d, s, xn, yn, ss, rs, lo, hi):
    def own(part, i):
        return [remote(buf.at[d, part], buf.at[d, part], ss.at[2 * i + n], rs.at[2 * i + n], (chip, s)) for n, chip in enumerate((xn, yn))]

    fwd_y = remote(buf.at[xn, lo], buf.at[xn, lo], ss.at[4], rs.at[4], (yn, s))
    fwd_x = remote(buf.at[yn, hi], buf.at[yn, hi], ss.at[5], rs.at[5], (xn, s))
    return own(lo, 0), own(hi, 1), fwd_y, fwd_x


def near_share(share):
    own_lo, own_hi, fwd_y, fwd_x = share
    own_lo[0].wait_recv()
    fwd_y.start()
    own_hi[1].wait_recv()
    fwd_x.start()


def far_share(share):
    own_lo, own_hi, fwd_y, fwd_x = share
    own_hi[0].wait_recv()
    own_lo[1].wait_recv()
    fwd_y.wait_recv()
    fwd_x.wait_recv()
    for copy in own_lo + own_hi + [fwd_y, fwd_x]:
        copy.wait_send()


def forward_kernel(act, cot, slot, w_gate, w_in, w_out,
                   sel_o, a_s, b_s, u_s, ho_s, no_s, r_s, other,
                   wv, wov, hb, nb, ub, zp, acc, ab, rv, near_in, far_in, inpv,
                   wss, wrs, iss, irs, xss, xrs, hss, hrs, ass, ars, zss, zrs, lw, lo, lab, lsv, lin, go):
    d, s, xn, yn, dg = place()
    T = nb.shape[0]
    half = T // 2
    piece = T if T <= 512 else half
    cols = ub.shape[1]
    tiles = cols // LANES
    dm = hb.shape[3]
    rows_in = act.shape[0]
    lo_rows, hi_rows = pl.ds(0, half), pl.ds(half, half)
    chips = (dg, xn, yn)
    early_tiles, held_tiles = (1, 2) if T <= 448 else (3, 3) if T <= 480 else (4, 3)

    def block_of(chip):
        return pl.ds(pl.multiple_of(chip * dm, dm), dm)

    def input_rows(chip):
        return pl.ds(pl.multiple_of(chip * rows_in, LANES), rows_in)

    def own_loads(j):
        return [pltpu.make_async_copy(w.at[j, :, pl.ds(pl.multiple_of(d * cols, LANES), cols)], wv.at[j, m, block_of(d)], lw.at[j, m])
                for m, w in enumerate((w_gate, w_in))]

    def start_weights(layer, src, core, sem, first, last):
        def body(k, carry):
            col = pl.ds(pl.multiple_of(k * LANES, LANES), LANES)
            for chip in chips:
                from_col = pl.ds(pl.multiple_of(chip * cols + k * LANES, LANES), LANES)
                for m in range(2):
                    remote(src[m].at[:, from_col], wv.at[layer, m, block_of(d), col], wss.at[sem], wrs.at[layer, k], (chip, core)).start()
            return carry
        lax.fori_loop(first, last, body, 0)

    def wait_sent(sem, count):
        sent = wv.at[0, :, pl.ds(0, 3 * dm), pl.ds(0, count * LANES)]
        pltpu.make_async_copy(sent, sent, wss.at[sem]).wait()

    def wait_tile(layer, k, col):
        came = wv.at[layer, :, pl.ds(0, 3 * dm), col]
        pltpu.make_async_copy(came, came, wrs.at[layer, k]).wait()

    other_pair = (other.at[0], other.at[1])
    first_pair = (w_gate.at[0], w_in.at[0])

    def input_sends(src):
        return [remote(src.at[:, block_of(chip)], inpv.at[input_rows(d)], iss.at[i], irs.at[i], (chip, s)) for i, chip in enumerate(chips)]

    def own_input(src):
        return pltpu.make_async_copy(src.at[:, block_of(d)], inpv.at[input_rows(d)], lin.at[0])
    share = share_rows(hb.at[s], d, s, xn, yn, ass, ars, lo_rows, hi_rows)

    def first_weights(first, last):
        @pl.when(s == 0)
        def _():
            start_weights(0, first_pair, 0, 0, first, last)
    meet()
    for n, src in enumerate((act, cot)):
        @pl.when(s == n)
        def _():
            for copy in input_sends(src) + [own_input(src)]:
                copy.start()
    swaps = [remote(w.at[1], other.at[m], xss.at[m], xrs.at[m], (d, 1 - s)) for m, w in enumerate((w_gate, w_in))]
    for copy in own_loads(0) + own_loads(1) + swaps:
        copy.start()
    pltpu.make_async_copy(w_out.at[0], wov, lo.at[0]).start()
    tokens = slot.shape[1]

    def pick_body(i, carry):
        base = pl.multiple_of(lax.div(i, 2) * half, 16)
        pick = (lax.broadcasted_iota(jnp.int32, (half, tokens), 0) + base == slot[...]).astype(BF16)
        lane = pl.ds(pl.multiple_of(lax.rem(i, 2) * (dm // 2), LANES), dm // 2)
        hb[s, d, pl.ds(base, half), lane] = jnp.dot(pick, inpv[:, lane], preferred_element_type=F32).astype(BF16)
        return carry

    def opening(q, carry):
        @pl.when(q == 1)
        def _():
            for copy in input_sends(act):
                copy.wait()
            own_input(act).wait()
            lax.fori_loop(0, 4, pick_body, 0)
            for copy in share[0] + share[1]:
                copy.start()

        @pl.when(q == 2)
        def _():
            near_share(share)
        first_weights(3 * q, 3 * q + 3 + lax.div(q, 2) * (tiles - 9))
        return carry
    lax.fori_loop(0, 3, opening, 0)
    far_share(share)
    for copy in swaps:
        copy.wait()

    def hand_over():
        return [remote(hb.at[0, c], hb.at[0, c], hss.at[i], hrs.at[i], (d, 1 - s)) for i, c in enumerate((d, xn, yn, dg))]

    @pl.when(s == 1)
    def _():
        top = [pltpu.make_async_copy(hb.at[1, c], sel_o.at[:, pl.ds(c * dm, dm)], lin.at[c]) for c in range(4)]
        for copy in top:
            copy.start()
        pl.semaphore_wait(go, 1)
        start_weights(1, other_pair, 0, 0, 0, tiles)

        def own_layers(q, carry):
            start_weights(q, (w_gate.at[q], w_in.at[q]), 1, 1 + q, 0, tiles - q * (tiles - early_tiles))
            return carry
        lax.fori_loop(0, 2, own_layers, 0)
        for copy in top:
            copy.wait()
        for copy in hand_over():
            copy.wait_recv()

    def layer(j, carry):
        nxt = 1 - j
        step = 32

        def norm_body(i, carry):
            rows = pl.ds(pl.multiple_of(i * step, step), step)
            blocks = [hb[j, c, rows, :].astype(F32) for c in range(4)]
            total = sum(jnp.sum(b * b, axis=-1, keepdims=True) for b in blocks)
            inv = lax.rsqrt(total * (1.0 / (4 * dm)) + EPSILON)
            for c in range(4):
                nb[rows, c * dm:(c + 1) * dm] = (blocks[c] * inv).astype(BF16)
            rv[rows, :] = jnp.broadcast_to(inv, (step, LANES))
            return carry
        lax.fori_loop(0, T // step, norm_body, 0)
        saves = [
            pltpu.make_async_copy(hb.at[j, d], ho_s.at[j], lsv.at[0]),
            pltpu.make_async_copy(nb.at[:, block_of(d)], no_s.at[j], lsv.at[1]),
            pltpu.make_async_copy(rv, r_s.at[j], lsv.at[2]),
        ]
        for copy in saves:
            copy.start()
        for copy in own_loads(j):
            copy.wait()

        def ab_copies(k, side):
            return [pltpu.make_async_copy(ab.at[side, 0], a_s.at[j, k], lab.at[side, 0]),
                    pltpu.make_async_copy(ab.at[side, 1], b_s.at[j, k], lab.at[side, 1])]

        def ab_body(k, carry):
            col = pl.ds(pl.multiple_of(k * LANES, LANES), LANES)
            wait_tile(j, k, col)

            @pl.when((j == 0) & (s == 0) & (k == tiles - 2))
            def _():
                pl.semaphore_signal(go, inc=1, device_id=(d, 1), device_id_type=MESH)

            def ab_rows(i, carry):
                rows = pl.ds(pl.multiple_of(i * piece, 16), piece)
                acc[rows, :] = jnp.dot(nb[rows, :], jnp.concatenate([wv[j, 0, :, col], wv[j, 1, :, col]], axis=1), preferred_element_type=F32)
                return carry
            lax.fori_loop(0, T // piece, ab_rows, 0)
            side = lax.rem(k, 2)

            @pl.when(k >= 2)
            def _():
                for copy in ab_copies(k, side):
                    copy.wait()
            a, b = acc[:, :LANES], acc[:, LANES:]
            ab[side, 0] = a
            ab[side, 1] = b
            ub[:, col] = (a * jax.nn.sigmoid(a) * b).astype(BF16)
            for copy in ab_copies(k, side):
                copy.start()
            return carry
        lax.fori_loop(0, tiles, ab_body, 0)
        for k in (tiles - 2, tiles - 1):
            for copy in ab_copies(k, k % 2):
                copy.wait()
        save_u = pltpu.make_async_copy(ub, u_s.at[j], lsv.at[3])
        save_u.start()

        @pl.when((j == 0) | (s == 0))
        def _():
            pltpu.make_async_copy(w_out.at[j], wov, lo.at[0]).wait()

            def send(i, c, rows, dst, chip):
                return remote(zp.at[c, rows], dst, zss.at[i], zrs.at[i], (chip, s))
            first = [send(0, dg, lo_rows, near_in.at[0, 0], xn), send(1, dg, hi_rows, near_in.at[1, 0], yn)]
            second = [send(2, xn, lo_rows, near_in.at[0, 1], xn), send(3, yn, hi_rows, near_in.at[1, 1], yn)]
            third = [send(4, yn, lo_rows, far_in.at[0], yn), send(5, xn, hi_rows, far_in.at[1], xn)]
            x, y = lax.rem(d, 2), lax.div(d, 2)
            wide = 2 * LANES

            def block_body(i, carry):
                rel, part_of = 3 - lax.div(i, 2), lax.rem(i, 2)
                c = 2 * lax.rem(y + lax.rem(rel, 2), 2) + lax.rem(x + lax.div(rel, 2), 2)

                def zp_rows(n, carry):
                    rows = pl.ds(pl.multiple_of(n * half, 16), half)
                    zp[c, rows, pl.ds(pl.multiple_of(part_of * wide, wide), wide)] = jnp.dot(
                        ub[rows, :], wov[:, pl.ds(pl.multiple_of(c * dm + part_of * wide, wide), wide)], preferred_element_type=F32)
                    return carry
                lax.fori_loop(0, 2, zp_rows, 0)
                for at, copies in ((1, first), (3, second[:1]), (5, second[1:])):
                    @pl.when(i == at)
                    def _():
                        for copy in copies:
                            copy.start()
                return carry
            lax.fori_loop(0, 8, block_body, 0)
            share = share_rows(hb.at[nxt], d, s, xn, yn, ass, ars, lo_rows, hi_rows)

            def both(n, stage):
                for at in range(2):
                    @pl.when(n == at)
                    def _():
                        stage(at)

            def half_rows(n):
                return pl.ds(pl.multiple_of(n * half, 16), half)

            def relay(n, carry):
                both(n, lambda at: first[at].wait_recv())
                c, rows = yn + n * (xn - yn), half_rows(n)
                zp[c, rows, :] += near_in[n, 0]
                both(n, lambda at: third[at].start())
                return carry
            lax.fori_loop(0, 2, relay, 0)

            def settle(n, carry):
                both(n, lambda at: (second[at].wait_recv(), third[at].wait_recv()))
                rows = half_rows(n)
                branch = (zp[d, rows, :] + near_in[n, 1] + far_in[n]).astype(BF16).astype(F32)
                hb[nxt, d, rows, :] = (hb[j, d, rows, :].astype(F32) + branch).astype(BF16)
                both(n, lambda at: [copy.start() for copy in share[at]])
                return carry
            lax.fori_loop(0, 2, settle, 0)
            near_share(share)

            @pl.when((j == 0) & (s == 1))
            def _():
                pl.semaphore_signal(go, inc=1, device_id=(d, 0), device_id_type=MESH)
            far_share(share)
            for copy in first + second + third:
                copy.wait_send()

        @pl.when((j == 0) & (s == 0))
        def _():
            pltpu.make_async_copy(w_out.at[1], wov, lo.at[0]).start()

        @pl.when((j == 1) & (s == 0))
        def _():
            hands = hand_over()
            for copy in hands:
                copy.start()

            def last_layer(q, carry):
                @pl.when(q == 1)
                def _():
                    pl.semaphore_wait(go, 1)
                start_weights(1, other_pair, 1, 1, early_tiles + q * (tiles - held_tiles - early_tiles), tiles - held_tiles + q * held_tiles)
                return carry
            lax.fori_loop(0, 2, last_layer, 0)
            for copy in hands:
                copy.wait_send()
        for copy in saves:
            copy.wait()
        save_u.wait()
        return carry
    lax.fori_loop(0, 2, layer, 0)
    wait_sent(0, tiles)

    @pl.when(s == 0)
    def _():
        wait_sent(1, tiles - early_tiles)

    @pl.when(s == 1)
    def _():
        wait_sent(1, tiles)
        wait_sent(2, early_tiles)


def backward_kernel(sel, slot, w_gate, w_in, w_out, a_s, b_s, ho_s, r_s,
                    da_o, db_o, e_o, act_o,
                    wgv, wov, eb, daf, ab, dn, hov, rv, sq, sv, agv, back_v,
                    dss, drs, fss, frs, ess, ers, hss, hrs, sss, srs, ass, ars, lw, lab, lout, lh, le, lsm):
    d, s, xn, yn, dg = place()
    T = sel.shape[0]
    part_rows = T // 2
    lo_n = -(-part_rows // 32) * 16
    cols = daf.shape[3]
    dm = dn.shape[1]
    wide = 2 * LANES
    n_full = cols // wide
    tail = cols - n_full * wide
    n_early = n_full // 2
    n_mid = n_early + 2
    splits, one_loop = (1 if T <= 640 else 2), T > 512
    pad = sq.shape[1]
    w_slots = wgv.shape[0]
    ab_slots = ab.shape[0]

    def wo_load(j):
        return pltpu.make_async_copy(w_out.at[j], wov, lw.at[0, 0])

    def slot_of(j, n):
        return j if n == 2 else 0

    def gate_loads(j):
        return [pltpu.make_async_copy(w.at[j], wgv.at[slot_of(j, w_slots), m], lw.at[1 + slot_of(j, w_slots), m]) for m, w in enumerate((w_gate, w_in))]

    def rows_of(g, base=0, size=part_rows):
        return pl.ds(pl.multiple_of(g * part_rows + base, 16), size)

    def in_copies(g):
        return [pltpu.make_async_copy(sel.at[rows_of(g), pl.ds(c * dm, dm)], eb.at[2, c, rows_of(g)], lh.at[g, c]) for c in range(4)]

    def hand_over(g):
        return [remote(eb.at[0, c, rows_of(g)], eb.at[2, c, rows_of(g)], hss.at[g, i], hrs.at[g, i], (d, 1 - s)) for i, c in enumerate((d, xn, yn, dg))]

    def ab_loads(j, g):
        side = slot_of(g, ab_slots)
        return [pltpu.make_async_copy(src.at[j, :, rows_of(g)], ab.at[side, m], lab.at[side, m]) for m, src in enumerate((a_s, b_s))]

    @pl.when(s == 1)
    def _():
        for copy in in_copies(0):
            copy.start()
    wo_load(1).start()
    small = [pltpu.make_async_copy(ho_s, hov, lsm.at[0]), pltpu.make_async_copy(r_s, rv, lsm.at[1])]
    for copy in ab_loads(1, 0):
        copy.start()
    meet()

    def columns(c, width):
        return pl.ds(pl.multiple_of(c * wide, LANES), width)

    def each_chunk(body, first=0, last=n_full):
        lax.fori_loop(first, last, lambda c, carry: (body(c, wide), carry)[1], 0)

    class Piece:
        def __init__(self, j, g):
            self.j, self.g, self.rows = j, g, rows_of(g)
            parts = (rows_of(g, 0, lo_n), rows_of(g, lo_n, part_rows - lo_n))
            self.share = share_rows(eb.at[j], d, s, xn, yn, ess.at[g], ers.at[g], *parts)
            self.e_saves = [pltpu.make_async_copy(eb.at[j + 1, c, self.rows], e_o.at[j, self.rows, pl.ds(c * dm, dm)], le.at[j, g, c]) for c in range(4)]
            self.sums = [remote(sv.at[g, 0], sv.at[g, 1 + i], sss.at[g, i], srs.at[g, i], (chip, s)) for i, chip in enumerate((xn, yn, dg))]

        def own_sends(self, c, col):
            g, out = self.g, []
            for m in range(2):
                for n, chip in enumerate((xn, yn)):
                    here = daf.at[m, d, self.rows, col]
                    out.append(remote(here, here, dss.at[g, m, n, c], drs.at[g, m, n, c], (chip, s)))
            return out

        def forwards(self, c, col):
            g = self.g
            from_x, from_y = daf.at[0, xn, self.rows, col], daf.at[1, yn, self.rows, col]
            return [remote(from_x, from_x, fss.at[g, 1, c], frs.at[g, 1, c], (yn, s)), remote(from_y, from_y, fss.at[g, 0, c], frs.at[g, 0, c], (xn, s))]

        def make(self):
            j, g, rows, side = self.j, self.g, self.rows, slot_of(self.g, ab_slots)
            for copy in self.e_saves:
                copy.start()

            @pl.when(g == 0)
            def _():
                wo_load(j).wait()
            for copy in ab_loads(j, g):
                copy.wait()

            @pl.when((j == 1) & (g == 0))
            def _():
                if ab_slots == 2:
                    for copy in ab_loads(1, 1):
                        copy.start()

                @pl.when(s == 1)
                def _():
                    for copy in in_copies(1):
                        copy.start()
                for copy in gate_loads(1) + small:
                    copy.start()
            if w_slots == 2:
                @pl.when((j == 1) & (g == 1))
                def _():
                    for copy in gate_loads(0):
                        copy.start()

            def tile(c, width=wide):
                base = jnp.minimum(c * wide, cols - wide) if one_loop else c * wide
                def du(blocks, lanes):
                    e_part = jnp.concatenate([eb[j + 1, n, rows, :] for n in blocks], axis=1)
                    return nt_dot(e_part, wov[pl.ds(pl.multiple_of(base, LANES), width), lanes])
                if splits == 1:
                    dn[rows, :width] = du(range(4), slice(None))
                else:
                    dn[rows, :width] = jnp.zeros((part_rows, width), F32)

                    def du_part(n, carry):
                        dn[rows, :width] += du((2 * n, 2 * n + 1), pl.ds(pl.multiple_of(n * 2 * dm, dm), 2 * dm))
                        return carry
                    lax.fori_loop(0, 2, du_part, 0)
                def lanes(n):
                    lane = pl.ds(pl.multiple_of(base + n * LANES, LANES), LANES)
                    at = lax.div(base, LANES) + n
                    a, b, du = ab[side, 0, at], ab[side, 1, at], dn[rows, n * LANES:(n + 1) * LANES]
                    sig = jax.nn.sigmoid(a)
                    daf[0, d, rows, lane] = (du * b * sig * (1.0 + a * (1.0 - sig))).astype(BF16)
                    daf[1, d, rows, lane] = (du * (a * sig)).astype(BF16)

                if one_loop:
                    @pl.when(c < n_full)
                    def _():
                        lanes(0)
                    lanes(1)
                else:
                    for n in range(width // LANES):
                        lanes(n)

            def body(c, width):
                tile(c, wide)

                @pl.when(c < n_early)
                def _():
                    for copy in self.own_sends(c, columns(c, wide)):
                        copy.start()
            each_chunk(body, 0, n_full + 1 if one_loop else n_full)
            if not one_loop:
                tile(n_full, tail)

        def send(self, first, last):
            def body(c, width):
                for copy in self.own_sends(c, columns(c, width)):
                    copy.start()
            each_chunk(body, first, last)

        def save_tile(self, m, chip, col, c, width):
            dst = (da_o, db_o)[m].at[self.j, self.rows, pl.ds(pl.multiple_of(chip * cols + c * wide, LANES), width)]
            pltpu.make_async_copy(daf.at[m, chip, self.rows, col], dst, lout.at[self.g]).start()

        def add(self, chip, c, width):
            def body(i, carry):
                m, at = lax.div(i, splits), pl.ds(pl.multiple_of(lax.rem(i, splits) * (dm // splits), LANES), dm // splits)
                w = wgv[slot_of(self.j, w_slots), m, at, pl.ds(pl.multiple_of(chip * cols + c * wide, LANES), width)]
                dn[self.rows, at] += nt_dot(daf[m, chip, self.rows, columns(c, width)], w)
                return carry
            lax.fori_loop(0, 2 * splits, body, 0)

        def own(self):
            @pl.when(self.g == 0)
            def _():
                for copy in gate_loads(self.j):
                    copy.wait()
            for m in range(2):
                self.save_tile(m, d, pl.ds(0, cols), 0, cols)
            dn[self.rows, :] = jnp.zeros((part_rows, dm), F32)
            each_chunk(lambda c, width: self.add(d, c, width))
            self.add(d, n_full, tail)

        def near(self, c, width):
            col = columns(c, width)
            fwd_y, fwd_x = self.forwards(c, col)

            def came(m, n, chip):
                there = daf.at[m, chip, self.rows, col]
                remote(there, there, dss.at[self.g, m, n, c], drs.at[self.g, m, n, c], (chip, s)).wait_recv()
            came(0, 0, xn)
            fwd_y.start()
            came(1, 1, yn)
            fwd_x.start()
            came(1, 0, xn)
            came(0, 1, yn)
            for chip in (xn, yn):
                for m in range(2):
                    self.save_tile(m, chip, col, c, width)
            lax.fori_loop(0, 2, lambda i, carry: (self.add(xn + i * (yn - xn), c, width), carry)[1], 0)

        def far(self):
            j, g, rows = self.j, self.g, self.rows

            def body(c, width):
                col = columns(c, width)
                there = [daf.at[m, dg, rows, col] for m in range(2)]
                remote(there[0], there[0], fss.at[g, 1, c], frs.at[g, 1, c], (yn, s)).wait_recv()
                remote(there[1], there[1], fss.at[g, 0, c], frs.at[g, 0, c], (xn, s)).wait_recv()
                for m in range(2):
                    self.save_tile(m, dg, col, c, width)
                self.add(dg, c, width)
            each_chunk(body)
            body(n_full, tail)

            @pl.when((j == 1) & (g == 0))
            def _():
                for copy in small:
                    copy.wait()
            prod = dn[rows, :] * hov[j, rows, :].astype(F32)
            sq[g, :part_rows, :] = (prod[:, :LANES] + prod[:, LANES:2 * LANES]) + (prod[:, 2 * LANES:3 * LANES] + prod[:, 3 * LANES:])
            sv[g, 0] = jnp.broadcast_to(jnp.sum(sq[g].T, axis=0, keepdims=True), (8, pad))
            for copy in self.sums:
                copy.start()
            if w_slots == 1:
                @pl.when((j == 1) & (g == 1))
                def _():
                    for copy in gate_loads(0):
                        copy.start()

        def finish(self):
            j, g = self.j, self.g
            whole = daf.at[:, :, self.rows]
            pltpu.make_async_copy(whole, whole, lout.at[g]).wait()

            def drain(c, width):
                col = columns(c, width)
                for copy in self.own_sends(c, col) + self.forwards(c, col):
                    copy.wait_send()
            each_chunk(drain)
            drain(n_full, tail)
            for copy in self.sums:
                copy.wait()
            mean = ((sv[g, 0, 0:1, :] + sv[g, 1, 0:1, :]) + (sv[g, 2, 0:1, :] + sv[g, 3, 0:1, :])) * (1.0 / (4 * dm))
            sq[g] = jnp.broadcast_to(mean, (LANES, pad)).T
            for n, (base, size) in enumerate(((0, lo_n), (lo_n, part_rows - lo_n))):
                at = rows_of(g, base, size)
                inv, avg = rv[j, at, :], sq[g, base:base + size, :]
                for c in range(4):
                    lane = slice(c * LANES, (c + 1) * LANES)
                    resid = inv * dn[at, lane] - hov[j, at, lane].astype(F32) * (inv * inv * inv) * avg
                    eb[j, d, at, lane] = (eb[j + 1, d, at, lane].astype(F32) + resid).astype(BF16)
                for copy in self.share[n]:
                    copy.start()

    def give(g):
        own_lo, own_hi, fwd_y, fwd_x = Piece(0, g).share
        for copy, came in zip(hand_over(g), ((), (own_hi[0],), (own_lo[1],), (fwd_y, fwd_x))):
            for part in came:
                part.wait_recv()
            copy.start()
        for copy in own_lo + own_hi + [fwd_y, fwd_x]:
            copy.wait_send()

    def step(i, carry):
        g = lax.rem(i, 2)
        cur = Piece(1 - lax.div(i, 2), g)
        prev = Piece(1 - lax.div(i - 1, 2), 1 - g)
        live, later = i < 4, i > 0

        ending = (i == 4) & (s == 1)

        @pl.when(ending)
        def _():
            give(0)

        @pl.when((i >= 2) & jnp.logical_not(ending))
        def _():
            far_share(Piece(1 - lax.div(i - 2, 2), g).share)

        @pl.when(live)
        def _():
            @pl.when((i < 2) & (s == 0))
            def _():
                for copy in hand_over(g):
                    copy.wait_recv()

            @pl.when((i < 2) & (s == 1))
            def _():
                for copy in in_copies(g):
                    copy.wait()

            cur.make()

            @pl.when(i == 1)
            def _():
                wo_load(0).start()
            coming = i + ab_slots

            @pl.when(coming < 4)
            def _():
                for copy in ab_loads(1 - lax.div(coming, 2), lax.rem(coming, 2)):
                    copy.start()

        @pl.when(later)
        def _():
            prev.far()

        def halves(h, carry):
            @pl.when(live)
            def _():
                cur.send(n_early + h * (n_mid - n_early), n_mid + h * (n_full - n_mid))

            @pl.when(live & (h == 0))
            def _():
                cur.own()

            @pl.when(live & (h == 1))
            def _():
                for copy in cur.own_sends(n_full, columns(n_full, tail)):
                    copy.start()

            @pl.when(later & (h == 1))
            def _():
                near_share(prev.share)

            @pl.when(live & (h == 1))
            def _():
                each_chunk(cur.near)

            @pl.when(later & (h == 0))
            def _():
                prev.finish()
            return carry
        lax.fori_loop(0, 2, halves, 0)

        @pl.when(live)
        def _():
            cur.near(n_full, tail)
        return carry
    lax.fori_loop(0, 5, step, 0)

    def act_copies(i, c):
        col = pl.ds(pl.multiple_of(c * dm, dm), dm)
        return remote(agv.at[c], act_o.at[:, col], ass.at[i], ars.at[i], (d, 1 - s)), pltpu.make_async_copy(agv.at[c], act_o.at[:, col], lh.at[0, i])

    @pl.when(s == 1)
    def _():
        give(1)
        for i, c in enumerate((d, xn, yn, dg)):
            act_copies(i, c)[0].wait_recv()

    @pl.when(s == 0)
    def _():
        own_lo, own_hi, fwd_y, fwd_x = Piece(0, 1).share
        rows_out = agv.shape[1]
        own_slots = slot[:, pl.ds(pl.multiple_of(d * rows_out, LANES), rows_out)]
        back = (lax.broadcasted_iota(jnp.int32, (T, rows_out), 0) == own_slots).astype(BF16)
        back_v[...] = back
        came = ((), (own_hi[0],), (own_lo[1],), (fwd_y, fwd_x))
        x, y = lax.rem(d, 2), lax.div(d, 2)

        def spread(i, carry):
            for n in range(1, 4):
                @pl.when(i == n)
                def _():
                    for copy in came[n]:
                        copy.wait_recv()
            c = 2 * lax.rem(y + lax.div(i, 2), 2) + lax.rem(x + lax.rem(i, 2), 2)
            agv[c] = lax.dot_general(back_v[...], eb[0, c], (((0,), (0,)), ((), ())), preferred_element_type=F32).astype(BF16)
            for copy in act_copies(i, c):
                copy.start()
            return carry
        lax.fori_loop(0, 4, spread, 0)
        for copy in own_lo + own_hi + [fwd_y, fwd_x]:
            copy.wait_send()
        for i, c in enumerate((d, xn, yn, dg)):
            away, here = act_copies(i, c)
            away.wait_send()
            here.wait()
    def saved(i, carry):
        for copy in Piece(lax.div(i, 2), lax.rem(i, 2)).e_saves:
            copy.wait()
        return carry
    lax.fori_loop(0, 4, saved, 0)

    @pl.when(s == 1)
    def _():
        for g in range(2):
            for copy in hand_over(g):
                copy.wait_send()


def grads_kernel(no_s, u_s, da, db, e_o, act, gate_o, in_o, out_o, act_o, nv, uv, ev, av, nt, ut, ring, og, oo, ln, lr, lg, lo):
    layers = nv.shape[0]
    wide = ring.shape[3]
    n_gate, n_out = da.shape[2] // wide, e_o.shape[2] // wide
    slots, g_slots, o_slots = ring.shape[0], og.shape[0], oo.shape[0]
    rows = oo.shape[2]
    n_flip = ut.shape[1] // LANES
    first_flip = 1
    first_out = max(first_flip + n_flip, layers * n_gate - layers * n_out - 2)

    def put(ref, at, value):
        ref[at] = value

    def for_rows(count, body):
        parts = 1 if nv.shape[1] <= 640 else 2
        size = count // parts
        if parts == 1:
            body(pl.ds(0, size))
        else:
            lax.fori_loop(0, parts, lambda i, carry: (body(pl.ds(pl.multiple_of(i * size, 32), size)), carry)[1], 0)

    def flip(src, dst):
        def body(i, carry):
            lane = pl.ds(pl.multiple_of(i * LANES, LANES), LANES)
            dst[lane, :] = src[:, lane].T
            return carry
        lax.fori_loop(0, dst.shape[0] // LANES, body, 0)
    wholes = [pltpu.make_async_copy(src, dst, ln.at[i]) for i, (src, dst) in enumerate(((no_s, nv), (u_s, uv), (e_o, ev), (act, av)))]
    act_store = pltpu.make_async_copy(av, act_o, ln.at[4])

    def tile_at(c):
        return pl.ds(pl.multiple_of(c * wide, wide), wide)

    def loads(t):
        slot = lax.rem(t, slots)
        return [pltpu.make_async_copy(src.at[lax.div(t, n_gate), :, tile_at(lax.rem(t, n_gate))], ring.at[slot, m], lr.at[slot, m]) for m, src in enumerate((da, db))]

    def gate_stores(t):
        slot = lax.rem(t, g_slots)
        return [pltpu.make_async_copy(og.at[slot, m], dst.at[lax.div(t, n_gate), :, tile_at(lax.rem(t, n_gate))], lg.at[slot, m]) for m, dst in enumerate((gate_o, in_o))]

    def out_stores(t):
        slot = lax.rem(t, o_slots)
        return [pltpu.make_async_copy(oo.at[slot, m], out_o.at[lax.div(t, n_out), pl.ds(m * rows, rows), tile_at(lax.rem(t, n_out))], lo.at[slot, m]) for m in range(2)]

    def start(copies):
        for copy in copies:
            copy.start()

    def wait(copies):
        for copy in copies:
            copy.wait()
    wholes[0].start()
    for t in range(slots - 1):
        start(loads(t))
    start(wholes[1:])
    wholes[0].wait()

    def out_tile(t):
        j, c, at = lax.div(t, n_out), lax.rem(t, n_out), lax.rem(t, o_slots)

        @pl.when(t >= o_slots)
        def _():
            wait(out_stores(t - o_slots))

        def half(m, carry):
            for_rows(rows, lambda at_rows: put(oo, (at, m, at_rows), jnp.dot(
                ut[j, pl.ds(pl.multiple_of(m * rows + at_rows.start, 32), at_rows.size), :], ev[j, :, tile_at(c)], preferred_element_type=F32)))
            return carry
        lax.fori_loop(0, 2, half, 0)
        start(out_stores(t))

    def gate_body(t, carry):
        j, c, slot, at = lax.div(t, n_gate), lax.rem(t, n_gate), lax.rem(t, slots), lax.rem(t, g_slots)

        @pl.when(t + slots - 1 < layers * n_gate)
        def _():
            start(loads(t + slots - 1))

        @pl.when(c == 0)
        def _():
            flip(nv.at[j], nt)
        wait(loads(t))

        @pl.when(t >= g_slots)
        def _():
            wait(gate_stores(t - g_slots))

        def side(m, carry):
            for_rows(og.shape[2], lambda at_rows: put(og, (at, m, at_rows), jnp.dot(nt[at_rows, :], ring[slot, m], preferred_element_type=F32)))
            return carry
        lax.fori_loop(0, 2, side, 0)
        start(gate_stores(t))

        @pl.when(t == first_flip)
        def _():
            wholes[1].wait()

        @pl.when((t >= first_flip) & (t < first_out))
        def _():
            lane = pl.ds(pl.multiple_of((t - first_flip) * LANES, LANES), LANES)

            def turn(n, carry):
                ut[n, lane, :] = uv[n, :, lane].T
                return carry
            lax.fori_loop(0, layers, turn, 0)

        @pl.when(t == first_out)
        def _():
            wait(wholes[2:])
            act_store.start()

        @pl.when((t >= first_out) & (t < first_out + layers * n_out))
        def _():
            out_tile(t - first_out)
        return carry
    lax.fori_loop(0, layers * n_gate, gate_body, 0)
    act_store.wait()
    for t in range(layers * n_gate - g_slots, layers * n_gate):
        wait(gate_stores(t))
    for t in range(layers * n_out - o_slots, layers * n_out):
        wait(out_stores(t))


def grads_call(no_s, u_s, da, db, e_o, act):
    layers, T, dsh = no_s.shape
    cols, dff, dmod = u_s.shape[2], da.shape[2], e_o.shape[2]
    V, wide = pltpu.VMEM, 4 * LANES
    moved = 2 * layers * T * (dsh + cols + 2 * dff + dmod) + 4 * layers * (2 * dsh * dff + cols * dmod)
    return pl.pallas_call(
        grads_kernel, name=f'grads_{T}', in_specs=[ANY] * 6, out_specs=[ANY] * 4,
        out_shape=[jax.ShapeDtypeStruct((layers, dsh, dff), F32), jax.ShapeDtypeStruct((layers, dsh, dff), F32), jax.ShapeDtypeStruct((layers, cols, dmod), F32),
                   jax.ShapeDtypeStruct(act.shape, BF16)],
        scratch_shapes=[V((layers, T, dsh), BF16), V((layers, T, cols), BF16), V((layers, T, dmod), BF16), V(act.shape, BF16), V((dsh, T), BF16), V((layers, cols, T), BF16),
                        V((6, 2, T, wide), BF16), V((4, 2, dsh, wide), F32), V((3, 2, cols // 2, wide), F32), DMA((5,)), DMA((6, 2)), DMA((4, 2)), DMA((3, 2))],
        cost_estimate=pl.CostEstimate(flops=2 * layers * T * (2 * dsh * dff + cols * dmod), bytes_accessed=moved, transcendentals=0),
        compiler_params=pltpu.CompilerParams(vmem_limit_bytes=VMEM_LIMIT))(no_s, u_s, da, db, e_o, act)


ANY = pl.BlockSpec(memory_space=pl.ANY)
DMA = pltpu.SemaphoreType.DMA


def comm_call(kernel, name, cid, outs, in_specs, scratch):
    return pl.pallas_call(
        kernel, name=name, out_shape=[jax.ShapeDtypeStruct(*o) for o in outs], in_specs=in_specs, out_specs=[ANY] * len(outs),
        scratch_shapes=scratch, compiler_params=pltpu.CompilerParams(collective_id=cid, has_side_effects=True, vmem_limit_bytes=VMEM_LIMIT))


def lens_call(lens, tokens, sizes):
    smem, vmem = pl.BlockSpec(memory_space=pltpu.SMEM), pl.BlockSpec(memory_space=pltpu.VMEM)
    rows = tokens // LANES
    return pl.pallas_call(
        functools.partial(lens_kernel, sizes), name='lens', out_shape=[jax.ShapeDtypeStruct((1, 4 * tokens), jnp.int32), jax.ShapeDtypeStruct((1,), jnp.int32)],
        in_specs=[smem], out_specs=[vmem, smem],
        scratch_shapes=[pltpu.VMEM((rows, LANES), jnp.int32), pltpu.VMEM((4, rows, LANES), jnp.int32), DMA((3,)), DMA((3,))],
        compiler_params=pltpu.CompilerParams(collective_id=0, has_side_effects=True))(lens)


def forward_call(cid, T, act, cot, slot, w_gate, w_in, w_out):
    rows, dmod = act.shape
    _, dsh, dff = w_gate.shape
    cols = dff // 4
    half = T // 2
    tiles = cols // LANES
    outs = [((T, dmod), BF16), ((2, tiles, T, LANES), F32), ((2, tiles, T, LANES), F32), ((2, T, cols), BF16),
            ((2, T, dsh), BF16), ((2, T, dsh), BF16), ((2, T, LANES), F32), ((2, dsh, dff), BF16)]
    V = pltpu.VMEM
    scratch = [V((2, 2, dmod, cols), BF16), V((cols, dmod), BF16), V((2, 4, T, dsh), BF16), V((T, dmod), BF16), V((T, cols), BF16),
               V((4, T, dsh), F32), V((T, 2 * LANES), F32), V((2, 2, T, LANES), F32), V((T, LANES), F32),
               V((2, 2, half, dsh), F32), V((2, half, dsh), F32), V((4 * rows, dsh), BF16),
               DMA((3,)), DMA((2, tiles)), DMA((3,)), DMA((3,)), DMA((2,)), DMA((2,)), DMA((4,)), DMA((4,)), DMA((6,)), DMA((6,)), DMA((6,)), DMA((6,)),
               DMA((2, 2)), DMA((1,)), DMA((2, 2)), DMA((4,)), DMA((4,)), pltpu.SemaphoreType.REGULAR]
    specs = [ANY, ANY, pl.BlockSpec(memory_space=pltpu.VMEM)] + [ANY] * 3
    return comm_call(forward_kernel, f'forward_{T}', cid, outs, specs, scratch)(act, cot, slot, w_gate, w_in, w_out)


def backward_call(cid, sel, slot, w_gate, w_in, w_out, a_s, b_s, ho_s, r_s):
    T, dmod = sel.shape
    _, dsh, dff = w_gate.shape
    cols = dff // 4
    tiles = cols // LANES
    chunks = (tiles + 1) // 2
    pad = -(-(T // 2) // LANES) * LANES
    slots = 2 if T <= 640 else 1
    ab_slots = 2 if T <= 832 else 1
    outs = [((2, T, dff), BF16), ((2, T, dff), BF16), ((2, T, dmod), BF16), ((slot.shape[1] // 4, dmod), BF16)]
    V = pltpu.VMEM
    scratch = [V((slots, 2, dsh, dff), BF16), V((cols, dmod), BF16), V((3, 4, T, dsh), BF16), V((2, 4, T, cols), BF16),
               V((ab_slots, 2, tiles, T // 2, LANES), F32), V((T, dsh), F32), V((2, T, dsh), BF16), V((2, T, LANES), F32), V((2, pad, LANES), F32), V((2, 4, 8, pad), F32), V((4, slot.shape[1] // 4, dsh), BF16), V((T, slot.shape[1] // 4), BF16),
               DMA((2, 2, 2, chunks)), DMA((2, 2, 2, chunks)), DMA((2, 2, chunks)), DMA((2, 2, chunks)), DMA((2, 6)), DMA((2, 6)), DMA((2, 4)), DMA((2, 4)),
               DMA((2, 3)), DMA((2, 3)), DMA((4,)), DMA((4,)), DMA((3, 2)), DMA((2, 2)), DMA((2,)), DMA((2, 4)), DMA((2, 2, 4)), DMA((2,))]
    return comm_call(backward_kernel, f'backward_{T}', cid, outs, [ANY, pl.BlockSpec(memory_space=pltpu.VMEM)] + [ANY] * 7, scratch)(sel, slot, w_gate, w_in, w_out, a_s, b_s, ho_s, r_s)


def solution(mesh, buckets=BUCKETS):
    act_spec = P(None, 'data')
    weight_spec = P('stage', None, 'data', None)

    def local_step(act_in, cot_out, seq_lens, w_gate, w_in, w_out):
        n_micro, n_rows, seq_len, dmod = act_in.shape
        rows = n_micro * n_rows * seq_len
        w_gate, w_in, w_out = w_gate[0], w_in[0], w_out[0]
        act, cot = act_in.reshape(rows, dmod), cot_out.reshape(rows, dmod)
        slot, which = lens_call(seq_lens.reshape(n_micro), rows, buckets)

        def branch(which, T):
            def run(_):
                sel, a_s, b_s, u_s, ho_s, no_s, r_s, _ = forward_call(1 + 2 * which, T, act, cot, slot, w_gate, w_in, w_out)
                da, db, e_o, act_grad = backward_call(2 + 2 * which, sel, slot, w_gate, w_in, w_out, a_s, b_s, ho_s, r_s)
                gate_grad, in_grad, out_grad, act_grad = grads_call(no_s, u_s, da, db, e_o, act_grad)
                return act_grad.reshape(act_in.shape), gate_grad[None], in_grad[None], out_grad[None]
            return run
        if len(buckets) == 1:
            return branch(0, buckets[0])(0)
        return lax.switch(which[0], [branch(i, b) for i, b in enumerate(buckets)], 0)

    return jax.shard_map(local_step, mesh=mesh, in_specs=(act_spec, act_spec, act_spec, weight_spec, weight_spec, weight_spec), out_specs=(act_spec, weight_spec, weight_spec, weight_spec), check_vma=False)
```

```python
import functools

import jax
import jax.numpy as jnp
from jax import lax
from jax.experimental import pallas as pl
from jax.experimental.pallas import tpu as pltpu
from jax.sharding import PartitionSpec as P

EPSILON = 1e-6
MESH = pl.DeviceIdType.MESH
BF16, F32 = jnp.bfloat16, jnp.float32
LANES = 128
VMEM_LIMIT = 67043328
BUCKETS = (448, 480, 512, 544, 608, 992)


def nt_dot(left, right):
    return lax.dot_general(left, right, (((1,), (1,)), ((), ())), preferred_element_type=F32)


def place():
    d = lax.axis_index('data')
    s = lax.axis_index('stage')
    x = lax.rem(d, 2)
    y = lax.div(d, 2)
    return d, s, 2 * y + 1 - x, 2 * (1 - y) + x, 3 - d


def meet(same_core=False):
    d, s, xn, yn, dg = place()
    barrier = pltpu.get_barrier_semaphore()
    peers = [(xn, s), (yn, s), (dg, s)]
    if not same_core:
        peers += [(xn, 1 - s), (yn, 1 - s), (dg, 1 - s), (d, 1 - s)]
    for chip, core in peers:
        pl.semaphore_signal(barrier, inc=1, device_id=(chip, core), device_id_type=MESH)
    pl.semaphore_wait(barrier, len(peers))


def remote(src, dst, send_sem, recv_sem, device):
    return pltpu.make_async_remote_copy(src_ref=src, dst_ref=dst, send_sem=send_sem, recv_sem=recv_sem, device_id=device, device_id_type=MESH)


def lens_kernel(sizes, lens, slot, which, mine, everyone, ss, rs):
    d, s, xn, yn, dg = place()
    seqs, tokens = lens.shape[0], mine.shape[0] * LANES
    each = tokens // seqs
    index = lax.broadcasted_iota(jnp.int32, mine.shape, 0) * LANES + lax.broadcasted_iota(jnp.int32, mine.shape, 1)
    length = jnp.zeros(mine.shape, jnp.int32)
    for i in range(seqs):
        length = jnp.where((index >= i * each) & (index < (i + 1) * each), lens[i], length)
    mine[...] = jnp.where(lax.rem(index, each) < length, 1, 0)
    everyone[d] = mine[...]
    meet(same_core=True)
    sends = [remote(mine, everyone.at[d], ss.at[i], rs.at[i], (chip, s)) for i, chip in enumerate((xn, yn, dg))]
    for copy in sends:
        copy.start()
    for copy in sends:
        copy.wait()
    rows = 4 * mine.shape[0]
    live = everyone[...].reshape(rows, LANES)
    lane, row = lax.broadcasted_iota(jnp.int32, live.shape, 1), lax.broadcasted_iota(jnp.int32, live.shape, 0)
    upto = live
    shift = 1
    while shift < LANES:
        upto = upto + jnp.where(lane >= shift, pltpu.roll(upto, shift, 1), 0)
        shift *= 2
    whole = jnp.broadcast_to(jnp.sum(live, axis=1, keepdims=True), live.shape)
    before = whole
    shift = 1
    while shift < rows:
        before = before + jnp.where(row >= shift, pltpu.roll(before, shift, 0), 0)
        shift *= 2
    place_of = jnp.where(live > 0, before - whole + upto - 1, -1)
    for i in range(rows):
        slot[:, i * LANES:(i + 1) * LANES] = place_of[i:i + 1, :]
    total = jnp.sum(live)
    which[0] = sum((total > size).astype(jnp.int32) for size in sizes[:-1]) if len(sizes) > 1 else 0


def share_rows(buf, d, s, xn, yn, ss, rs, lo, hi):
    def own(part, i):
        return [remote(buf.at[d, part], buf.at[d, part], ss.at[2 * i + n], rs.at[2 * i + n], (chip, s)) for n, chip in enumerate((xn, yn))]

    fwd_y = remote(buf.at[xn, lo], buf.at[xn, lo], ss.at[4], rs.at[4], (yn, s))
    fwd_x = remote(buf.at[yn, hi], buf.at[yn, hi], ss.at[5], rs.at[5], (xn, s))
    return own(lo, 0), own(hi, 1), fwd_y, fwd_x


def near_share(share):
    own_lo, own_hi, fwd_y, fwd_x = share
    own_lo[0].wait_recv()
    fwd_y.start()
    own_hi[1].wait_recv()
    fwd_x.start()


def far_share(share):
    own_lo, own_hi, fwd_y, fwd_x = share
    own_hi[0].wait_recv()
    own_lo[1].wait_recv()
    fwd_y.wait_recv()
    fwd_x.wait_recv()
    for copy in own_lo + own_hi + [fwd_y, fwd_x]:
        copy.wait_send()


def forward_kernel(act, cot, slot, w_gate, w_in, w_out,
                   sel_o, a_s, b_s, u_s, ho_s, no_s, r_s, other,
                   wv, wov, hb, nb, ub, zp, acc, ab, rv, near_in, far_in, inpv,
                   wss, wrs, iss, irs, xss, xrs, hss, hrs, ass, ars, zss, zrs, lw, lo, lab, lsv, lin, go):
    d, s, xn, yn, dg = place()
    T = nb.shape[0]
    half = T // 2
    piece = T if T <= 512 else half
    cols = ub.shape[1]
    tiles = cols // LANES
    dm = hb.shape[3]
    rows_in = act.shape[0]
    lo_rows, hi_rows = pl.ds(0, half), pl.ds(half, half)
    chips = (dg, xn, yn)
    early_tiles, held_tiles = (1, 2) if T <= 448 else (3, 3) if T <= 480 else (4, 3)

    def block_of(chip):
        return pl.ds(pl.multiple_of(chip * dm, dm), dm)

    def input_rows(chip):
        return pl.ds(pl.multiple_of(chip * rows_in, LANES), rows_in)

    def own_loads(j):
        return [pltpu.make_async_copy(w.at[j, :, pl.ds(pl.multiple_of(d * cols, LANES), cols)], wv.at[j, m, block_of(d)], lw.at[j, m])
                for m, w in enumerate((w_gate, w_in))]

    def start_weights(layer, src, core, sem, first, last):
        def body(k, carry):
            col = pl.ds(pl.multiple_of(k * LANES, LANES), LANES)
            for chip in chips:
                from_col = pl.ds(pl.multiple_of(chip * cols + k * LANES, LANES), LANES)
                for m in range(2):
                    remote(src[m].at[:, from_col], wv.at[layer, m, block_of(d), col], wss.at[sem], wrs.at[layer, k], (chip, core)).start()
            return carry
        lax.fori_loop(first, last, body, 0)

    def wait_sent(sem, count):
        sent = wv.at[0, :, pl.ds(0, 3 * dm), pl.ds(0, count * LANES)]
        pltpu.make_async_copy(sent, sent, wss.at[sem]).wait()

    def wait_tile(layer, k, col):
        came = wv.at[layer, :, pl.ds(0, 3 * dm), col]
        pltpu.make_async_copy(came, came, wrs.at[layer, k]).wait()

    other_pair = (other.at[0], other.at[1])
    first_pair = (w_gate.at[0], w_in.at[0])

    def input_sends(src):
        return [remote(src.at[:, block_of(chip)], inpv.at[input_rows(d)], iss.at[i], irs.at[i], (chip, s)) for i, chip in enumerate(chips)]

    def own_input(src):
        return pltpu.make_async_copy(src.at[:, block_of(d)], inpv.at[input_rows(d)], lin.at[0])
    share = share_rows(hb.at[s], d, s, xn, yn, ass, ars, lo_rows, hi_rows)

    def first_weights(first, last):
        @pl.when(s == 0)
        def _():
            start_weights(0, first_pair, 0, 0, first, last)
    meet()
    for n, src in enumerate((act, cot)):
        @pl.when(s == n)
        def _():
            for copy in input_sends(src) + [own_input(src)]:
                copy.start()
    swaps = [remote(w.at[1], other.at[m], xss.at[m], xrs.at[m], (d, 1 - s)) for m, w in enumerate((w_gate, w_in))]
    for copy in own_loads(0) + own_loads(1) + swaps:
        copy.start()
    pltpu.make_async_copy(w_out.at[0], wov, lo.at[0]).start()
    tokens = slot.shape[1]

    def pick_body(i, carry):
        base = pl.multiple_of(lax.div(i, 2) * half, 16)
        pick = (lax.broadcasted_iota(jnp.int32, (half, tokens), 0) + base == slot[...]).astype(BF16)
        lane = pl.ds(pl.multiple_of(lax.rem(i, 2) * (dm // 2), LANES), dm // 2)
        hb[s, d, pl.ds(base, half), lane] = jnp.dot(pick, inpv[:, lane], preferred_element_type=F32).astype(BF16)
        return carry

    def opening(q, carry):
        @pl.when(q == 1)
        def _():
            for copy in input_sends(act):
                copy.wait()
            own_input(act).wait()
            lax.fori_loop(0, 4, pick_body, 0)
            for copy in share[0] + share[1]:
                copy.start()

        @pl.when(q == 2)
        def _():
            near_share(share)
        first_weights(3 * q, 3 * q + 3 + lax.div(q, 2) * (tiles - 9))
        return carry
    lax.fori_loop(0, 3, opening, 0)
    far_share(share)
    for copy in swaps:
        copy.wait()

    def hand_over():
        return [remote(hb.at[0, c], hb.at[0, c], hss.at[i], hrs.at[i], (d, 1 - s)) for i, c in enumerate((d, xn, yn, dg))]

    @pl.when(s == 1)
    def _():
        top = [pltpu.make_async_copy(hb.at[1, c], sel_o.at[:, pl.ds(c * dm, dm)], lin.at[c]) for c in range(4)]
        for copy in top:
            copy.start()
        pl.semaphore_wait(go, 1)
        start_weights(1, other_pair, 0, 0, 0, tiles)

        def own_layers(q, carry):
            start_weights(q, (w_gate.at[q], w_in.at[q]), 1, 1 + q, 0, tiles - q * (tiles - early_tiles))
            return carry
        lax.fori_loop(0, 2, own_layers, 0)
        for copy in top:
            copy.wait()
        for copy in hand_over():
            copy.wait_recv()

    def layer(j, carry):
        nxt = 1 - j
        step = 32

        def norm_body(i, carry):
            rows = pl.ds(pl.multiple_of(i * step, step), step)
            blocks = [hb[j, c, rows, :].astype(F32) for c in range(4)]
            total = sum(jnp.sum(b * b, axis=-1, keepdims=True) for b in blocks)
            inv = lax.rsqrt(total * (1.0 / (4 * dm)) + EPSILON)
            for c in range(4):
                nb[rows, c * dm:(c + 1) * dm] = (blocks[c] * inv).astype(BF16)
            rv[rows, :] = jnp.broadcast_to(inv, (step, LANES))
            return carry
        lax.fori_loop(0, T // step, norm_body, 0)
        saves = [
            pltpu.make_async_copy(hb.at[j, d], ho_s.at[j], lsv.at[0]),
            pltpu.make_async_copy(nb.at[:, block_of(d)], no_s.at[j], lsv.at[1]),
            pltpu.make_async_copy(rv, r_s.at[j], lsv.at[2]),
        ]
        for copy in saves:
            copy.start()
        for copy in own_loads(j):
            copy.wait()

        def ab_copies(k, side):
            return [pltpu.make_async_copy(ab.at[side, 0], a_s.at[j, k], lab.at[side, 0]),
                    pltpu.make_async_copy(ab.at[side, 1], b_s.at[j, k], lab.at[side, 1])]

        def ab_body(k, carry):
            col = pl.ds(pl.multiple_of(k * LANES, LANES), LANES)
            wait_tile(j, k, col)

            @pl.when((j == 0) & (s == 0) & (k == tiles - 2))
            def _():
                pl.semaphore_signal(go, inc=1, device_id=(d, 1), device_id_type=MESH)

            def ab_rows(i, carry):
                rows = pl.ds(pl.multiple_of(i * piece, 16), piece)
                acc[rows, :] = jnp.dot(nb[rows, :], jnp.concatenate([wv[j, 0, :, col], wv[j, 1, :, col]], axis=1), preferred_element_type=F32)
                return carry
            lax.fori_loop(0, T // piece, ab_rows, 0)
            side = lax.rem(k, 2)

            @pl.when(k >= 2)
            def _():
                for copy in ab_copies(k, side):
                    copy.wait()
            a, b = acc[:, :LANES], acc[:, LANES:]
            ab[side, 0] = a
            ab[side, 1] = b
            ub[:, col] = (a * jax.nn.sigmoid(a) * b).astype(BF16)
            for copy in ab_copies(k, side):
                copy.start()
            return carry
        lax.fori_loop(0, tiles, ab_body, 0)
        for k in (tiles - 2, tiles - 1):
            for copy in ab_copies(k, k % 2):
                copy.wait()
        save_u = pltpu.make_async_copy(ub, u_s.at[j], lsv.at[3])
        save_u.start()

        @pl.when((j == 0) | (s == 0))
        def _():
            pltpu.make_async_copy(w_out.at[j], wov, lo.at[0]).wait()

            def send(i, c, rows, dst, chip):
                return remote(zp.at[c, rows], dst, zss.at[i], zrs.at[i], (chip, s))
            first = [send(0, dg, lo_rows, near_in.at[0, 0], xn), send(1, dg, hi_rows, near_in.at[1, 0], yn)]
            second = [send(2, xn, lo_rows, near_in.at[0, 1], xn), send(3, yn, hi_rows, near_in.at[1, 1], yn)]
            third = [send(4, yn, lo_rows, far_in.at[0], yn), send(5, xn, hi_rows, far_in.at[1], xn)]
            x, y = lax.rem(d, 2), lax.div(d, 2)
            wide = 2 * LANES

            def block_body(i, carry):
                rel, part_of = 3 - lax.div(i, 2), lax.rem(i, 2)
                c = 2 * lax.rem(y + lax.rem(rel, 2), 2) + lax.rem(x + lax.div(rel, 2), 2)

                def zp_rows(n, carry):
                    rows = pl.ds(pl.multiple_of(n * half, 16), half)
                    zp[c, rows, pl.ds(pl.multiple_of(part_of * wide, wide), wide)] = jnp.dot(
                        ub[rows, :], wov[:, pl.ds(pl.multiple_of(c * dm + part_of * wide, wide), wide)], preferred_element_type=F32)
                    return carry
                lax.fori_loop(0, 2, zp_rows, 0)
                for at, copies in ((1, first), (3, second[:1]), (5, second[1:])):
                    @pl.when(i == at)
                    def _():
                        for copy in copies:
                            copy.start()
                return carry
            lax.fori_loop(0, 8, block_body, 0)
            share = share_rows(hb.at[nxt], d, s, xn, yn, ass, ars, lo_rows, hi_rows)

            def both(n, stage):
                for at in range(2):
                    @pl.when(n == at)
                    def _():
                        stage(at)

            def half_rows(n):
                return pl.ds(pl.multiple_of(n * half, 16), half)

            def relay(n, carry):
                both(n, lambda at: first[at].wait_recv())
                c, rows = yn + n * (xn - yn), half_rows(n)
                zp[c, rows, :] += near_in[n, 0]
                both(n, lambda at: third[at].start())
                return carry
            lax.fori_loop(0, 2, relay, 0)

            def settle(n, carry):
                both(n, lambda at: (second[at].wait_recv(), third[at].wait_recv()))
                rows = half_rows(n)
                branch = (zp[d, rows, :] + near_in[n, 1] + far_in[n]).astype(BF16).astype(F32)
                hb[nxt, d, rows, :] = (hb[j, d, rows, :].astype(F32) + branch).astype(BF16)
                both(n, lambda at: [copy.start() for copy in share[at]])
                return carry
            lax.fori_loop(0, 2, settle, 0)
            near_share(share)

            @pl.when((j == 0) & (s == 1))
            def _():
                pl.semaphore_signal(go, inc=1, device_id=(d, 0), device_id_type=MESH)
            far_share(share)
            for copy in first + second + third:
                copy.wait_send()

        @pl.when((j == 0) & (s == 0))
        def _():
            pltpu.make_async_copy(w_out.at[1], wov, lo.at[0]).start()

        @pl.when((j == 1) & (s == 0))
        def _():
            hands = hand_over()
            for copy in hands:
                copy.start()

            def last_layer(q, carry):
                @pl.when(q == 1)
                def _():
                    pl.semaphore_wait(go, 1)
                start_weights(1, other_pair, 1, 1, early_tiles + q * (tiles - held_tiles - early_tiles), tiles - held_tiles + q * held_tiles)
                return carry
            lax.fori_loop(0, 2, last_layer, 0)
            for copy in hands:
                copy.wait_send()
        for copy in saves:
            copy.wait()
        save_u.wait()
        return carry
    lax.fori_loop(0, 2, layer, 0)
    wait_sent(0, tiles)

    @pl.when(s == 0)
    def _():
        wait_sent(1, tiles - early_tiles)

    @pl.when(s == 1)
    def _():
        wait_sent(1, tiles)
        wait_sent(2, early_tiles)


def backward_kernel(sel, slot, w_gate, w_in, w_out, a_s, b_s, ho_s, r_s,
                    da_o, db_o, e_o, act_o,
                    wgv, wov, eb, daf, ab, dn, hov, rv, sq, sv, agv, back_v,
                    dss, drs, fss, frs, ess, ers, hss, hrs, sss, srs, ass, ars, lw, lab, lout, lh, le, lsm):
    d, s, xn, yn, dg = place()
    T = sel.shape[0]
    part_rows = T // 2
    lo_n = -(-part_rows // 32) * 16
    cols = daf.shape[3]
    dm = dn.shape[1]
    wide = 2 * LANES
    n_full = cols // wide
    tail = cols - n_full * wide
    n_early = n_full // 2
    n_mid = n_early + 2
    splits, one_loop = (1 if T <= 640 else 2), T > 512
    pad = sq.shape[1]
    w_slots = wgv.shape[0]
    ab_slots = ab.shape[0]

    def wo_load(j):
        return pltpu.make_async_copy(w_out.at[j], wov, lw.at[0, 0])

    def slot_of(j, n):
        return j if n == 2 else 0

    def gate_loads(j):
        return [pltpu.make_async_copy(w.at[j], wgv.at[slot_of(j, w_slots), m], lw.at[1 + slot_of(j, w_slots), m]) for m, w in enumerate((w_gate, w_in))]

    def rows_of(g, base=0, size=part_rows):
        return pl.ds(pl.multiple_of(g * part_rows + base, 16), size)

    def in_copies(g):
        return [pltpu.make_async_copy(sel.at[rows_of(g), pl.ds(c * dm, dm)], eb.at[2, c, rows_of(g)], lh.at[g, c]) for c in range(4)]

    def hand_over(g):
        return [remote(eb.at[0, c, rows_of(g)], eb.at[2, c, rows_of(g)], hss.at[g, i], hrs.at[g, i], (d, 1 - s)) for i, c in enumerate((d, xn, yn, dg))]

    def ab_loads(j, g):
        side = slot_of(g, ab_slots)
        return [pltpu.make_async_copy(src.at[j, :, rows_of(g)], ab.at[side, m], lab.at[side, m]) for m, src in enumerate((a_s, b_s))]

    @pl.when(s == 1)
    def _():
        for copy in in_copies(0):
            copy.start()
    wo_load(1).start()
    small = [pltpu.make_async_copy(ho_s, hov, lsm.at[0]), pltpu.make_async_copy(r_s, rv, lsm.at[1])]
    for copy in ab_loads(1, 0):
        copy.start()
    meet()

    def columns(c, width):
        return pl.ds(pl.multiple_of(c * wide, LANES), width)

    def each_chunk(body, first=0, last=n_full):
        lax.fori_loop(first, last, lambda c, carry: (body(c, wide), carry)[1], 0)

    class Piece:
        def __init__(self, j, g):
            self.j, self.g, self.rows = j, g, rows_of(g)
            parts = (rows_of(g, 0, lo_n), rows_of(g, lo_n, part_rows - lo_n))
            self.share = share_rows(eb.at[j], d, s, xn, yn, ess.at[g], ers.at[g], *parts)
            self.e_saves = [pltpu.make_async_copy(eb.at[j + 1, c, self.rows], e_o.at[j, self.rows, pl.ds(c * dm, dm)], le.at[j, g, c]) for c in range(4)]
            self.sums = [remote(sv.at[g, 0], sv.at[g, 1 + i], sss.at[g, i], srs.at[g, i], (chip, s)) for i, chip in enumerate((xn, yn, dg))]

        def own_sends(self, c, col):
            g, out = self.g, []
            for m in range(2):
                for n, chip in enumerate((xn, yn)):
                    here = daf.at[m, d, self.rows, col]
                    out.append(remote(here, here, dss.at[g, m, n, c], drs.at[g, m, n, c], (chip, s)))
            return out

        def forwards(self, c, col):
            g = self.g
            from_x, from_y = daf.at[0, xn, self.rows, col], daf.at[1, yn, self.rows, col]
            return [remote(from_x, from_x, fss.at[g, 1, c], frs.at[g, 1, c], (yn, s)), remote(from_y, from_y, fss.at[g, 0, c], frs.at[g, 0, c], (xn, s))]

        def make(self):
            j, g, rows, side = self.j, self.g, self.rows, slot_of(self.g, ab_slots)
            for copy in self.e_saves:
                copy.start()

            @pl.when(g == 0)
            def _():
                wo_load(j).wait()
            for copy in ab_loads(j, g):
                copy.wait()

            @pl.when((j == 1) & (g == 0))
            def _():
                if ab_slots == 2:
                    for copy in ab_loads(1, 1):
                        copy.start()

                @pl.when(s == 1)
                def _():
                    for copy in in_copies(1):
                        copy.start()
                for copy in gate_loads(1) + small:
                    copy.start()
            if w_slots == 2:
                @pl.when((j == 1) & (g == 1))
                def _():
                    for copy in gate_loads(0):
                        copy.start()

            def tile(c, width=wide):
                base = jnp.minimum(c * wide, cols - wide) if one_loop else c * wide
                def du(blocks, lanes):
                    e_part = jnp.concatenate([eb[j + 1, n, rows, :] for n in blocks], axis=1)
                    return nt_dot(e_part, wov[pl.ds(pl.multiple_of(base, LANES), width), lanes])
                if splits == 1:
                    dn[rows, :width] = du(range(4), slice(None))
                else:
                    dn[rows, :width] = jnp.zeros((part_rows, width), F32)

                    def du_part(n, carry):
                        dn[rows, :width] += du((2 * n, 2 * n + 1), pl.ds(pl.multiple_of(n * 2 * dm, dm), 2 * dm))
                        return carry
                    lax.fori_loop(0, 2, du_part, 0)
                def lanes(n):
                    lane = pl.ds(pl.multiple_of(base + n * LANES, LANES), LANES)
                    at = lax.div(base, LANES) + n
                    a, b, du = ab[side, 0, at], ab[side, 1, at], dn[rows, n * LANES:(n + 1) * LANES]
                    sig = jax.nn.sigmoid(a)
                    daf[0, d, rows, lane] = (du * b * sig * (1.0 + a * (1.0 - sig))).astype(BF16)
                    daf[1, d, rows, lane] = (du * (a * sig)).astype(BF16)

                if one_loop:
                    @pl.when(c < n_full)
                    def _():
                        lanes(0)
                    lanes(1)
                else:
                    for n in range(width // LANES):
                        lanes(n)

            def body(c, width):
                tile(c, wide)

                @pl.when(c < n_early)
                def _():
                    for copy in self.own_sends(c, columns(c, wide)):
                        copy.start()
            each_chunk(body, 0, n_full + 1 if one_loop else n_full)
            if not one_loop:
                tile(n_full, tail)

        def send(self, first, last):
            def body(c, width):
                for copy in self.own_sends(c, columns(c, width)):
                    copy.start()
            each_chunk(body, first, last)

        def save_tile(self, m, chip, col, c, width):
            dst = (da_o, db_o)[m].at[self.j, self.rows, pl.ds(pl.multiple_of(chip * cols + c * wide, LANES), width)]
            pltpu.make_async_copy(daf.at[m, chip, self.rows, col], dst, lout.at[self.g]).start()

        def add(self, chip, c, width):
            def body(i, carry):
                m, at = lax.div(i, splits), pl.ds(pl.multiple_of(lax.rem(i, splits) * (dm // splits), LANES), dm // splits)
                w = wgv[slot_of(self.j, w_slots), m, at, pl.ds(pl.multiple_of(chip * cols + c * wide, LANES), width)]
                dn[self.rows, at] += nt_dot(daf[m, chip, self.rows, columns(c, width)], w)
                return carry
            lax.fori_loop(0, 2 * splits, body, 0)

        def own(self):
            @pl.when(self.g == 0)
            def _():
                for copy in gate_loads(self.j):
                    copy.wait()
            for m in range(2):
                self.save_tile(m, d, pl.ds(0, cols), 0, cols)
            dn[self.rows, :] = jnp.zeros((part_rows, dm), F32)
            each_chunk(lambda c, width: self.add(d, c, width))
            self.add(d, n_full, tail)

        def near(self, c, width):
            col = columns(c, width)
            fwd_y, fwd_x = self.forwards(c, col)

            def came(m, n, chip):
                there = daf.at[m, chip, self.rows, col]
                remote(there, there, dss.at[self.g, m, n, c], drs.at[self.g, m, n, c], (chip, s)).wait_recv()
            came(0, 0, xn)
            fwd_y.start()
            came(1, 1, yn)
            fwd_x.start()
            came(1, 0, xn)
            came(0, 1, yn)
            for chip in (xn, yn):
                for m in range(2):
                    self.save_tile(m, chip, col, c, width)
            lax.fori_loop(0, 2, lambda i, carry: (self.add(xn + i * (yn - xn), c, width), carry)[1], 0)

        def far(self):
            j, g, rows = self.j, self.g, self.rows

            def body(c, width):
                col = columns(c, width)
                there = [daf.at[m, dg, rows, col] for m in range(2)]
                remote(there[0], there[0], fss.at[g, 1, c], frs.at[g, 1, c], (yn, s)).wait_recv()
                remote(there[1], there[1], fss.at[g, 0, c], frs.at[g, 0, c], (xn, s)).wait_recv()
                for m in range(2):
                    self.save_tile(m, dg, col, c, width)
                self.add(dg, c, width)
            each_chunk(body)
            body(n_full, tail)

            @pl.when((j == 1) & (g == 0))
            def _():
                for copy in small:
                    copy.wait()
            prod = dn[rows, :] * hov[j, rows, :].astype(F32)
            sq[g, :part_rows, :] = (prod[:, :LANES] + prod[:, LANES:2 * LANES]) + (prod[:, 2 * LANES:3 * LANES] + prod[:, 3 * LANES:])
            sv[g, 0] = jnp.broadcast_to(jnp.sum(sq[g].T, axis=0, keepdims=True), (8, pad))
            for copy in self.sums:
                copy.start()
            if w_slots == 1:
                @pl.when((j == 1) & (g == 1))
                def _():
                    for copy in gate_loads(0):
                        copy.start()

        def finish(self):
            j, g = self.j, self.g
            whole = daf.at[:, :, self.rows]
            pltpu.make_async_copy(whole, whole, lout.at[g]).wait()

            def drain(c, width):
                col = columns(c, width)
                for copy in self.own_sends(c, col) + self.forwards(c, col):
                    copy.wait_send()
            each_chunk(drain)
            drain(n_full, tail)
            for copy in self.sums:
                copy.wait()
            mean = ((sv[g, 0, 0:1, :] + sv[g, 1, 0:1, :]) + (sv[g, 2, 0:1, :] + sv[g, 3, 0:1, :])) * (1.0 / (4 * dm))
            sq[g] = jnp.broadcast_to(mean, (LANES, pad)).T
            for n, (base, size) in enumerate(((0, lo_n), (lo_n, part_rows - lo_n))):
                at = rows_of(g, base, size)
                inv, avg = rv[j, at, :], sq[g, base:base + size, :]
                for c in range(4):
                    lane = slice(c * LANES, (c + 1) * LANES)
                    resid = inv * dn[at, lane] - hov[j, at, lane].astype(F32) * (inv * inv * inv) * avg
                    eb[j, d, at, lane] = (eb[j + 1, d, at, lane].astype(F32) + resid).astype(BF16)
                for copy in self.share[n]:
                    copy.start()

    def give(g):
        own_lo, own_hi, fwd_y, fwd_x = Piece(0, g).share
        for copy, came in zip(hand_over(g), ((), (own_hi[0],), (own_lo[1],), (fwd_y, fwd_x))):
            for part in came:
                part.wait_recv()
            copy.start()
        for copy in own_lo + own_hi + [fwd_y, fwd_x]:
            copy.wait_send()

    def step(i, carry):
        g = lax.rem(i, 2)
        cur = Piece(1 - lax.div(i, 2), g)
        prev = Piece(1 - lax.div(i - 1, 2), 1 - g)
        live, later = i < 4, i > 0

        ending = (i == 4) & (s == 1)

        @pl.when(ending)
        def _():
            give(0)

        @pl.when((i >= 2) & jnp.logical_not(ending))
        def _():
            far_share(Piece(1 - lax.div(i - 2, 2), g).share)

        @pl.when(live)
        def _():
            @pl.when((i < 2) & (s == 0))
            def _():
                for copy in hand_over(g):
                    copy.wait_recv()

            @pl.when((i < 2) & (s == 1))
            def _():
                for copy in in_copies(g):
                    copy.wait()

            cur.make()

            @pl.when(i == 1)
            def _():
                wo_load(0).start()
            coming = i + ab_slots

            @pl.when(coming < 4)
            def _():
                for copy in ab_loads(1 - lax.div(coming, 2), lax.rem(coming, 2)):
                    copy.start()

        @pl.when(later)
        def _():
            prev.far()

        def halves(h, carry):
            @pl.when(live)
            def _():
                cur.send(n_early + h * (n_mid - n_early), n_mid + h * (n_full - n_mid))

            @pl.when(live & (h == 0))
            def _():
                cur.own()

            @pl.when(live & (h == 1))
            def _():
                for copy in cur.own_sends(n_full, columns(n_full, tail)):
                    copy.start()

            @pl.when(later & (h == 1))
            def _():
                near_share(prev.share)

            @pl.when(live & (h == 1))
            def _():
                each_chunk(cur.near)

            @pl.when(later & (h == 0))
            def _():
                prev.finish()
            return carry
        lax.fori_loop(0, 2, halves, 0)

        @pl.when(live)
        def _():
            cur.near(n_full, tail)
        return carry
    lax.fori_loop(0, 5, step, 0)

    def act_copies(i, c):
        col = pl.ds(pl.multiple_of(c * dm, dm), dm)
        return remote(agv.at[c], act_o.at[:, col], ass.at[i], ars.at[i], (d, 1 - s)), pltpu.make_async_copy(agv.at[c], act_o.at[:, col], lh.at[0, i])

    @pl.when(s == 1)
    def _():
        give(1)
        for i, c in enumerate((d, xn, yn, dg)):
            act_copies(i, c)[0].wait_recv()

    @pl.when(s == 0)
    def _():
        own_lo, own_hi, fwd_y, fwd_x = Piece(0, 1).share
        rows_out = agv.shape[1]
        own_slots = slot[:, pl.ds(pl.multiple_of(d * rows_out, LANES), rows_out)]
        back = (lax.broadcasted_iota(jnp.int32, (T, rows_out), 0) == own_slots).astype(BF16)
        back_v[...] = back
        came = ((), (own_hi[0],), (own_lo[1],), (fwd_y, fwd_x))
        x, y = lax.rem(d, 2), lax.div(d, 2)

        def spread(i, carry):
            for n in range(1, 4):
                @pl.when(i == n)
                def _():
                    for copy in came[n]:
                        copy.wait_recv()
            c = 2 * lax.rem(y + lax.div(i, 2), 2) + lax.rem(x + lax.rem(i, 2), 2)
            agv[c] = lax.dot_general(back_v[...], eb[0, c], (((0,), (0,)), ((), ())), preferred_element_type=F32).astype(BF16)
            for copy in act_copies(i, c):
                copy.start()
            return carry
        lax.fori_loop(0, 4, spread, 0)
        for copy in own_lo + own_hi + [fwd_y, fwd_x]:
            copy.wait_send()
        for i, c in enumerate((d, xn, yn, dg)):
            away, here = act_copies(i, c)
            away.wait_send()
            here.wait()
    def saved(i, carry):
        for copy in Piece(lax.div(i, 2), lax.rem(i, 2)).e_saves:
            copy.wait()
        return carry
    lax.fori_loop(0, 4, saved, 0)

    @pl.when(s == 1)
    def _():
        for g in range(2):
            for copy in hand_over(g):
                copy.wait_send()


def grads_kernel(no_s, u_s, da, db, e_o, act, gate_o, in_o, out_o, act_o, nv, uv, ev, av, nt, ut, ring, og, oo, ln, lr, lg, lo):
    layers = nv.shape[0]
    wide = ring.shape[3]
    n_gate, n_out = da.shape[2] // wide, e_o.shape[2] // wide
    slots, g_slots, o_slots = ring.shape[0], og.shape[0], oo.shape[0]
    rows = oo.shape[2]
    n_flip = ut.shape[1] // LANES
    first_flip = 1
    first_out = max(first_flip + n_flip, layers * n_gate - layers * n_out - 2)

    def put(ref, at, value):
        ref[at] = value

    def for_rows(count, body):
        parts = 1 if nv.shape[1] <= 640 else 2
        size = count // parts
        if parts == 1:
            body(pl.ds(0, size))
        else:
            lax.fori_loop(0, parts, lambda i, carry: (body(pl.ds(pl.multiple_of(i * size, 32), size)), carry)[1], 0)

    def flip(src, dst):
        def body(i, carry):
            lane = pl.ds(pl.multiple_of(i * LANES, LANES), LANES)
            dst[lane, :] = src[:, lane].T
            return carry
        lax.fori_loop(0, dst.shape[0] // LANES, body, 0)
    wholes = [pltpu.make_async_copy(src, dst, ln.at[i]) for i, (src, dst) in enumerate(((no_s, nv), (u_s, uv), (e_o, ev), (act, av)))]
    act_store = pltpu.make_async_copy(av, act_o, ln.at[4])

    def tile_at(c):
        return pl.ds(pl.multiple_of(c * wide, wide), wide)

    def loads(t):
        slot = lax.rem(t, slots)
        return [pltpu.make_async_copy(src.at[lax.div(t, n_gate), :, tile_at(lax.rem(t, n_gate))], ring.at[slot, m], lr.at[slot, m]) for m, src in enumerate((da, db))]

    def gate_stores(t):
        slot = lax.rem(t, g_slots)
        return [pltpu.make_async_copy(og.at[slot, m], dst.at[lax.div(t, n_gate), :, tile_at(lax.rem(t, n_gate))], lg.at[slot, m]) for m, dst in enumerate((gate_o, in_o))]

    def out_stores(t):
        slot = lax.rem(t, o_slots)
        return [pltpu.make_async_copy(oo.at[slot, m], out_o.at[lax.div(t, n_out), pl.ds(m * rows, rows), tile_at(lax.rem(t, n_out))], lo.at[slot, m]) for m in range(2)]

    def start(copies):
        for copy in copies:
            copy.start()

    def wait(copies):
        for copy in copies:
            copy.wait()
    wholes[0].start()
    for t in range(slots - 1):
        start(loads(t))
    start(wholes[1:])
    wholes[0].wait()

    def out_tile(t):
        j, c, at = lax.div(t, n_out), lax.rem(t, n_out), lax.rem(t, o_slots)

        @pl.when(t >= o_slots)
        def _():
            wait(out_stores(t - o_slots))

        def half(m, carry):
            for_rows(rows, lambda at_rows: put(oo, (at, m, at_rows), jnp.dot(
                ut[j, pl.ds(pl.multiple_of(m * rows + at_rows.start, 32), at_rows.size), :], ev[j, :, tile_at(c)], preferred_element_type=F32)))
            return carry
        lax.fori_loop(0, 2, half, 0)
        start(out_stores(t))

    def gate_body(t, carry):
        j, c, slot, at = lax.div(t, n_gate), lax.rem(t, n_gate), lax.rem(t, slots), lax.rem(t, g_slots)

        @pl.when(t + slots - 1 < layers * n_gate)
        def _():
            start(loads(t + slots - 1))

        @pl.when(c == 0)
        def _():
            flip(nv.at[j], nt)
        wait(loads(t))

        @pl.when(t >= g_slots)
        def _():
            wait(gate_stores(t - g_slots))

        def side(m, carry):
            for_rows(og.shape[2], lambda at_rows: put(og, (at, m, at_rows), jnp.dot(nt[at_rows, :], ring[slot, m], preferred_element_type=F32)))
            return carry
        lax.fori_loop(0, 2, side, 0)
        start(gate_stores(t))

        @pl.when(t == first_flip)
        def _():
            wholes[1].wait()

        @pl.when((t >= first_flip) & (t < first_out))
        def _():
            lane = pl.ds(pl.multiple_of((t - first_flip) * LANES, LANES), LANES)

            def turn(n, carry):
                ut[n, lane, :] = uv[n, :, lane].T
                return carry
            lax.fori_loop(0, layers, turn, 0)

        @pl.when(t == first_out)
        def _():
            wait(wholes[2:])
            act_store.start()

        @pl.when((t >= first_out) & (t < first_out + layers * n_out))
        def _():
            out_tile(t - first_out)
        return carry
    lax.fori_loop(0, layers * n_gate, gate_body, 0)
    act_store.wait()
    for t in range(layers * n_gate - g_slots, layers * n_gate):
        wait(gate_stores(t))
    for t in range(layers * n_out - o_slots, layers * n_out):
        wait(out_stores(t))


def grads_call(no_s, u_s, da, db, e_o, act):
    layers, T, dsh = no_s.shape
    cols, dff, dmod = u_s.shape[2], da.shape[2], e_o.shape[2]
    V, wide = pltpu.VMEM, 4 * LANES
    moved = 2 * layers * T * (dsh + cols + 2 * dff + dmod) + 4 * layers * (2 * dsh * dff + cols * dmod)
    return pl.pallas_call(
        grads_kernel, name=f'grads_{T}', in_specs=[ANY] * 6, out_specs=[ANY] * 4,
        out_shape=[jax.ShapeDtypeStruct((layers, dsh, dff), F32), jax.ShapeDtypeStruct((layers, dsh, dff), F32), jax.ShapeDtypeStruct((layers, cols, dmod), F32),
                   jax.ShapeDtypeStruct(act.shape, BF16)],
        scratch_shapes=[V((layers, T, dsh), BF16), V((layers, T, cols), BF16), V((layers, T, dmod), BF16), V(act.shape, BF16), V((dsh, T), BF16), V((layers, cols, T), BF16),
                        V((6, 2, T, wide), BF16), V((4, 2, dsh, wide), F32), V((3, 2, cols // 2, wide), F32), DMA((5,)), DMA((6, 2)), DMA((4, 2)), DMA((3, 2))],
        cost_estimate=pl.CostEstimate(flops=2 * layers * T * (2 * dsh * dff + cols * dmod), bytes_accessed=moved, transcendentals=0),
        compiler_params=pltpu.CompilerParams(vmem_limit_bytes=VMEM_LIMIT))(no_s, u_s, da, db, e_o, act)


ANY = pl.BlockSpec(memory_space=pl.ANY)
DMA = pltpu.SemaphoreType.DMA


def comm_call(kernel, name, cid, outs, in_specs, scratch):
    return pl.pallas_call(
        kernel, name=name, out_shape=[jax.ShapeDtypeStruct(*o) for o in outs], in_specs=in_specs, out_specs=[ANY] * len(outs),
        scratch_shapes=scratch, compiler_params=pltpu.CompilerParams(collective_id=cid, has_side_effects=True, vmem_limit_bytes=VMEM_LIMIT))


def lens_call(lens, tokens, sizes):
    smem, vmem = pl.BlockSpec(memory_space=pltpu.SMEM), pl.BlockSpec(memory_space=pltpu.VMEM)
    rows = tokens // LANES
    return pl.pallas_call(
        functools.partial(lens_kernel, sizes), name='lens', out_shape=[jax.ShapeDtypeStruct((1, 4 * tokens), jnp.int32), jax.ShapeDtypeStruct((1,), jnp.int32)],
        in_specs=[smem], out_specs=[vmem, smem],
        scratch_shapes=[pltpu.VMEM((rows, LANES), jnp.int32), pltpu.VMEM((4, rows, LANES), jnp.int32), DMA((3,)), DMA((3,))],
        compiler_params=pltpu.CompilerParams(collective_id=0, has_side_effects=True))(lens)


def forward_call(cid, T, act, cot, slot, w_gate, w_in, w_out):
    rows, dmod = act.shape
    _, dsh, dff = w_gate.shape
    cols = dff // 4
    half = T // 2
    tiles = cols // LANES
    outs = [((T, dmod), BF16), ((2, tiles, T, LANES), F32), ((2, tiles, T, LANES), F32), ((2, T, cols), BF16),
            ((2, T, dsh), BF16), ((2, T, dsh), BF16), ((2, T, LANES), F32), ((2, dsh, dff), BF16)]
    V = pltpu.VMEM
    scratch = [V((2, 2, dmod, cols), BF16), V((cols, dmod), BF16), V((2, 4, T, dsh), BF16), V((T, dmod), BF16), V((T, cols), BF16),
               V((4, T, dsh), F32), V((T, 2 * LANES), F32), V((2, 2, T, LANES), F32), V((T, LANES), F32),
               V((2, 2, half, dsh), F32), V((2, half, dsh), F32), V((4 * rows, dsh), BF16),
               DMA((3,)), DMA((2, tiles)), DMA((3,)), DMA((3,)), DMA((2,)), DMA((2,)), DMA((4,)), DMA((4,)), DMA((6,)), DMA((6,)), DMA((6,)), DMA((6,)),
               DMA((2, 2)), DMA((1,)), DMA((2, 2)), DMA((4,)), DMA((4,)), pltpu.SemaphoreType.REGULAR]
    specs = [ANY, ANY, pl.BlockSpec(memory_space=pltpu.VMEM)] + [ANY] * 3
    return comm_call(forward_kernel, f'forward_{T}', cid, outs, specs, scratch)(act, cot, slot, w_gate, w_in, w_out)


def backward_call(cid, sel, slot, w_gate, w_in, w_out, a_s, b_s, ho_s, r_s):
    T, dmod = sel.shape
    _, dsh, dff = w_gate.shape
    cols = dff // 4
    tiles = cols // LANES
    chunks = (tiles + 1) // 2
    pad = -(-(T // 2) // LANES) * LANES
    slots = 2 if T <= 640 else 1
    ab_slots = 2 if T <= 832 else 1
    outs = [((2, T, dff), BF16), ((2, T, dff), BF16), ((2, T, dmod), BF16), ((slot.shape[1] // 4, dmod), BF16)]
    V = pltpu.VMEM
    scratch = [V((slots, 2, dsh, dff), BF16), V((cols, dmod), BF16), V((3, 4, T, dsh), BF16), V((2, 4, T, cols), BF16),
               V((ab_slots, 2, tiles, T // 2, LANES), F32), V((T, dsh), F32), V((2, T, dsh), BF16), V((2, T, LANES), F32), V((2, pad, LANES), F32), V((2, 4, 8, pad), F32), V((4, slot.shape[1] // 4, dsh), BF16), V((T, slot.shape[1] // 4), BF16),
               DMA((2, 2, 2, chunks)), DMA((2, 2, 2, chunks)), DMA((2, 2, chunks)), DMA((2, 2, chunks)), DMA((2, 6)), DMA((2, 6)), DMA((2, 4)), DMA((2, 4)),
               DMA((2, 3)), DMA((2, 3)), DMA((4,)), DMA((4,)), DMA((3, 2)), DMA((2, 2)), DMA((2,)), DMA((2, 4)), DMA((2, 2, 4)), DMA((2,))]
    return comm_call(backward_kernel, f'backward_{T}', cid, outs, [ANY, pl.BlockSpec(memory_space=pltpu.VMEM)] + [ANY] * 7, scratch)(sel, slot, w_gate, w_in, w_out, a_s, b_s, ho_s, r_s)


def solution(mesh, buckets=BUCKETS):
    act_spec = P(None, 'data')
    weight_spec = P('stage', None, 'data', None)

    def local_step(act_in, cot_out, seq_lens, w_gate, w_in, w_out):
        n_micro, n_rows, seq_len, dmod = act_in.shape
        rows = n_micro * n_rows * seq_len
        w_gate, w_in, w_out = w_gate[0], w_in[0], w_out[0]
        act, cot = act_in.reshape(rows, dmod), cot_out.reshape(rows, dmod)
        slot, which = lens_call(seq_lens.reshape(n_micro), rows, buckets)

        def branch(which, T):
            def run(_):
                sel, a_s, b_s, u_s, ho_s, no_s, r_s, _ = forward_call(1 + 2 * which, T, act, cot, slot, w_gate, w_in, w_out)
                da, db, e_o, act_grad = backward_call(2 + 2 * which, sel, slot, w_gate, w_in, w_out, a_s, b_s, ho_s, r_s)
                gate_grad, in_grad, out_grad, act_grad = grads_call(no_s, u_s, da, db, e_o, act_grad)
                return act_grad.reshape(act_in.shape), gate_grad[None], in_grad[None], out_grad[None]
            return run
        if len(buckets) == 1:
            return branch(0, buckets[0])(0)
        return lax.switch(which[0], [branch(i, b) for i, b in enumerate(buckets)], 0)

    return jax.shard_map(local_step, mesh=mesh, in_specs=(act_spec, act_spec, act_spec, weight_spec, weight_spec, weight_spec), out_specs=(act_spec, weight_spec, weight_spec, weight_spec), check_vma=False)
```
